32 devices in a mesh: dp: 8 (over y, x, core), tensor: 4 (over z).
Axes of the slice: x: 2, y: 2, z: 4, core: 2. Of those that a mesh axis runs over, the one named last changes fastest.
Arguments:
- tokens: float32 [12544, 768], P(('dp', 'tensor')), may hold values from -6 to 6
- live_clips: int32 [8], P('dp'), may hold values from 1 to 2, as said below
- norm_gains: bfloat16 [3, 768], P(None, 'dp'), may hold values from 0.099609375 to 1.8984375
- qkv_time: bfloat16 [3, 768, 768], P(None, 'dp', 'tensor'), may hold values from -0.21875 to 0.21875
- out_time: bfloat16 [768, 768], P('tensor', 'dp'), may hold values from -0.625 to 0.625
- qkv_space: bfloat16 [3, 768, 768], P(None, 'dp', 'tensor'), may hold values from -0.21875 to 0.21875
- out_space: bfloat16 [768, 768], P('tensor', 'dp'), may hold values from -3.5 to 3.5
- up_weight: bfloat16 [768, 3072], P('dp', 'tensor'), may hold values from -0.21875 to 0.21875
- down_weight: bfloat16 [3072, 768], P('tensor', 'dp'), may hold values from -0.109375 to 0.109375
- cotangent: float32 [12544, 768], P(('dp', 'tensor')), may hold values from -6 to 6
Outputs:
- output: float32 [12544, 768], P(('dp', 'tensor'))
- grad_tokens: float32 [12544, 768], P(('dp', 'tensor'))
- grad_gains: float32 [3, 768], P(None, 'dp')
- grad_qkv_time: float32 [3, 768, 768], P(None, 'dp', 'tensor')
- grad_out_time: float32 [768, 768], P('tensor', 'dp')
- grad_qkv_space: float32 [3, 768, 768], P(None, 'dp', 'tensor')
- grad_out_space: float32 [768, 768], P('tensor', 'dp')
- grad_up: float32 [768, 3072], P('dp', 'tensor')
- grad_down: float32 [3072, 768], P('tensor', 'dp')
The draws below stay inside these ranges and needn't reach their ends.
Inputs may be any that keep to these rules, and one draw needn't show every extreme that they name: `live_clips`: groups 2i and 2i+1 have equal counts; slots below a group's count are live, the others are padding; some pair of groups has all 2 slots live.
All inputs are finite; a program needn't handle non-finite values.
Results may differ from the reference program's by a relative error of at most 0.038.
Values may be sent and summed in bfloat16 or wider, within the bound.
A program may use at most 128 MiB of HBM per device.

```python
import jax
import jax.numpy as jnp
from jax import lax

D = 768
HEADS = 12
HEAD_DIM = 64
FF = 3072
FRAMES = 8
PATCHES = 196
SLOTS = 2
HALF = 4
NPAIR = 4
TOKENS = 12544
N_DP = 8


def draw_live_clips(key, part):
    counts = jax.random.randint(key, (NPAIR,), SLOTS // 2, SLOTS + 1)
    fullest = jax.random.randint(jax.random.fold_in(key, 7), (), 0, NPAIR)
    counts = jnp.where(jnp.arange(NPAIR) == fullest, SLOTS, counts)
    return jnp.repeat(counts, 2).astype(jnp.int32)


def raised(array, stream_key, source, target, parts, factor):
    def block_of(axis_at):
        return (jnp.arange(array.shape[axis_at]) // (array.shape[axis_at] // parts)).reshape((-1,) + (1,) * (array.ndim - 1 - axis_at))

    near = jax.random.permutation(stream_key, parts)[block_of(target)]
    far = (block_of(target) + parts // 2) % parts
    return jnp.where((block_of(source) == near) | (block_of(source) == far), factor * array, array)


def levels(stream_key, extent, cuts, smallest, largest):
    def one(position, blocks):
        draws = jax.random.uniform(jax.random.fold_in(jax.random.fold_in(stream_key, 6), position), (blocks,), jnp.float32, smallest / len(cuts), largest / len(cuts))
        return jnp.repeat(jnp.exp(draws), extent[position] // blocks).reshape((-1,) + (1,) * (len(extent) - position - 1))

    factor_of = one(*cuts[0])
    for cut in cuts[1:]:
        factor_of = factor_of * one(*cut)
    return factor_of


def normal_values(stream_key, dims, deviation, bound, shards=(), held_as=jnp.bfloat16):
    level = levels(stream_key, dims, shards, -0.22, 0.18) if shards else 1.0
    entries = jax.random.normal(stream_key, dims, jnp.float32) * deviation * level
    return jnp.minimum(jnp.maximum(entries, -bound), bound).astype(held_as)


def heavy_noise(stream_key, dims, scale, bound, cuts, heavy, held_as=jnp.bfloat16):
    result = scale * jax.random.normal(stream_key, dims, jnp.float32)
    if cuts:
        result = result * levels(stream_key, dims, cuts, -0.22, 0.18)
    return jnp.clip(raised(result, jax.random.fold_in(stream_key, 3), *heavy), -bound, bound).astype(held_as)


def setup_inputs(seed: int = 0) -> dict:
    key_list = jax.random.split(jax.random.key(seed), 11)
    tokens = normal_values(key_list[0], (TOKENS, D), 1.0, 6.0, ((0, 32),), jnp.float32)
    live_clips = draw_live_clips(jax.random.fold_in(key_list[10], 71), 0)
    norm_gains = jnp.clip(1.0 + 0.18 * jax.random.normal(key_list[2], (3, D), jnp.float32), 0.099609375, 1.8984375).astype(jnp.bfloat16)
    qkv_time = normal_values(key_list[3], (3, D, D), D ** -0.5, 0.21875, ((1, 8), (2, 4)))
    out_time = normal_values(key_list[4], (D, D), (D // FRAMES) ** -0.5, 0.625, ((0, 4), (1, 8)))
    qkv_space = normal_values(key_list[5], (3, D, D), D ** -0.5, 0.21875, ((1, 8), (2, 4)))
    out_space = normal_values(key_list[6], (D, D), (D // PATCHES) ** -0.5, 3.5, ((0, 4), (1, 8)))
    up_weight = normal_values(key_list[7], (D, FF), D ** -0.5, 0.21875, ((0, 8), (1, 4)))
    down_weight = normal_values(key_list[8], (FF, D), FF ** -0.5, 0.109375, ((0, 4), (1, 8)))
    cotangent = heavy_noise(key_list[9], (TOKENS, D), 1.0, 6.0, ((0, 32),), (0, 1, 32, 2.75), jnp.float32)
    return dict(tokens=tokens, live_clips=live_clips, norm_gains=norm_gains, qkv_time=qkv_time, out_time=out_time, qkv_space=qkv_space, out_space=out_space, up_weight=up_weight, down_weight=down_weight, cotangent=cotangent)


@jax.custom_vjp
def low(v):
    return lax.optimization_barrier(v.astype(jnp.bfloat16)).astype(jnp.float32)

@jax.custom_vjp
def low_back(v):
    return v

def low_keep(v):
    return (low(v), None)

def low_pass(kept, grad):
    return (grad,)

def back_keep(v):
    return (v, None)

def back_low(kept, grad):
    return (low(grad),)
low.defvjp(low_keep, low_pass)
low_back.defvjp(back_keep, back_low)
epsilon = 1e-06
highest = lax.Precision.HIGHEST

def normalize(rows, scale_row):
    average = lax.optimization_barrier(jnp.mean(rows, -1, keepdims=True))
    centred = rows - average
    spread = lax.optimization_barrier(jnp.mean(centred * centred, -1, keepdims=True))
    return centred * lax.rsqrt(spread + epsilon) * scale_row

def clip_keys(flat):
    shaped = flat.reshape(NPAIR, 2, SLOTS, HALF, PATCHES, HEADS, HEAD_DIM)
    return shaped.transpose(0, 2, 4, 5, 1, 3, 6).reshape(NPAIR, SLOTS, PATCHES, HEADS, FRAMES, HEAD_DIM)

def time_attend(query_rows, key_rows, value_rows):
    shaped = query_rows.reshape(NPAIR, 2, SLOTS, HALF, PATCHES, HEADS, HEAD_DIM)
    scores = low_back(jnp.einsum('absfphd,asphkd->absfphk', shaped, clip_keys(key_rows), precision=highest) * HEAD_DIM ** (-0.5))
    weights = jax.nn.softmax(scores, axis=-1)
    blended = jnp.einsum('absfphk,asphkd->absfphd', low(weights), clip_keys(value_rows), precision=highest)
    return blended.reshape(TOKENS, D)

def frame_attend(operands):
    query_rows, key_rows, value_rows = operands
    scores = low_back(jnp.einsum('phd,qhd->hpq', query_rows, key_rows, precision=highest) * HEAD_DIM ** (-0.5))
    weights = jax.nn.softmax(scores, axis=-1)
    return jnp.einsum('hpq,qhd->phd', low(weights), value_rows, precision=highest)

def space_attend(query_rows, key_rows, value_rows):
    frame_count = TOKENS // PATCHES
    shaped = (query_rows.reshape(frame_count, PATCHES, HEADS, HEAD_DIM), key_rows.reshape(frame_count, PATCHES, HEADS, HEAD_DIM), value_rows.reshape(frame_count, PATCHES, HEADS, HEAD_DIM))
    blended = lax.map(jax.checkpoint(frame_attend), shaped)
    return blended.reshape(TOKENS, D)

def reference(tokens, live_clips, norm_gains, qkv_time, out_time, qkv_space, out_space, up_weight, down_weight, cotangent):
    slot_live = jnp.arange(SLOTS, dtype=jnp.int32)[None, :] < live_clips[:, None]
    slot_mask = jnp.where(slot_live, 1.0, 0.0).astype(jnp.float32)
    row_mask = jnp.broadcast_to(slot_mask[:, :, None], (N_DP, SLOTS, HALF * PATCHES)).reshape(TOKENS, 1)

    def layer(stream, gain_rows, time_in, time_out, space_in, space_out, up_full, down_full):
        normed = low(normalize(stream, gain_rows[0]))
        heads = low_back(low(jnp.einsum('td,cde->cte', normed, time_in, precision=highest)))
        blended = low_back(low(time_attend(heads[0], heads[1], heads[2])))
        after_time = stream + low_back(jnp.dot(blended, time_out, precision=highest))
        normed = low(normalize(after_time, gain_rows[1]))
        heads = low_back(low(jnp.einsum('td,cde->cte', normed, space_in, precision=highest)))
        blended = low_back(low(space_attend(heads[0], heads[1], heads[2])))
        after_space = after_time + low_back(jnp.dot(blended, space_out, precision=highest))
        normed = low(normalize(after_space, gain_rows[2]))
        pre_act = low_back(jnp.dot(normed, up_full, precision=highest))
        hidden = low(jax.nn.gelu(pre_act, approximate=False))
        after_mlp = after_space + low_back(jnp.dot(hidden, down_full, precision=highest))
        return after_mlp * row_mask
    output, pullback = jax.vjp(layer, tokens, norm_gains.astype(jnp.float32), qkv_time.astype(jnp.float32), out_time.astype(jnp.float32), qkv_space.astype(jnp.float32), out_space.astype(jnp.float32), up_weight.astype(jnp.float32), down_weight.astype(jnp.float32))
    grads = pullback(cotangent)
    return (output, grads[0], grads[1], grads[2], grads[3], grads[4], grads[5], grads[6], grads[7])
```

```python
import functools

import jax
import jax.numpy as jnp
from jax import lax
from jax.experimental import pallas as pl
from jax.experimental.pallas import tpu as pltpu
from jax.sharding import Mesh, PartitionSpec as P

HEAD_DIM = 64
PATCHES = 196
HALF = 4
FRAMES = 8
EPSILON = 1e-06
F32 = jnp.float32
BF16 = jnp.bfloat16
ALL = ("o", "c", "s", "h")
DP = ("o", "c")
TENSOR = ("s", "h")
CLIP = ("c", "h")

NN = (((1,), (0,)), ((), ()))
NT = (((1,), (1,)), ((), ()))


def mm(a, b, dims=NN):
    return lax.dot_general(a, b, dims, preferred_element_type=F32)


def row_ids(shape, dim, start):
    return lax.broadcasted_iota(jnp.int32, shape, dim) + start


def windows(kind, count):
    if kind == "time":
        return [(0, count, None)]
    found = []
    for frame in range(count // PATCHES):
        low = frame * PATCHES // 16 * 16
        high = min(count, -(-(frame + 1) * PATCHES // 16) * 16)
        found.append((low, high - low, frame))
    return found


def key_bias(start, size, group, stride):
    keys = row_ids((size, size), 0, start)
    if group is None:
        together = keys % stride == row_ids((size, size), 1, start) % stride
    else:
        together = (keys >= group * PATCHES) & (keys < (group + 1) * PATCHES)
    return jnp.where(together, 0.0, -1e30)


def row_valid(start, size, group, width):
    rows = row_ids((size, width), 0, start)
    return (rows >= group * PATCHES) & (rows < (group + 1) * PATCHES)


def attend_kernel(kind, stride, heads_ref, mixed_ref, sums):
    count = heads_ref.shape[0]
    width = mixed_ref.shape[1]
    sums[...] = jnp.zeros_like(sums)
    for start, size, group in windows(kind, count):
        bias = key_bias(start, size, group, stride)
        rows = pl.ds(start, size)
        for head in range(width // HEAD_DIM):
            low = head * HEAD_DIM
            query = heads_ref[rows, low : low + HEAD_DIM] * HEAD_DIM**-0.5
            key = heads_ref[rows, width + low : width + low + HEAD_DIM]
            value = heads_ref[rows, 2 * width + low : 2 * width + low + HEAD_DIM]
            scores = mm(key, query, NT) + bias
            weights = jnp.exp(scores - jnp.max(scores, 0, keepdims=True))
            total = jnp.sum(weights, 0, keepdims=True)
            blended = mm(value.T, weights.astype(BF16)) / total
            blended = blended.T
            if group is not None:
                blended = jnp.where(row_valid(start, size, group, HEAD_DIM), blended, 0.0)
            sums[rows, low : low + HEAD_DIM] += blended
    mixed_ref[...] = sums[...].astype(BF16)


def attend_back_kernel(kind, stride, heads_ref, grad_ref, out_ref, sums):
    count = heads_ref.shape[0]
    width = grad_ref.shape[1]
    scale = HEAD_DIM**-0.5
    sums[...] = jnp.zeros_like(sums)
    for start, size, group in windows(kind, count):
        bias = key_bias(start, size, group, stride)
        rows = pl.ds(start, size)
        for head in range(width // HEAD_DIM):
            low = head * HEAD_DIM
            query = heads_ref[rows, low : low + HEAD_DIM] * scale
            key = heads_ref[rows, width + low : width + low + HEAD_DIM]
            value = heads_ref[rows, 2 * width + low : 2 * width + low + HEAD_DIM]
            grad = grad_ref[rows, low : low + HEAD_DIM]
            if group is not None:
                grad = jnp.where(
                    row_valid(start, size, group, HEAD_DIM), grad.astype(F32), 0.0
                ).astype(BF16)
            scores = mm(key, query, NT) + bias
            weights = jnp.exp(scores - jnp.max(scores, 0, keepdims=True))
            weights = weights / jnp.sum(weights, 0, keepdims=True)
            grad_weights = mm(value, grad, NT)
            row_terms = jnp.sum(weights * grad_weights, 0, keepdims=True)
            grad_scores = (weights * (grad_weights - row_terms)).astype(BF16)
            grad_query = (mm(key.T, grad_scores) * scale).T
            grad_key = mm(grad_scores, query)
            grad_value = mm(weights.astype(BF16), grad)
            sums[rows, low : low + HEAD_DIM] += grad_query
            sums[rows, width + low : width + low + HEAD_DIM] += grad_key
            sums[rows, 2 * width + low : 2 * width + low + HEAD_DIM] += grad_value
    out_ref[...] = sums[...].astype(BF16)


def attend(kind, heads, stride=1):
    blocks, count, columns = heads.shape
    width = columns // 3
    spec = lambda lanes: pl.BlockSpec((None, count, lanes), lambda i: (i, 0, 0))
    return pl.pallas_call(
        functools.partial(attend_kernel, kind, stride),
        grid=(blocks,),
        in_specs=[spec(columns)],
        out_specs=spec(width),
        out_shape=jax.ShapeDtypeStruct((blocks, count, width), BF16),
        scratch_shapes=[pltpu.VMEM((count, width), F32)],
        name=kind + "_attend",
    )(heads)


def attend_back(kind, heads, grad, stride=1):
    blocks, count, columns = heads.shape
    width = columns // 3
    spec = lambda lanes: pl.BlockSpec((None, count, lanes), lambda i: (i, 0, 0))
    return pl.pallas_call(
        functools.partial(attend_back_kernel, kind, stride),
        grid=(blocks,),
        in_specs=[spec(columns), spec(width)],
        out_specs=spec(columns),
        out_shape=jax.ShapeDtypeStruct((blocks, count, columns), BF16),
        scratch_shapes=[pltpu.VMEM((count, columns), F32)],
        name=kind + "_attend_back",
    )(heads, grad)


def normalize(rows, scale_row):
    average = jnp.mean(rows, -1, keepdims=True)
    centred = rows - average
    spread = jnp.mean(centred * centred, -1, keepdims=True)
    return centred * lax.rsqrt(spread + EPSILON) * scale_row


def norm_back(rows, scale_row, grad_normed):
    unused, pullback = jax.vjp(normalize, rows, scale_row)
    return pullback(grad_normed)


def gather_weights(shard):
    every = lax.all_gather(shard, TENSOR, axis=0, tiled=False)
    every = every.reshape(-1, *shard.shape)
    return lax.all_gather(every, DP, axis=1, tiled=True)


def reduce_grads(blocks):
    part = lax.psum_scatter(blocks.astype(BF16), TENSOR, scatter_dimension=0, tiled=True)[0]
    return lax.psum_scatter(part, DP, scatter_dimension=0, tiled=True)


def to_patches(rows, members):
    share = PATCHES // members
    columns = rows.shape[1]
    parts = rows.reshape(-1, members, share, columns).transpose(1, 0, 2, 3)
    return lax.all_to_all(parts, CLIP, 0, 0, tiled=True).reshape(-1, columns)


def to_frames(rows, members):
    share = PATCHES // members
    columns = rows.shape[1]
    parts = rows.reshape(members, -1, share, columns)
    parts = lax.all_to_all(parts, CLIP, 0, 0, tiled=True)
    return parts.transpose(1, 0, 2, 3).reshape(-1, columns)


def on_device(
    tokens,
    live_clips,
    norm_gains,
    qkv_time,
    out_time,
    qkv_space,
    out_space,
    up_weight,
    down_weight,
    cotangent,
):
    members = lax.axis_size("c") * lax.axis_size("h")
    share = PATCHES // members
    live = jnp.where(lax.axis_index("s") < live_clips[0], 1.0, 0.0).astype(F32)

    def pack_heads(qkv, out):
        rows = qkv.shape[1]
        return jnp.concatenate([qkv.transpose(1, 0, 2).reshape(rows, -1), out.T], 1)

    time_all = gather_weights(pack_heads(qkv_time, out_time))
    space_all = gather_weights(pack_heads(qkv_space, out_space))
    up_all = gather_weights(up_weight)
    down_all = gather_weights(down_weight.T)
    gains = lax.all_gather(norm_gains, DP, axis=1, tiled=True).astype(F32)
    width = qkv_time.shape[2]
    time_in, time_out = time_all[:, :, : 3 * width], time_all[:, :, 3 * width :]
    space_in, space_out = space_all[:, :, : 3 * width], space_all[:, :, 3 * width :]

    def heads_of(normed, weight):
        return jnp.einsum("gd,tde->tge", normed, weight, preferred_element_type=F32).astype(BF16)

    def project(mixed, weight):
        return jnp.einsum("tge,tne->gn", mixed, weight, preferred_element_type=F32)

    def project_back(grad, weight):
        return jnp.einsum("gn,tne->tge", grad, weight, preferred_element_type=F32)

    def heads_back(grad_heads, weight):
        return jnp.einsum("tge,tde->gd", grad_heads, weight, preferred_element_type=F32)

    def outer(rows, blocks):
        return jnp.einsum("gd,tge->tde", rows, blocks, preferred_element_type=F32)

    normed_time = to_patches(normalize(tokens, gains[0]).astype(BF16), members)
    time_heads = heads_of(normed_time, time_in)
    time_mixed = attend("time", time_heads, share)
    after_time = tokens + to_frames(project(time_mixed, time_out).astype(BF16), members).astype(F32)
    normed_space = normalize(after_time, gains[1]).astype(BF16)
    space_heads = heads_of(normed_space, space_in)
    space_mixed = attend("space", space_heads)
    after_space = after_time + project(space_mixed, space_out)
    normed_mlp = normalize(after_space, gains[2]).astype(BF16)
    pre_act = jnp.einsum("gd,tde->tge", normed_mlp, up_all, preferred_element_type=F32)
    cdf = 0.5 * (1.0 + lax.erf(pre_act * 0.5**0.5))
    hidden = (pre_act * cdf).astype(BF16)
    slope = cdf + pre_act * (jnp.exp(-0.5 * pre_act * pre_act) * (0.5 / jnp.pi) ** 0.5)
    output = (after_space + project(hidden, down_all)) * live

    grad_stream = cotangent * live
    grad_low = grad_stream.astype(BF16)
    grad_down = outer(grad_low, hidden)
    grad_pre = (project_back(grad_low, down_all) * slope).astype(BF16)
    grad_up = outer(normed_mlp, grad_pre)
    grad_part, gain_mlp = norm_back(after_space, gains[2], heads_back(grad_pre, up_all))
    grad_stream = grad_stream + grad_part
    grad_low = grad_stream.astype(BF16)
    grad_space_out = outer(grad_low, space_mixed)
    grad_mixed = project_back(grad_low, space_out).astype(BF16)
    grad_heads = attend_back("space", space_heads, grad_mixed)
    grad_space_in = outer(normed_space, grad_heads)
    grad_part, gain_space = norm_back(after_time, gains[1], heads_back(grad_heads, space_in))
    grad_stream = grad_stream + grad_part
    grad_low = to_patches(grad_stream.astype(BF16), members)
    grad_time_out = outer(grad_low, time_mixed)
    grad_mixed = project_back(grad_low, time_out).astype(BF16)
    grad_heads = attend_back("time", time_heads, grad_mixed, share)
    grad_time_in = outer(normed_time, grad_heads)
    grad_normed = to_frames(heads_back(grad_heads, time_in).astype(BF16), members).astype(F32)
    grad_part, gain_time = norm_back(tokens, gains[0], grad_normed)
    grad_tokens = grad_stream + grad_part

    down_own = reduce_grads(grad_down).T
    up_own = reduce_grads(grad_up)
    space_own = reduce_grads(jnp.concatenate([grad_space_in, grad_space_out], 2))
    time_own = reduce_grads(jnp.concatenate([grad_time_in, grad_time_out], 2))
    gains_own = lax.psum(jnp.stack([gain_time, gain_space, gain_mlp]), TENSOR)
    gains_own = lax.psum_scatter(gains_own, DP, scatter_dimension=1, tiled=True)

    def unpack(own):
        rows = own.shape[0]
        return own[:, : 3 * width].reshape(rows, 3, width).transpose(1, 0, 2), own[:, 3 * width :].T

    time_in_own, time_out_own = unpack(time_own.astype(F32))
    space_in_own, space_out_own = unpack(space_own.astype(F32))
    return (
        output,
        grad_tokens,
        gains_own,
        time_in_own,
        time_out_own,
        space_in_own,
        space_out_own,
        up_own.astype(F32),
        down_own.astype(F32),
    )


def solution(mesh):
    n_dp, n_tensor = mesh.devices.shape

    def run(*args):
        slots = args[0].shape[0] // (n_dp * HALF * PATCHES)
        fine = Mesh(mesh.devices.reshape(n_dp // 2, 2, slots, n_tensor // slots), ALL)
        in_specs = (
            P(ALL, None),
            P(DP),
            P(None, DP),
            P(None, DP, TENSOR),
            P(TENSOR, DP),
            P(None, DP, TENSOR),
            P(TENSOR, DP),
            P(DP, TENSOR),
            P(TENSOR, DP),
            P(ALL, None),
        )
        out_specs = (in_specs[0], in_specs[0]) + in_specs[2:9]
        return jax.shard_map(
            on_device, mesh=fine, in_specs=in_specs, out_specs=out_specs, check_vma=False
        )(*args)

    return run
```

```python
import functools
import math

import jax
import jax.numpy as jnp
from jax import lax
from jax.experimental import pallas as pl
from jax.experimental.pallas import tpu as pltpu
from jax.sharding import Mesh, PartitionSpec as P

HEAD_DIM = 64
PATCHES = 196
HALF = 4
FRAMES = 8
EPSILON = 1e-06
F32 = jnp.float32
BF16 = jnp.bfloat16
ALL = ("o", "c", "s", "h")
DP = ("o", "c")
TENSOR = ("s", "h")
CLIP = ("c", "h")

NN = (((1,), (0,)), ((), ()))
NT = (((1,), (1,)), ((), ()))
TN = (((0,), (0,)), ((), ()))
BLOCK_ROWS = 96


def mm(a, b, dims=NN):
    return lax.dot_general(a, b, dims, preferred_element_type=F32)


def row_ids(shape, dim, start):
    return lax.broadcasted_iota(jnp.int32, shape, dim) + start


def windows(kind, count):
    if kind == "time":
        return [(0, count, None)]
    found = []
    for frame in range(count // PATCHES):
        low = frame * PATCHES // 16 * 16
        high = min(count, -(-(frame + 1) * PATCHES // 16) * 16)
        found.append((low, high - low, frame))
    return found


def key_bias(start, size, group, stride):
    keys = row_ids((size, size), 0, start)
    if group is None:
        together = keys % stride == row_ids((size, size), 1, start) % stride
    else:
        together = (keys >= group * PATCHES) & (keys < (group + 1) * PATCHES)
    return jnp.where(together, 0.0, -1e30)


def row_valid(start, size, group, width):
    rows = row_ids((size, width), 0, start)
    return (rows >= group * PATCHES) & (rows < (group + 1) * PATCHES)


def normalize(rows, scale_row):
    average = jnp.mean(rows, -1, keepdims=True)
    centred = rows - average
    spread = jnp.mean(centred * centred, -1, keepdims=True)
    return centred * lax.rsqrt(spread + EPSILON) * scale_row


def norm_back(rows, scale_row, grad_normed):
    unused, pullback = jax.vjp(normalize, rows, scale_row)
    return pullback(grad_normed)


def row_block(core, part, quad):
    quad_me = lax.axis_index("o")
    block = jnp.bitwise_xor(quad_me, quad) * 2 + jnp.bitwise_xor(core, part)
    return pl.multiple_of(block * BLOCK_ROWS, BLOCK_ROWS)


def head_slices(ref, rows, width, head):
    low = head * HEAD_DIM
    return tuple(ref[rows, part * width + low : part * width + low + HEAD_DIM] for part in range(3))


def put_grads(work, outs):
    if len(outs) == 1:
        outs[0][...] = work[...]
        return
    core = lax.axis_index("c")
    for part, out in enumerate(outs):
        for quad in range(out.shape[0]):
            out[quad] = work[pl.ds(row_block(core, part, quad), out.shape[1]), :]


def attend_kernel(kind, stride, normed_ref, weight_ref, heads_ref, mixed_ref, out_ref, sums, total_ref):
    step = pl.program_id(0)
    count, width = mixed_ref.shape
    heads_ref[...] = mm(normed_ref[...], weight_ref[:, : 3 * width]).astype(BF16)
    sums[...] = jnp.zeros_like(sums)
    for start, size, group in windows(kind, count):
        bias = key_bias(start, size, group, stride)
        rows = pl.ds(start, size)
        for head in range(width // HEAD_DIM):
            low = head * HEAD_DIM
            query, key, value = head_slices(heads_ref, rows, width, head)
            scores = mm(key, query * HEAD_DIM**-0.5, NT) + bias
            weights = jnp.exp(scores - jnp.max(scores, 0, keepdims=True))
            total = jnp.sum(weights, 0, keepdims=True)
            blended = (mm(value.T, weights.astype(BF16)) / total).T
            if group is not None:
                blended = jnp.where(row_valid(start, size, group, HEAD_DIM), blended, 0.0)
            sums[rows, low : low + HEAD_DIM] += blended
    mixed_ref[...] = sums[...].astype(BF16)
    share = mm(mixed_ref[...], weight_ref[:, 3 * width :], NT)

    @pl.when(step == 0)
    def _():
        total_ref[...] = share

    @pl.when(step > 0)
    def _():
        total_ref[...] += share

    @pl.when(step == pl.num_programs(0) - 1)
    def _():
        out_ref[...] = total_ref[...].astype(out_ref.dtype)


def attend_back_kernel(
    kind, stride, normed_ref, weight_ref, heads_ref, mixed_ref, grad_ref, *rest
):
    outs, (out_ref, sums, total_ref, grad_mixed, grad_heads, work) = rest[:-6], rest[-6:]
    step = pl.program_id(0)
    count, width = mixed_ref.shape
    scale = HEAD_DIM**-0.5
    grad_mixed[...] = mm(grad_ref[...], weight_ref[:, 3 * width :]).astype(BF16)
    sums[...] = jnp.zeros_like(sums)
    for start, size, group in windows(kind, count):
        bias = key_bias(start, size, group, stride)
        rows = pl.ds(start, size)
        for head in range(width // HEAD_DIM):
            low = head * HEAD_DIM
            query, key, value = head_slices(heads_ref, rows, width, head)
            query = query * scale
            grad = grad_mixed[rows, low : low + HEAD_DIM]
            if group is not None:
                valid = row_valid(start, size, group, HEAD_DIM)
                grad = jnp.where(valid, grad.astype(F32), 0.0).astype(BF16)
            scores = mm(key, query, NT) + bias
            weights = jnp.exp(scores - jnp.max(scores, 0, keepdims=True))
            weights = weights / jnp.sum(weights, 0, keepdims=True)
            grad_weights = mm(value, grad, NT)
            row_terms = jnp.sum(weights * grad_weights, 0, keepdims=True)
            grad_scores = (weights * (grad_weights - row_terms)).astype(BF16)
            sums[rows, low : low + HEAD_DIM] += (mm(key.T, grad_scores) * scale).T
            low += width
            sums[rows, low : low + HEAD_DIM] += mm(grad_scores, query)
            low += width
            sums[rows, low : low + HEAD_DIM] += mm(weights.astype(BF16), grad)
    grad_heads[...] = sums[...].astype(BF16)
    share = mm(grad_heads[...], weight_ref[:, : 3 * width], NT)

    @pl.when(step == 0)
    def _():
        total_ref[...] = share

    @pl.when(step > 0)
    def _():
        total_ref[...] += share

    @pl.when(step == pl.num_programs(0) - 1)
    def _():
        out_ref[...] = total_ref[...].astype(out_ref.dtype)

    work[:, : 3 * width] = mm(normed_ref[...], grad_heads[...], TN).astype(BF16)
    work[:, 3 * width :] = mm(grad_ref[...], mixed_ref[...], TN).astype(BF16)
    put_grads(work, outs)


def up_kernel(normed_ref, weight_ref, hidden_ref, slope_ref):
    pre_act = mm(normed_ref[...], weight_ref[...])
    cdf = 0.5 * (1.0 + lax.erf(pre_act * 0.5**0.5))
    hidden_ref[...] = (pre_act * cdf).astype(BF16)
    density = jnp.exp(-0.5 * pre_act * pre_act) * (0.5 / math.pi) ** 0.5
    slope_ref[...] = (cdf + pre_act * density).astype(slope_ref.dtype)


def down_kernel(hidden_ref, weight_ref, out_ref):
    share = mm(hidden_ref[...], weight_ref[...], NT)

    @pl.when(pl.program_id(0) == 0)
    def _():
        out_ref[...] = share

    @pl.when(pl.program_id(0) > 0)
    def _():
        out_ref[...] += share


def down_back_kernel(grad_ref, weight_ref, hidden_ref, slope_ref, *rest):
    outs, (grad_pre_ref, work) = rest[:-2], rest[-2:]
    grad_hidden = mm(grad_ref[...], weight_ref[...])
    grad_pre_ref[...] = (grad_hidden * slope_ref[...].astype(F32)).astype(BF16)
    work[...] = mm(grad_ref[...], hidden_ref[...], TN).astype(BF16)
    put_grads(work, outs)


def up_back_kernel(normed_ref, weight_ref, grad_pre_ref, *rest):
    outs, (out_ref, work) = rest[:-2], rest[-2:]
    share = mm(grad_pre_ref[...], weight_ref[...], NT)

    @pl.when(pl.program_id(0) == 0)
    def _():
        out_ref[...] = share

    @pl.when(pl.program_id(0) > 0)
    def _():
        out_ref[...] += share

    work[...] = mm(normed_ref[...], grad_pre_ref[...], TN).astype(BF16)
    put_grads(work, outs)


def whole_spec(array):
    return pl.BlockSpec(array.shape, lambda i: (0,) * array.ndim)


def step_spec(array):
    rest = array.shape[1:]
    return pl.BlockSpec((None,) + rest, lambda i: (i,) + (0,) * len(rest))


def phase(kernel, name, inputs, outputs, scratch=(), cost=0):
    blocks = [a for a in inputs if a.ndim > 2][0].shape[0]
    spec = lambda a: whole_spec(a) if a.ndim == 2 else step_spec(a)
    return pl.pallas_call(
        kernel,
        grid=(blocks,),
        in_specs=[spec(a) for a in inputs],
        out_specs=[spec(a) for a in outputs],
        out_shape=outputs,
        scratch_shapes=list(scratch),
        cost_estimate=pl.CostEstimate(
            flops=int(cost * 800e6), bytes_accessed=int(cost * 1e6), transcendentals=0
        ),
        name=name,
    )(*inputs)


def shaped(*shape, dtype=BF16):
    return jax.ShapeDtypeStruct(shape, dtype)


def grad_shapes(weight, routed):
    blocks, depth, lanes = weight.shape
    if not routed:
        return [shaped(blocks, depth, lanes)]
    rows = BLOCK_ROWS
    return [shaped(blocks, depth // rows // 2, rows, lanes) for part in range(2)]


def attend(kind, normed, weight, stride, out_dtype):
    blocks, depth, lanes = weight.shape
    count, width = normed.shape[0], lanes // 4
    return phase(
        functools.partial(attend_kernel, kind, stride),
        kind + "_attend",
        (normed, weight),
        (
            shaped(blocks, count, 3 * width),
            shaped(blocks, count, width),
            shaped(count, depth, dtype=out_dtype),
        ),
        (pltpu.VMEM((count, width), F32), pltpu.VMEM((count, depth), F32)),
        cost=14,
    )


def attend_back(kind, normed, weight, heads, mixed, grad, stride, out_dtype, routed):
    blocks, depth, lanes = weight.shape
    count, width = normed.shape[0], lanes // 4
    *grads, out = phase(
        functools.partial(attend_back_kernel, kind, stride),
        kind + "_attend_back",
        (normed, weight, heads, mixed, grad),
        (*grad_shapes(weight, routed), shaped(count, depth, dtype=out_dtype)),
        (
            pltpu.VMEM((count, 3 * width), F32),
            pltpu.VMEM((count, depth), F32),
            pltpu.VMEM((count, width), BF16),
            pltpu.VMEM((count, 3 * width), BF16),
            pltpu.VMEM((depth, lanes), BF16),
        ),
        cost=20,
    )
    return grads, out


def along(piece, axes, distance):
    size = lax.axis_size(axes)
    return lax.ppermute(piece, axes, [(i, i ^ distance) for i in range(size)])


def after(piece, earlier):
    return piece + earlier[:1, :1] * 0


def gather_routed(shard):
    line = [shard] + [along(shard, TENSOR, k) for k in range(1, 4)]
    quads = [line]
    beside = [along(piece, "o", 1) for piece in line]
    above = [along(piece, "o", 2) for piece in line]
    across = [along(piece, "o", 2) for piece in beside[:2]]
    across += [along(piece, "o", 1) for piece in above[2:]]
    quads = [line, beside, above, across]
    other = [[along(piece, "c", 1) for piece in quad] for quad in quads]
    return quads, other


def assemble_kernel(*refs):
    (*pieces, out_ref, sems) = refs
    core = lax.axis_index("c")
    quads, blocks = 4, out_ref.shape[0]
    copies = []
    for part in range(2):
        for quad in range(quads):
            row = row_block(core, part, quad)
            for block in range(blocks):
                index = (part * quads + quad) * blocks + block
                copies.append(
                    pltpu.make_async_copy(
                        pieces[index],
                        out_ref.at[block, pl.ds(row, BLOCK_ROWS)],
                        sems.at[index],
                    )
                )
    for copy in copies:
        copy.start()
    for copy in copies:
        copy.wait()


def assemble(own, other):
    pieces = [piece for part in (own, other) for quad in part for piece in quad]
    rows, lanes = pieces[0].shape
    blocks = len(own[0])
    return pl.pallas_call(
        assemble_kernel,
        in_specs=[pl.BlockSpec(memory_space=pl.ANY)] * len(pieces),
        out_specs=pl.BlockSpec(memory_space=pltpu.VMEM),
        out_shape=shaped(blocks, rows * len(pieces) // blocks, lanes),
        scratch_shapes=[pltpu.SemaphoreType.DMA((len(pieces),))],
        cost_estimate=pl.CostEstimate(flops=0, bytes_accessed=9_000_000, transcendentals=0),
        name="assemble",
    )(*pieces)


def gather_plain(shard):
    every = lax.all_gather(shard, TENSOR, axis=0, tiled=False)
    return lax.all_gather(every.reshape(-1, *shard.shape), DP, axis=1, tiled=True)


def add(*parts):
    return sum(part.astype(F32) for part in parts)


def reduce_routed(grads):
    keep, send = grads
    came = along(send, "c", 1)
    both = lambda t, q: add(keep[t, q], came[t, q]).astype(BF16)
    late, early = slice(0, 2), slice(2, 4)
    first = along(both(slice(0, 2), slice(2, 4)), "o", 2)
    second = along(both(slice(2, 4), slice(1, 4, 2)), "o", 1)
    low = add(keep[:2, :2], came[:2, :2], first)
    high = add(keep[2:, ::2], came[2:, ::2], second)
    first = along(low[:, 1].astype(BF16), "o", 1)
    second = along(high[:, 1].astype(BF16), "o", 2)
    low = add(low[:, 0], first)
    high = add(high[:, 0], second)
    far = [along(low[1].astype(BF16), TENSOR, 1)]
    far += [along(high[k].astype(BF16), TENSOR, k + 2) for k in range(2)]
    return add(low[0], *far)


def reduce_plain(grads):
    part = lax.psum_scatter(grads[0], TENSOR, scatter_dimension=0, tiled=True)[0]
    return lax.psum_scatter(part, DP, scatter_dimension=0, tiled=True).astype(F32)


def to_patches(rows, members):
    share, columns = PATCHES // members, rows.shape[1]
    me = lax.axis_index(CLIP)
    parts = rows.reshape(-1, members, share, columns).transpose(1, 0, 2, 3)
    parts = [
        lax.dynamic_index_in_dim(parts, jnp.bitwise_xor(me, k), 0, keepdims=False)
        for k in range(members)
    ]
    parts = [parts[0]] + [along(parts[k], CLIP, k) for k in range(1, members)]
    return jnp.stack(parts).reshape(-1, columns)


def to_frames(rows, members):
    share, columns = PATCHES // members, rows.shape[1]
    me = lax.axis_index(CLIP)
    parts = rows.reshape(members, -1, share, columns)
    parts = [parts[0]] + [along(parts[k], CLIP, k) for k in range(1, members)]
    parts = jnp.stack(parts)
    order = jnp.bitwise_xor(me, jnp.arange(members))
    parts = [
        lax.dynamic_index_in_dim(parts, jnp.bitwise_xor(me, k), 0, keepdims=False)
        for k in range(members)
    ]
    return jnp.stack(parts, 1).reshape(-1, columns)


def all_gains(norm_gains, columns):
    own = norm_gains.shape[1]
    place = lax.axis_index(DP) * own
    total = lax.dynamic_update_slice(jnp.zeros((3, columns), F32), norm_gains.astype(F32), (0, place))
    total = total + along(total, "c", 1)
    bit = 1
    while bit < lax.axis_size("o"):
        total = total + along(total, "o", bit)
        bit *= 2
    return total


def sum_gains(total, own):
    for axes in ("c", "o", TENSOR):
        bit = 1
        while bit < lax.axis_size(axes):
            total = total + along(total, axes, bit)
            bit *= 2
    return lax.dynamic_slice_in_dim(total, lax.axis_index(DP) * own, own, 1)


def on_device(
    routed,
    tokens,
    live_clips,
    norm_gains,
    qkv_time,
    out_time,
    qkv_space,
    out_space,
    up_weight,
    down_weight,
    cotangent,
):
    members = lax.axis_size("c") * lax.axis_size("h")
    share = PATCHES // members
    count, columns = tokens.shape
    width = qkv_time.shape[2]
    live = jnp.where(lax.axis_index("s") < live_clips[0], 1.0, 0.0).astype(F32)

    def pack_heads(qkv, out):
        rows = qkv.shape[1]
        return jnp.concatenate([qkv.transpose(1, 0, 2).reshape(rows, -1), out.T], 1)

    shards = [
        pack_heads(qkv_time, out_time),
        pack_heads(qkv_space, out_space),
        up_weight,
        down_weight.T,
    ]
    gains = all_gains(norm_gains, columns)
    if routed:
        gathered = []
        for shard in shards:
            if gathered:
                shard = after(shard, gathered[-1][0][3][3])
            gathered.append(gather_routed(shard))
        time_all, space_all, up_all, down_all = [assemble(*found) for found in gathered]
        reduce_grads = reduce_routed
    else:
        time_all, space_all, up_all, down_all = [gather_plain(shard) for shard in shards]
        reduce_grads = reduce_plain

    blocks, depth, lanes = up_all.shape
    normed_time = to_patches(normalize(tokens, gains[0]).astype(BF16), members)
    time_heads, time_mixed, change = attend("time", normed_time, time_all, share, BF16)
    after_time = tokens + to_frames(change, members).astype(F32)
    normed_space = normalize(after_time, gains[1]).astype(BF16)
    space_heads, space_mixed, change = attend("space", normed_space, space_all, 1, F32)
    after_space = after_time + change
    normed_mlp = normalize(after_space, gains[2]).astype(BF16)
    hidden, slope = phase(
        up_kernel,
        "up",
        (normed_mlp, up_all),
        (shaped(blocks, count, lanes), shaped(blocks, count, lanes)),
        cost=12,
    )
    (change,) = phase(
        down_kernel, "down", (hidden, down_all), (shaped(count, depth, dtype=F32),), cost=4
    )
    output = (after_space + change) * live

    grad_stream = cotangent * live
    grad_low = grad_stream.astype(BF16)
    work = (pltpu.VMEM((depth, lanes), BF16),)
    *down_grads, grad_pre = phase(
        down_back_kernel,
        "down_back",
        (grad_low, down_all, hidden, slope),
        (*grad_shapes(down_all, routed), shaped(blocks, count, lanes)),
        work,
        cost=8,
    )
    *up_grads, grad_normed = phase(
        up_back_kernel,
        "up_back",
        (normed_mlp, up_all, grad_pre),
        (*grad_shapes(up_all, routed), shaped(count, depth, dtype=F32)),
        work,
        cost=8,
    )
    grad_part, gain_mlp = norm_back(after_space, gains[2], grad_normed)
    grad_stream = grad_stream + grad_part
    space_grads, grad_normed = attend_back(
        "space",
        normed_space,
        space_all,
        space_heads,
        space_mixed,
        grad_stream.astype(BF16),
        1,
        F32,
        routed,
    )
    grad_part, gain_space = norm_back(after_time, gains[1], grad_normed)
    grad_stream = grad_stream + grad_part
    grad_low = to_patches(grad_stream.astype(BF16), members)
    time_grads, grad_normed = attend_back(
        "time", normed_time, time_all, time_heads, time_mixed, grad_low, share, BF16, routed
    )
    grad_normed = to_frames(grad_normed, members).astype(F32)
    grad_part, gain_time = norm_back(tokens, gains[0], grad_normed)
    grad_tokens = grad_stream + grad_part

    down_own = reduce_grads(down_grads).T
    up_own = reduce_grads(up_grads)
    space_own = reduce_grads(space_grads)
    time_own = reduce_grads(time_grads)
    gains_own = sum_gains(jnp.stack([gain_time, gain_space, gain_mlp]), norm_gains.shape[1])

    def unpack(own):
        rows = own.shape[0]
        return own[:, : 3 * width].reshape(rows, 3, width).transpose(1, 0, 2), own[:, 3 * width :].T

    time_in_own, time_out_own = unpack(time_own)
    space_in_own, space_out_own = unpack(space_own)
    return (
        output,
        grad_tokens,
        gains_own,
        time_in_own,
        time_out_own,
        space_in_own,
        space_out_own,
        up_own,
        down_own,
    )


def solution(mesh):
    n_dp, n_tensor = mesh.devices.shape

    def run(*args):
        slots = args[0].shape[0] // (n_dp * HALF * PATCHES)
        fine = Mesh(mesh.devices.reshape(n_dp // 2, 2, slots, n_tensor // slots), ALL)
        in_specs = (
            P(ALL, None),
            P(DP),
            P(None, DP),
            P(None, DP, TENSOR),
            P(TENSOR, DP),
            P(None, DP, TENSOR),
            P(TENSOR, DP),
            P(DP, TENSOR),
            P(TENSOR, DP),
            P(ALL, None),
        )
        out_specs = (in_specs[0], in_specs[0]) + in_specs[2:9]
        routed = fine.devices.shape == (4, 2, 2, 2)
        return jax.shard_map(
            functools.partial(on_device, routed), mesh=fine, in_specs=in_specs, out_specs=out_specs, check_vma=False
        )(*args)

    return run
```

```python
import functools
import math

import jax
import jax.numpy as jnp
from jax import lax
from jax.experimental import pallas as pl
from jax.experimental.pallas import tpu as pltpu
from jax.sharding import Mesh, PartitionSpec as P

HEAD_DIM = 64
PATCHES = 196
HALF = 4
FRAMES = 8
EPSILON = 1e-06
F32 = jnp.float32
BF16 = jnp.bfloat16
ALL = ("y", "x", "c", "s", "h")
DP = ("y", "x", "c")
TENSOR = ("s", "h")
CLIP = ("c", "h")

NN = (((1,), (0,)), ((), ()))
NT = (((1,), (1,)), ((), ()))
TN = (((0,), (0,)), ((), ()))
BLOCK_ROWS = 96


def mm(a, b, dims=NN):
    return lax.dot_general(a, b, dims, preferred_element_type=F32)


def row_ids(shape, dim, start):
    return lax.broadcasted_iota(jnp.int32, shape, dim) + start


def windows(kind, count):
    if kind == "time":
        return [(0, count, None)]
    found = []
    for frame in range(count // PATCHES):
        low = frame * PATCHES // 16 * 16
        high = min(count, -(-(frame + 1) * PATCHES // 16) * 16)
        found.append((low, high - low, frame))
    return found


def key_bias(start, size, group, stride):
    keys = row_ids((size, size), 0, start)
    if group is None:
        together = keys % stride == row_ids((size, size), 1, start) % stride
    else:
        together = (keys >= group * PATCHES) & (keys < (group + 1) * PATCHES)
    return jnp.where(together, 0.0, -1e30)


def row_valid(start, size, group, width):
    rows = row_ids((size, width), 0, start)
    return (rows >= group * PATCHES) & (rows < (group + 1) * PATCHES)


def normalize(rows, scale_row):
    average = jnp.mean(rows, -1, keepdims=True)
    centred = rows - average
    spread = jnp.mean(centred * centred, -1, keepdims=True)
    return centred * lax.rsqrt(spread + EPSILON) * scale_row


def norm_back(rows, scale_row, grad_normed):
    unused, pullback = jax.vjp(normalize, rows, scale_row)
    return pullback(grad_normed)


def row_block(core, part, quad):
    quad_me = lax.axis_index(("y", "x"))
    block = jnp.bitwise_xor(quad_me, quad) * 2 + jnp.bitwise_xor(core, part)
    return pl.multiple_of(block * BLOCK_ROWS, BLOCK_ROWS)


def head_slices(ref, rows, width, head):
    low = head * HEAD_DIM
    return tuple(ref[rows, part * width + low : part * width + low + HEAD_DIM] for part in range(3))


def put_grads(work, outs):
    if len(outs) == 1:
        outs[0][...] = work[...]
        return
    core = lax.axis_index("c")
    for part, out in enumerate(outs):
        for quad in range(out.shape[0]):
            out[quad] = work[pl.ds(row_block(core, part, quad), out.shape[1]), :]


def attend_kernel(kind, stride, normed_ref, weight_ref, heads_ref, mixed_ref, out_ref, sums, total_ref):
    step = pl.program_id(0)
    count, width = mixed_ref.shape
    heads_ref[...] = mm(normed_ref[...], weight_ref[:, : 3 * width]).astype(BF16)
    sums[...] = jnp.zeros_like(sums)
    for start, size, group in windows(kind, count):
        bias = key_bias(start, size, group, stride)
        rows = pl.ds(start, size)
        for head in range(width // HEAD_DIM):
            low = head * HEAD_DIM
            query, key, value = head_slices(heads_ref, rows, width, head)
            scores = mm(key, query * HEAD_DIM**-0.5, NT) + bias
            weights = jnp.exp(scores - jnp.max(scores, 0, keepdims=True))
            total = jnp.sum(weights, 0, keepdims=True)
            blended = (mm(value.T, weights.astype(BF16)) / total).T
            if group is not None:
                blended = jnp.where(row_valid(start, size, group, HEAD_DIM), blended, 0.0)
            sums[rows, low : low + HEAD_DIM] += blended
    mixed_ref[...] = sums[...].astype(BF16)
    share = mm(mixed_ref[...], weight_ref[:, 3 * width :], NT)

    @pl.when(step == 0)
    def _():
        total_ref[...] = share

    @pl.when(step > 0)
    def _():
        total_ref[...] += share

    @pl.when(step == pl.num_programs(0) - 1)
    def _():
        out_ref[...] = total_ref[...].astype(out_ref.dtype)


def attend_back_kernel(
    kind, stride, normed_ref, weight_ref, heads_ref, mixed_ref, grad_ref, *rest
):
    outs, (out_ref, sums, total_ref, grad_mixed, grad_heads, work) = rest[:-6], rest[-6:]
    step = pl.program_id(0)
    count, width = mixed_ref.shape
    scale = HEAD_DIM**-0.5
    grad_mixed[...] = mm(grad_ref[...], weight_ref[:, 3 * width :]).astype(BF16)
    sums[...] = jnp.zeros_like(sums)
    for start, size, group in windows(kind, count):
        bias = key_bias(start, size, group, stride)
        rows = pl.ds(start, size)
        for head in range(width // HEAD_DIM):
            low = head * HEAD_DIM
            query, key, value = head_slices(heads_ref, rows, width, head)
            query = query * scale
            grad = grad_mixed[rows, low : low + HEAD_DIM]
            if group is not None:
                valid = row_valid(start, size, group, HEAD_DIM)
                grad = jnp.where(valid, grad.astype(F32), 0.0).astype(BF16)
            scores = mm(key, query, NT) + bias
            weights = jnp.exp(scores - jnp.max(scores, 0, keepdims=True))
            weights = weights / jnp.sum(weights, 0, keepdims=True)
            grad_weights = mm(value, grad, NT)
            row_terms = jnp.sum(weights * grad_weights, 0, keepdims=True)
            grad_scores = (weights * (grad_weights - row_terms)).astype(BF16)
            sums[rows, low : low + HEAD_DIM] += (mm(key.T, grad_scores) * scale).T
            low += width
            sums[rows, low : low + HEAD_DIM] += mm(grad_scores, query)
            low += width
            sums[rows, low : low + HEAD_DIM] += mm(weights.astype(BF16), grad)
    grad_heads[...] = sums[...].astype(BF16)
    share = mm(grad_heads[...], weight_ref[:, : 3 * width], NT)

    @pl.when(step == 0)
    def _():
        total_ref[...] = share

    @pl.when(step > 0)
    def _():
        total_ref[...] += share

    @pl.when(step == pl.num_programs(0) - 1)
    def _():
        out_ref[...] = total_ref[...].astype(out_ref.dtype)

    work[:, : 3 * width] = mm(normed_ref[...], grad_heads[...], TN).astype(BF16)
    work[:, 3 * width :] = mm(grad_ref[...], mixed_ref[...], TN).astype(BF16)
    put_grads(work, outs)


def up_kernel(normed_ref, weight_ref, hidden_ref, slope_ref):
    pre_act = mm(normed_ref[...], weight_ref[...])
    cdf = 0.5 * (1.0 + lax.erf(pre_act * 0.5**0.5))
    hidden_ref[...] = (pre_act * cdf).astype(BF16)
    density = jnp.exp(-0.5 * pre_act * pre_act) * (0.5 / math.pi) ** 0.5
    slope_ref[...] = (cdf + pre_act * density).astype(slope_ref.dtype)


def down_kernel(hidden_ref, weight_ref, out_ref):
    share = mm(hidden_ref[...], weight_ref[...], NT)

    @pl.when(pl.program_id(0) == 0)
    def _():
        out_ref[...] = share

    @pl.when(pl.program_id(0) > 0)
    def _():
        out_ref[...] += share


def down_back_kernel(grad_ref, weight_ref, hidden_ref, slope_ref, *rest):
    outs, (grad_pre_ref, work) = rest[:-2], rest[-2:]
    grad_hidden = mm(grad_ref[...], weight_ref[...])
    grad_pre_ref[...] = (grad_hidden * slope_ref[...].astype(F32)).astype(BF16)
    work[...] = mm(grad_ref[...], hidden_ref[...], TN).astype(BF16)
    put_grads(work, outs)


def up_back_kernel(normed_ref, weight_ref, grad_pre_ref, *rest):
    outs, (out_ref, work) = rest[:-2], rest[-2:]
    share = mm(grad_pre_ref[...], weight_ref[...], NT)

    @pl.when(pl.program_id(0) == 0)
    def _():
        out_ref[...] = share

    @pl.when(pl.program_id(0) > 0)
    def _():
        out_ref[...] += share

    work[...] = mm(normed_ref[...], grad_pre_ref[...], TN).astype(BF16)
    put_grads(work, outs)


def whole_spec(array):
    return pl.BlockSpec(array.shape, lambda i: (0,) * array.ndim)


def step_spec(array):
    rest = array.shape[1:]
    return pl.BlockSpec((None,) + rest, lambda i: (i,) + (0,) * len(rest))


def phase(kernel, name, inputs, outputs, scratch=(), cost=0):
    blocks = [a for a in inputs if a.ndim > 2][0].shape[0]
    spec = lambda a: whole_spec(a) if a.ndim == 2 else step_spec(a)
    return pl.pallas_call(
        kernel,
        grid=(blocks,),
        in_specs=[spec(a) for a in inputs],
        out_specs=[spec(a) for a in outputs],
        out_shape=outputs,
        scratch_shapes=list(scratch),
        cost_estimate=pl.CostEstimate(
            flops=int(cost * 800e6), bytes_accessed=int(cost * 1e6), transcendentals=0
        ),
        name=name,
    )(*inputs)


def shaped(*shape, dtype=BF16):
    return jax.ShapeDtypeStruct(shape, dtype)


def grad_shapes(weight, routed):
    blocks, depth, lanes = weight.shape
    if not routed:
        return [shaped(blocks, depth, lanes)]
    rows = BLOCK_ROWS
    return [shaped(blocks, depth // rows // 2, rows, lanes) for part in range(2)]


def attend(kind, normed, weight, stride, out_dtype):
    blocks, depth, lanes = weight.shape
    count, width = normed.shape[0], lanes // 4
    return phase(
        functools.partial(attend_kernel, kind, stride),
        kind + "_attend",
        (normed, weight),
        (
            shaped(blocks, count, 3 * width),
            shaped(blocks, count, width),
            shaped(count, depth, dtype=out_dtype),
        ),
        (pltpu.VMEM((count, width), F32), pltpu.VMEM((count, depth), F32)),
        cost=14,
    )


def attend_back(kind, normed, weight, heads, mixed, grad, stride, out_dtype, routed):
    blocks, depth, lanes = weight.shape
    count, width = normed.shape[0], lanes // 4
    *grads, out = phase(
        functools.partial(attend_back_kernel, kind, stride),
        kind + "_attend_back",
        (normed, weight, heads, mixed, grad),
        (*grad_shapes(weight, routed), shaped(count, depth, dtype=out_dtype)),
        (
            pltpu.VMEM((count, 3 * width), F32),
            pltpu.VMEM((count, depth), F32),
            pltpu.VMEM((count, width), BF16),
            pltpu.VMEM((count, 3 * width), BF16),
            pltpu.VMEM((depth, lanes), BF16),
        ),
        cost=20,
    )
    return grads, out


def along(piece, axes, distance):
    size = lax.axis_size(axes)
    return lax.ppermute(piece, axes, [(i, i ^ distance) for i in range(size)])


def after(piece, earlier):
    return piece + earlier[:1, :1] * 0


def gather_plain(shard):
    every = lax.all_gather(shard, TENSOR, axis=0, tiled=False)
    return lax.all_gather(every.reshape(-1, *shard.shape), DP, axis=1, tiled=True)


def add(*parts):
    return sum(part.astype(F32) for part in parts)


def reduce_routed(grads):
    keep, send = grads
    came = along(send, "c", 1)
    both = lambda t, q: add(keep[t, q], came[t, q]).astype(BF16)
    late, early = slice(0, 2), slice(2, 4)
    first = along(both(slice(0, 2), slice(2, 4)), "y", 1)
    second = along(both(slice(2, 4), slice(1, 4, 2)), "x", 1)
    low = add(keep[:2, :2], came[:2, :2], first)
    high = add(keep[2:, ::2], came[2:, ::2], second)
    first = along(low[:, 1].astype(BF16), "x", 1)
    second = along(high[:, 1].astype(BF16), "y", 1)
    low = add(low[:, 0], first)
    high = add(high[:, 0], second)
    far = [along(low[1].astype(BF16), TENSOR, 1)]
    far += [along(high[k].astype(BF16), TENSOR, k + 2) for k in range(2)]
    return add(low[0], *far)


def reduce_plain(grads):
    part = lax.psum_scatter(grads[0], TENSOR, scatter_dimension=0, tiled=True)[0]
    return lax.psum_scatter(part, DP, scatter_dimension=0, tiled=True).astype(F32)


def by_member(parts, me):
    return jnp.stack(
        [
            lax.dynamic_index_in_dim(parts, jnp.bitwise_xor(me, k), 0, keepdims=False)
            for k in range(parts.shape[0])
        ]
    )


def to_patches(rows, members):
    share, columns = PATCHES // members, rows.shape[1]
    me = lax.axis_index(CLIP)
    parts = rows.reshape(-1, members, share, columns).transpose(1, 0, 2, 3)
    parts = [
        lax.dynamic_index_in_dim(parts, jnp.bitwise_xor(me, k), 0, keepdims=False)
        for k in range(members)
    ]
    parts = [parts[0]] + [along(parts[k], CLIP, k) for k in range(1, members)]
    return by_member(jnp.stack(parts), me).reshape(-1, columns)


def to_frames(rows, members):
    share, columns = PATCHES // members, rows.shape[1]
    me = lax.axis_index(CLIP)
    parts = by_member(rows.reshape(members, -1, share, columns), me)
    parts = [parts[0]] + [along(parts[k], CLIP, k) for k in range(1, members)]
    parts = jnp.stack(parts)
    order = jnp.bitwise_xor(me, jnp.arange(members))
    parts = [
        lax.dynamic_index_in_dim(parts, jnp.bitwise_xor(me, k), 0, keepdims=False)
        for k in range(members)
    ]
    return jnp.stack(parts, 1).reshape(-1, columns)


CHUNKS = 4
STEPS = 4
PAD = 56


def place():
    return {axis: lax.axis_index(axis) for axis in ALL}


def moved(here, **flips):
    return tuple(here[a] + flips.get(a, 0) * (1 - 2 * here[a]) for a in ALL)


def dp_row(here, y=0, x=0, c=0):
    to = lambda a, flip: here[a] + flip * (1 - 2 * here[a])
    return to("y", y) * 4 + to("x", x) * 2 + to("c", c)


def remote(source, target, sent, received, device):
    return pltpu.make_async_remote_copy(
        src_ref=source,
        dst_ref=target,
        send_sem=sent,
        recv_sem=received,
        device_id=device,
        device_id_type=pl.DeviceIdType.MESH,
    )


def peers(here):
    found = [moved(here, s=j // 2, h=j % 2) for j in range(1, 4)]
    found += [moved(here, y=r // 4, x=r // 2 % 2, c=r % 2) for r in range(1, 8)]
    return found + [moved(here, c=1, h=1)]


def greet(here):
    barrier = pltpu.get_barrier_semaphore()
    everyone = peers(here)
    for device in everyone:
        pl.semaphore_signal(
            barrier, inc=1, device_id=device, device_id_type=pl.DeviceIdType.MESH
        )
    pl.semaphore_wait(barrier, len(everyone))


class Exchange:
    def __init__(self, here, out, back, sent, received):
        self.here, self.out, self.back = here, out, back
        self.sent, self.received = sent, received
        self.me = here["c"] * 2 + here["h"]

    def device(self, member):
        return tuple({"c": member // 2, "h": member % 2}.get(a, self.here[a]) for a in ALL)

    def start(self, member):
        @pl.when(self.me != member)
        def _():
            remote(
                self.out.at[member],
                self.back.at[self.me],
                self.sent.at[member],
                self.received.at[self.me],
                self.device(member),
            ).start()

        @pl.when(self.me == member)
        def _():
            self.back[member] = self.out[member]

    def finish(self, member):
        @pl.when(self.me != member)
        def _():
            remote(
                self.out.at[member],
                self.back.at[member],
                self.sent.at[member],
                self.received.at[member],
                self.device(member),
            ).wait()

    def send(self, rows_ref, first_row):
        share = PATCHES // 4
        for member in range(4):
            for frame in range(2):
                low = first_row(member, frame)
                self.out[member, frame, :share, :] = rows_ref[low : low + share, :].astype(BF16)
            self.start(member)

    def take(self, rows_ref, first_row):
        share = PATCHES // 4
        for member in range(4):
            self.finish(member)
            for frame in range(2):
                low = first_row(member, frame)
                rows_ref[low : low + share, :] = self.back[member, frame, :share, :].astype(F32)

    @staticmethod
    def by_frame(member, frame):
        return frame * PATCHES + member * (PATCHES // 4)

    @staticmethod
    def by_share(member, frame):
        return (member * 2 + frame) * (PATCHES // 4)

    def send_frames(self, rows_ref):
        self.send(rows_ref, self.by_frame)

    def take_patches(self, rows_ref):
        self.take(rows_ref, self.by_share)

    def send_patches(self, rows_ref):
        self.send(rows_ref, self.by_share)

    def take_frames(self, rows_ref):
        self.take(rows_ref, self.by_frame)


def by_rows(count, body, size=56):
    def step(i, carry):
        body(pl.ds(pl.multiple_of(i * size, size), size))
        return carry

    lax.fori_loop(0, count // size, step, 0)


def row_stats(rows):
    average = jnp.mean(rows, -1, keepdims=True)
    centred = rows - average
    spread = jnp.mean(centred * centred, -1, keepdims=True)
    return centred, lax.rsqrt(spread + EPSILON)


def attend_block(kind, stride, t, normed, weight, heads_ref, mixed_ref, sums):
    count, width = mixed_ref.shape[1:]
    heads_ref[t] = mm(normed, weight[:, : 3 * width]).astype(BF16)
    heads = heads_ref.at[t]
    sums[...] = jnp.zeros_like(sums)
    for start, size, group in windows(kind, count):
        bias = key_bias(start, size, group, stride)
        rows = pl.ds(start, size)
        for head in range(width // HEAD_DIM):
            low = head * HEAD_DIM
            query, key, value = head_slices(heads, rows, width, head)
            scores = mm(key, query * HEAD_DIM**-0.5, NT) + bias
            weights = jnp.exp(scores - jnp.max(scores, 0, keepdims=True))
            total = jnp.sum(weights, 0, keepdims=True)
            blended = (mm(value.T, weights.astype(BF16)) / total).T
            if group is not None:
                blended = jnp.where(row_valid(start, size, group, HEAD_DIM), blended, 0.0)
            sums[rows, low : low + HEAD_DIM] += blended
    mixed_ref[t] = sums[...].astype(BF16)
    return mm(mixed_ref[t], weight[:, 3 * width :], NT)


def forward_kernel(
    tokens_ref,
    shard_ref,
    gain_ref,
    weight_ref,
    normed_time_ref,
    time_heads_ref,
    time_mixed_ref,
    after_time_ref,
    normed_space_ref,
    space_heads_ref,
    space_mixed_ref,
    after_space_ref,
    normed_mlp_ref,
    hidden_ref,
    slope_ref,
    out_ref,
    gains_ref,
    held,
    rows_ref,
    total_ref,
    sums,
    gain_parts,
    swap_out,
    swap_back,
    piece_sent,
    piece_here,
    gain_sent,
    gain_here,
    swap_sent,
    swap_here,
    held_sem,
    own_sem,
):
    here = place()
    count = tokens_ref.shape[0]
    own_row = dp_row(here)
    greet(here)

    def row_of(part, r):
        return dp_row(here, y=r // 2, x=r % 2, c=part)

    def slot_of(k, j, row):
        return weight_ref.at[k, j, pl.ds(pl.multiple_of(row * BLOCK_ROWS, BLOCK_ROWS), BLOCK_ROWS)]

    def arrived(k, part, r, j):
        slot = slot_of(k, j, row_of(part, r))
        remote(
            slot, slot, piece_sent.at[k, 0, 0], piece_here.at[k, part, r, j], moved(here, c=1)
        ).wait_recv()

    def send(source, k, j, r, sem, part, r_there, **flips):
        remote(
            source,
            slot_of(k, j, row_of(0, r)),
            piece_sent.at[k, sem, j],
            piece_here.at[k, part, r_there, j],
            moved(here, **flips),
        ).start()

    def piece(k, j, r):
        return slot_of(k, j, row_of(0, r))

    def start_line(k):
        for j in range(1, 4):
            remote(
                shard_ref.at[k],
                slot_of(k, j, own_row),
                piece_sent.at[k, 0, j],
                piece_here.at[k, 0, 0, j],
                moved(here, s=j // 2, h=j % 2),
            ).start()

    def spread(source, k, j):
        send(source, k, j, 0, 1, 0, 1, x=1)
        send(source, k, j, 0, 2, 0, 2, y=1)
        send(source, k, j, 0, 4, 1, 0, c=1)

    def line(k, j):
        arrived(k, 0, 0, j)
        spread(piece(k, j, 0), k, j)

    def relay(k, j):
        up = j // 2
        arrived(k, 0, 1, j)
        send(piece(k, j, 1), k, j, 1, 5, 1, 1, c=1)
        arrived(k, 0, 2, j)
        send(piece(k, j, 2), k, j, 2, 6, 1, 2, c=1)
        source = slot_of(k, j, dp_row(here, y=up, x=1 - up))
        remote(
            source,
            source,
            piece_sent.at[k, 3, j],
            piece_here.at[k, 0, 3, j],
            moved(here, y=1 - up, x=up),
        ).start()

    def across(k, j):
        arrived(k, 0, 3, j)
        send(piece(k, j, 3), k, j, 3, 7, 1, 3, c=1)

    def fetch(k, t):
        return pltpu.make_async_copy(weight_ref.at[k, t], held.at[t], held_sem.at[t])

    def ready(k):
        for j in range(STEPS):
            for r in range(4):
                arrived(k, 1, r, j)
        for t in range(STEPS):
            fetch(k, t).start()

    def weight(k, t):
        fetch(k, t).wait()
        return held.at[t]

    def stored(k):
        return pltpu.make_async_copy(
            shard_ref.at[k], slot_of(k, 0, own_row), own_sem.at[k]
        )

    for k in range(CHUNKS):
        start_line(k)
        stored(k).start()
        if k == 0:
            spread(shard_ref.at[0], 0, 0)
    spread(shard_ref.at[1], 1, 0)

    def gain_copy(r):
        return remote(
            gain_ref,
            gain_parts.at[own_row],
            gain_sent.at[r],
            gain_here.at[r],
            moved(here, y=r // 4, x=r // 2 % 2, c=r % 2),
        )

    for r in range(1, 8):
        gain_copy(r).start()
    gain_parts[own_row] = gain_ref[...]
    for r in range(1, 8):
        gain_copy(r).wait()
    own = gains_ref.shape[1] // 8
    for d in range(8):
        gains_ref[:, d * own : (d + 1) * own] = gain_parts[d, :, :own].astype(F32)

    def layer_norm(source_ref, gain, target_ref):
        def body(rows):
            centred, scale = row_stats(source_ref[rows, :])
            target_ref[rows, :] = (centred * scale * gains_ref[gain : gain + 1, :]).astype(
                target_ref.dtype
            )

        by_rows(count, body)

    def exchange(index):
        return Exchange(
            here,
            swap_out.at[index],
            swap_back.at[index],
            swap_sent.at[index],
            swap_here.at[index],
        )

    def heads_phase(kind, stride, k, normed_ref, heads_ref, mixed_ref):
        total_ref[...] = jnp.zeros_like(total_ref)

        def step(t, carry):
            total_ref[...] += attend_block(
                kind, stride, t, normed_ref[...], weight(k, t), heads_ref, mixed_ref, sums
            )
            relay(k + 1, t)
            return carry

        lax.fori_loop(0, STEPS, step, 0)

    def loop(body):
        lax.fori_loop(0, STEPS, lambda t, carry: (body(t), carry)[1], 0)

    layer_norm(tokens_ref, 0, rows_ref)
    there = exchange(0)
    there.send_frames(rows_ref)
    for j in range(1, 4):
        line(0, j)
    there.take_patches(rows_ref)
    normed_time_ref[...] = rows_ref[...].astype(BF16)
    for j in range(4):
        relay(0, j)
    for j in range(1, 4):
        line(1, j)
    for j in range(4):
        across(0, j)
    for k in range(CHUNKS):
        stored(k).wait()
    ready(0)
    spread(shard_ref.at[2], 2, 0)
    heads_phase("time", PATCHES // 4, 0, normed_time_ref, time_heads_ref, time_mixed_ref)
    back = exchange(1)
    back.send_patches(total_ref)
    for j in range(1, 4):
        line(2, j)
    back.take_frames(rows_ref)
    after_time_ref[...] = tokens_ref[...] + rows_ref[...]

    layer_norm(after_time_ref, 1, normed_space_ref)
    for j in range(4):
        across(1, j)
    ready(1)
    spread(shard_ref.at[3], 3, 0)
    heads_phase("space", 1, 1, normed_space_ref, space_heads_ref, space_mixed_ref)
    for j in range(1, 4):
        line(3, j)
    after_space_ref[...] = after_time_ref[...] + total_ref[...]

    layer_norm(after_space_ref, 2, normed_mlp_ref)
    for j in range(4):
        across(2, j)
    ready(2)

    def up(t):
        pre_act = mm(normed_mlp_ref[...], weight(2, t)[...])
        cdf = 0.5 * (1.0 + lax.erf(pre_act * 0.5**0.5))
        hidden_ref[t] = (pre_act * cdf).astype(BF16)
        density = jnp.exp(-0.5 * pre_act * pre_act) * (0.5 / math.pi) ** 0.5
        slope_ref[t] = (cdf + pre_act * density).astype(BF16)
        relay(3, t)

    loop(up)
    for j in range(4):
        across(3, j)
    ready(3)
    out_ref[...] = after_space_ref[...]

    def down(t):
        out_ref[...] += mm(hidden_ref[t], weight(3, t)[...], NT)

    loop(down)

    for k in range(CHUNKS):
        for sem in range(8):
            for j in range(4):
                if sem or j:
                    slot = slot_of(k, 0, own_row)
                    remote(
                        slot,
                        slot,
                        piece_sent.at[k, sem, j],
                        piece_here.at[k, 0, 0, 0],
                        moved(here, c=1),
                    ).wait_send()


def forward(tokens, shards, gain_shard):
    count, columns = tokens.shape
    rows, lanes = shards.shape[1:]
    width = lanes // 4
    outputs = (
        shaped(CHUNKS, STEPS, columns, lanes),
        shaped(count, columns),
        shaped(STEPS, count, 3 * width),
        shaped(STEPS, count, width),
        shaped(count, columns, dtype=F32),
        shaped(count, columns),
        shaped(STEPS, count, 3 * width),
        shaped(STEPS, count, width),
        shaped(count, columns, dtype=F32),
        shaped(count, columns),
        shaped(STEPS, count, lanes),
        shaped(STEPS, count, lanes),
        shaped(count, columns, dtype=F32),
        shaped(8, columns, dtype=F32),
    )
    here = pl.BlockSpec(memory_space=pltpu.VMEM)
    return pl.pallas_call(
        forward_kernel,
        in_specs=[here] * 3,
        out_specs=[pl.BlockSpec(memory_space=pl.ANY)] + [here] * (len(outputs) - 1),
        out_shape=outputs,
        scratch_shapes=[
            pltpu.VMEM((STEPS, columns, lanes), BF16),
            pltpu.VMEM((count, columns), F32),
            pltpu.VMEM((count, columns), F32),
            pltpu.VMEM((count, width), F32),
            pltpu.VMEM((8,) + gain_shard.shape, F32),
            pltpu.VMEM((2, 4, 2, PAD, columns), BF16),
            pltpu.VMEM((2, 4, 2, PAD, columns), BF16),
            pltpu.SemaphoreType.DMA((CHUNKS, 8, 4)),
            pltpu.SemaphoreType.DMA((CHUNKS, 2, 4, 4)),
            pltpu.SemaphoreType.DMA((8,)),
            pltpu.SemaphoreType.DMA((8,)),
            pltpu.SemaphoreType.DMA((2, 4)),
            pltpu.SemaphoreType.DMA((2, 4)),
            pltpu.SemaphoreType.DMA((STEPS,)),
            pltpu.SemaphoreType.DMA((CHUNKS,)),
        ],
        compiler_params=pltpu.CompilerParams(
            collective_id=0, has_side_effects=True, vmem_limit_bytes=60 * 2**20
        ),
        name="forward",
    )(tokens, shards, gain_shard)


def sum_gains(total, own):
    for axes in ("c", "x", "y", TENSOR):
        bit = 1
        while bit < lax.axis_size(axes):
            total = total + along(total, axes, bit)
            bit *= 2
    return lax.dynamic_slice_in_dim(total, lax.axis_index(DP) * own, own, 1)


def on_device(
    routed,
    tokens,
    live_clips,
    norm_gains,
    qkv_time,
    out_time,
    qkv_space,
    out_space,
    up_weight,
    down_weight,
    cotangent,
):
    members = lax.axis_size("c") * lax.axis_size("h")
    share = PATCHES // members
    count, columns = tokens.shape
    width = qkv_time.shape[2]
    live = jnp.where(lax.axis_index("s") < live_clips[0], 1.0, 0.0).astype(F32)

    def pack_heads(qkv, out):
        rows = qkv.shape[1]
        return jnp.concatenate([qkv.transpose(1, 0, 2).reshape(rows, -1), out.T], 1)

    shards = [
        pack_heads(qkv_time, out_time),
        pack_heads(qkv_space, out_space),
        up_weight,
        down_weight.T,
    ]
    if routed:
        reduce_grads = reduce_routed
        gain_shard = jnp.pad(
            norm_gains.astype(F32), ((0, 8 - 3), (0, -norm_gains.shape[1] % 128))
        )
        (
            weights_all,
            normed_time,
            time_heads,
            time_mixed,
            after_time,
            normed_space,
            space_heads,
            space_mixed,
            after_space,
            normed_mlp,
            hidden,
            slope,
            after_mlp,
            gains,
        ) = forward(tokens, jnp.stack(shards), gain_shard)
        time_all, space_all, up_all, down_all = weights_all
        blocks, depth, lanes = up_all.shape
    else:
        reduce_grads = reduce_plain
        time_all, space_all, up_all, down_all = [gather_plain(shard) for shard in shards]
        blocks, depth, lanes = up_all.shape
        gains = lax.all_gather(norm_gains, DP, axis=1, tiled=True).astype(F32)
        normed_time = to_patches(normalize(tokens, gains[0]).astype(BF16), members)
        time_heads, time_mixed, change = attend("time", normed_time, time_all, share, BF16)
        after_time = tokens + to_frames(change, members).astype(F32)
        normed_space = normalize(after_time, gains[1]).astype(BF16)
        space_heads, space_mixed, change = attend("space", normed_space, space_all, 1, F32)
        after_space = after_time + change
        normed_mlp = normalize(after_space, gains[2]).astype(BF16)
        hidden, slope = phase(
            up_kernel,
            "up",
            (normed_mlp, up_all),
            (shaped(blocks, count, lanes), shaped(blocks, count, lanes)),
            cost=12,
        )
        (change,) = phase(
            down_kernel, "down", (hidden, down_all), (shaped(count, depth, dtype=F32),), cost=4
        )
        after_mlp = after_space + change
    output = after_mlp * live

    grad_stream = cotangent * live
    grad_low = grad_stream.astype(BF16)
    work = (pltpu.VMEM((depth, lanes), BF16),)
    *down_grads, grad_pre = phase(
        down_back_kernel,
        "down_back",
        (grad_low, down_all, hidden, slope),
        (*grad_shapes(down_all, routed), shaped(blocks, count, lanes)),
        work,
        cost=8,
    )
    *up_grads, grad_normed = phase(
        up_back_kernel,
        "up_back",
        (normed_mlp, up_all, grad_pre),
        (*grad_shapes(up_all, routed), shaped(count, depth, dtype=F32)),
        work,
        cost=8,
    )
    grad_part, gain_mlp = norm_back(after_space, gains[2], grad_normed)
    grad_stream = grad_stream + grad_part
    space_grads, grad_normed = attend_back(
        "space",
        normed_space,
        space_all,
        space_heads,
        space_mixed,
        grad_stream.astype(BF16),
        1,
        F32,
        routed,
    )
    grad_part, gain_space = norm_back(after_time, gains[1], grad_normed)
    grad_stream = grad_stream + grad_part
    grad_low = to_patches(grad_stream.astype(BF16), members)
    time_grads, grad_normed = attend_back(
        "time", normed_time, time_all, time_heads, time_mixed, grad_low, share, BF16, routed
    )
    grad_normed = to_frames(grad_normed, members).astype(F32)
    grad_part, gain_time = norm_back(tokens, gains[0], grad_normed)
    grad_tokens = grad_stream + grad_part

    down_own = reduce_grads(down_grads).T
    up_own = reduce_grads(up_grads)
    space_own = reduce_grads(space_grads)
    time_own = reduce_grads(time_grads)
    gains_own = sum_gains(jnp.stack([gain_time, gain_space, gain_mlp]), norm_gains.shape[1])

    def unpack(own):
        rows = own.shape[0]
        return own[:, : 3 * width].reshape(rows, 3, width).transpose(1, 0, 2), own[:, 3 * width :].T

    time_in_own, time_out_own = unpack(time_own)
    space_in_own, space_out_own = unpack(space_own)
    return (
        output,
        grad_tokens,
        gains_own,
        time_in_own,
        time_out_own,
        space_in_own,
        space_out_own,
        up_own,
        down_own,
    )


def solution(mesh):
    n_dp, n_tensor = mesh.devices.shape

    def run(*args):
        slots = args[0].shape[0] // (n_dp * HALF * PATCHES)
        fine = Mesh(mesh.devices.reshape(n_dp // 4, 2, 2, slots, n_tensor // slots), ALL)
        in_specs = (
            P(ALL, None),
            P(DP),
            P(None, DP),
            P(None, DP, TENSOR),
            P(TENSOR, DP),
            P(None, DP, TENSOR),
            P(TENSOR, DP),
            P(DP, TENSOR),
            P(TENSOR, DP),
            P(ALL, None),
        )
        out_specs = (in_specs[0], in_specs[0]) + in_specs[2:9]
        routed = fine.devices.shape == (2, 2, 2, 2, 2)
        return jax.shard_map(
            functools.partial(on_device, routed), mesh=fine, in_specs=in_specs, out_specs=out_specs, check_vma=False
        )(*args)

    return run
```

```python
import functools
import math

import jax
import jax.numpy as jnp
from jax import lax
from jax.experimental import pallas as pl
from jax.experimental.pallas import tpu as pltpu
from jax.sharding import Mesh, PartitionSpec as P

HEAD_DIM = 64
PATCHES = 196
HALF = 4
FRAMES = 8
EPSILON = 1e-06
F32 = jnp.float32
BF16 = jnp.bfloat16
ALL = ("y", "x", "c", "s", "h")
DP = ("y", "x", "c")
TENSOR = ("s", "h")
CLIP = ("c", "h")

NN = (((1,), (0,)), ((), ()))
NT = (((1,), (1,)), ((), ()))
TN = (((0,), (0,)), ((), ()))
BLOCK_ROWS = 96


def mm(a, b, dims=NN):
    return lax.dot_general(a, b, dims, preferred_element_type=F32)


def row_ids(shape, dim, start):
    return lax.broadcasted_iota(jnp.int32, shape, dim) + start


def windows(kind, count):
    if kind == "time":
        return [(0, count, None)]
    found = []
    for frame in range(count // PATCHES):
        low = frame * PATCHES // 16 * 16
        high = min(count, -(-(frame + 1) * PATCHES // 16) * 16)
        found.append((low, high - low, frame))
    return found


def key_bias(start, size, group, stride):
    keys = row_ids((size, size), 0, start)
    if group is None:
        together = keys % stride == row_ids((size, size), 1, start) % stride
    else:
        together = (keys >= group * PATCHES) & (keys < (group + 1) * PATCHES)
    return jnp.where(together, 0.0, -1e30)


def row_valid(start, size, group, width):
    rows = row_ids((size, width), 0, start)
    return (rows >= group * PATCHES) & (rows < (group + 1) * PATCHES)


def normalize(rows, scale_row):
    average = jnp.mean(rows, -1, keepdims=True)
    centred = rows - average
    spread = jnp.mean(centred * centred, -1, keepdims=True)
    return centred * lax.rsqrt(spread + EPSILON) * scale_row


def norm_back(rows, scale_row, grad_normed):
    unused, pullback = jax.vjp(normalize, rows, scale_row)
    return pullback(grad_normed)


def row_block(core, part, quad):
    quad_me = lax.axis_index(("y", "x"))
    block = jnp.bitwise_xor(quad_me, quad) * 2 + jnp.bitwise_xor(core, part)
    return pl.multiple_of(block * BLOCK_ROWS, BLOCK_ROWS)


def head_slices(ref, rows, width, head):
    low = head * HEAD_DIM
    return tuple(ref[rows, part * width + low : part * width + low + HEAD_DIM] for part in range(3))


def put_grads(work, outs):
    if len(outs) == 1:
        outs[0][...] = work[...]
        return
    core = lax.axis_index("c")
    for part, out in enumerate(outs):
        for quad in range(out.shape[0]):
            out[quad] = work[pl.ds(row_block(core, part, quad), out.shape[1]), :]


def attend_kernel(kind, stride, normed_ref, weight_ref, heads_ref, mixed_ref, out_ref, sums, total_ref):
    step = pl.program_id(0)
    count, width = mixed_ref.shape
    heads_ref[...] = mm(normed_ref[...], weight_ref[:, : 3 * width]).astype(BF16)
    sums[...] = jnp.zeros_like(sums)
    for start, size, group in windows(kind, count):
        bias = key_bias(start, size, group, stride)
        rows = pl.ds(start, size)
        for head in range(width // HEAD_DIM):
            low = head * HEAD_DIM
            query, key, value = head_slices(heads_ref, rows, width, head)
            scores = mm(key, query * HEAD_DIM**-0.5, NT) + bias
            weights = jnp.exp(scores - jnp.max(scores, 0, keepdims=True))
            total = jnp.sum(weights, 0, keepdims=True)
            blended = (mm(value.T, weights.astype(BF16)) / total).T
            if group is not None:
                blended = jnp.where(row_valid(start, size, group, HEAD_DIM), blended, 0.0)
            sums[rows, low : low + HEAD_DIM] += blended
    mixed_ref[...] = sums[...].astype(BF16)
    share = mm(mixed_ref[...], weight_ref[:, 3 * width :], NT)

    @pl.when(step == 0)
    def _():
        total_ref[...] = share

    @pl.when(step > 0)
    def _():
        total_ref[...] += share

    @pl.when(step == pl.num_programs(0) - 1)
    def _():
        out_ref[...] = total_ref[...].astype(out_ref.dtype)


def attend_back_kernel(
    kind, stride, normed_ref, weight_ref, heads_ref, mixed_ref, grad_ref, *rest
):
    outs, (out_ref, sums, total_ref, grad_mixed, grad_heads, work) = rest[:-6], rest[-6:]
    step = pl.program_id(0)
    count, width = mixed_ref.shape
    scale = HEAD_DIM**-0.5
    grad_mixed[...] = mm(grad_ref[...], weight_ref[:, 3 * width :]).astype(BF16)
    sums[...] = jnp.zeros_like(sums)
    for start, size, group in windows(kind, count):
        bias = key_bias(start, size, group, stride)
        rows = pl.ds(start, size)
        for head in range(width // HEAD_DIM):
            low = head * HEAD_DIM
            query, key, value = head_slices(heads_ref, rows, width, head)
            query = query * scale
            grad = grad_mixed[rows, low : low + HEAD_DIM]
            if group is not None:
                valid = row_valid(start, size, group, HEAD_DIM)
                grad = jnp.where(valid, grad.astype(F32), 0.0).astype(BF16)
            scores = mm(key, query, NT) + bias
            weights = jnp.exp(scores - jnp.max(scores, 0, keepdims=True))
            weights = weights / jnp.sum(weights, 0, keepdims=True)
            grad_weights = mm(value, grad, NT)
            row_terms = jnp.sum(weights * grad_weights, 0, keepdims=True)
            grad_scores = (weights * (grad_weights - row_terms)).astype(BF16)
            sums[rows, low : low + HEAD_DIM] += (mm(key.T, grad_scores) * scale).T
            low += width
            sums[rows, low : low + HEAD_DIM] += mm(grad_scores, query)
            low += width
            sums[rows, low : low + HEAD_DIM] += mm(weights.astype(BF16), grad)
    grad_heads[...] = sums[...].astype(BF16)
    share = mm(grad_heads[...], weight_ref[:, : 3 * width], NT)

    @pl.when(step == 0)
    def _():
        total_ref[...] = share

    @pl.when(step > 0)
    def _():
        total_ref[...] += share

    @pl.when(step == pl.num_programs(0) - 1)
    def _():
        out_ref[...] = total_ref[...].astype(out_ref.dtype)

    work[:, : 3 * width] = mm(normed_ref[...], grad_heads[...], TN).astype(BF16)
    work[:, 3 * width :] = mm(grad_ref[...], mixed_ref[...], TN).astype(BF16)
    put_grads(work, outs)


def up_kernel(normed_ref, weight_ref, hidden_ref, slope_ref):
    pre_act = mm(normed_ref[...], weight_ref[...])
    cdf = 0.5 * (1.0 + lax.erf(pre_act * 0.5**0.5))
    hidden_ref[...] = (pre_act * cdf).astype(BF16)
    density = jnp.exp(-0.5 * pre_act * pre_act) * (0.5 / math.pi) ** 0.5
    slope_ref[...] = (cdf + pre_act * density).astype(slope_ref.dtype)


def down_kernel(hidden_ref, weight_ref, out_ref):
    share = mm(hidden_ref[...], weight_ref[...], NT)

    @pl.when(pl.program_id(0) == 0)
    def _():
        out_ref[...] = share

    @pl.when(pl.program_id(0) > 0)
    def _():
        out_ref[...] += share


def down_back_kernel(grad_ref, weight_ref, hidden_ref, slope_ref, *rest):
    outs, (grad_pre_ref, work) = rest[:-2], rest[-2:]
    grad_hidden = mm(grad_ref[...], weight_ref[...])
    grad_pre_ref[...] = (grad_hidden * slope_ref[...].astype(F32)).astype(BF16)
    work[...] = mm(grad_ref[...], hidden_ref[...], TN).astype(BF16)
    put_grads(work, outs)


def up_back_kernel(normed_ref, weight_ref, grad_pre_ref, *rest):
    outs, (out_ref, work) = rest[:-2], rest[-2:]
    share = mm(grad_pre_ref[...], weight_ref[...], NT)

    @pl.when(pl.program_id(0) == 0)
    def _():
        out_ref[...] = share

    @pl.when(pl.program_id(0) > 0)
    def _():
        out_ref[...] += share

    work[...] = mm(normed_ref[...], grad_pre_ref[...], TN).astype(BF16)
    put_grads(work, outs)


def whole_spec(array):
    return pl.BlockSpec(array.shape, lambda i: (0,) * array.ndim)


def step_spec(array):
    rest = array.shape[1:]
    return pl.BlockSpec((None,) + rest, lambda i: (i,) + (0,) * len(rest))


def phase(kernel, name, inputs, outputs, scratch=(), cost=0):
    blocks = [a for a in inputs if a.ndim > 2][0].shape[0]
    spec = lambda a: whole_spec(a) if a.ndim == 2 else step_spec(a)
    return pl.pallas_call(
        kernel,
        grid=(blocks,),
        in_specs=[spec(a) for a in inputs],
        out_specs=[spec(a) for a in outputs],
        out_shape=outputs,
        scratch_shapes=list(scratch),
        cost_estimate=pl.CostEstimate(
            flops=int(cost * 800e6), bytes_accessed=int(cost * 1e6), transcendentals=0
        ),
        name=name,
    )(*inputs)


def shaped(*shape, dtype=BF16):
    return jax.ShapeDtypeStruct(shape, dtype)


def grad_shapes(weight, routed):
    blocks, depth, lanes = weight.shape
    if not routed:
        return [shaped(blocks, depth, lanes)]
    rows = BLOCK_ROWS
    return [shaped(blocks, depth // rows // 2, rows, lanes) for part in range(2)]


def attend(kind, normed, weight, stride, out_dtype):
    blocks, depth, lanes = weight.shape
    count, width = normed.shape[0], lanes // 4
    return phase(
        functools.partial(attend_kernel, kind, stride),
        kind + "_attend",
        (normed, weight),
        (
            shaped(blocks, count, 3 * width),
            shaped(blocks, count, width),
            shaped(count, depth, dtype=out_dtype),
        ),
        (pltpu.VMEM((count, width), F32), pltpu.VMEM((count, depth), F32)),
        cost=14,
    )


def attend_back(kind, normed, weight, heads, mixed, grad, stride, out_dtype, routed):
    blocks, depth, lanes = weight.shape
    count, width = normed.shape[0], lanes // 4
    *grads, out = phase(
        functools.partial(attend_back_kernel, kind, stride),
        kind + "_attend_back",
        (normed, weight, heads, mixed, grad),
        (*grad_shapes(weight, routed), shaped(count, depth, dtype=out_dtype)),
        (
            pltpu.VMEM((count, 3 * width), F32),
            pltpu.VMEM((count, depth), F32),
            pltpu.VMEM((count, width), BF16),
            pltpu.VMEM((count, 3 * width), BF16),
            pltpu.VMEM((depth, lanes), BF16),
        ),
        cost=20,
    )
    return grads, out


def along(piece, axes, distance):
    size = lax.axis_size(axes)
    return lax.ppermute(piece, axes, [(i, i ^ distance) for i in range(size)])


def after(piece, earlier):
    return piece + earlier[:1, :1] * 0


def gather_plain(shard):
    every = lax.all_gather(shard, TENSOR, axis=0, tiled=False)
    return lax.all_gather(every.reshape(-1, *shard.shape), DP, axis=1, tiled=True)


def reduce_plain(grads):
    part = lax.psum_scatter(grads[0], TENSOR, scatter_dimension=0, tiled=True)[0]
    return lax.psum_scatter(part, DP, scatter_dimension=0, tiled=True).astype(F32)


def by_member(parts, me):
    return jnp.stack(
        [
            lax.dynamic_index_in_dim(parts, jnp.bitwise_xor(me, k), 0, keepdims=False)
            for k in range(parts.shape[0])
        ]
    )


def to_patches(rows, members):
    share, columns = PATCHES // members, rows.shape[1]
    me = lax.axis_index(CLIP)
    parts = rows.reshape(-1, members, share, columns).transpose(1, 0, 2, 3)
    parts = [
        lax.dynamic_index_in_dim(parts, jnp.bitwise_xor(me, k), 0, keepdims=False)
        for k in range(members)
    ]
    parts = [parts[0]] + [along(parts[k], CLIP, k) for k in range(1, members)]
    return by_member(jnp.stack(parts), me).reshape(-1, columns)


def to_frames(rows, members):
    share, columns = PATCHES // members, rows.shape[1]
    me = lax.axis_index(CLIP)
    parts = by_member(rows.reshape(members, -1, share, columns), me)
    parts = [parts[0]] + [along(parts[k], CLIP, k) for k in range(1, members)]
    parts = jnp.stack(parts)
    order = jnp.bitwise_xor(me, jnp.arange(members))
    parts = [
        lax.dynamic_index_in_dim(parts, jnp.bitwise_xor(me, k), 0, keepdims=False)
        for k in range(members)
    ]
    return jnp.stack(parts, 1).reshape(-1, columns)


CHUNKS = 4
STEPS = 4
PAD = 56


def place():
    return {axis: lax.axis_index(axis) for axis in ALL}


def moved(here, **flips):
    return tuple(here[a] + flips.get(a, 0) * (1 - 2 * here[a]) for a in ALL)


def dp_row(here, y=0, x=0, c=0):
    to = lambda a, flip: here[a] + flip * (1 - 2 * here[a])
    return to("y", y) * 4 + to("x", x) * 2 + to("c", c)


def remote(source, target, sent, received, device):
    return pltpu.make_async_remote_copy(
        src_ref=source,
        dst_ref=target,
        send_sem=sent,
        recv_sem=received,
        device_id=device,
        device_id_type=pl.DeviceIdType.MESH,
    )


def peers(here):
    found = [moved(here, s=j // 2, h=j % 2) for j in range(1, 4)]
    found += [moved(here, y=r // 4, x=r // 2 % 2, c=r % 2) for r in range(1, 8)]
    return found + [moved(here, c=1, h=1)]


def greet(here):
    barrier = pltpu.get_barrier_semaphore()
    everyone = peers(here)
    for device in everyone:
        pl.semaphore_signal(
            barrier, inc=1, device_id=device, device_id_type=pl.DeviceIdType.MESH
        )
    pl.semaphore_wait(barrier, len(everyone))


class Exchange:
    def __init__(self, here, out, back, sent, received):
        self.here, self.out, self.back = here, out, back
        self.sent, self.received = sent, received
        self.me = here["c"] * 2 + here["h"]

    def device(self, member):
        return tuple({"c": member // 2, "h": member % 2}.get(a, self.here[a]) for a in ALL)

    def start(self, member):
        @pl.when(self.me != member)
        def _():
            remote(
                self.out.at[member],
                self.back.at[self.me],
                self.sent.at[member],
                self.received.at[self.me],
                self.device(member),
            ).start()

        @pl.when(self.me == member)
        def _():
            self.back[member] = self.out[member]

    def finish(self, member):
        @pl.when(self.me != member)
        def _():
            remote(
                self.out.at[member],
                self.back.at[member],
                self.sent.at[member],
                self.received.at[member],
                self.device(member),
            ).wait()

    def send(self, rows_ref, first_row):
        share = PATCHES // 4
        for member in range(4):
            for frame in range(2):
                low = first_row(member, frame)
                self.out[member, frame, :share, :] = rows_ref[low : low + share, :].astype(BF16)
            self.start(member)

    def take(self, rows_ref, first_row):
        share = PATCHES // 4
        for member in range(4):
            self.finish(member)
            for frame in range(2):
                low = first_row(member, frame)
                rows_ref[low : low + share, :] = self.back[member, frame, :share, :].astype(F32)

    @staticmethod
    def by_frame(member, frame):
        return frame * PATCHES + member * (PATCHES // 4)

    @staticmethod
    def by_share(member, frame):
        return (member * 2 + frame) * (PATCHES // 4)

    def send_frames(self, rows_ref):
        self.send(rows_ref, self.by_frame)

    def take_patches(self, rows_ref):
        self.take(rows_ref, self.by_share)

    def send_patches(self, rows_ref):
        self.send(rows_ref, self.by_share)

    def take_frames(self, rows_ref):
        self.take(rows_ref, self.by_frame)


def by_rows(count, body, size=56):
    def step(i, carry):
        body(pl.ds(pl.multiple_of(i * size, size), size))
        return carry

    lax.fori_loop(0, count // size, step, 0)


def row_stats(rows):
    average = jnp.mean(rows, -1, keepdims=True)
    centred = rows - average
    spread = jnp.mean(centred * centred, -1, keepdims=True)
    return centred, lax.rsqrt(spread + EPSILON)


def attend_block(kind, stride, t, normed, weight, heads_ref, mixed_ref, sums, bias_ref):
    count, width = mixed_ref.shape[1:]
    heads_ref[t] = mm(normed, weight[:, : 3 * width]).astype(BF16)
    heads = heads_ref.at[t]
    sums[...] = jnp.zeros_like(sums)
    for start, size, group in windows(kind, count):
        bias = bias_ref[...] if group is None else key_bias(start, size, group, stride)
        rows = pl.ds(start, size)
        for head in range(width // HEAD_DIM):
            low = head * HEAD_DIM
            query, key, value = head_slices(heads, rows, width, head)
            scores = mm(key, query * HEAD_DIM**-0.5, NT) + bias
            weights = jnp.exp(scores - jnp.max(scores, 0, keepdims=True))
            total = jnp.sum(weights, 0, keepdims=True)
            blended = (mm(value.T, weights.astype(BF16)) / total).T
            if group is not None:
                blended = jnp.where(row_valid(start, size, group, HEAD_DIM), blended, 0.0)
            sums[rows, low : low + HEAD_DIM] += blended
    mixed_ref[t] = sums[...].astype(BF16)
    return mm(mixed_ref[t], weight[:, 3 * width :], NT)


def forward_kernel(
    tokens_ref,
    shard_ref,
    gain_ref,
    weight_ref,
    normed_time_ref,
    time_heads_ref,
    time_mixed_ref,
    after_time_ref,
    normed_space_ref,
    space_heads_ref,
    space_mixed_ref,
    after_space_ref,
    normed_mlp_ref,
    hidden_ref,
    slope_ref,
    out_ref,
    gains_ref,
    held,
    rows_ref,
    total_ref,
    sums,
    bias_ref,
    gain_parts,
    swap_out,
    swap_back,
    piece_sent,
    piece_here,
    gain_sent,
    gain_here,
    swap_sent,
    swap_here,
    held_sem,
    own_sem,
):
    here = place()
    count = tokens_ref.shape[0]
    own_row = dp_row(here)
    greet(here)

    def row_of(part, r):
        return dp_row(here, y=r // 2, x=r % 2, c=part)

    def slot_of(k, j, row):
        return weight_ref.at[k, j, pl.ds(pl.multiple_of(row * BLOCK_ROWS, BLOCK_ROWS), BLOCK_ROWS)]

    def arrived(k, part, r, j):
        slot = slot_of(k, j, row_of(part, r))
        remote(
            slot, slot, piece_sent.at[k, 0, 0], piece_here.at[k, part, r, j], moved(here, c=1)
        ).wait_recv()

    def send(source, k, j, r, sem, part, r_there, **flips):
        remote(
            source,
            slot_of(k, j, row_of(0, r)),
            piece_sent.at[k, sem, j],
            piece_here.at[k, part, r_there, j],
            moved(here, **flips),
        ).start()

    def piece(k, j, r):
        return slot_of(k, j, row_of(0, r))

    def start_line(k):
        for j in range(1, 4):
            remote(
                shard_ref.at[k],
                slot_of(k, j, own_row),
                piece_sent.at[k, 0, j],
                piece_here.at[k, 0, 0, j],
                moved(here, s=j // 2, h=j % 2),
            ).start()

    def spread(source, k, j):
        send(source, k, j, 0, 1, 0, 1, x=1)
        send(source, k, j, 0, 2, 0, 2, y=1)
        send(source, k, j, 0, 4, 1, 0, c=1)

    def line(k, j):
        arrived(k, 0, 0, j)
        spread(piece(k, j, 0), k, j)

    def relay(k, j):
        up = j // 2
        arrived(k, 0, 1, j)
        send(piece(k, j, 1), k, j, 1, 5, 1, 1, c=1)
        arrived(k, 0, 2, j)
        send(piece(k, j, 2), k, j, 2, 6, 1, 2, c=1)
        source = slot_of(k, j, dp_row(here, y=up, x=1 - up))
        remote(
            source,
            source,
            piece_sent.at[k, 3, j],
            piece_here.at[k, 0, 3, j],
            moved(here, y=1 - up, x=up),
        ).start()

    def across(k, j):
        arrived(k, 0, 3, j)
        send(piece(k, j, 3), k, j, 3, 7, 1, 3, c=1)

    def fetch(k, t):
        return pltpu.make_async_copy(weight_ref.at[k, t], held.at[t], held_sem.at[t])

    def ready(k):
        for j in range(STEPS):
            for r in range(4):
                arrived(k, 1, r, j)
        for t in range(STEPS):
            fetch(k, t).start()

    def weight(k, t):
        fetch(k, t).wait()
        return held.at[t]

    def stored(k):
        return pltpu.make_async_copy(
            shard_ref.at[k], slot_of(k, 0, own_row), own_sem.at[k]
        )

    for k in range(CHUNKS):
        start_line(k)
        stored(k).start()
        if k == 0:
            spread(shard_ref.at[0], 0, 0)
    spread(shard_ref.at[1], 1, 0)

    def gain_copy(r):
        return remote(
            gain_ref,
            gain_parts.at[own_row],
            gain_sent.at[r],
            gain_here.at[r],
            moved(here, y=r // 4, x=r // 2 % 2, c=r % 2),
        )

    for r in range(1, 8):
        gain_copy(r).start()
    gain_parts[own_row] = gain_ref[...]
    for r in range(1, 8):
        gain_copy(r).wait()
    own = gains_ref.shape[1] // 8
    for d in range(8):
        gains_ref[:, d * own : (d + 1) * own] = gain_parts[d, :, :own].astype(F32)

    def layer_norm(source_ref, gain, target_ref):
        def body(rows):
            centred, scale = row_stats(source_ref[rows, :])
            target_ref[rows, :] = (centred * scale * gains_ref[gain : gain + 1, :]).astype(
                target_ref.dtype
            )

        by_rows(count, body)

    def exchange(index):
        return Exchange(
            here,
            swap_out.at[index],
            swap_back.at[index],
            swap_sent.at[index],
            swap_here.at[index],
        )

    def heads_phase(kind, stride, k, normed_ref, heads_ref, mixed_ref):
        total_ref[...] = jnp.zeros_like(total_ref)

        def step(t, carry):
            total_ref[...] += attend_block(
                kind, stride, t, normed_ref[...], weight(k, t), heads_ref, mixed_ref, sums, bias_ref
            )
            relay(k + 1, t)
            return carry

        lax.fori_loop(0, STEPS, step, 0)

    def loop(body):
        lax.fori_loop(0, STEPS, lambda t, carry: (body(t), carry)[1], 0)

    bias_ref[...] = key_bias(0, count, None, PATCHES // 4)
    layer_norm(tokens_ref, 0, rows_ref)
    there = exchange(0)
    there.send_frames(rows_ref)
    for j in range(1, 4):
        line(0, j)
    there.take_patches(rows_ref)
    normed_time_ref[...] = rows_ref[...].astype(BF16)
    for j in range(4):
        relay(0, j)
    for j in range(1, 4):
        line(1, j)
    for j in range(4):
        across(0, j)
    for k in range(CHUNKS):
        stored(k).wait()
    ready(0)
    spread(shard_ref.at[2], 2, 0)
    heads_phase("time", PATCHES // 4, 0, normed_time_ref, time_heads_ref, time_mixed_ref)
    back = exchange(1)
    back.send_patches(total_ref)
    for j in range(1, 4):
        line(2, j)
    back.take_frames(rows_ref)
    after_time_ref[...] = tokens_ref[...] + rows_ref[...]

    layer_norm(after_time_ref, 1, normed_space_ref)
    for j in range(4):
        across(1, j)
    ready(1)
    spread(shard_ref.at[3], 3, 0)
    heads_phase("space", 1, 1, normed_space_ref, space_heads_ref, space_mixed_ref)
    for j in range(1, 4):
        line(3, j)
    after_space_ref[...] = after_time_ref[...] + total_ref[...]

    layer_norm(after_space_ref, 2, normed_mlp_ref)
    for j in range(4):
        across(2, j)
    ready(2)

    def up(t):
        pre_act = mm(normed_mlp_ref[...], weight(2, t)[...])
        cdf = 0.5 * (1.0 + lax.erf(pre_act * 0.5**0.5))
        hidden_ref[t] = (pre_act * cdf).astype(BF16)
        density = jnp.exp(-0.5 * pre_act * pre_act) * (0.5 / math.pi) ** 0.5
        slope_ref[t] = (cdf + pre_act * density).astype(BF16)
        relay(3, t)

    loop(up)
    for j in range(4):
        across(3, j)
    ready(3)
    out_ref[...] = after_space_ref[...]

    def down(t):
        out_ref[...] += mm(hidden_ref[t], weight(3, t)[...], NT)

    loop(down)

    for k in range(CHUNKS):
        for sem in range(8):
            for j in range(4):
                if sem or j:
                    slot = slot_of(k, 0, own_row)
                    remote(
                        slot,
                        slot,
                        piece_sent.at[k, sem, j],
                        piece_here.at[k, 0, 0, 0],
                        moved(here, c=1),
                    ).wait_send()


def forward(tokens, shards, gain_shard):
    count, columns = tokens.shape
    rows, lanes = shards.shape[1:]
    width = lanes // 4
    outputs = (
        shaped(CHUNKS, STEPS, columns, lanes),
        shaped(count, columns),
        shaped(STEPS, count, 3 * width),
        shaped(STEPS, count, width),
        shaped(count, columns, dtype=F32),
        shaped(count, columns),
        shaped(STEPS, count, 3 * width),
        shaped(STEPS, count, width),
        shaped(count, columns, dtype=F32),
        shaped(count, columns),
        shaped(STEPS, count, lanes),
        shaped(STEPS, count, lanes),
        shaped(count, columns, dtype=F32),
        shaped(8, columns, dtype=F32),
    )
    here = pl.BlockSpec(memory_space=pltpu.VMEM)
    return pl.pallas_call(
        forward_kernel,
        in_specs=[here] * 3,
        out_specs=[pl.BlockSpec(memory_space=pl.ANY)] + [here] * (len(outputs) - 1),
        out_shape=outputs,
        scratch_shapes=[
            pltpu.VMEM((STEPS, columns, lanes), BF16),
            pltpu.VMEM((count, columns), F32),
            pltpu.VMEM((count, columns), F32),
            pltpu.VMEM((count, width), F32),
            pltpu.VMEM((count, count), F32),
            pltpu.VMEM((8,) + gain_shard.shape, F32),
            pltpu.VMEM((2, 4, 2, PAD, columns), BF16),
            pltpu.VMEM((2, 4, 2, PAD, columns), BF16),
            pltpu.SemaphoreType.DMA((CHUNKS, 8, 4)),
            pltpu.SemaphoreType.DMA((CHUNKS, 2, 4, 4)),
            pltpu.SemaphoreType.DMA((8,)),
            pltpu.SemaphoreType.DMA((8,)),
            pltpu.SemaphoreType.DMA((2, 4)),
            pltpu.SemaphoreType.DMA((2, 4)),
            pltpu.SemaphoreType.DMA((STEPS,)),
            pltpu.SemaphoreType.DMA((CHUNKS,)),
        ],
        compiler_params=pltpu.CompilerParams(
            collective_id=0, has_side_effects=True, vmem_limit_bytes=60 * 2**20
        ),
        name="forward",
    )(tokens, shards, gain_shard)


def attend_back_block(
    kind, stride, heads, mixed, grad, normed, weight, grad_mixed, sums, grad_heads, bias_ref
):
    count, width = mixed.shape
    scale = HEAD_DIM**-0.5
    grad_mixed[...] = mm(grad[...], weight[:, 3 * width :]).astype(BF16)
    sums[...] = jnp.zeros_like(sums)
    for start, size, group in windows(kind, count):
        bias = bias_ref[...] if group is None else key_bias(start, size, group, stride)
        rows = pl.ds(start, size)
        for head in range(width // HEAD_DIM):
            low = head * HEAD_DIM
            query, key, value = head_slices(heads, rows, width, head)
            query = query * scale
            grad_here = grad_mixed[rows, low : low + HEAD_DIM]
            if group is not None:
                valid = row_valid(start, size, group, HEAD_DIM)
                grad_here = jnp.where(valid, grad_here.astype(F32), 0.0).astype(BF16)
            scores = mm(key, query, NT) + bias
            weights = jnp.exp(scores - jnp.max(scores, 0, keepdims=True))
            weights = weights * (1.0 / jnp.sum(weights, 0, keepdims=True))
            grad_weights = mm(value, grad_here, NT)
            row_terms = jnp.sum(weights * grad_weights, 0, keepdims=True)
            grad_scores = (weights * (grad_weights - row_terms)).astype(BF16)
            sums[rows, low : low + HEAD_DIM] += (mm(key.T, grad_scores) * scale).T
            low += width
            sums[rows, low : low + HEAD_DIM] += mm(grad_scores, query)
            low += width
            sums[rows, low : low + HEAD_DIM] += mm(weights.astype(BF16), grad_here)
    grad_heads[...] = sums[...].astype(BF16)
    return mm(grad_heads[...], weight[:, : 3 * width], NT)


def backward_kernel(
    grad_ref,
    weight_ref,
    tokens_ref,
    normed_time_ref,
    time_heads_ref,
    time_mixed_ref,
    after_time_ref,
    normed_space_ref,
    space_heads_ref,
    space_mixed_ref,
    after_space_ref,
    normed_mlp_ref,
    hidden_ref,
    slope_ref,
    gains_ref,
    stream_ref,
    own_ref,
    own_gain_ref,
    held,
    work,
    keep,
    came,
    first,
    second,
    third,
    grad_pre,
    low_ref,
    total_ref,
    rows_ref,
    grad_mixed,
    sums,
    grad_heads,
    bias_ref,
    gain_sums,
    gain_line,
    gain_out,
    gain_parts,
    swap_out,
    swap_back,
    held_sem,
    core_sent,
    core_here,
    first_sent,
    first_here,
    second_sent,
    second_here,
    third_sent,
    third_here,
    gain_sent,
    gain_here,
    swap_sent,
    swap_here,
    credit,
):
    here = place()
    count = grad_ref.shape[0]
    greet(here)

    def turn(step):
        return step % STEPS // 2

    def row_of(step, part, i):
        u = turn(step)
        y = (1 - u) * (i // 2) + u * (i % 2)
        x = (1 - u) * (i % 2) + u * (i // 2)
        row = dp_row(here, y=y, x=x, c=part)
        return pl.ds(pl.multiple_of(row * BLOCK_ROWS, BLOCK_ROWS), BLOCK_ROWS)

    def core_copy(step, i):
        return remote(
            work.at[step % 2, row_of(step, 1, i)],
            came.at[step % 4, i],
            core_sent.at[step % 2, i],
            core_here.at[step % 4, i],
            moved(here, c=1),
        )

    def first_copy(step):
        u = turn(step)
        return remote(
            keep.at[step, pl.ds(2, 2)],
            first.at[step],
            first_sent.at[step],
            first_here.at[step],
            moved(here, y=1 - u, x=u),
        )

    def second_copy(step):
        u = turn(step)
        return remote(
            keep.at[step, 1],
            second.at[step],
            second_sent.at[step],
            second_here.at[step],
            moved(here, y=u, x=1 - u),
        )

    def third_copy(step):
        return remote(
            keep.at[step, 0],
            third.at[step],
            third_sent.at[step],
            third_here.at[step],
            moved(here, s=step % STEPS // 2, h=step % 2),
        )

    def fetch(step):
        return pltpu.make_async_copy(
            weight_ref.at[CHUNKS - 1 - step // STEPS, step % STEPS],
            held.at[step % 2],
            held_sem.at[step % 2],
        )

    def begin(step):
        fetch(step).wait()

        @pl.when(step < CHUNKS * STEPS - 1)
        def _():
            fetch(step + 1).start()

        @pl.when(step >= 2)
        def _():
            for i in range(4):
                core_copy(step - 2, i).wait_send()

        return held.at[step % 2]

    def emit(step):
        @pl.when(step >= 4)
        def _():
            pl.semaphore_wait(credit, 1)

        for i in range(4):
            core_copy(step, i).start()

    def take_core(step):
        for i in range(4):
            core_copy(step, i).wait_recv()
        for i in (2, 3, 0, 1):
            own = work[step % 2, row_of(step, 0, i), :].astype(F32)
            keep[step, i] = (own + came[step % 4, i].astype(F32)).astype(BF16)
            if i == 3:
                first_copy(step).start()

        @pl.when(step < CHUNKS * STEPS - 4)
        def _():
            pl.semaphore_signal(
                credit,
                inc=1,
                device_id=moved(here, c=1),
                device_id_type=pl.DeviceIdType.MESH,
            )

    def take_first(step):
        first_copy(step).wait_recv()
        for i in (1, 0):
            both = keep[step, i].astype(F32) + first[step, i].astype(F32)
            keep[step, i] = both.astype(BF16)
            if i:
                second_copy(step).start()

    def take_second(step):
        second_copy(step).wait_recv()
        keep[step, 0] = (keep[step, 0].astype(F32) + second[step].astype(F32)).astype(BF16)

        @pl.when(step % STEPS > 0)
        def _():
            third_copy(step).start()

    def take_third(phase_index):
        low = phase_index * STEPS
        total = keep[low, 0].astype(F32)
        for j in range(1, STEPS):
            third_copy(low + j).wait_recv()
            total = total + third[low + j].astype(F32)
        own_ref[phase_index] = total

    def loop(index, compute, *events):
        def body(t, carry):
            step = index * STEPS + t
            compute(t, begin(step), work.at[step % 2])
            emit(step)
            for event, low, start in events:
                if start:

                    @pl.when(t >= start)
                    def _(event=event, low=low):
                        event(low + t)

                else:
                    event(low + t)
            return carry

        lax.fori_loop(0, STEPS, body, 0)

    def norm_back(source_ref, gain, grad_normed_ref):
        def body(rows):
            centred, scale = row_stats(source_ref[rows, :])
            unit = centred * scale
            grad_normed = grad_normed_ref[rows, :]
            e = grad_normed * gains_ref[gain : gain + 1, :]
            mean = jnp.mean(e, -1, keepdims=True)
            tilt = jnp.mean(e * unit, -1, keepdims=True)
            stream_ref[rows, :] += scale * (e - mean - unit * tilt)
            gain_sums[gain : gain + 1, :] += jnp.sum(grad_normed * unit, 0, keepdims=True)

        by_rows(count, body)

    def exchange(index):
        return Exchange(
            here,
            swap_out.at[index],
            swap_back.at[index],
            swap_sent.at[index],
            swap_here.at[index],
        )

    fetch(0).start()
    gain_sums[...] = jnp.zeros_like(gain_sums)
    stream_ref[...] = grad_ref[...]
    low_ref[...] = grad_ref[...].astype(BF16)
    bias_ref[...] = key_bias(0, count, None, PATCHES // 4)

    def down(t, weight, out):
        grad_hidden = mm(low_ref[...], weight[...])
        grad_pre[t] = (grad_hidden * slope_ref[t].astype(F32)).astype(BF16)
        out[...] = mm(low_ref[...], hidden_ref[t], TN).astype(BF16)

    loop(0, down, (take_core, -1, 1))
    total_ref[...] = jnp.zeros_like(total_ref)

    def up(t, weight, out):
        total_ref[...] += mm(grad_pre[t], weight[...], NT)
        out[...] = mm(normed_mlp_ref[...], grad_pre[t], TN).astype(BF16)

    loop(1, up, (take_core, 3, 0), (take_first, -1, 1))
    norm_back(after_space_ref, 2, total_ref)
    low_ref[...] = stream_ref[...].astype(BF16)

    def attention(kind, heads_ref, mixed_ref, normed_ref):
        total_ref[...] = jnp.zeros_like(total_ref)
        width = mixed_ref.shape[2]

        def compute(t, weight, out):
            total_ref[...] += attend_back_block(
                kind,
                PATCHES // 4,
                heads_ref.at[t],
                mixed_ref.at[t],
                low_ref,
                normed_ref,
                weight,
                grad_mixed,
                sums,
                grad_heads,
                bias_ref,
            )
            out[:, : 3 * width] = mm(normed_ref[...], grad_heads[...], TN).astype(BF16)
            out[:, 3 * width :] = mm(low_ref[...], mixed_ref[t], TN).astype(BF16)

        return compute

    loop(
        2,
        attention("space", space_heads_ref, space_mixed_ref, normed_space_ref),
        (take_core, 7, 0),
        (take_first, 3, 0),
        (take_second, 0, 0),
    )
    norm_back(after_time_ref, 1, total_ref)
    there = exchange(0)
    there.send_frames(stream_ref)
    take_core(11)
    take_first(7)
    take_second(4)
    take_third(0)
    there.take_patches(rows_ref)
    low_ref[...] = rows_ref[...].astype(BF16)
    loop(
        3,
        attention("time", time_heads_ref, time_mixed_ref, normed_time_ref),
        (take_core, 11, 1),
        (take_first, 8, 0),
        (take_second, 5, 0),
    )
    back = exchange(1)
    back.send_patches(total_ref)
    take_core(15)
    for step in range(12, 15):
        take_first(step)
    for step in range(9, 12):
        take_second(step)
    take_third(1)
    back.take_frames(rows_ref)
    norm_back(tokens_ref, 0, rows_ref)

    line_index = here["s"] * 2 + here["h"]
    own_row = dp_row(here)

    def gain_line_copy(j):
        return remote(
            gain_sums,
            gain_line.at[line_index],
            gain_sent.at[0, j],
            gain_here.at[0, j],
            moved(here, s=j // 2, h=j % 2),
        )

    def gain_copy(r):
        flips = {"y": r // 4, "x": r // 2 % 2, "c": r % 2}
        return remote(
            gain_out.at[dp_row(here, **flips)],
            gain_parts.at[own_row],
            gain_sent.at[1, r],
            gain_here.at[1, r],
            moved(here, **flips),
        )

    for j in range(1, 4):
        gain_line_copy(j).start()
    gain_line[line_index] = gain_sums[...]
    take_first(15)
    for step in range(12, 15):
        take_second(step)
    for j in range(1, 4):
        gain_line_copy(j).wait()
    total = gain_line[0] + gain_line[1] + gain_line[2] + gain_line[3]
    own = own_gain_ref.shape[1]
    span = total.shape[1] // 8
    for d in range(8):
        gain_out[d, :, :span] = total[:, d * span : (d + 1) * span]
    for r in range(1, 8):
        gain_copy(r).start()
    gain_parts[own_row] = gain_out[own_row]
    take_second(15)
    take_third(2)
    for r in range(1, 8):
        gain_copy(r).wait()
    total = gain_parts[0]
    for d in range(1, 8):
        total = total + gain_parts[d]
    own_gain_ref[...] = total
    take_third(3)

    for step in range(CHUNKS * STEPS):
        if step >= CHUNKS * STEPS - 2:
            for i in range(4):
                core_copy(step, i).wait_send()
        first_copy(step).wait_send()
        second_copy(step).wait_send()
        if step % STEPS:
            third_copy(step).wait_send()


def backward(grad, weights, tokens, kept, gains):
    count, columns = grad.shape
    lanes = weights.shape[3]
    rows, width, steps = BLOCK_ROWS, lanes // 4, CHUNKS * STEPS
    here = pl.BlockSpec(memory_space=pltpu.VMEM)
    outputs = (
        shaped(count, columns, dtype=F32),
        shaped(CHUNKS, rows, lanes, dtype=F32),
        shaped(8, 128, dtype=F32),
    )
    return pl.pallas_call(
        backward_kernel,
        in_specs=[here, pl.BlockSpec(memory_space=pl.ANY)] + [here] * (len(kept) + 2),
        out_specs=[here] * len(outputs),
        out_shape=outputs,
        scratch_shapes=[
            pltpu.VMEM((2, columns, lanes), BF16),
            pltpu.VMEM((2, columns, lanes), BF16),
            pltpu.VMEM((steps, 4, rows, lanes), BF16),
            pltpu.VMEM((4, 4, rows, lanes), BF16),
            pltpu.VMEM((steps, 2, rows, lanes), BF16),
            pltpu.VMEM((steps, rows, lanes), BF16),
            pltpu.VMEM((steps, rows, lanes), BF16),
            pltpu.VMEM((STEPS, count, lanes), BF16),
            pltpu.VMEM((count, columns), BF16),
            pltpu.VMEM((count, columns), F32),
            pltpu.VMEM((count, columns), F32),
            pltpu.VMEM((count, width), BF16),
            pltpu.VMEM((count, 3 * width), F32),
            pltpu.VMEM((count, 3 * width), BF16),
            pltpu.VMEM((count, count), F32),
            pltpu.VMEM((8, columns), F32),
            pltpu.VMEM((4, 8, columns), F32),
            pltpu.VMEM((8, 8, 128), F32),
            pltpu.VMEM((8, 8, 128), F32),
            pltpu.VMEM((2, 4, 2, PAD, columns), BF16),
            pltpu.VMEM((2, 4, 2, PAD, columns), BF16),
            pltpu.SemaphoreType.DMA((2,)),
            pltpu.SemaphoreType.DMA((2, 4)),
            pltpu.SemaphoreType.DMA((4, 4)),
            pltpu.SemaphoreType.DMA((steps,)),
            pltpu.SemaphoreType.DMA((steps,)),
            pltpu.SemaphoreType.DMA((steps,)),
            pltpu.SemaphoreType.DMA((steps,)),
            pltpu.SemaphoreType.DMA((steps,)),
            pltpu.SemaphoreType.DMA((steps,)),
            pltpu.SemaphoreType.DMA((2, 8)),
            pltpu.SemaphoreType.DMA((2, 8)),
            pltpu.SemaphoreType.DMA((2, 4)),
            pltpu.SemaphoreType.DMA((2, 4)),
            pltpu.SemaphoreType.REGULAR,
        ],
        compiler_params=pltpu.CompilerParams(
            collective_id=1, has_side_effects=True, vmem_limit_bytes=60 * 2**20
        ),
        name="backward",
    )(grad, weights, tokens, *kept, gains)


def sum_gains(total, own):
    for axes in ("c", "x", "y", TENSOR):
        bit = 1
        while bit < lax.axis_size(axes):
            total = total + along(total, axes, bit)
            bit *= 2
    return lax.dynamic_slice_in_dim(total, lax.axis_index(DP) * own, own, 1)


def on_device(
    routed,
    tokens,
    live_clips,
    norm_gains,
    qkv_time,
    out_time,
    qkv_space,
    out_space,
    up_weight,
    down_weight,
    cotangent,
):
    members = lax.axis_size("c") * lax.axis_size("h")
    share = PATCHES // members
    count, columns = tokens.shape
    width = qkv_time.shape[2]
    live = jnp.where(lax.axis_index("s") < live_clips[0], 1.0, 0.0).astype(F32)

    def pack_heads(qkv, out):
        rows = qkv.shape[1]
        return jnp.concatenate([qkv.transpose(1, 0, 2).reshape(rows, -1), out.T], 1)

    shards = [
        pack_heads(qkv_time, out_time),
        pack_heads(qkv_space, out_space),
        up_weight,
        down_weight.T,
    ]
    grad_stream = cotangent * live
    if routed:
        gain_shard = jnp.pad(
            norm_gains.astype(F32), ((0, 8 - 3), (0, -norm_gains.shape[1] % 128))
        )
        weights, *kept, after_mlp, gains = forward(tokens, jnp.stack(shards), gain_shard)
        grad_tokens, own, gains_own = backward(grad_stream, weights, tokens, kept, gains)
        down_own, up_own, space_own, time_own = own
        down_own = down_own.T
        gains_own = gains_own[:3, : norm_gains.shape[1]]
    else:
        time_all, space_all, up_all, down_all = [gather_plain(shard) for shard in shards]
        blocks, depth, lanes = up_all.shape
        gains = lax.all_gather(norm_gains, DP, axis=1, tiled=True).astype(F32)
        normed_time = to_patches(normalize(tokens, gains[0]).astype(BF16), members)
        time_heads, time_mixed, change = attend("time", normed_time, time_all, share, BF16)
        after_time = tokens + to_frames(change, members).astype(F32)
        normed_space = normalize(after_time, gains[1]).astype(BF16)
        space_heads, space_mixed, change = attend("space", normed_space, space_all, 1, F32)
        after_space = after_time + change
        normed_mlp = normalize(after_space, gains[2]).astype(BF16)
        hidden, slope = phase(
            up_kernel,
            "up",
            (normed_mlp, up_all),
            (shaped(blocks, count, lanes), shaped(blocks, count, lanes)),
            cost=12,
        )
        (change,) = phase(
            down_kernel, "down", (hidden, down_all), (shaped(count, depth, dtype=F32),), cost=4
        )
        after_mlp = after_space + change
        grad_low = grad_stream.astype(BF16)
        work = (pltpu.VMEM((depth, lanes), BF16),)
        *down_grads, grad_pre = phase(
            down_back_kernel,
            "down_back",
            (grad_low, down_all, hidden, slope),
            (*grad_shapes(down_all, False), shaped(blocks, count, lanes)),
            work,
            cost=8,
        )
        *up_grads, grad_normed = phase(
            up_back_kernel,
            "up_back",
            (normed_mlp, up_all, grad_pre),
            (*grad_shapes(up_all, False), shaped(count, depth, dtype=F32)),
            work,
            cost=8,
        )
        grad_part, gain_mlp = norm_back(after_space, gains[2], grad_normed)
        grad_stream = grad_stream + grad_part
        space_grads, grad_normed = attend_back(
            "space",
            normed_space,
            space_all,
            space_heads,
            space_mixed,
            grad_stream.astype(BF16),
            1,
            F32,
            False,
        )
        grad_part, gain_space = norm_back(after_time, gains[1], grad_normed)
        grad_stream = grad_stream + grad_part
        grad_low = to_patches(grad_stream.astype(BF16), members)
        time_grads, grad_normed = attend_back(
            "time", normed_time, time_all, time_heads, time_mixed, grad_low, share, BF16, routed
        )
        grad_normed = to_frames(grad_normed, members).astype(F32)
        grad_part, gain_time = norm_back(tokens, gains[0], grad_normed)
        grad_tokens = grad_stream + grad_part
        down_own = reduce_plain(down_grads).T
        up_own = reduce_plain(up_grads)
        space_own = reduce_plain(space_grads)
        time_own = reduce_plain(time_grads)
        gains_own = sum_gains(jnp.stack([gain_time, gain_space, gain_mlp]), norm_gains.shape[1])
    output = after_mlp * live

    def unpack(own):
        rows = own.shape[0]
        return own[:, : 3 * width].reshape(rows, 3, width).transpose(1, 0, 2), own[:, 3 * width :].T

    time_in_own, time_out_own = unpack(time_own)
    space_in_own, space_out_own = unpack(space_own)
    return (
        output,
        grad_tokens,
        gains_own,
        time_in_own,
        time_out_own,
        space_in_own,
        space_out_own,
        up_own,
        down_own,
    )


def solution(mesh):
    n_dp, n_tensor = mesh.devices.shape

    def run(*args):
        slots = args[0].shape[0] // (n_dp * HALF * PATCHES)
        fine = Mesh(mesh.devices.reshape(n_dp // 4, 2, 2, slots, n_tensor // slots), ALL)
        in_specs = (
            P(ALL, None),
            P(DP),
            P(None, DP),
            P(None, DP, TENSOR),
            P(TENSOR, DP),
            P(None, DP, TENSOR),
            P(TENSOR, DP),
            P(DP, TENSOR),
            P(TENSOR, DP),
            P(ALL, None),
        )
        out_specs = (in_specs[0], in_specs[0]) + in_specs[2:9]
        routed = fine.devices.shape == (2, 2, 2, 2, 2)
        return jax.shard_map(
            functools.partial(on_device, routed), mesh=fine, in_specs=in_specs, out_specs=out_specs, check_vma=False
        )(*args)

    return run
```

```python
import functools
import math

import jax
import jax.numpy as jnp
from jax import lax
from jax.experimental import pallas as pl
from jax.experimental.pallas import tpu as pltpu
from jax.sharding import Mesh, PartitionSpec as P

HEAD_DIM = 64
PATCHES = 196
HALF = 4
FRAMES = 8
EPSILON = 1e-06
F32 = jnp.float32
BF16 = jnp.bfloat16
ALL = ("y", "x", "c", "s", "h")
DP = ("y", "x", "c")
TENSOR = ("s", "h")
CLIP = ("c", "h")

NN = (((1,), (0,)), ((), ()))
NT = (((1,), (1,)), ((), ()))
TN = (((0,), (0,)), ((), ()))
BLOCK_ROWS = 96


def mm(a, b, dims=NN):
    return lax.dot_general(a, b, dims, preferred_element_type=F32)


def row_ids(shape, dim, start):
    return lax.broadcasted_iota(jnp.int32, shape, dim) + start


def windows(kind, count):
    if kind == "time":
        return [(0, count, None)]
    found = []
    for frame in range(count // PATCHES):
        low = frame * PATCHES // 16 * 16
        high = min(count, -(-(frame + 1) * PATCHES // 16) * 16)
        found.append((low, high - low, frame))
    return found


def key_bias(start, size, group, stride):
    keys = row_ids((size, size), 0, start)
    if group is None:
        together = keys % stride == row_ids((size, size), 1, start) % stride
    else:
        together = (keys >= group * PATCHES) & (keys < (group + 1) * PATCHES)
    return jnp.where(together, 0.0, -1e30)


def row_valid(start, size, group, width):
    rows = row_ids((size, width), 0, start)
    return (rows >= group * PATCHES) & (rows < (group + 1) * PATCHES)


def normalize(rows, scale_row):
    average = jnp.mean(rows, -1, keepdims=True)
    centred = rows - average
    spread = jnp.mean(centred * centred, -1, keepdims=True)
    return centred * lax.rsqrt(spread + EPSILON) * scale_row


def norm_back(rows, scale_row, grad_normed):
    unused, pullback = jax.vjp(normalize, rows, scale_row)
    return pullback(grad_normed)


def row_block(core, part, quad):
    quad_me = lax.axis_index(("y", "x"))
    block = jnp.bitwise_xor(quad_me, quad) * 2 + jnp.bitwise_xor(core, part)
    return pl.multiple_of(block * BLOCK_ROWS, BLOCK_ROWS)


def head_slices(ref, rows, width, head):
    low = head * HEAD_DIM
    return tuple(ref[rows, part * width + low : part * width + low + HEAD_DIM] for part in range(3))


def put_grads(work, outs):
    if len(outs) == 1:
        outs[0][...] = work[...]
        return
    core = lax.axis_index("c")
    for part, out in enumerate(outs):
        for quad in range(out.shape[0]):
            out[quad] = work[pl.ds(row_block(core, part, quad), out.shape[1]), :]


def attend_kernel(kind, stride, normed_ref, weight_ref, heads_ref, mixed_ref, out_ref, sums, total_ref):
    step = pl.program_id(0)
    count, width = mixed_ref.shape
    heads_ref[...] = mm(normed_ref[...], weight_ref[:, : 3 * width]).astype(BF16)
    sums[...] = jnp.zeros_like(sums)
    for start, size, group in windows(kind, count):
        bias = key_bias(start, size, group, stride)
        rows = pl.ds(start, size)
        for head in range(width // HEAD_DIM):
            low = head * HEAD_DIM
            query, key, value = head_slices(heads_ref, rows, width, head)
            scores = mm(key, query * HEAD_DIM**-0.5, NT) + bias
            weights = jnp.exp(scores - jnp.max(scores, 0, keepdims=True))
            total = jnp.sum(weights, 0, keepdims=True)
            blended = (mm(value.T, weights.astype(BF16)) / total).T
            if group is not None:
                blended = jnp.where(row_valid(start, size, group, HEAD_DIM), blended, 0.0)
            sums[rows, low : low + HEAD_DIM] += blended
    mixed_ref[...] = sums[...].astype(BF16)
    share = mm(mixed_ref[...], weight_ref[:, 3 * width :], NT)

    @pl.when(step == 0)
    def _():
        total_ref[...] = share

    @pl.when(step > 0)
    def _():
        total_ref[...] += share

    @pl.when(step == pl.num_programs(0) - 1)
    def _():
        out_ref[...] = total_ref[...].astype(out_ref.dtype)


def attend_back_kernel(
    kind, stride, normed_ref, weight_ref, heads_ref, mixed_ref, grad_ref, *rest
):
    outs, (out_ref, sums, total_ref, grad_mixed, grad_heads, work) = rest[:-6], rest[-6:]
    step = pl.program_id(0)
    count, width = mixed_ref.shape
    scale = HEAD_DIM**-0.5
    grad_mixed[...] = mm(grad_ref[...], weight_ref[:, 3 * width :]).astype(BF16)
    sums[...] = jnp.zeros_like(sums)
    for start, size, group in windows(kind, count):
        bias = key_bias(start, size, group, stride)
        rows = pl.ds(start, size)
        for head in range(width // HEAD_DIM):
            low = head * HEAD_DIM
            query, key, value = head_slices(heads_ref, rows, width, head)
            query = query * scale
            grad = grad_mixed[rows, low : low + HEAD_DIM]
            if group is not None:
                valid = row_valid(start, size, group, HEAD_DIM)
                grad = jnp.where(valid, grad.astype(F32), 0.0).astype(BF16)
            scores = mm(key, query, NT) + bias
            weights = jnp.exp(scores - jnp.max(scores, 0, keepdims=True))
            weights = weights / jnp.sum(weights, 0, keepdims=True)
            grad_weights = mm(value, grad, NT)
            row_terms = jnp.sum(weights * grad_weights, 0, keepdims=True)
            grad_scores = (weights * (grad_weights - row_terms)).astype(BF16)
            sums[rows, low : low + HEAD_DIM] += (mm(key.T, grad_scores) * scale).T
            low += width
            sums[rows, low : low + HEAD_DIM] += mm(grad_scores, query)
            low += width
            sums[rows, low : low + HEAD_DIM] += mm(weights.astype(BF16), grad)
    grad_heads[...] = sums[...].astype(BF16)
    share = mm(grad_heads[...], weight_ref[:, : 3 * width], NT)

    @pl.when(step == 0)
    def _():
        total_ref[...] = share

    @pl.when(step > 0)
    def _():
        total_ref[...] += share

    @pl.when(step == pl.num_programs(0) - 1)
    def _():
        out_ref[...] = total_ref[...].astype(out_ref.dtype)

    work[:, : 3 * width] = mm(normed_ref[...], grad_heads[...], TN).astype(BF16)
    work[:, 3 * width :] = mm(grad_ref[...], mixed_ref[...], TN).astype(BF16)
    put_grads(work, outs)


def up_kernel(normed_ref, weight_ref, hidden_ref, slope_ref):
    pre_act = mm(normed_ref[...], weight_ref[...])
    cdf = 0.5 * (1.0 + lax.erf(pre_act * 0.5**0.5))
    hidden_ref[...] = (pre_act * cdf).astype(BF16)
    density = jnp.exp(-0.5 * pre_act * pre_act) * (0.5 / math.pi) ** 0.5
    slope_ref[...] = (cdf + pre_act * density).astype(slope_ref.dtype)


def down_kernel(hidden_ref, weight_ref, out_ref):
    share = mm(hidden_ref[...], weight_ref[...], NT)

    @pl.when(pl.program_id(0) == 0)
    def _():
        out_ref[...] = share

    @pl.when(pl.program_id(0) > 0)
    def _():
        out_ref[...] += share


def down_back_kernel(grad_ref, weight_ref, hidden_ref, slope_ref, *rest):
    outs, (grad_pre_ref, work) = rest[:-2], rest[-2:]
    grad_hidden = mm(grad_ref[...], weight_ref[...])
    grad_pre_ref[...] = (grad_hidden * slope_ref[...].astype(F32)).astype(BF16)
    work[...] = mm(grad_ref[...], hidden_ref[...], TN).astype(BF16)
    put_grads(work, outs)


def up_back_kernel(normed_ref, weight_ref, grad_pre_ref, *rest):
    outs, (out_ref, work) = rest[:-2], rest[-2:]
    share = mm(grad_pre_ref[...], weight_ref[...], NT)

    @pl.when(pl.program_id(0) == 0)
    def _():
        out_ref[...] = share

    @pl.when(pl.program_id(0) > 0)
    def _():
        out_ref[...] += share

    work[...] = mm(normed_ref[...], grad_pre_ref[...], TN).astype(BF16)
    put_grads(work, outs)


def whole_spec(array):
    return pl.BlockSpec(array.shape, lambda i: (0,) * array.ndim)


def step_spec(array):
    rest = array.shape[1:]
    return pl.BlockSpec((None,) + rest, lambda i: (i,) + (0,) * len(rest))


def phase(kernel, name, inputs, outputs, scratch=(), cost=0):
    blocks = [a for a in inputs if a.ndim > 2][0].shape[0]
    spec = lambda a: whole_spec(a) if a.ndim == 2 else step_spec(a)
    return pl.pallas_call(
        kernel,
        grid=(blocks,),
        in_specs=[spec(a) for a in inputs],
        out_specs=[spec(a) for a in outputs],
        out_shape=outputs,
        scratch_shapes=list(scratch),
        cost_estimate=pl.CostEstimate(
            flops=int(cost * 800e6), bytes_accessed=int(cost * 1e6), transcendentals=0
        ),
        name=name,
    )(*inputs)


def shaped(*shape, dtype=BF16):
    return jax.ShapeDtypeStruct(shape, dtype)


def grad_shapes(weight, routed):
    blocks, depth, lanes = weight.shape
    if not routed:
        return [shaped(blocks, depth, lanes)]
    rows = BLOCK_ROWS
    return [shaped(blocks, depth // rows // 2, rows, lanes) for part in range(2)]


def attend(kind, normed, weight, stride, out_dtype):
    blocks, depth, lanes = weight.shape
    count, width = normed.shape[0], lanes // 4
    return phase(
        functools.partial(attend_kernel, kind, stride),
        kind + "_attend",
        (normed, weight),
        (
            shaped(blocks, count, 3 * width),
            shaped(blocks, count, width),
            shaped(count, depth, dtype=out_dtype),
        ),
        (pltpu.VMEM((count, width), F32), pltpu.VMEM((count, depth), F32)),
        cost=14,
    )


def attend_back(kind, normed, weight, heads, mixed, grad, stride, out_dtype, routed):
    blocks, depth, lanes = weight.shape
    count, width = normed.shape[0], lanes // 4
    *grads, out = phase(
        functools.partial(attend_back_kernel, kind, stride),
        kind + "_attend_back",
        (normed, weight, heads, mixed, grad),
        (*grad_shapes(weight, routed), shaped(count, depth, dtype=out_dtype)),
        (
            pltpu.VMEM((count, 3 * width), F32),
            pltpu.VMEM((count, depth), F32),
            pltpu.VMEM((count, width), BF16),
            pltpu.VMEM((count, 3 * width), BF16),
            pltpu.VMEM((depth, lanes), BF16),
        ),
        cost=20,
    )
    return grads, out


def along(piece, axes, distance):
    size = lax.axis_size(axes)
    return lax.ppermute(piece, axes, [(i, i ^ distance) for i in range(size)])


def after(piece, earlier):
    return piece + earlier[:1, :1] * 0


def gather_plain(shard):
    every = lax.all_gather(shard, TENSOR, axis=0, tiled=False)
    return lax.all_gather(every.reshape(-1, *shard.shape), DP, axis=1, tiled=True)


def reduce_plain(grads):
    part = lax.psum_scatter(grads[0], TENSOR, scatter_dimension=0, tiled=True)[0]
    return lax.psum_scatter(part, DP, scatter_dimension=0, tiled=True).astype(F32)


def by_member(parts, me):
    return jnp.stack(
        [
            lax.dynamic_index_in_dim(parts, jnp.bitwise_xor(me, k), 0, keepdims=False)
            for k in range(parts.shape[0])
        ]
    )


def to_patches(rows, members):
    share, columns = PATCHES // members, rows.shape[1]
    me = lax.axis_index(CLIP)
    parts = rows.reshape(-1, members, share, columns).transpose(1, 0, 2, 3)
    parts = [
        lax.dynamic_index_in_dim(parts, jnp.bitwise_xor(me, k), 0, keepdims=False)
        for k in range(members)
    ]
    parts = [parts[0]] + [along(parts[k], CLIP, k) for k in range(1, members)]
    return by_member(jnp.stack(parts), me).reshape(-1, columns)


def to_frames(rows, members):
    share, columns = PATCHES // members, rows.shape[1]
    me = lax.axis_index(CLIP)
    parts = by_member(rows.reshape(members, -1, share, columns), me)
    parts = [parts[0]] + [along(parts[k], CLIP, k) for k in range(1, members)]
    parts = jnp.stack(parts)
    order = jnp.bitwise_xor(me, jnp.arange(members))
    parts = [
        lax.dynamic_index_in_dim(parts, jnp.bitwise_xor(me, k), 0, keepdims=False)
        for k in range(members)
    ]
    return jnp.stack(parts, 1).reshape(-1, columns)


CHUNKS = 4
STEPS = 4
PAD = 56


def place():
    return {axis: lax.axis_index(axis) for axis in ALL}


def moved(here, **flips):
    return tuple(here[a] + flips.get(a, 0) * (1 - 2 * here[a]) for a in ALL)


def dp_row(here, y=0, x=0, c=0):
    to = lambda a, flip: here[a] + flip * (1 - 2 * here[a])
    return to("y", y) * 4 + to("x", x) * 2 + to("c", c)


def remote(source, target, sent, received, device):
    return pltpu.make_async_remote_copy(
        src_ref=source,
        dst_ref=target,
        send_sem=sent,
        recv_sem=received,
        device_id=device,
        device_id_type=pl.DeviceIdType.MESH,
    )


def peers(here):
    found = [moved(here, s=j // 2, h=j % 2) for j in range(1, 4)]
    found += [moved(here, y=r // 4, x=r // 2 % 2, c=r % 2) for r in range(1, 8)]
    return found + [moved(here, c=1, h=1)]


def greet(here):
    barrier = pltpu.get_barrier_semaphore()
    everyone = peers(here)
    for device in everyone:
        pl.semaphore_signal(
            barrier, inc=1, device_id=device, device_id_type=pl.DeviceIdType.MESH
        )
    pl.semaphore_wait(barrier, len(everyone))


class Exchange:
    def __init__(self, here, out, back, sent, received):
        self.here, self.out, self.back = here, out, back
        self.sent, self.received = sent, received
        self.me = here["c"] * 2 + here["h"]

    def device(self, member):
        return tuple({"c": member // 2, "h": member % 2}.get(a, self.here[a]) for a in ALL)

    def start(self, member):
        @pl.when(self.me != member)
        def _():
            remote(
                self.out.at[member],
                self.back.at[self.me],
                self.sent.at[member],
                self.received.at[self.me],
                self.device(member),
            ).start()

        @pl.when(self.me == member)
        def _():
            self.back[member] = self.out[member]

    def finish(self, member):
        @pl.when(self.me != member)
        def _():
            remote(
                self.out.at[member],
                self.back.at[member],
                self.sent.at[member],
                self.received.at[member],
                self.device(member),
            ).wait()

    def send(self, rows_ref, first_row):
        share = PATCHES // 4
        for member in range(4):
            for frame in range(2):
                low = first_row(member, frame)
                self.out[member, frame, :share, :] = rows_ref[low : low + share, :].astype(BF16)
            self.start(member)

    def take(self, rows_ref, first_row):
        share = PATCHES // 4
        for member in range(4):
            self.finish(member)
            for frame in range(2):
                low = first_row(member, frame)
                rows_ref[low : low + share, :] = self.back[member, frame, :share, :].astype(F32)

    @staticmethod
    def by_frame(member, frame):
        return frame * PATCHES + member * (PATCHES // 4)

    @staticmethod
    def by_share(member, frame):
        return (member * 2 + frame) * (PATCHES // 4)

    def send_frames(self, rows_ref):
        self.send(rows_ref, self.by_frame)

    def take_patches(self, rows_ref):
        self.take(rows_ref, self.by_share)

    def send_patches(self, rows_ref):
        self.send(rows_ref, self.by_share)

    def take_frames(self, rows_ref):
        self.take(rows_ref, self.by_frame)


def by_rows(count, body, size=56):
    def step(i, carry):
        body(pl.ds(pl.multiple_of(i * size, size), size))
        return carry

    lax.fori_loop(0, count // size, step, 0)


def row_stats(rows):
    average = jnp.mean(rows, -1, keepdims=True)
    centred = rows - average
    spread = jnp.mean(centred * centred, -1, keepdims=True)
    return centred, lax.rsqrt(spread + EPSILON)


def attend_block(kind, stride, t, normed, weight, heads_ref, mixed_ref, sums, bias_ref):
    count, width = mixed_ref.shape[1:]
    heads_ref[t] = mm(normed, weight[:, : 3 * width]).astype(BF16)
    heads = heads_ref.at[t]
    sums[...] = jnp.zeros_like(sums)
    for start, size, group in windows(kind, count):
        bias = bias_ref[...] if group is None else key_bias(start, size, group, stride)
        rows = pl.ds(start, size)
        for head in range(width // HEAD_DIM):
            low = head * HEAD_DIM
            query, key, value = head_slices(heads, rows, width, head)
            scores = mm(key, query * HEAD_DIM**-0.5, NT) + bias
            weights = jnp.exp(scores - jnp.max(scores, 0, keepdims=True))
            total = jnp.sum(weights, 0, keepdims=True)
            blended = (mm(value.T, weights.astype(BF16)) / total).T
            if group is not None:
                blended = jnp.where(row_valid(start, size, group, HEAD_DIM), blended, 0.0)
            sums[rows, low : low + HEAD_DIM] += blended
    mixed_ref[t] = sums[...].astype(BF16)
    return mm(mixed_ref[t], weight[:, 3 * width :], NT)


def attend_back_block(
    kind, stride, heads, mixed, grad, normed, weight, grad_mixed, sums, grad_heads, bias_ref
):
    count, width = mixed.shape
    scale = HEAD_DIM**-0.5
    grad_mixed[...] = mm(grad[...], weight[:, 3 * width :]).astype(BF16)
    sums[...] = jnp.zeros_like(sums)
    for start, size, group in windows(kind, count):
        bias = bias_ref[...] if group is None else key_bias(start, size, group, stride)
        rows = pl.ds(start, size)
        for head in range(width // HEAD_DIM):
            low = head * HEAD_DIM
            query, key, value = head_slices(heads, rows, width, head)
            query = query * scale
            grad_here = grad_mixed[rows, low : low + HEAD_DIM]
            if group is not None:
                valid = row_valid(start, size, group, HEAD_DIM)
                grad_here = jnp.where(valid, grad_here.astype(F32), 0.0).astype(BF16)
            scores = mm(key, query, NT) + bias
            weights = jnp.exp(scores - jnp.max(scores, 0, keepdims=True))
            weights = weights * (1.0 / jnp.sum(weights, 0, keepdims=True))
            grad_weights = mm(value, grad_here, NT)
            row_terms = jnp.sum(weights * grad_weights, 0, keepdims=True)
            grad_scores = (weights * (grad_weights - row_terms)).astype(BF16)
            sums[rows, low : low + HEAD_DIM] += (mm(key.T, grad_scores) * scale).T
            low += width
            sums[rows, low : low + HEAD_DIM] += mm(grad_scores, query)
            low += width
            sums[rows, low : low + HEAD_DIM] += mm(weights.astype(BF16), grad_here)
    grad_heads[...] = sums[...].astype(BF16)
    return mm(grad_heads[...], weight[:, : 3 * width], NT)


def layer_kernel(
    live_ref,
    tokens_hbm,
    cotangent_hbm,
    gain_ref,
    qkv_time_ref,
    out_time_ref,
    qkv_space_ref,
    out_space_ref,
    up_ref,
    down_ref,
    weight_ref,
    out_ref,
    stream_ref,
    own_ref,
    own_gain_ref,
    tokens_ref,
    shard_ref,
    held,
    normed_time_ref,
    time_heads_ref,
    time_mixed_ref,
    after_time_ref,
    normed_space_ref,
    space_heads_ref,
    space_mixed_ref,
    after_space_ref,
    normed_mlp_ref,
    hidden_ref,
    slope_ref,
    low_ref,
    rows_ref,
    total_ref,
    mixed_sums,
    sums,
    grad_mixed,
    grad_heads,
    bias_ref,
    work,
    keep,
    came,
    first,
    second,
    third,
    gains_ref,
    gain_sums,
    gain_line,
    gain_out,
    gain_parts,
    swap_out,
    swap_back,
    piece_sent,
    piece_here,
    core_sent,
    core_here,
    first_sent,
    first_here,
    second_sent,
    second_here,
    third_sent,
    third_here,
    gain_sent,
    gain_here,
    swap_sent,
    swap_here,
    held_sem,
    own_sem,
    load_sem,
    credit,
):
    here = place()
    count, columns = tokens_ref.shape
    width = time_mixed_ref.shape[2]
    own_row = dp_row(here)
    last = CHUNKS * STEPS - 1
    live = jnp.where(here["s"] < live_ref[0], 1.0, 0.0).astype(F32)

    load_tokens = pltpu.make_async_copy(tokens_hbm, tokens_ref, load_sem.at[0])
    load_cotangent = pltpu.make_async_copy(cotangent_hbm, stream_ref, load_sem.at[1])
    load_tokens.start()
    load_cotangent.start()

    for k, qkv, out in ((0, qkv_time_ref, out_time_ref), (1, qkv_space_ref, out_space_ref)):
        for c in range(3):
            shard_ref[k, :, c * width : (c + 1) * width] = qkv[c]
        shard_ref[k, :, 3 * width :] = out[...].astype(F32).T.astype(BF16)
    shard_ref[2] = up_ref[...]
    shard_ref[3] = down_ref[...].astype(F32).T.astype(BF16)
    own_gains = gain_ref.shape[1]
    gain_out[0, : gain_ref.shape[0], :own_gains] = gain_ref[...].astype(F32)
    greet(here)

    def row_of(part, r):
        return dp_row(here, y=r // 2, x=r % 2, c=part)

    def slot_of(k, j, row):
        return weight_ref.at[k, j, pl.ds(pl.multiple_of(row * BLOCK_ROWS, BLOCK_ROWS), BLOCK_ROWS)]

    def arrived(k, part, r, j):
        slot = slot_of(k, j, row_of(part, r))
        remote(
            slot, slot, piece_sent.at[k, 0, 0], piece_here.at[k, part, r, j], moved(here, c=1)
        ).wait_recv()

    def send(source, k, j, r, sem, part, r_there, **flips):
        remote(
            source,
            slot_of(k, j, row_of(0, r)),
            piece_sent.at[k, sem, j],
            piece_here.at[k, part, r_there, j],
            moved(here, **flips),
        ).start()

    def piece(k, j, r):
        return slot_of(k, j, row_of(0, r))

    def start_line(k):
        for j in range(1, 4):
            remote(
                shard_ref.at[k],
                slot_of(k, j, own_row),
                piece_sent.at[k, 0, j],
                piece_here.at[k, 0, 0, j],
                moved(here, s=j // 2, h=j % 2),
            ).start()

    def spread(source, k, j):
        send(source, k, j, 0, 1, 0, 1, x=1)
        send(source, k, j, 0, 2, 0, 2, y=1)
        send(source, k, j, 0, 4, 1, 0, c=1)

    def line(k, j):
        arrived(k, 0, 0, j)
        spread(piece(k, j, 0), k, j)

    def relay(k, j):
        up = j // 2
        arrived(k, 0, 1, j)
        send(piece(k, j, 1), k, j, 1, 5, 1, 1, c=1)
        arrived(k, 0, 2, j)
        send(piece(k, j, 2), k, j, 2, 6, 1, 2, c=1)
        source = slot_of(k, j, dp_row(here, y=up, x=1 - up))
        remote(
            source,
            source,
            piece_sent.at[k, 3, j],
            piece_here.at[k, 0, 3, j],
            moved(here, y=1 - up, x=up),
        ).start()

    def across(k):
        for j in range(STEPS):
            arrived(k, 0, 3, j)
            send(piece(k, j, 3), k, j, 3, 7, 1, 3, c=1)

    def fetch(k, t):
        return pltpu.make_async_copy(weight_ref.at[k, t], held.at[t], held_sem.at[t])

    def ready(k):
        for j in range(STEPS):
            for r in range(4):
                arrived(k, 1, r, j)
        for t in range(STEPS):
            fetch(k, t).start()

    def weight(k, t):
        fetch(k, t).wait()
        return held.at[t]

    def stored(k):
        return pltpu.make_async_copy(shard_ref.at[k], slot_of(k, 0, own_row), own_sem.at[k])

    def turn(step):
        return step % 2

    def grad_rows(step, part, i):
        u = turn(step)
        y = (1 - u) * (i // 2) + u * (i % 2)
        x = (1 - u) * (i % 2) + u * (i // 2)
        row = dp_row(here, y=y, x=x, c=part)
        return pl.ds(pl.multiple_of(row * BLOCK_ROWS, BLOCK_ROWS), BLOCK_ROWS)

    def core_copy(step, i):
        return remote(
            work.at[step % 2, grad_rows(step, 1, i)],
            came.at[step % 4, i],
            core_sent.at[step % 2, i],
            core_here.at[step % 4, i],
            moved(here, c=1),
        )

    def first_copy(step):
        u = turn(step)
        return remote(
            keep.at[step, pl.ds(2, 2)],
            first.at[step],
            first_sent.at[step],
            first_here.at[step],
            moved(here, y=1 - u, x=u),
        )

    def second_copy(step):
        u = turn(step)
        return remote(
            keep.at[step, 1],
            second.at[step],
            second_sent.at[step],
            second_here.at[step],
            moved(here, y=u, x=1 - u),
        )

    def third_copy(step):
        return remote(
            keep.at[step, 0],
            third.at[step],
            third_sent.at[step],
            third_here.at[step],
            moved(here, s=step % STEPS // 2, h=step % 2),
        )

    def begin(step):
        @pl.when(step >= 2)
        def _():
            for i in range(4):
                core_copy(step - 2, i).wait_send()

        return work.at[step % 2]

    def emit(step):
        @pl.when(step >= 4)
        def _():
            pl.semaphore_wait(credit, 1)

        for i in range(4):
            core_copy(step, i).start()

    def take_core(step):
        for i in range(4):
            core_copy(step, i).wait_recv()
        for i in (2, 3, 0, 1):
            own = work[step % 2, grad_rows(step, 0, i), :].astype(F32)
            keep[step, i] = (own + came[step % 4, i].astype(F32)).astype(BF16)
            if i == 3:
                first_copy(step).start()

        @pl.when(step <= last - 4)
        def _():
            pl.semaphore_signal(
                credit,
                inc=1,
                device_id=moved(here, c=1),
                device_id_type=pl.DeviceIdType.MESH,
            )

    def take_first(step):
        first_copy(step).wait_recv()
        for i in (1, 0):
            both = keep[step, i].astype(F32) + first[step, i].astype(F32)
            keep[step, i] = both.astype(BF16)
            if i:
                second_copy(step).start()

    def take_second(step):
        second_copy(step).wait_recv()
        keep[step, 0] = (keep[step, 0].astype(F32) + second[step].astype(F32)).astype(BF16)

        @pl.when(step % STEPS > 0)
        def _():
            third_copy(step).start()

    def take_third(index):
        low = index * STEPS
        total = keep[low, 0].astype(F32)
        for j in range(1, STEPS):
            third_copy(low + j).wait_recv()
            total = total + third[low + j].astype(F32)
        own_ref[index] = total

    def loop(body, *events):
        def step(t, carry):
            body(t)
            for event, low, start in events:
                if start:

                    @pl.when(t >= start)
                    def _(event=event, low=low):
                        event(low + t)

                else:
                    event(low + t)
            return carry

        lax.fori_loop(0, STEPS, step, 0)

    def layer_norm(source_ref, gain, target_ref):
        def body(rows):
            centred, scale = row_stats(source_ref[rows, :])
            target_ref[rows, :] = (centred * scale * gains_ref[gain : gain + 1, :]).astype(
                target_ref.dtype
            )

        by_rows(count, body)

    def norm_back(source_ref, gain, grad_normed_ref):
        def body(rows):
            centred, scale = row_stats(source_ref[rows, :])
            unit = centred * scale
            grad_normed = grad_normed_ref[rows, :]
            e = grad_normed * gains_ref[gain : gain + 1, :]
            mean = jnp.mean(e, -1, keepdims=True)
            tilt = jnp.mean(e * unit, -1, keepdims=True)
            stream_ref[rows, :] += scale * (e - mean - unit * tilt)
            gain_sums[gain : gain + 1, :] += jnp.sum(grad_normed * unit, 0, keepdims=True)

        by_rows(count, body)

    def exchange(index):
        return Exchange(
            here,
            swap_out.at[index % 2],
            swap_back.at[index % 2],
            swap_sent.at[index],
            swap_here.at[index],
        )

    def attention(kind, k, normed_ref, heads_ref, mixed_ref):
        total_ref[...] = jnp.zeros_like(total_ref)

        def compute(t):
            total_ref[...] += attend_block(
                kind,
                PATCHES // 4,
                t,
                normed_ref[...],
                weight(k, t),
                heads_ref,
                mixed_ref,
                mixed_sums,
                bias_ref,
            )

        return compute

    def attention_back(kind, k, normed_ref, heads_ref, mixed_ref):
        total_ref[...] = jnp.zeros_like(total_ref)

        def compute(t):
            step = (CHUNKS - 1 - k) * STEPS + t
            out = begin(step)
            total_ref[...] += attend_back_block(
                kind,
                PATCHES // 4,
                heads_ref.at[t],
                mixed_ref.at[t],
                low_ref,
                normed_ref,
                weight(k, t),
                grad_mixed,
                sums,
                grad_heads,
                bias_ref,
            )
            if k:
                fetch(k - 1, t).start()
            out[:, : 3 * width] = mm(normed_ref[...], grad_heads[...], TN).astype(BF16)
            out[:, 3 * width :] = mm(low_ref[...], mixed_ref[t], TN).astype(BF16)
            emit(step)

        return compute

    gain_parts[0, own_row] = gain_out[0]

    def gain_copy(r):
        flips = {"y": r // 4, "x": r // 2 % 2, "c": r % 2}
        return remote(
            gain_out.at[0],
            gain_parts.at[0, own_row],
            gain_sent.at[0, r],
            gain_here.at[0, r],
            moved(here, **flips),
        )

    for r in range(1, 8):
        gain_copy(r).start()
    start_line(0)
    spread(shard_ref.at[0], 0, 0)
    spread(shard_ref.at[1], 1, 0)
    for k in range(CHUNKS):
        stored(k).start()
    load_tokens.wait()

    def unit_rows(rows):
        centred, scale = row_stats(tokens_ref[rows, :])
        rows_ref[rows, :] = centred * scale

    by_rows(count, unit_rows)
    swap = exchange(0)
    for r in range(1, 8):
        gain_copy(r).wait()
    for d in range(8):
        gains_ref[:, d * own_gains : (d + 1) * own_gains] = gain_parts[0, d, :, :own_gains]

    def scale_rows(rows):
        rows_ref[rows, :] = rows_ref[rows, :] * gains_ref[0:1, :]

    by_rows(count, scale_rows)
    swap.send_frames(rows_ref)
    start_line(1)
    bias_ref[...] = key_bias(0, count, None, PATCHES // 4)
    gain_sums[...] = jnp.zeros_like(gain_sums)
    line(0, 1)
    spread(shard_ref.at[2], 2, 0)
    line(0, 2)
    line(0, 3)
    load_cotangent.wait()

    def mask_rows(rows):
        stream_ref[rows, :] = stream_ref[rows, :] * live
        low_ref[rows, :] = stream_ref[rows, :].astype(BF16)

    by_rows(count, mask_rows)
    swap.take_patches(rows_ref)
    start_line(2)
    normed_time_ref[...] = rows_ref[...].astype(BF16)
    for j in range(STEPS):
        relay(0, j)
    line(1, 1)
    line(1, 2)
    line(1, 3)
    spread(shard_ref.at[3], 3, 0)
    across(0)
    for k in range(CHUNKS):
        stored(k).wait()
    ready(0)

    loop(
        attention("time", 0, normed_time_ref, time_heads_ref, time_mixed_ref),
        (lambda t: relay(1, t), 0, 0),
        (lambda t: line(2, t), 0, 1),
    )
    swap = exchange(1)
    swap.send_patches(total_ref)
    start_line(3)
    across(1)
    swap.take_frames(rows_ref)
    after_time_ref[...] = tokens_ref[...] + rows_ref[...]

    layer_norm(after_time_ref, 1, normed_space_ref)
    ready(1)
    loop(
        attention("space", 1, normed_space_ref, space_heads_ref, space_mixed_ref),
        (lambda t: relay(2, t), 0, 0),
        (lambda t: line(3, t), 0, 1),
    )
    after_space_ref[...] = after_time_ref[...] + total_ref[...]

    layer_norm(after_space_ref, 2, normed_mlp_ref)
    across(2)
    ready(2)

    def up(t):
        out = begin(t)
        pre_act = mm(normed_mlp_ref[...], weight(2, t)[...])
        cdf = 0.5 * (1.0 + lax.erf(pre_act * 0.5**0.5))
        hidden_ref[t] = (pre_act * cdf).astype(BF16)
        density = jnp.exp(-0.5 * pre_act * pre_act) * (0.5 / math.pi) ** 0.5
        slope_ref[t] = (cdf + pre_act * density).astype(BF16)
        out[...] = mm(low_ref[...], hidden_ref[t], TN).astype(BF16)
        emit(t)

    loop(up, (lambda t: relay(3, t), 0, 0), (take_core, -1, 1))
    take_core(3)
    across(3)
    ready(3)
    out_ref[...] = after_space_ref[...]

    def down(t):
        out_ref[...] += mm(hidden_ref[t], weight(3, t)[...], NT)
        grad_hidden = mm(low_ref[...], held[t])
        slope_ref[t] = (grad_hidden * slope_ref[t].astype(F32)).astype(BF16)
        fetch(2, t).start()

    loop(down)
    out_ref[...] = out_ref[...] * live
    total_ref[...] = jnp.zeros_like(total_ref)

    def up_back(t):
        step = STEPS + t
        out = begin(step)
        total_ref[...] += mm(slope_ref[t], weight(2, t)[...], NT)
        fetch(1, t).start()
        out[...] = mm(normed_mlp_ref[...], slope_ref[t], TN).astype(BF16)
        emit(step)

    loop(up_back, (take_core, 3, 1), (take_first, -2, 2))
    norm_back(after_space_ref, 2, total_ref)
    low_ref[...] = stream_ref[...].astype(BF16)
    loop(
        attention_back("space", 1, normed_space_ref, space_heads_ref, space_mixed_ref),
        (take_core, 7, 0),
        (take_first, 2, 0),
        (take_second, 0, 0),
    )
    norm_back(after_time_ref, 1, total_ref)
    swap = exchange(2)
    swap.send_frames(stream_ref)
    take_core(11)
    for step in (6, 7, 8):
        take_first(step)
    for step in (4, 5, 6):
        take_second(step)
    take_third(0)
    swap.take_patches(rows_ref)
    low_ref[...] = rows_ref[...].astype(BF16)
    loop(
        attention_back("time", 0, normed_time_ref, time_heads_ref, time_mixed_ref),
        (take_core, 11, 1),
        (take_first, 9, 0),
        (take_second, 7, 0),
    )
    swap = exchange(3)
    swap.send_patches(total_ref)
    take_core(15)
    take_first(13)
    take_second(11)
    take_third(1)
    swap.take_frames(rows_ref)
    norm_back(tokens_ref, 0, rows_ref)

    line_index = here["s"] * 2 + here["h"]

    def gain_line_copy(j):
        return remote(
            gain_sums,
            gain_line.at[line_index],
            gain_sent.at[1, j],
            gain_here.at[1, j],
            moved(here, s=j // 2, h=j % 2),
        )

    def gain_back(r):
        flips = {"y": r // 4, "x": r // 2 % 2, "c": r % 2}
        return remote(
            gain_out.at[dp_row(here, **flips)],
            gain_parts.at[1, own_row],
            gain_sent.at[2, r],
            gain_here.at[2, r],
            moved(here, **flips),
        )

    for j in range(1, 4):
        gain_line_copy(j).start()
    gain_line[line_index] = gain_sums[...]
    take_first(14)
    take_second(12)
    take_first(15)
    for j in range(1, 4):
        gain_line_copy(j).wait()
    total = gain_line[0] + gain_line[1] + gain_line[2] + gain_line[3]
    for d in range(8):
        gain_out[d, :, :own_gains] = total[:, d * own_gains : (d + 1) * own_gains]
    for r in range(1, 8):
        gain_back(r).start()
    gain_parts[1, own_row] = gain_out[own_row]
    take_second(13)
    take_second(14)
    take_third(2)
    take_second(15)
    for r in range(1, 8):
        gain_back(r).wait()
    total = gain_parts[1, 0]
    for d in range(1, 8):
        total = total + gain_parts[1, d]
    own_gain_ref[...] = total
    take_third(3)

    for k in range(CHUNKS):
        for sem in range(8):
            for j in range(4):
                if sem or j:
                    slot = slot_of(k, 0, own_row)
                    remote(
                        slot,
                        slot,
                        piece_sent.at[k, sem, j],
                        piece_here.at[k, 0, 0, 0],
                        moved(here, c=1),
                    ).wait_send()
    for step in range(last + 1):
        if step > last - 2:
            for i in range(4):
                core_copy(step, i).wait_send()
        first_copy(step).wait_send()
        second_copy(step).wait_send()
        if step % STEPS:
            third_copy(step).wait_send()


def layer(live_clips, tokens, cotangent, norm_gains, *weights):
    count, columns = tokens.shape
    rows, lanes = weights[4].shape
    width, steps = lanes // 4, CHUNKS * STEPS
    here = pl.BlockSpec(memory_space=pltpu.VMEM)
    there = pl.BlockSpec(memory_space=pl.ANY)
    outputs = (
        shaped(CHUNKS, STEPS, columns, lanes),
        shaped(count, columns, dtype=F32),
        shaped(count, columns, dtype=F32),
        shaped(CHUNKS, rows, lanes, dtype=F32),
        shaped(8, 128, dtype=F32),
    )
    return pl.pallas_call(
        layer_kernel,
        in_specs=[pl.BlockSpec(memory_space=pltpu.SMEM), there, there] + [here] * 7,
        out_specs=[there] + [here] * (len(outputs) - 1),
        out_shape=outputs,
        scratch_shapes=[
            pltpu.VMEM((count, columns), F32),
            pltpu.VMEM((CHUNKS, rows, lanes), BF16),
            pltpu.VMEM((STEPS, columns, lanes), BF16),
            pltpu.VMEM((count, columns), BF16),
            pltpu.VMEM((STEPS, count, 3 * width), BF16),
            pltpu.VMEM((STEPS, count, width), BF16),
            pltpu.VMEM((count, columns), F32),
            pltpu.VMEM((count, columns), BF16),
            pltpu.VMEM((STEPS, count, 3 * width), BF16),
            pltpu.VMEM((STEPS, count, width), BF16),
            pltpu.VMEM((count, columns), F32),
            pltpu.VMEM((count, columns), BF16),
            pltpu.VMEM((STEPS, count, lanes), BF16),
            pltpu.VMEM((STEPS, count, lanes), BF16),
            pltpu.VMEM((count, columns), BF16),
            pltpu.VMEM((count, columns), F32),
            pltpu.VMEM((count, columns), F32),
            pltpu.VMEM((count, width), F32),
            pltpu.VMEM((count, 3 * width), F32),
            pltpu.VMEM((count, width), BF16),
            pltpu.VMEM((count, 3 * width), BF16),
            pltpu.VMEM((count, count), F32),
            pltpu.VMEM((2, columns, lanes), BF16),
            pltpu.VMEM((steps, 4, rows, lanes), BF16),
            pltpu.VMEM((4, 4, rows, lanes), BF16),
            pltpu.VMEM((steps, 2, rows, lanes), BF16),
            pltpu.VMEM((steps, rows, lanes), BF16),
            pltpu.VMEM((steps, rows, lanes), BF16),
            pltpu.VMEM((8, columns), F32),
            pltpu.VMEM((8, columns), F32),
            pltpu.VMEM((4, 8, columns), F32),
            pltpu.VMEM((8, 8, 128), F32),
            pltpu.VMEM((2, 8, 8, 128), F32),
            pltpu.VMEM((2, 4, 2, PAD, columns), BF16),
            pltpu.VMEM((2, 4, 2, PAD, columns), BF16),
            pltpu.SemaphoreType.DMA((CHUNKS, 8, 4)),
            pltpu.SemaphoreType.DMA((CHUNKS, 2, 4, 4)),
            pltpu.SemaphoreType.DMA((2, 4)),
            pltpu.SemaphoreType.DMA((4, 4)),
            pltpu.SemaphoreType.DMA((steps,)),
            pltpu.SemaphoreType.DMA((steps,)),
            pltpu.SemaphoreType.DMA((steps,)),
            pltpu.SemaphoreType.DMA((steps,)),
            pltpu.SemaphoreType.DMA((steps,)),
            pltpu.SemaphoreType.DMA((steps,)),
            pltpu.SemaphoreType.DMA((3, 8)),
            pltpu.SemaphoreType.DMA((3, 8)),
            pltpu.SemaphoreType.DMA((4, 4)),
            pltpu.SemaphoreType.DMA((4, 4)),
            pltpu.SemaphoreType.DMA((STEPS,)),
            pltpu.SemaphoreType.DMA((CHUNKS,)),
            pltpu.SemaphoreType.DMA((2,)),
            pltpu.SemaphoreType.REGULAR,
        ],
        compiler_params=pltpu.CompilerParams(
            collective_id=0, has_side_effects=True, vmem_limit_bytes=67043328
        ),
        name="layer",
    )(live_clips, tokens, cotangent, norm_gains, *weights)[1:]


def sum_gains(total, own):
    for axes in ("c", "x", "y", TENSOR):
        bit = 1
        while bit < lax.axis_size(axes):
            total = total + along(total, axes, bit)
            bit *= 2
    return lax.dynamic_slice_in_dim(total, lax.axis_index(DP) * own, own, 1)


def on_device(
    routed,
    tokens,
    live_clips,
    norm_gains,
    qkv_time,
    out_time,
    qkv_space,
    out_space,
    up_weight,
    down_weight,
    cotangent,
):
    members = lax.axis_size("c") * lax.axis_size("h")
    share = PATCHES // members
    count, columns = tokens.shape
    width = qkv_time.shape[2]
    live = jnp.where(lax.axis_index("s") < live_clips[0], 1.0, 0.0).astype(F32)

    def pack_heads(qkv, out):
        rows = qkv.shape[1]
        return jnp.concatenate([qkv.transpose(1, 0, 2).reshape(rows, -1), out.T], 1)

    if routed:
        output, grad_tokens, own, gains_own = layer(
            live_clips,
            tokens,
            cotangent,
            norm_gains,
            qkv_time,
            out_time,
            qkv_space,
            out_space,
            up_weight,
            down_weight,
        )
        down_own, up_own, space_own, time_own = own
        down_own = down_own.T
        gains_own = gains_own[:3, : norm_gains.shape[1]]
    else:
        shards = [
            pack_heads(qkv_time, out_time),
            pack_heads(qkv_space, out_space),
            up_weight,
            down_weight.T,
        ]
        grad_stream = cotangent * live
        time_all, space_all, up_all, down_all = [gather_plain(shard) for shard in shards]
        blocks, depth, lanes = up_all.shape
        gains = lax.all_gather(norm_gains, DP, axis=1, tiled=True).astype(F32)
        normed_time = to_patches(normalize(tokens, gains[0]).astype(BF16), members)
        time_heads, time_mixed, change = attend("time", normed_time, time_all, share, BF16)
        after_time = tokens + to_frames(change, members).astype(F32)
        normed_space = normalize(after_time, gains[1]).astype(BF16)
        space_heads, space_mixed, change = attend("space", normed_space, space_all, 1, F32)
        after_space = after_time + change
        normed_mlp = normalize(after_space, gains[2]).astype(BF16)
        hidden, slope = phase(
            up_kernel,
            "up",
            (normed_mlp, up_all),
            (shaped(blocks, count, lanes), shaped(blocks, count, lanes)),
            cost=12,
        )
        (change,) = phase(
            down_kernel, "down", (hidden, down_all), (shaped(count, depth, dtype=F32),), cost=4
        )
        after_mlp = after_space + change
        grad_low = grad_stream.astype(BF16)
        work = (pltpu.VMEM((depth, lanes), BF16),)
        *down_grads, grad_pre = phase(
            down_back_kernel,
            "down_back",
            (grad_low, down_all, hidden, slope),
            (*grad_shapes(down_all, False), shaped(blocks, count, lanes)),
            work,
            cost=8,
        )
        *up_grads, grad_normed = phase(
            up_back_kernel,
            "up_back",
            (normed_mlp, up_all, grad_pre),
            (*grad_shapes(up_all, False), shaped(count, depth, dtype=F32)),
            work,
            cost=8,
        )
        grad_part, gain_mlp = norm_back(after_space, gains[2], grad_normed)
        grad_stream = grad_stream + grad_part
        space_grads, grad_normed = attend_back(
            "space",
            normed_space,
            space_all,
            space_heads,
            space_mixed,
            grad_stream.astype(BF16),
            1,
            F32,
            False,
        )
        grad_part, gain_space = norm_back(after_time, gains[1], grad_normed)
        grad_stream = grad_stream + grad_part
        grad_low = to_patches(grad_stream.astype(BF16), members)
        time_grads, grad_normed = attend_back(
            "time", normed_time, time_all, time_heads, time_mixed, grad_low, share, BF16, routed
        )
        grad_normed = to_frames(grad_normed, members).astype(F32)
        grad_part, gain_time = norm_back(tokens, gains[0], grad_normed)
        grad_tokens = grad_stream + grad_part
        down_own = reduce_plain(down_grads).T
        up_own = reduce_plain(up_grads)
        space_own = reduce_plain(space_grads)
        time_own = reduce_plain(time_grads)
        gains_own = sum_gains(jnp.stack([gain_time, gain_space, gain_mlp]), norm_gains.shape[1])
        output = after_mlp * live

    def unpack(own):
        rows = own.shape[0]
        return own[:, : 3 * width].reshape(rows, 3, width).transpose(1, 0, 2), own[:, 3 * width :].T

    time_in_own, time_out_own = unpack(time_own)
    space_in_own, space_out_own = unpack(space_own)
    return (
        output,
        grad_tokens,
        gains_own,
        time_in_own,
        time_out_own,
        space_in_own,
        space_out_own,
        up_own,
        down_own,
    )


def solution(mesh):
    n_dp, n_tensor = mesh.devices.shape

    def run(*args):
        slots = args[0].shape[0] // (n_dp * HALF * PATCHES)
        fine = Mesh(mesh.devices.reshape(n_dp // 4, 2, 2, slots, n_tensor // slots), ALL)
        in_specs = (
            P(ALL, None),
            P(DP),
            P(None, DP),
            P(None, DP, TENSOR),
            P(TENSOR, DP),
            P(None, DP, TENSOR),
            P(TENSOR, DP),
            P(DP, TENSOR),
            P(TENSOR, DP),
            P(ALL, None),
        )
        out_specs = (in_specs[0], in_specs[0]) + in_specs[2:9]
        routed = fine.devices.shape == (2, 2, 2, 2, 2)
        return jax.shard_map(
            functools.partial(on_device, routed), mesh=fine, in_specs=in_specs, out_specs=out_specs, check_vma=False
        )(*args)

    return run
```

```python
import functools
import math

import jax
import jax.numpy as jnp
from jax import lax
from jax.experimental import pallas as pl
from jax.experimental.pallas import tpu as pltpu
from jax.sharding import Mesh, PartitionSpec as P

HEAD_DIM = 64
PATCHES = 196
HALF = 4
FRAMES = 8
EPSILON = 1e-06
F32 = jnp.float32
BF16 = jnp.bfloat16
ALL = ("y", "x", "c", "s", "h")
DP = ("y", "x", "c")
TENSOR = ("s", "h")
CLIP = ("c", "h")

NN = (((1,), (0,)), ((), ()))
NT = (((1,), (1,)), ((), ()))
TN = (((0,), (0,)), ((), ()))
BLOCK_ROWS = 96


def mm(a, b, dims=NN):
    return lax.dot_general(a, b, dims, preferred_element_type=F32)


def row_ids(shape, dim, start):
    return lax.broadcasted_iota(jnp.int32, shape, dim) + start


def windows(kind, count):
    if kind == "time":
        return [(0, count, None)]
    found = []
    for frame in range(count // PATCHES):
        low = frame * PATCHES // 16 * 16
        high = min(count, -(-(frame + 1) * PATCHES // 16) * 16)
        found.append((low, high - low, frame))
    return found


def key_bias(start, size, group, stride):
    keys = row_ids((size, size), 0, start)
    if group is None:
        together = keys % stride == row_ids((size, size), 1, start) % stride
    else:
        together = (keys >= group * PATCHES) & (keys < (group + 1) * PATCHES)
    return jnp.where(together, 0.0, -1e30)


def row_valid(start, size, group, width):
    rows = row_ids((size, width), 0, start)
    return (rows >= group * PATCHES) & (rows < (group + 1) * PATCHES)


def normalize(rows, scale_row):
    average = jnp.mean(rows, -1, keepdims=True)
    centred = rows - average
    spread = jnp.mean(centred * centred, -1, keepdims=True)
    return centred * lax.rsqrt(spread + EPSILON) * scale_row


def norm_back(rows, scale_row, grad_normed):
    unused, pullback = jax.vjp(normalize, rows, scale_row)
    return pullback(grad_normed)


def row_block(core, part, quad):
    quad_me = lax.axis_index(("y", "x"))
    block = jnp.bitwise_xor(quad_me, quad) * 2 + jnp.bitwise_xor(core, part)
    return pl.multiple_of(block * BLOCK_ROWS, BLOCK_ROWS)


def head_slices(ref, rows, width, head):
    low = head * HEAD_DIM
    return tuple(ref[rows, part * width + low : part * width + low + HEAD_DIM] for part in range(3))


def put_grads(work, outs):
    if len(outs) == 1:
        outs[0][...] = work[...]
        return
    core = lax.axis_index("c")
    for part, out in enumerate(outs):
        for quad in range(out.shape[0]):
            out[quad] = work[pl.ds(row_block(core, part, quad), out.shape[1]), :]


def attend_kernel(kind, stride, normed_ref, weight_ref, heads_ref, mixed_ref, out_ref, sums, total_ref):
    step = pl.program_id(0)
    count, width = mixed_ref.shape
    heads_ref[...] = mm(normed_ref[...], weight_ref[:, : 3 * width]).astype(BF16)
    sums[...] = jnp.zeros_like(sums)
    for start, size, group in windows(kind, count):
        bias = key_bias(start, size, group, stride)
        rows = pl.ds(start, size)
        for head in range(width // HEAD_DIM):
            low = head * HEAD_DIM
            query, key, value = head_slices(heads_ref, rows, width, head)
            scores = mm(key, query * HEAD_DIM**-0.5, NT) + bias
            weights = jnp.exp(scores - jnp.max(scores, 0, keepdims=True))
            total = jnp.sum(weights, 0, keepdims=True)
            blended = (mm(value.T, weights.astype(BF16)) / total).T
            if group is not None:
                blended = jnp.where(row_valid(start, size, group, HEAD_DIM), blended, 0.0)
            sums[rows, low : low + HEAD_DIM] += blended
    mixed_ref[...] = sums[...].astype(BF16)
    share = mm(mixed_ref[...], weight_ref[:, 3 * width :], NT)

    @pl.when(step == 0)
    def _():
        total_ref[...] = share

    @pl.when(step > 0)
    def _():
        total_ref[...] += share

    @pl.when(step == pl.num_programs(0) - 1)
    def _():
        out_ref[...] = total_ref[...].astype(out_ref.dtype)


def attend_back_kernel(
    kind, stride, normed_ref, weight_ref, heads_ref, mixed_ref, grad_ref, *rest
):
    outs, (out_ref, sums, total_ref, grad_mixed, grad_heads, work) = rest[:-6], rest[-6:]
    step = pl.program_id(0)
    count, width = mixed_ref.shape
    scale = HEAD_DIM**-0.5
    grad_mixed[...] = mm(grad_ref[...], weight_ref[:, 3 * width :]).astype(BF16)
    sums[...] = jnp.zeros_like(sums)
    for start, size, group in windows(kind, count):
        bias = key_bias(start, size, group, stride)
        rows = pl.ds(start, size)
        for head in range(width // HEAD_DIM):
            low = head * HEAD_DIM
            query, key, value = head_slices(heads_ref, rows, width, head)
            query = query * scale
            grad = grad_mixed[rows, low : low + HEAD_DIM]
            if group is not None:
                valid = row_valid(start, size, group, HEAD_DIM)
                grad = jnp.where(valid, grad.astype(F32), 0.0).astype(BF16)
            scores = mm(key, query, NT) + bias
            weights = jnp.exp(scores - jnp.max(scores, 0, keepdims=True))
            weights = weights / jnp.sum(weights, 0, keepdims=True)
            grad_weights = mm(value, grad, NT)
            row_terms = jnp.sum(weights * grad_weights, 0, keepdims=True)
            grad_scores = (weights * (grad_weights - row_terms)).astype(BF16)
            sums[rows, low : low + HEAD_DIM] += (mm(key.T, grad_scores) * scale).T
            low += width
            sums[rows, low : low + HEAD_DIM] += mm(grad_scores, query)
            low += width
            sums[rows, low : low + HEAD_DIM] += mm(weights.astype(BF16), grad)
    grad_heads[...] = sums[...].astype(BF16)
    share = mm(grad_heads[...], weight_ref[:, : 3 * width], NT)

    @pl.when(step == 0)
    def _():
        total_ref[...] = share

    @pl.when(step > 0)
    def _():
        total_ref[...] += share

    @pl.when(step == pl.num_programs(0) - 1)
    def _():
        out_ref[...] = total_ref[...].astype(out_ref.dtype)

    work[:, : 3 * width] = mm(normed_ref[...], grad_heads[...], TN).astype(BF16)
    work[:, 3 * width :] = mm(grad_ref[...], mixed_ref[...], TN).astype(BF16)
    put_grads(work, outs)


def up_kernel(normed_ref, weight_ref, hidden_ref, slope_ref):
    pre_act = mm(normed_ref[...], weight_ref[...])
    cdf = 0.5 * (1.0 + lax.erf(pre_act * 0.5**0.5))
    hidden_ref[...] = (pre_act * cdf).astype(BF16)
    density = jnp.exp(-0.5 * pre_act * pre_act) * (0.5 / math.pi) ** 0.5
    slope_ref[...] = (cdf + pre_act * density).astype(slope_ref.dtype)


def down_kernel(hidden_ref, weight_ref, out_ref):
    share = mm(hidden_ref[...], weight_ref[...], NT)

    @pl.when(pl.program_id(0) == 0)
    def _():
        out_ref[...] = share

    @pl.when(pl.program_id(0) > 0)
    def _():
        out_ref[...] += share


def down_back_kernel(grad_ref, weight_ref, hidden_ref, slope_ref, *rest):
    outs, (grad_pre_ref, work) = rest[:-2], rest[-2:]
    grad_hidden = mm(grad_ref[...], weight_ref[...])
    grad_pre_ref[...] = (grad_hidden * slope_ref[...].astype(F32)).astype(BF16)
    work[...] = mm(grad_ref[...], hidden_ref[...], TN).astype(BF16)
    put_grads(work, outs)


def up_back_kernel(normed_ref, weight_ref, grad_pre_ref, *rest):
    outs, (out_ref, work) = rest[:-2], rest[-2:]
    share = mm(grad_pre_ref[...], weight_ref[...], NT)

    @pl.when(pl.program_id(0) == 0)
    def _():
        out_ref[...] = share

    @pl.when(pl.program_id(0) > 0)
    def _():
        out_ref[...] += share

    work[...] = mm(normed_ref[...], grad_pre_ref[...], TN).astype(BF16)
    put_grads(work, outs)


def whole_spec(array):
    return pl.BlockSpec(array.shape, lambda i: (0,) * array.ndim)


def step_spec(array):
    rest = array.shape[1:]
    return pl.BlockSpec((None,) + rest, lambda i: (i,) + (0,) * len(rest))


def phase(kernel, name, inputs, outputs, scratch=(), cost=0):
    blocks = [a for a in inputs if a.ndim > 2][0].shape[0]
    spec = lambda a: whole_spec(a) if a.ndim == 2 else step_spec(a)
    return pl.pallas_call(
        kernel,
        grid=(blocks,),
        in_specs=[spec(a) for a in inputs],
        out_specs=[spec(a) for a in outputs],
        out_shape=outputs,
        scratch_shapes=list(scratch),
        cost_estimate=pl.CostEstimate(
            flops=int(cost * 800e6), bytes_accessed=int(cost * 1e6), transcendentals=0
        ),
        name=name,
    )(*inputs)


def shaped(*shape, dtype=BF16):
    return jax.ShapeDtypeStruct(shape, dtype)


def grad_shapes(weight, routed):
    blocks, depth, lanes = weight.shape
    if not routed:
        return [shaped(blocks, depth, lanes)]
    rows = BLOCK_ROWS
    return [shaped(blocks, depth // rows // 2, rows, lanes) for part in range(2)]


def attend(kind, normed, weight, stride, out_dtype):
    blocks, depth, lanes = weight.shape
    count, width = normed.shape[0], lanes // 4
    return phase(
        functools.partial(attend_kernel, kind, stride),
        kind + "_attend",
        (normed, weight),
        (
            shaped(blocks, count, 3 * width),
            shaped(blocks, count, width),
            shaped(count, depth, dtype=out_dtype),
        ),
        (pltpu.VMEM((count, width), F32), pltpu.VMEM((count, depth), F32)),
        cost=14,
    )


def attend_back(kind, normed, weight, heads, mixed, grad, stride, out_dtype, routed):
    blocks, depth, lanes = weight.shape
    count, width = normed.shape[0], lanes // 4
    *grads, out = phase(
        functools.partial(attend_back_kernel, kind, stride),
        kind + "_attend_back",
        (normed, weight, heads, mixed, grad),
        (*grad_shapes(weight, routed), shaped(count, depth, dtype=out_dtype)),
        (
            pltpu.VMEM((count, 3 * width), F32),
            pltpu.VMEM((count, depth), F32),
            pltpu.VMEM((count, width), BF16),
            pltpu.VMEM((count, 3 * width), BF16),
            pltpu.VMEM((depth, lanes), BF16),
        ),
        cost=20,
    )
    return grads, out


def along(piece, axes, distance):
    size = lax.axis_size(axes)
    return lax.ppermute(piece, axes, [(i, i ^ distance) for i in range(size)])


def after(piece, earlier):
    return piece + earlier[:1, :1] * 0


def gather_plain(shard):
    every = lax.all_gather(shard, TENSOR, axis=0, tiled=False)
    return lax.all_gather(every.reshape(-1, *shard.shape), DP, axis=1, tiled=True)


def reduce_plain(grads):
    part = lax.psum_scatter(grads[0], TENSOR, scatter_dimension=0, tiled=True)[0]
    return lax.psum_scatter(part, DP, scatter_dimension=0, tiled=True).astype(F32)


def by_member(parts, me):
    return jnp.stack(
        [
            lax.dynamic_index_in_dim(parts, jnp.bitwise_xor(me, k), 0, keepdims=False)
            for k in range(parts.shape[0])
        ]
    )


def to_patches(rows, members):
    share, columns = PATCHES // members, rows.shape[1]
    me = lax.axis_index(CLIP)
    parts = rows.reshape(-1, members, share, columns).transpose(1, 0, 2, 3)
    parts = [
        lax.dynamic_index_in_dim(parts, jnp.bitwise_xor(me, k), 0, keepdims=False)
        for k in range(members)
    ]
    parts = [parts[0]] + [along(parts[k], CLIP, k) for k in range(1, members)]
    return by_member(jnp.stack(parts), me).reshape(-1, columns)


def to_frames(rows, members):
    share, columns = PATCHES // members, rows.shape[1]
    me = lax.axis_index(CLIP)
    parts = by_member(rows.reshape(members, -1, share, columns), me)
    parts = [parts[0]] + [along(parts[k], CLIP, k) for k in range(1, members)]
    parts = jnp.stack(parts)
    order = jnp.bitwise_xor(me, jnp.arange(members))
    parts = [
        lax.dynamic_index_in_dim(parts, jnp.bitwise_xor(me, k), 0, keepdims=False)
        for k in range(members)
    ]
    return jnp.stack(parts, 1).reshape(-1, columns)


CHUNKS = 4
STEPS = 4
PAD = 56


def place():
    return {axis: lax.axis_index(axis) for axis in ALL}


def moved(here, **flips):
    return tuple(here[a] + flips.get(a, 0) * (1 - 2 * here[a]) for a in ALL)


def dp_row(here, y=0, x=0, c=0):
    to = lambda a, flip: here[a] + flip * (1 - 2 * here[a])
    return to("y", y) * 4 + to("x", x) * 2 + to("c", c)


def remote(source, target, sent, received, device):
    return pltpu.make_async_remote_copy(
        src_ref=source,
        dst_ref=target,
        send_sem=sent,
        recv_sem=received,
        device_id=device,
        device_id_type=pl.DeviceIdType.MESH,
    )


def peers(here):
    found = [moved(here, s=j // 2, h=j % 2) for j in range(1, 4)]
    found += [moved(here, y=r // 4, x=r // 2 % 2, c=r % 2) for r in range(1, 8)]
    return found + [moved(here, c=1, h=1)]


def greet(here, what):
    barrier = pltpu.get_barrier_semaphore()
    everyone = peers(here)
    if what == "answer":
        pl.semaphore_wait(barrier, len(everyone))
        return
    for device in everyone:
        pl.semaphore_signal(
            barrier, inc=1, device_id=device, device_id_type=pl.DeviceIdType.MESH
        )


class Exchange:
    def __init__(self, here, out, back, sent, received):
        self.here, self.out, self.back = here, out, back
        self.sent, self.received = sent, received
        self.me = here["c"] * 2 + here["h"]

    def device(self, member):
        return tuple({"c": member // 2, "h": member % 2}.get(a, self.here[a]) for a in ALL)

    def start(self, member):
        @pl.when(self.me != member)
        def _():
            remote(
                self.out.at[member],
                self.back.at[self.me],
                self.sent.at[member],
                self.received.at[self.me],
                self.device(member),
            ).start()

        @pl.when(self.me == member)
        def _():
            self.back[member] = self.out[member]

    def finish(self, member):
        @pl.when(self.me != member)
        def _():
            remote(
                self.out.at[member],
                self.back.at[member],
                self.sent.at[member],
                self.received.at[member],
                self.device(member),
            ).wait()

    def send(self, rows_ref, first_row):
        share = PATCHES // 4
        for member in range(4):
            for frame in range(2):
                low = first_row(member, frame)
                self.out[member, frame, :share, :] = rows_ref[low : low + share, :].astype(BF16)
            self.start(member)

    def take(self, rows_ref, first_row):
        share = PATCHES // 4
        for member in range(4):
            self.finish(member)
            for frame in range(2):
                low = first_row(member, frame)
                rows_ref[low : low + share, :] = self.back[member, frame, :share, :].astype(F32)

    @staticmethod
    def by_frame(member, frame):
        return frame * PATCHES + member * (PATCHES // 4)

    @staticmethod
    def by_share(member, frame):
        return (member * 2 + frame) * (PATCHES // 4)

    def send_frames(self, rows_ref):
        self.send(rows_ref, self.by_frame)

    def take_patches(self, rows_ref):
        self.take(rows_ref, self.by_share)

    def send_patches(self, rows_ref):
        self.send(rows_ref, self.by_share)

    def take_frames(self, rows_ref):
        self.take(rows_ref, self.by_frame)


def by_rows(count, body, size=56):
    def step(i, carry):
        body(pl.ds(pl.multiple_of(i * size, size), size))
        return carry

    lax.fori_loop(0, count // size, step, 0)


def row_stats(rows):
    average = jnp.mean(rows, -1, keepdims=True)
    centred = rows - average
    spread = jnp.mean(centred * centred, -1, keepdims=True)
    return centred, lax.rsqrt(spread + EPSILON)


def attend_block(kind, stride, t, normed, weight, heads_ref, mixed_ref, sums, bias_ref):
    count, width = mixed_ref.shape[1:]
    heads_ref[t] = mm(normed, weight[:, : 3 * width]).astype(BF16)
    heads = heads_ref.at[t]
    sums[...] = jnp.zeros_like(sums)
    for start, size, group in windows(kind, count):
        bias = bias_ref[...] if group is None else key_bias(start, size, group, stride)
        rows = pl.ds(start, size)
        for head in range(width // HEAD_DIM):
            low = head * HEAD_DIM
            query, key, value = head_slices(heads, rows, width, head)
            scores = mm(key, query * HEAD_DIM**-0.5, NT) + bias
            weights = jnp.exp(scores - jnp.max(scores, 0, keepdims=True))
            total = jnp.sum(weights, 0, keepdims=True)
            blended = (mm(value.T, weights.astype(BF16)) / total).T
            if group is not None:
                blended = jnp.where(row_valid(start, size, group, HEAD_DIM), blended, 0.0)
            sums[rows, low : low + HEAD_DIM] += blended
    mixed_ref[t] = sums[...].astype(BF16)
    return mm(mixed_ref[t], weight[:, 3 * width :], NT)


def attend_back_block(
    kind, stride, heads, mixed, grad, normed, weight, grad_mixed, sums, grad_heads, bias_ref
):
    count, width = mixed.shape
    scale = HEAD_DIM**-0.5
    grad_mixed[...] = mm(grad[...], weight[:, 3 * width :]).astype(BF16)
    sums[...] = jnp.zeros_like(sums)
    for start, size, group in windows(kind, count):
        bias = bias_ref[...] if group is None else key_bias(start, size, group, stride)
        rows = pl.ds(start, size)
        for head in range(width // HEAD_DIM):
            low = head * HEAD_DIM
            query, key, value = head_slices(heads, rows, width, head)
            query = query * scale
            grad_here = grad_mixed[rows, low : low + HEAD_DIM]
            if group is not None:
                valid = row_valid(start, size, group, HEAD_DIM)
                grad_here = jnp.where(valid, grad_here.astype(F32), 0.0).astype(BF16)
            scores = mm(key, query, NT) + bias
            weights = jnp.exp(scores - jnp.max(scores, 0, keepdims=True))
            weights = weights * (1.0 / jnp.sum(weights, 0, keepdims=True))
            grad_weights = mm(value, grad_here, NT)
            row_terms = jnp.sum(weights * grad_weights, 0, keepdims=True)
            grad_scores = (weights * (grad_weights - row_terms)).astype(BF16)
            sums[rows, low : low + HEAD_DIM] += (mm(key.T, grad_scores) * scale).T
            low += width
            sums[rows, low : low + HEAD_DIM] += mm(grad_scores, query)
            low += width
            sums[rows, low : low + HEAD_DIM] += mm(weights.astype(BF16), grad_here)
    grad_heads[...] = sums[...].astype(BF16)
    return mm(grad_heads[...], weight[:, : 3 * width], NT)


EVENT_NAMES = ("zs", "line", "relay", "across", "core", "first", "second", "third")
BLOCK_ORDER = (1, 2, 3, 0)
ORDER = (
    ("go",),
    ("zs", 0, 1), ("zs", 0, 2), ("zs", 0, 3), ("line", 0, 0), ("line", 1, 0), ("ln0",),
    ("line", 2, 0), ("mask",), ("line", 3, 0), ("line", 0, 1), ("zs", 1, 1), ("line", 0, 2),
    ("zs", 1, 2), ("relay", 0, 0), ("zs", 1, 3), ("line", 0, 3), ("takeE0",), ("relay", 0, 1),
    ("zs", 2, 1), ("relay", 0, 2), ("line", 1, 1), ("zs", 2, 2), ("across", 0, 0),
    ("relay", 1, 0), ("relay", 0, 3), ("across", 0, 2), ("zs", 2, 3), ("line", 1, 2),
    ("across", 0, 1), ("line", 1, 3), ("zs", 3, 1), ("across", 0, 3), ("P0", 0), ("relay", 1, 1),
    ("across", 1, 0), ("zs", 3, 2), ("P0", 1), ("relay", 1, 2), ("line", 2, 1), ("zs", 3, 3),
    ("P0", 2), ("relay", 1, 3), ("relay", 2, 0), ("P0", 3), ("across", 1, 1), ("across", 1, 2),
    ("line", 2, 2), ("exch1",), ("relay", 3, 0), ("line", 2, 3), ("across", 2, 0),
    ("across", 1, 3), ("relay", 2, 1), ("relay", 2, 2), ("line", 3, 1), ("across", 3, 0),
    ("ln1",), ("relay", 2, 3), ("line", 3, 2), ("P1", 0), ("across", 2, 1), ("across", 2, 2),
    ("line", 3, 3), ("P1", 1), ("relay", 3, 1), ("P1", 2), ("across", 2, 3), ("P1", 3),
    ("relay", 3, 2), ("ln2",), ("relay", 3, 3), ("up", 0), ("across", 3, 1), ("up", 1),
    ("across", 3, 2), ("core", 0), ("up", 2), ("across", 3, 3), ("core", 1), ("up", 3),
    ("core", 2), ("dn", 0), ("first", 0), ("core", 3), ("dn", 1), ("first", 1), ("dn", 2),
    ("dn", 3), ("first", 2), ("B1", 0), ("second", 0), ("B1", 1), ("first", 3), ("core", 4),
    ("B1", 2), ("second", 1), ("core", 5), ("second", 2), ("B1", 3), ("second", 3), ("nb2",),
    ("core", 6), ("core", 7), ("B2", 0), ("first", 4), ("first", 5), ("B2", 1), ("third", 0),
    ("first", 6), ("first", 7), ("core", 8), ("B2", 2), ("second", 4), ("second", 5),
    ("second", 6), ("core", 9), ("B2", 3), ("second", 7), ("first", 8), ("core", 10), ("nb1",),
    ("first", 9), ("core", 11), ("second", 8), ("first", 10), ("second", 9), ("third", 1),
    ("first", 11), ("second", 10), ("takeE2",), ("B3", 0), ("second", 11), ("B3", 1),
    ("core", 12), ("B3", 2), ("third", 2), ("core", 13), ("B3", 3), ("first", 12), ("core", 14),
    ("exch3",), ("first", 13), ("core", 15), ("second", 12), ("first", 14), ("nb0",),
    ("second", 13), ("gain",), ("first", 15), ("second", 14), ("second", 15), ("third", 3),
)


def after_each(order):
    found, events = {}, []
    for item in order:
        if item[0] in EVENT_NAMES:
            events.append(item)
        else:
            events = found.setdefault(item, [])
    return found


AFTER = after_each(ORDER)


def layer_kernel(
    live_ref,
    tokens_hbm,
    cotangent_hbm,
    gain_hbm,
    qkv_time_hbm,
    out_time_hbm,
    qkv_space_hbm,
    out_space_hbm,
    up_hbm,
    down_hbm,
    weight_ref,
    out_ref,
    stream_ref,
    own_ref,
    own_gain_ref,
    tokens_ref,
    gain_ref,
    qkv_time_ref,
    out_time_ref,
    qkv_space_ref,
    out_space_ref,
    shard_ref,
    held,
    normed_time_ref,
    time_heads_ref,
    time_mixed_ref,
    after_time_ref,
    normed_space_ref,
    space_heads_ref,
    space_mixed_ref,
    after_space_ref,
    normed_mlp_ref,
    hidden_ref,
    slope_ref,
    low_ref,
    rows_ref,
    total_ref,
    mixed_sums,
    sums,
    grad_mixed,
    grad_heads,
    bias_ref,
    work,
    keep,
    came,
    first,
    second,
    third,
    gains_ref,
    gain_sums,
    gain_line,
    gain_out,
    gain_parts,
    swap_out,
    swap_back,
    piece_sent,
    piece_here,
    core_sent,
    core_here,
    first_sent,
    first_here,
    second_sent,
    second_here,
    third_sent,
    third_here,
    gain_sent,
    gain_here,
    swap_sent,
    swap_here,
    held_sem,
    own_sem,
    load_sem,
    credit,
):
    here = place()
    count, columns = tokens_ref.shape
    width = time_mixed_ref.shape[2]
    own_row = dp_row(here)
    last = CHUNKS * STEPS - 1
    live = jnp.where(here["s"] < live_ref[0], 1.0, 0.0).astype(F32)

    loads = [
        pltpu.make_async_copy(source, target, load_sem.at[i])
        for i, (source, target) in enumerate(
            (
                (gain_hbm, gain_ref),
                (qkv_time_hbm, qkv_time_ref),
                (out_time_hbm, out_time_ref),
                (qkv_space_hbm, qkv_space_ref),
                (out_space_hbm, out_space_ref),
                (up_hbm, shard_ref.at[2]),
                (down_hbm, shard_ref.at[3]),
                (tokens_hbm, tokens_ref),
                (cotangent_hbm, stream_ref),
            )
        )
    ]
    greet(here, "call")
    for load in loads:
        load.start()
    for load in loads[:5]:
        load.wait()

    for k, qkv, out in ((0, qkv_time_ref, out_time_ref), (1, qkv_space_ref, out_space_ref)):
        for c in range(3):
            shard_ref[k, :, c * width : (c + 1) * width] = qkv[c]
        shard_ref[k, :, 3 * width :] = out[...].astype(F32).T.astype(BF16)
    own_gains = gain_ref.shape[1]
    gain_out[0, : gain_ref.shape[0], :own_gains] = gain_ref[...].astype(F32)
    for load in loads[5:7]:
        load.wait()
    greet(here, "answer")

    def row_of(part, r):
        return dp_row(here, y=r // 2, x=r % 2, c=part)

    def slot_of(k, j, row):
        return weight_ref.at[k, j, pl.ds(pl.multiple_of(row * BLOCK_ROWS, BLOCK_ROWS), BLOCK_ROWS)]

    def arrived(k, part, r, j):
        slot = slot_of(k, j, row_of(part, r))
        remote(
            slot, slot, piece_sent.at[k, 0, 0], piece_here.at[k, part, r, j], moved(here, c=1)
        ).wait_recv()

    def send(source, k, j, r, sem, part, r_there, **flips):
        remote(
            source,
            slot_of(k, j, row_of(0, r)),
            piece_sent.at[k, sem, j],
            piece_here.at[k, part, r_there, j],
            moved(here, **flips),
        ).start()

    def piece(k, j, r):
        return slot_of(k, j, row_of(0, r))

    def along_line(k, j):
        remote(
            shard_ref.at[k],
            slot_of(k, j, own_row),
            piece_sent.at[k, 0, j],
            piece_here.at[k, 0, 0, j],
            moved(here, s=j // 2, h=j % 2),
        ).start()

    def spread(source, k, j):
        send(source, k, j, 0, 1, 0, 1, x=1)
        send(source, k, j, 0, 2, 0, 2, y=1)
        send(source, k, j, 0, 4, 1, 0, c=1)

    def line(k, j):
        if j:
            arrived(k, 0, 0, j)
        spread(piece(k, j, 0) if j else shard_ref.at[k], k, j)

    def relay(k, j):
        up = j // 2
        arrived(k, 0, 1, j)
        send(piece(k, j, 1), k, j, 1, 5, 1, 1, c=1)
        arrived(k, 0, 2, j)
        send(piece(k, j, 2), k, j, 2, 6, 1, 2, c=1)
        source = slot_of(k, j, dp_row(here, y=up, x=1 - up))
        remote(
            source,
            source,
            piece_sent.at[k, 3, j],
            piece_here.at[k, 0, 3, j],
            moved(here, y=1 - up, x=up),
        ).start()

    def across(k, j):
        arrived(k, 0, 3, j)
        send(piece(k, j, 3), k, j, 3, 7, 1, 3, c=1)

    def fetch(k, t):
        return pltpu.make_async_copy(weight_ref.at[k, t], held.at[t], held_sem.at[t])

    def ready(k):
        for j in range(STEPS):
            for r in range(4):
                arrived(k, 1, r, j)
        for t in BLOCK_ORDER:
            fetch(k, t).start()

    def weight(k, t):
        fetch(k, t).wait()
        return held.at[t]

    def stored(k):
        return pltpu.make_async_copy(shard_ref.at[k], slot_of(k, 0, own_row), own_sem.at[k])

    half_lanes = keep.shape[4]
    swapped = (0, 2, 1, 3)

    def grad_rows(part, quad):
        row = dp_row(here, y=quad // 2, x=quad % 2, c=part)
        return pl.ds(pl.multiple_of(row * BLOCK_ROWS, BLOCK_ROWS), BLOCK_ROWS)

    def core_copy(step, quad):
        return remote(
            work.at[step % 2, grad_rows(1, quad)],
            came.at[step % 4, quad],
            core_sent.at[step % 2, quad],
            core_here.at[step % 4, quad],
            moved(here, c=1),
        )

    def first_copy(step, half):
        return remote(
            keep.at[step, pl.ds(2, 2), half],
            first.at[step, half],
            first_sent.at[step, half],
            first_here.at[step, half],
            moved(here, y=1 - half, x=half),
        )

    def second_copy(step, half):
        return remote(
            keep.at[step, 1, half],
            second.at[step, half],
            second_sent.at[step, half],
            second_here.at[step, half],
            moved(here, y=half, x=1 - half),
        )

    def third_copy(step):
        j = BLOCK_ORDER[step % STEPS]
        return remote(
            keep.at[step, 0],
            third.at[step],
            third_sent.at[step],
            third_here.at[step],
            moved(here, s=j // 2, h=j % 2),
        )

    def begin(step):
        @pl.when(step >= 2)
        def _():
            for quad in range(4):
                core_copy(step - 2, quad).wait_send()

        return work.at[step % 2]

    def emit(step):
        @pl.when(step >= 4)
        def _():
            pl.semaphore_wait(credit, 1)

        for quad in range(4):
            core_copy(step, quad).start()

    def take_core(step):
        for quad in range(4):
            core_copy(step, quad).wait_recv()
        for index in (2, 3, 1, 0):
            for half in range(2):
                quad = swapped[index] if half else index
                lanes = slice(half * half_lanes, (half + 1) * half_lanes)
                own = work[step % 2, grad_rows(0, quad), lanes].astype(F32)
                both = own + came[step % 4, quad, :, lanes].astype(F32)
                keep[step, index, half] = both.astype(BF16)
                if index == 3:
                    first_copy(step, half).start()
        if step <= last - 4:
            pl.semaphore_signal(
                credit,
                inc=1,
                device_id=moved(here, c=1),
                device_id_type=pl.DeviceIdType.MESH,
            )

    def take_first(step):
        for half in range(2):
            first_copy(step, half).wait_recv()
            for index in (1, 0):
                both = keep[step, index, half].astype(F32) + first[step, half, index].astype(F32)
                keep[step, index, half] = both.astype(BF16)
                if index:
                    second_copy(step, half).start()

    def take_second(step):
        for half in range(2):
            second_copy(step, half).wait_recv()
            both = keep[step, 0, half].astype(F32) + second[step, half].astype(F32)
            keep[step, 0, half] = both.astype(BF16)
        if BLOCK_ORDER[step % STEPS]:
            third_copy(step).start()

    def take_third(index):
        steps = [index * STEPS + i for i in range(STEPS)]
        for step in steps:
            if BLOCK_ORDER[step % STEPS]:
                third_copy(step).wait_recv()
        for half in range(2):
            total = jnp.zeros((BLOCK_ROWS, half_lanes), F32)
            for step in steps:
                source = third[step, half] if BLOCK_ORDER[step % STEPS] else keep[step, 0, half]
                total = total + source.astype(F32)
            own_ref[index, :, half * half_lanes : (half + 1) * half_lanes] = total

    events = {
        "zs": along_line,
        "line": line,
        "relay": relay,
        "across": across,
        "core": take_core,
        "first": take_first,
        "second": take_second,
        "third": take_third,
    }

    def follow(item):
        for name, *args in AFTER.get(item, ()):
            events[name](*args)

    def loop(name, body):
        def step(i, carry):
            body(i, (i + 1) % STEPS)
            for c in range(STEPS - 1):
                if AFTER.get((name, c)):

                    @pl.when(i == c)
                    def _(c=c):
                        follow((name, c))

            return carry

        lax.fori_loop(0, STEPS, step, 0)
        follow((name, STEPS - 1))

    def layer_norm(source_ref, gain, target_ref):
        def body(rows):
            centred, scale = row_stats(source_ref[rows, :])
            target_ref[rows, :] = (centred * scale * gains_ref[gain : gain + 1, :]).astype(
                target_ref.dtype
            )

        by_rows(count, body)

    def norm_back(source_ref, gain, grad_normed_ref):
        def body(rows):
            centred, scale = row_stats(source_ref[rows, :])
            unit = centred * scale
            grad_normed = grad_normed_ref[rows, :]
            e = grad_normed * gains_ref[gain : gain + 1, :]
            mean = jnp.mean(e, -1, keepdims=True)
            tilt = jnp.mean(e * unit, -1, keepdims=True)
            stream_ref[rows, :] += scale * (e - mean - unit * tilt)
            gain_sums[gain : gain + 1, :] += jnp.sum(grad_normed * unit, 0, keepdims=True)

        by_rows(count, body)

    def exchange(index):
        return Exchange(
            here,
            swap_out.at[index % 2],
            swap_back.at[index % 2],
            swap_sent.at[index],
            swap_here.at[index],
        )

    def attention(kind, k, normed_ref, heads_ref, mixed_ref):
        total_ref[...] = jnp.zeros_like(total_ref)

        def compute(i, t):
            total_ref[...] += attend_block(
                kind,
                PATCHES // 4,
                t,
                normed_ref[...],
                weight(k, t),
                heads_ref,
                mixed_ref,
                mixed_sums,
                bias_ref,
            )

        return compute

    def attention_back(kind, k, normed_ref, heads_ref, mixed_ref):
        total_ref[...] = jnp.zeros_like(total_ref)

        def compute(i, t):
            step = (CHUNKS - 1 - k) * STEPS + i
            out = begin(step)
            total_ref[...] += attend_back_block(
                kind,
                PATCHES // 4,
                heads_ref.at[t],
                mixed_ref.at[t],
                low_ref,
                normed_ref,
                weight(k, t),
                grad_mixed,
                sums,
                grad_heads,
                bias_ref,
            )
            if k:
                fetch(k - 1, t).start()
            out[:, : 3 * width] = mm(normed_ref[...], grad_heads[...], TN).astype(BF16)
            out[:, 3 * width :] = mm(low_ref[...], mixed_ref[t], TN).astype(BF16)
            emit(step)

        return compute

    gain_parts[0, own_row] = gain_out[0]

    def gain_copy(r):
        flips = {"y": r // 4, "x": r // 2 % 2, "c": r % 2}
        return remote(
            gain_out.at[0],
            gain_parts.at[0, own_row],
            gain_sent.at[0, r],
            gain_here.at[0, r],
            moved(here, **flips),
        )

    for r in range(1, 8):
        gain_copy(r).start()
    for k in range(CHUNKS):
        stored(k).start()
    follow(("go",))
    loads[7].wait()

    def unit_rows(rows):
        centred, scale = row_stats(tokens_ref[rows, :])
        rows_ref[rows, :] = centred * scale

    by_rows(count, unit_rows)
    for r in range(1, 8):
        gain_copy(r).wait()
    for d in range(8):
        gains_ref[:, d * own_gains : (d + 1) * own_gains] = gain_parts[0, d, :, :own_gains]

    def scale_rows(rows):
        rows_ref[rows, :] = rows_ref[rows, :] * gains_ref[0:1, :]

    by_rows(count, scale_rows)
    swap = exchange(0)
    swap.send_frames(rows_ref)
    follow(("ln0",))
    loads[8].wait()

    def mask_rows(rows):
        stream_ref[rows, :] = stream_ref[rows, :] * live
        low_ref[rows, :] = stream_ref[rows, :].astype(BF16)

    by_rows(count, mask_rows)
    bias_ref[...] = key_bias(0, count, None, PATCHES // 4)
    gain_sums[...] = jnp.zeros_like(gain_sums)
    follow(("mask",))
    swap.take_patches(rows_ref)
    normed_time_ref[...] = rows_ref[...].astype(BF16)
    for k in range(CHUNKS):
        stored(k).wait()
    follow(("takeE0",))

    ready(0)
    loop("P0", attention("time", 0, normed_time_ref, time_heads_ref, time_mixed_ref))
    swap = exchange(1)
    swap.send_patches(total_ref)
    follow(("exch1",))
    swap.take_frames(rows_ref)
    after_time_ref[...] = tokens_ref[...] + rows_ref[...]
    layer_norm(after_time_ref, 1, normed_space_ref)
    follow(("ln1",))

    ready(1)
    loop("P1", attention("space", 1, normed_space_ref, space_heads_ref, space_mixed_ref))
    after_space_ref[...] = after_time_ref[...] + total_ref[...]
    layer_norm(after_space_ref, 2, normed_mlp_ref)
    follow(("ln2",))

    ready(2)

    def up(i, t):
        out = begin(i)
        pre_act = mm(normed_mlp_ref[...], weight(2, t)[...])
        cdf = 0.5 * (1.0 + lax.erf(pre_act * 0.5**0.5))
        hidden_ref[t] = (pre_act * cdf).astype(BF16)
        density = jnp.exp(-0.5 * pre_act * pre_act) * (0.5 / math.pi) ** 0.5
        slope_ref[t] = (cdf + pre_act * density).astype(BF16)
        out[...] = mm(low_ref[...], hidden_ref[t], TN).astype(BF16)
        emit(i)

    loop("up", up)
    ready(3)
    out_ref[...] = after_space_ref[...]

    def down(i, t):
        out_ref[...] += mm(hidden_ref[t], weight(3, t)[...], NT)
        grad_hidden = mm(low_ref[...], held[t])
        slope_ref[t] = (grad_hidden * slope_ref[t].astype(F32)).astype(BF16)
        fetch(2, t).start()

    loop("dn", down)
    out_ref[...] = out_ref[...] * live
    total_ref[...] = jnp.zeros_like(total_ref)

    def up_back(i, t):
        step = STEPS + i
        out = begin(step)
        total_ref[...] += mm(slope_ref[t], weight(2, t)[...], NT)
        fetch(1, t).start()
        out[...] = mm(normed_mlp_ref[...], slope_ref[t], TN).astype(BF16)
        emit(step)

    loop("B1", up_back)
    norm_back(after_space_ref, 2, total_ref)
    low_ref[...] = stream_ref[...].astype(BF16)
    follow(("nb2",))
    loop("B2", attention_back("space", 1, normed_space_ref, space_heads_ref, space_mixed_ref))
    norm_back(after_time_ref, 1, total_ref)
    swap = exchange(2)
    swap.send_frames(stream_ref)
    follow(("nb1",))
    swap.take_patches(rows_ref)
    low_ref[...] = rows_ref[...].astype(BF16)
    follow(("takeE2",))
    loop("B3", attention_back("time", 0, normed_time_ref, time_heads_ref, time_mixed_ref))
    swap = exchange(3)
    swap.send_patches(total_ref)
    follow(("exch3",))
    swap.take_frames(rows_ref)
    norm_back(tokens_ref, 0, rows_ref)

    line_index = here["s"] * 2 + here["h"]

    def gain_line_copy(j):
        return remote(
            gain_sums,
            gain_line.at[line_index],
            gain_sent.at[1, j],
            gain_here.at[1, j],
            moved(here, s=j // 2, h=j % 2),
        )

    def gain_back(r):
        flips = {"y": r // 4, "x": r // 2 % 2, "c": r % 2}
        return remote(
            gain_out.at[dp_row(here, **flips)],
            gain_parts.at[1, own_row],
            gain_sent.at[2, r],
            gain_here.at[2, r],
            moved(here, **flips),
        )

    for j in range(1, 4):
        gain_line_copy(j).start()
    gain_line[line_index] = gain_sums[...]
    follow(("nb0",))
    for j in range(1, 4):
        gain_line_copy(j).wait()
    total = gain_line[0] + gain_line[1] + gain_line[2] + gain_line[3]
    for d in range(8):
        gain_out[d, :, :own_gains] = total[:, d * own_gains : (d + 1) * own_gains]
    for r in range(1, 8):
        gain_back(r).start()
    gain_parts[1, own_row] = gain_out[own_row]
    follow(("gain",))
    for r in range(1, 8):
        gain_back(r).wait()
    total = gain_parts[1, 0]
    for d in range(1, 8):
        total = total + gain_parts[1, d]
    own_gain_ref[...] = total

    for k in range(CHUNKS):
        for sem in range(8):
            for j in range(4):
                if sem or j:
                    slot = slot_of(k, 0, own_row)
                    remote(
                        slot,
                        slot,
                        piece_sent.at[k, sem, j],
                        piece_here.at[k, 0, 0, 0],
                        moved(here, c=1),
                    ).wait_send()
    for step in range(last + 1):
        if step > last - 2:
            for quad in range(4):
                core_copy(step, quad).wait_send()
        for half in range(2):
            first_copy(step, half).wait_send()
            second_copy(step, half).wait_send()
        if BLOCK_ORDER[step % STEPS]:
            third_copy(step).wait_send()


def layer(live_clips, tokens, cotangent, norm_gains, *weights):
    count, columns = tokens.shape
    rows, lanes = weights[4].shape
    half = lanes // 2
    width, steps = lanes // 4, CHUNKS * STEPS
    here = pl.BlockSpec(memory_space=pltpu.VMEM)
    there = pl.BlockSpec(memory_space=pl.ANY)
    outputs = (
        shaped(CHUNKS, STEPS, columns, lanes),
        shaped(count, columns, dtype=F32),
        shaped(count, columns, dtype=F32),
        shaped(CHUNKS, rows, lanes, dtype=F32),
        shaped(8, 128, dtype=F32),
    )
    return pl.pallas_call(
        layer_kernel,
        in_specs=[pl.BlockSpec(memory_space=pltpu.SMEM)] + [there] * 9,
        out_specs=[there] + [here] * (len(outputs) - 1),
        out_shape=outputs,
        scratch_shapes=[
            pltpu.VMEM((count, columns), F32),
            pltpu.VMEM(norm_gains.shape, BF16),
            *[pltpu.VMEM(w.shape, BF16) for w in weights[:4]],
            pltpu.VMEM((CHUNKS, rows, lanes), BF16),
            pltpu.VMEM((STEPS, columns, lanes), BF16),
            pltpu.VMEM((count, columns), BF16),
            pltpu.VMEM((STEPS, count, 3 * width), BF16),
            pltpu.VMEM((STEPS, count, width), BF16),
            pltpu.VMEM((count, columns), F32),
            pltpu.VMEM((count, columns), BF16),
            pltpu.VMEM((STEPS, count, 3 * width), BF16),
            pltpu.VMEM((STEPS, count, width), BF16),
            pltpu.VMEM((count, columns), F32),
            pltpu.VMEM((count, columns), BF16),
            pltpu.VMEM((STEPS, count, lanes), BF16),
            pltpu.VMEM((STEPS, count, lanes), BF16),
            pltpu.VMEM((count, columns), BF16),
            pltpu.VMEM((count, columns), F32),
            pltpu.VMEM((count, columns), F32),
            pltpu.VMEM((count, width), F32),
            pltpu.VMEM((count, 3 * width), F32),
            pltpu.VMEM((count, width), BF16),
            pltpu.VMEM((count, 3 * width), BF16),
            pltpu.VMEM((count, count), F32),
            pltpu.VMEM((2, columns, lanes), BF16),
            pltpu.VMEM((steps, 4, 2, rows, half), BF16),
            pltpu.VMEM((4, 4, rows, lanes), BF16),
            pltpu.VMEM((steps, 2, 2, rows, half), BF16),
            pltpu.VMEM((steps, 2, rows, half), BF16),
            pltpu.VMEM((steps, 2, rows, half), BF16),
            pltpu.VMEM((8, columns), F32),
            pltpu.VMEM((8, columns), F32),
            pltpu.VMEM((4, 8, columns), F32),
            pltpu.VMEM((8, 8, 128), F32),
            pltpu.VMEM((2, 8, 8, 128), F32),
            pltpu.VMEM((2, 4, 2, PAD, columns), BF16),
            pltpu.VMEM((2, 4, 2, PAD, columns), BF16),
            pltpu.SemaphoreType.DMA((CHUNKS, 8, 4)),
            pltpu.SemaphoreType.DMA((CHUNKS, 2, 4, 4)),
            pltpu.SemaphoreType.DMA((2, 4)),
            pltpu.SemaphoreType.DMA((4, 4)),
            pltpu.SemaphoreType.DMA((steps, 2)),
            pltpu.SemaphoreType.DMA((steps, 2)),
            pltpu.SemaphoreType.DMA((steps, 2)),
            pltpu.SemaphoreType.DMA((steps, 2)),
            pltpu.SemaphoreType.DMA((steps,)),
            pltpu.SemaphoreType.DMA((steps,)),
            pltpu.SemaphoreType.DMA((3, 8)),
            pltpu.SemaphoreType.DMA((3, 8)),
            pltpu.SemaphoreType.DMA((4, 4)),
            pltpu.SemaphoreType.DMA((4, 4)),
            pltpu.SemaphoreType.DMA((STEPS,)),
            pltpu.SemaphoreType.DMA((CHUNKS,)),
            pltpu.SemaphoreType.DMA((9,)),
            pltpu.SemaphoreType.REGULAR,
        ],
        compiler_params=pltpu.CompilerParams(
            collective_id=0, has_side_effects=True, vmem_limit_bytes=67043328
        ),
        name="layer",
    )(live_clips, tokens, cotangent, norm_gains, *weights)[1:]


def finish_kernel(output_ref, grad_ref, own_ref, gain_ref, *outs):
    out_ref, stream_ref, gains, time_in, time_out, space_in, space_out, up, down = outs
    width = time_in.shape[2]
    out_ref[...] = output_ref[...]
    stream_ref[...] = grad_ref[...]
    gains[...] = gain_ref[: gains.shape[0], : gains.shape[1]]
    for k, into, out in ((3, time_in, time_out), (2, space_in, space_out)):
        for c in range(3):
            into[c] = own_ref[k, :, c * width : (c + 1) * width]
        out[...] = own_ref[k, :, 3 * width :].T
    up[...] = own_ref[1]
    down[...] = own_ref[0]


def finish(output, grad, own, gain, like):
    shapes = [jax.ShapeDtypeStruct(a.shape, F32) for a in like]
    here = pl.BlockSpec(memory_space=pltpu.VMEM)
    return pl.pallas_call(
        finish_kernel,
        in_specs=[here] * 4,
        out_specs=[here] * len(shapes),
        out_shape=shapes,
        name="finish",
    )(output, grad, own, gain)


def sum_gains(total, own):
    for axes in ("c", "x", "y", TENSOR):
        bit = 1
        while bit < lax.axis_size(axes):
            total = total + along(total, axes, bit)
            bit *= 2
    return lax.dynamic_slice_in_dim(total, lax.axis_index(DP) * own, own, 1)


def on_device(
    routed,
    tokens,
    live_clips,
    norm_gains,
    qkv_time,
    out_time,
    qkv_space,
    out_space,
    up_weight,
    down_weight,
    cotangent,
):
    members = lax.axis_size("c") * lax.axis_size("h")
    share = PATCHES // members
    count, columns = tokens.shape
    width = qkv_time.shape[2]
    live = jnp.where(lax.axis_index("s") < live_clips[0], 1.0, 0.0).astype(F32)

    def pack_heads(qkv, out):
        rows = qkv.shape[1]
        return jnp.concatenate([qkv.transpose(1, 0, 2).reshape(rows, -1), out.T], 1)

    if routed:
        weights = (qkv_time, out_time, qkv_space, out_space, up_weight, down_weight.T)
        done = layer(live_clips, tokens, cotangent, norm_gains, *weights)
        *found, down_own = finish(*done, (tokens, cotangent, norm_gains, *weights))
        return (*found, down_own.T)
    shards = [
        pack_heads(qkv_time, out_time),
        pack_heads(qkv_space, out_space),
        up_weight,
        down_weight.T,
    ]
    grad_stream = cotangent * live
    time_all, space_all, up_all, down_all = [gather_plain(shard) for shard in shards]
    blocks, depth, lanes = up_all.shape
    gains = lax.all_gather(norm_gains, DP, axis=1, tiled=True).astype(F32)
    normed_time = to_patches(normalize(tokens, gains[0]).astype(BF16), members)
    time_heads, time_mixed, change = attend("time", normed_time, time_all, share, BF16)
    after_time = tokens + to_frames(change, members).astype(F32)
    normed_space = normalize(after_time, gains[1]).astype(BF16)
    space_heads, space_mixed, change = attend("space", normed_space, space_all, 1, F32)
    after_space = after_time + change
    normed_mlp = normalize(after_space, gains[2]).astype(BF16)
    hidden, slope = phase(
        up_kernel,
        "up",
        (normed_mlp, up_all),
        (shaped(blocks, count, lanes), shaped(blocks, count, lanes)),
        cost=12,
    )
    (change,) = phase(
        down_kernel, "down", (hidden, down_all), (shaped(count, depth, dtype=F32),), cost=4
    )
    after_mlp = after_space + change
    grad_low = grad_stream.astype(BF16)
    work = (pltpu.VMEM((depth, lanes), BF16),)
    *down_grads, grad_pre = phase(
        down_back_kernel,
        "down_back",
        (grad_low, down_all, hidden, slope),
        (*grad_shapes(down_all, False), shaped(blocks, count, lanes)),
        work,
        cost=8,
    )
    *up_grads, grad_normed = phase(
        up_back_kernel,
        "up_back",
        (normed_mlp, up_all, grad_pre),
        (*grad_shapes(up_all, False), shaped(count, depth, dtype=F32)),
        work,
        cost=8,
    )
    grad_part, gain_mlp = norm_back(after_space, gains[2], grad_normed)
    grad_stream = grad_stream + grad_part
    space_grads, grad_normed = attend_back(
        "space",
        normed_space,
        space_all,
        space_heads,
        space_mixed,
        grad_stream.astype(BF16),
        1,
        F32,
        False,
    )
    grad_part, gain_space = norm_back(after_time, gains[1], grad_normed)
    grad_stream = grad_stream + grad_part
    grad_low = to_patches(grad_stream.astype(BF16), members)
    time_grads, grad_normed = attend_back(
        "time", normed_time, time_all, time_heads, time_mixed, grad_low, share, BF16, routed
    )
    grad_normed = to_frames(grad_normed, members).astype(F32)
    grad_part, gain_time = norm_back(tokens, gains[0], grad_normed)
    grad_tokens = grad_stream + grad_part
    down_own = reduce_plain(down_grads).T
    up_own = reduce_plain(up_grads)
    space_own = reduce_plain(space_grads)
    time_own = reduce_plain(time_grads)
    gains_own = sum_gains(jnp.stack([gain_time, gain_space, gain_mlp]), norm_gains.shape[1])
    output = after_mlp * live

    def unpack(own):
        rows = own.shape[0]
        return own[:, : 3 * width].reshape(rows, 3, width).transpose(1, 0, 2), own[:, 3 * width :].T

    time_in_own, time_out_own = unpack(time_own)
    space_in_own, space_out_own = unpack(space_own)
    return (
        output,
        grad_tokens,
        gains_own,
        time_in_own,
        time_out_own,
        space_in_own,
        space_out_own,
        up_own,
        down_own,
    )


def solution(mesh):
    n_dp, n_tensor = mesh.devices.shape

    def run(*args):
        slots = args[0].shape[0] // (n_dp * HALF * PATCHES)
        fine = Mesh(mesh.devices.reshape(n_dp // 4, 2, 2, slots, n_tensor // slots), ALL)
        in_specs = (
            P(ALL, None),
            P(DP),
            P(None, DP),
            P(None, DP, TENSOR),
            P(TENSOR, DP),
            P(None, DP, TENSOR),
            P(TENSOR, DP),
            P(DP, TENSOR),
            P(TENSOR, DP),
            P(ALL, None),
        )
        out_specs = (in_specs[0], in_specs[0]) + in_specs[2:9]
        routed = fine.devices.shape == (2, 2, 2, 2, 2)
        return jax.shard_map(
            functools.partial(on_device, routed), mesh=fine, in_specs=in_specs, out_specs=out_specs, check_vma=False
        )(*args)

    return run
```

```python
import functools
import math

import jax
import jax.numpy as jnp
from jax import lax
from jax.experimental import pallas as pl
from jax.experimental.pallas import tpu as pltpu
from jax.sharding import Mesh, PartitionSpec as P

HEAD_DIM = 64
PATCHES = 196
HALF = 4
FRAMES = 8
EPSILON = 1e-06
F32 = jnp.float32
BF16 = jnp.bfloat16
ALL = ("y", "x", "c", "s", "h")
DP = ("y", "x", "c")
TENSOR = ("s", "h")
CLIP = ("c", "h")

NN = (((1,), (0,)), ((), ()))
NT = (((1,), (1,)), ((), ()))
TN = (((0,), (0,)), ((), ()))
BLOCK_ROWS = 96


def mm(a, b, dims=NN):
    return lax.dot_general(a, b, dims, preferred_element_type=F32)


def row_ids(shape, dim, start):
    return lax.broadcasted_iota(jnp.int32, shape, dim) + start


def windows(kind, count):
    if kind == "time":
        return [(0, count, None)]
    found = []
    for frame in range(count // PATCHES):
        low = frame * PATCHES // 16 * 16
        high = min(count, -(-(frame + 1) * PATCHES // 16) * 16)
        found.append((low, high - low, frame))
    return found


def key_bias(start, size, group, stride):
    keys = row_ids((size, size), 0, start)
    if group is None:
        together = keys % stride == row_ids((size, size), 1, start) % stride
    else:
        together = (keys >= group * PATCHES) & (keys < (group + 1) * PATCHES)
    return jnp.where(together, 0.0, -1e30)


def row_valid(start, size, group, width):
    rows = row_ids((size, width), 0, start)
    return (rows >= group * PATCHES) & (rows < (group + 1) * PATCHES)


def normalize(rows, scale_row):
    average = jnp.mean(rows, -1, keepdims=True)
    centred = rows - average
    spread = jnp.mean(centred * centred, -1, keepdims=True)
    return centred * lax.rsqrt(spread + EPSILON) * scale_row


def norm_back(rows, scale_row, grad_normed):
    unused, pullback = jax.vjp(normalize, rows, scale_row)
    return pullback(grad_normed)


def row_block(core, part, quad):
    quad_me = lax.axis_index(("y", "x"))
    block = jnp.bitwise_xor(quad_me, quad) * 2 + jnp.bitwise_xor(core, part)
    return pl.multiple_of(block * BLOCK_ROWS, BLOCK_ROWS)


def head_slices(ref, rows, width, head):
    low = head * HEAD_DIM
    return tuple(ref[rows, part * width + low : part * width + low + HEAD_DIM] for part in range(3))


def put_grads(work, outs):
    if len(outs) == 1:
        outs[0][...] = work[...]
        return
    core = lax.axis_index("c")
    for part, out in enumerate(outs):
        for quad in range(out.shape[0]):
            out[quad] = work[pl.ds(row_block(core, part, quad), out.shape[1]), :]


def attend_kernel(kind, stride, normed_ref, weight_ref, heads_ref, mixed_ref, out_ref, sums, total_ref):
    step = pl.program_id(0)
    count, width = mixed_ref.shape
    heads_ref[...] = mm(normed_ref[...], weight_ref[:, : 3 * width]).astype(BF16)
    sums[...] = jnp.zeros_like(sums)
    for start, size, group in windows(kind, count):
        bias = key_bias(start, size, group, stride)
        rows = pl.ds(start, size)
        for head in range(width // HEAD_DIM):
            low = head * HEAD_DIM
            query, key, value = head_slices(heads_ref, rows, width, head)
            scores = mm(key, query * HEAD_DIM**-0.5, NT) + bias
            weights = jnp.exp(scores - jnp.max(scores, 0, keepdims=True))
            total = jnp.sum(weights, 0, keepdims=True)
            blended = (mm(value.T, weights.astype(BF16)) / total).T
            if group is not None:
                blended = jnp.where(row_valid(start, size, group, HEAD_DIM), blended, 0.0)
            sums[rows, low : low + HEAD_DIM] += blended
    mixed_ref[...] = sums[...].astype(BF16)
    share = mm(mixed_ref[...], weight_ref[:, 3 * width :], NT)

    @pl.when(step == 0)
    def _():
        total_ref[...] = share

    @pl.when(step > 0)
    def _():
        total_ref[...] += share

    @pl.when(step == pl.num_programs(0) - 1)
    def _():
        out_ref[...] = total_ref[...].astype(out_ref.dtype)


def attend_back_kernel(
    kind, stride, normed_ref, weight_ref, heads_ref, mixed_ref, grad_ref, *rest
):
    outs, (out_ref, sums, total_ref, grad_mixed, grad_heads, work) = rest[:-6], rest[-6:]
    step = pl.program_id(0)
    count, width = mixed_ref.shape
    scale = HEAD_DIM**-0.5
    grad_mixed[...] = mm(grad_ref[...], weight_ref[:, 3 * width :]).astype(BF16)
    sums[...] = jnp.zeros_like(sums)
    for start, size, group in windows(kind, count):
        bias = key_bias(start, size, group, stride)
        rows = pl.ds(start, size)
        for head in range(width // HEAD_DIM):
            low = head * HEAD_DIM
            query, key, value = head_slices(heads_ref, rows, width, head)
            query = query * scale
            grad = grad_mixed[rows, low : low + HEAD_DIM]
            if group is not None:
                valid = row_valid(start, size, group, HEAD_DIM)
                grad = jnp.where(valid, grad.astype(F32), 0.0).astype(BF16)
            scores = mm(key, query, NT) + bias
            weights = jnp.exp(scores - jnp.max(scores, 0, keepdims=True))
            weights = weights / jnp.sum(weights, 0, keepdims=True)
            grad_weights = mm(value, grad, NT)
            row_terms = jnp.sum(weights * grad_weights, 0, keepdims=True)
            grad_scores = (weights * (grad_weights - row_terms)).astype(BF16)
            sums[rows, low : low + HEAD_DIM] += (mm(key.T, grad_scores) * scale).T
            low += width
            sums[rows, low : low + HEAD_DIM] += mm(grad_scores, query)
            low += width
            sums[rows, low : low + HEAD_DIM] += mm(weights.astype(BF16), grad)
    grad_heads[...] = sums[...].astype(BF16)
    share = mm(grad_heads[...], weight_ref[:, : 3 * width], NT)

    @pl.when(step == 0)
    def _():
        total_ref[...] = share

    @pl.when(step > 0)
    def _():
        total_ref[...] += share

    @pl.when(step == pl.num_programs(0) - 1)
    def _():
        out_ref[...] = total_ref[...].astype(out_ref.dtype)

    work[:, : 3 * width] = mm(normed_ref[...], grad_heads[...], TN).astype(BF16)
    work[:, 3 * width :] = mm(grad_ref[...], mixed_ref[...], TN).astype(BF16)
    put_grads(work, outs)


def up_kernel(normed_ref, weight_ref, hidden_ref, slope_ref):
    pre_act = mm(normed_ref[...], weight_ref[...])
    cdf = 0.5 * (1.0 + lax.erf(pre_act * 0.5**0.5))
    hidden_ref[...] = (pre_act * cdf).astype(BF16)
    density = jnp.exp(-0.5 * pre_act * pre_act) * (0.5 / math.pi) ** 0.5
    slope_ref[...] = (cdf + pre_act * density).astype(slope_ref.dtype)


def down_kernel(hidden_ref, weight_ref, out_ref):
    share = mm(hidden_ref[...], weight_ref[...], NT)

    @pl.when(pl.program_id(0) == 0)
    def _():
        out_ref[...] = share

    @pl.when(pl.program_id(0) > 0)
    def _():
        out_ref[...] += share


def down_back_kernel(grad_ref, weight_ref, hidden_ref, slope_ref, *rest):
    outs, (grad_pre_ref, work) = rest[:-2], rest[-2:]
    grad_hidden = mm(grad_ref[...], weight_ref[...])
    grad_pre_ref[...] = (grad_hidden * slope_ref[...].astype(F32)).astype(BF16)
    work[...] = mm(grad_ref[...], hidden_ref[...], TN).astype(BF16)
    put_grads(work, outs)


def up_back_kernel(normed_ref, weight_ref, grad_pre_ref, *rest):
    outs, (out_ref, work) = rest[:-2], rest[-2:]
    share = mm(grad_pre_ref[...], weight_ref[...], NT)

    @pl.when(pl.program_id(0) == 0)
    def _():
        out_ref[...] = share

    @pl.when(pl.program_id(0) > 0)
    def _():
        out_ref[...] += share

    work[...] = mm(normed_ref[...], grad_pre_ref[...], TN).astype(BF16)
    put_grads(work, outs)


def whole_spec(array):
    return pl.BlockSpec(array.shape, lambda i: (0,) * array.ndim)


def step_spec(array):
    rest = array.shape[1:]
    return pl.BlockSpec((None,) + rest, lambda i: (i,) + (0,) * len(rest))


def phase(kernel, name, inputs, outputs, scratch=(), cost=0):
    blocks = [a for a in inputs if a.ndim > 2][0].shape[0]
    spec = lambda a: whole_spec(a) if a.ndim == 2 else step_spec(a)
    return pl.pallas_call(
        kernel,
        grid=(blocks,),
        in_specs=[spec(a) for a in inputs],
        out_specs=[spec(a) for a in outputs],
        out_shape=outputs,
        scratch_shapes=list(scratch),
        cost_estimate=pl.CostEstimate(
            flops=int(cost * 800e6), bytes_accessed=int(cost * 1e6), transcendentals=0
        ),
        name=name,
    )(*inputs)


def shaped(*shape, dtype=BF16):
    return jax.ShapeDtypeStruct(shape, dtype)


def grad_shapes(weight, routed):
    blocks, depth, lanes = weight.shape
    if not routed:
        return [shaped(blocks, depth, lanes)]
    rows = BLOCK_ROWS
    return [shaped(blocks, depth // rows // 2, rows, lanes) for part in range(2)]


def attend(kind, normed, weight, stride, out_dtype):
    blocks, depth, lanes = weight.shape
    count, width = normed.shape[0], lanes // 4
    return phase(
        functools.partial(attend_kernel, kind, stride),
        kind + "_attend",
        (normed, weight),
        (
            shaped(blocks, count, 3 * width),
            shaped(blocks, count, width),
            shaped(count, depth, dtype=out_dtype),
        ),
        (pltpu.VMEM((count, width), F32), pltpu.VMEM((count, depth), F32)),
        cost=14,
    )


def attend_back(kind, normed, weight, heads, mixed, grad, stride, out_dtype, routed):
    blocks, depth, lanes = weight.shape
    count, width = normed.shape[0], lanes // 4
    *grads, out = phase(
        functools.partial(attend_back_kernel, kind, stride),
        kind + "_attend_back",
        (normed, weight, heads, mixed, grad),
        (*grad_shapes(weight, routed), shaped(count, depth, dtype=out_dtype)),
        (
            pltpu.VMEM((count, 3 * width), F32),
            pltpu.VMEM((count, depth), F32),
            pltpu.VMEM((count, width), BF16),
            pltpu.VMEM((count, 3 * width), BF16),
            pltpu.VMEM((depth, lanes), BF16),
        ),
        cost=20,
    )
    return grads, out


def along(piece, axes, distance):
    size = lax.axis_size(axes)
    return lax.ppermute(piece, axes, [(i, i ^ distance) for i in range(size)])


def after(piece, earlier):
    return piece + earlier[:1, :1] * 0


def gather_plain(shard):
    every = lax.all_gather(shard, TENSOR, axis=0, tiled=False)
    return lax.all_gather(every.reshape(-1, *shard.shape), DP, axis=1, tiled=True)


def reduce_plain(grads):
    part = lax.psum_scatter(grads[0], TENSOR, scatter_dimension=0, tiled=True)[0]
    return lax.psum_scatter(part, DP, scatter_dimension=0, tiled=True).astype(F32)


def by_member(parts, me):
    return jnp.stack(
        [
            lax.dynamic_index_in_dim(parts, jnp.bitwise_xor(me, k), 0, keepdims=False)
            for k in range(parts.shape[0])
        ]
    )


def to_patches(rows, members):
    share, columns = PATCHES // members, rows.shape[1]
    me = lax.axis_index(CLIP)
    parts = rows.reshape(-1, members, share, columns).transpose(1, 0, 2, 3)
    parts = [
        lax.dynamic_index_in_dim(parts, jnp.bitwise_xor(me, k), 0, keepdims=False)
        for k in range(members)
    ]
    parts = [parts[0]] + [along(parts[k], CLIP, k) for k in range(1, members)]
    return by_member(jnp.stack(parts), me).reshape(-1, columns)


def to_frames(rows, members):
    share, columns = PATCHES // members, rows.shape[1]
    me = lax.axis_index(CLIP)
    parts = by_member(rows.reshape(members, -1, share, columns), me)
    parts = [parts[0]] + [along(parts[k], CLIP, k) for k in range(1, members)]
    parts = jnp.stack(parts)
    order = jnp.bitwise_xor(me, jnp.arange(members))
    parts = [
        lax.dynamic_index_in_dim(parts, jnp.bitwise_xor(me, k), 0, keepdims=False)
        for k in range(members)
    ]
    return jnp.stack(parts, 1).reshape(-1, columns)


CHUNKS = 4
STEPS = 4
PAD = 56


def place():
    return {axis: lax.axis_index(axis) for axis in ALL}


def moved(here, **flips):
    return tuple(here[a] + flips.get(a, 0) * (1 - 2 * here[a]) for a in ALL)


def dp_row(here, y=0, x=0, c=0):
    to = lambda a, flip: here[a] + flip * (1 - 2 * here[a])
    return to("y", y) * 4 + to("x", x) * 2 + to("c", c)


def remote(source, target, sent, received, device):
    return pltpu.make_async_remote_copy(
        src_ref=source,
        dst_ref=target,
        send_sem=sent,
        recv_sem=received,
        device_id=device,
        device_id_type=pl.DeviceIdType.MESH,
    )


def peers(here):
    found = [moved(here, s=j // 2, h=j % 2) for j in range(1, 4)]
    found += [moved(here, y=r // 4, x=r // 2 % 2, c=r % 2) for r in range(1, 8)]
    return found + [moved(here, c=1, h=1)]


def greet(here, what):
    barrier = pltpu.get_barrier_semaphore()
    everyone = peers(here)
    if what == "answer":
        pl.semaphore_wait(barrier, len(everyone))
        return
    for device in everyone:
        pl.semaphore_signal(
            barrier, inc=1, device_id=device, device_id_type=pl.DeviceIdType.MESH
        )


class Exchange:
    def __init__(self, here, out, back, sent, received):
        self.here, self.out, self.back = here, out, back
        self.sent, self.received = sent, received
        self.me = here["c"] * 2 + here["h"]

    def device(self, member):
        return tuple({"c": member // 2, "h": member % 2}.get(a, self.here[a]) for a in ALL)

    def start(self, member):
        @pl.when(self.me != member)
        def _():
            remote(
                self.out.at[member],
                self.back.at[self.me],
                self.sent.at[member],
                self.received.at[self.me],
                self.device(member),
            ).start()

        @pl.when(self.me == member)
        def _():
            self.back[member] = self.out[member]

    def finish(self, member):
        @pl.when(self.me != member)
        def _():
            remote(
                self.out.at[member],
                self.back.at[member],
                self.sent.at[member],
                self.received.at[member],
                self.device(member),
            ).wait()

    def send(self, rows_ref, rows_of):
        share = PATCHES // 4
        for member in range(4):
            for frame in range(2):
                rows = rows_of(member, frame)
                self.out[member, frame, :share, :] = rows_ref[rows, :].astype(BF16)
            self.start(member)

    def take(self, rows_ref, rows_of):
        share = PATCHES // 4
        for member in range(4):
            self.finish(member)
            for frame in range(2):
                rows = rows_of(member, frame)
                rows_ref[rows, :] = self.back[member, frame, :share, :].astype(F32)

    @staticmethod
    def by_frame(member, frame):
        low = frame * PATCHES + member * (PATCHES // 4)
        return slice(low, low + PATCHES // 4)

    @staticmethod
    def by_share(member, frame):
        return pl.ds(member * 2 + frame, PATCHES // 4, stride=FRAMES)

    def parts(self, patch_ref):
        for block in range(patch_ref.shape[0]):
            yield block, slice(block * 128, (block + 1) * 128)

    def send_frames(self, rows_ref):
        self.send(rows_ref, self.by_frame)

    def take_patches(self, patch_ref, low_ref):
        share = PATCHES // 4
        for member in range(4):
            self.finish(member)
            for frame in range(2):
                for block, lanes in self.parts(patch_ref):
                    patch_ref[block, self.by_share(member, frame), :] = self.back[
                        member, frame, :share, lanes
                    ].astype(F32)
        for block, lanes in self.parts(patch_ref):
            low_ref[:, lanes] = patch_ref[block].astype(BF16)

    def send_patches(self, rows_ref, patch_ref):
        share = PATCHES // 4
        for block, lanes in self.parts(patch_ref):
            patch_ref[block] = rows_ref[:, lanes]
        for member in range(4):
            for frame in range(2):
                for block, lanes in self.parts(patch_ref):
                    self.out[member, frame, :share, lanes] = patch_ref[
                        block, self.by_share(member, frame), :
                    ].astype(BF16)
            self.start(member)

    def take_frames(self, rows_ref):
        self.take(rows_ref, self.by_frame)


def by_rows(count, body, size=56):
    def step(i, carry):
        body(pl.ds(pl.multiple_of(i * size, size), size))
        return carry

    lax.fori_loop(0, count // size, step, 0)


def row_stats(rows):
    average = jnp.mean(rows, -1, keepdims=True)
    centred = rows - average
    spread = jnp.mean(centred * centred, -1, keepdims=True)
    return centred, lax.rsqrt(spread + EPSILON)


def attention_units(kind, count, width):
    found = []
    if kind == "time":
        tile = 96
        starts = list(range(0, count - tile, tile))
        ends = starts[1:] + [count]
    else:
        starts = [low for low, size, group in windows(kind, count)]
        ends = [low + size for low, size, group in windows(kind, count)]
    for index, (start, end) in enumerate(zip(starts, ends)):
        size = end - start
        keys = row_ids((size, size), 0, 0)
        first, final = 0, size
        if kind == "time":
            together = keys // FRAMES == row_ids((size, size), 1, 0) // FRAMES
        else:
            first = index * PATCHES - start
            final = first + PATCHES
            together = (keys >= first) & (keys < final)
        bias = jnp.where(together, 0.0, -1e30)
        found += [(start, size, first, final, bias, head) for head in range(width // HEAD_DIM)]
    return found


def attend_block(kind, t, normed, weight, heads_ref, mixed_ref, sums):
    count, width = mixed_ref.shape[1:]
    heads_ref[t] = mm(normed, weight[:, : 3 * width]).astype(BF16)
    heads = heads_ref.at[t]
    target = mixed_ref.at[t] if kind == "time" else sums
    units = attention_units(kind, count, width)
    for batch in range(0, len(units), 6):
        some = units[batch : batch + 6]
        parts = [head_slices(heads, pl.ds(u[0], u[1]), width, u[5]) for u in some]
        scores = [
            mm(key, query * HEAD_DIM**-0.5, NT) + u[4] for u, (query, key, value) in zip(some, parts)
        ]
        weights = [jnp.exp(x - jnp.max(x, 0, keepdims=True)) for x in scores]
        scales = [1.0 / jnp.sum(x, 0, keepdims=True) for x in weights]
        blended = [
            (mm(value.T, x.astype(BF16)) * scale).T
            for x, scale, (query, key, value) in zip(weights, scales, parts)
        ]
        for (start, size, first, final, bias, head), x in zip(some, blended):
            lanes = slice(head * HEAD_DIM, (head + 1) * HEAD_DIM)
            target[start + first : start + final, lanes] = x[first:final].astype(target.dtype)
    if kind != "time":
        mixed_ref[t] = sums[...].astype(BF16)
    return mm(mixed_ref[t], weight[:, 3 * width :], NT)


def attend_back_block(kind, heads, mixed, grad, weight, grad_mixed, sums, grad_heads):
    count, width = mixed.shape
    scale = HEAD_DIM**-0.5
    grad_mixed[...] = mm(grad[...], weight[:, 3 * width :]).astype(BF16)
    target = grad_heads if kind == "time" else sums
    units = attention_units(kind, count, width)
    batch_size = 12 if kind == "time" else 3
    for batch in range(0, len(units), batch_size):
        some = units[batch : batch + batch_size]
        parts = []
        for start, size, first, final, bias, head in some:
            rows = pl.ds(start, size)
            query, key, value = head_slices(heads, rows, width, head)
            grad_here = grad_mixed[rows, head * HEAD_DIM : (head + 1) * HEAD_DIM]
            if kind != "time":
                ids = row_ids((size, HEAD_DIM), 0, 0)
                valid = (ids >= first) & (ids < final)
                grad_here = jnp.where(valid, grad_here.astype(F32), 0.0).astype(BF16)
            parts.append((query * scale, key, value, grad_here))
        scores = [mm(p[1], p[0], NT) + u[4] for u, p in zip(some, parts)]
        grad_weights = [mm(p[2], p[3], NT) for p in parts]
        weights = [jnp.exp(x - jnp.max(x, 0, keepdims=True)) for x in scores]
        weights = [x * (1.0 / jnp.sum(x, 0, keepdims=True)) for x in weights]
        grad_values = [mm(x.astype(BF16), p[3]) for x, p in zip(weights, parts)]
        grad_scores = [
            (x * (y - jnp.sum(x * y, 0, keepdims=True))).astype(BF16)
            for x, y in zip(weights, grad_weights)
        ]
        grad_keys = [mm(x, p[0]) for x, p in zip(grad_scores, parts)]
        grad_queries = [(mm(p[1].T, x) * scale).T for x, p in zip(grad_scores, parts)]
        for u, *grads in zip(some, grad_queries, grad_keys, grad_values):
            start, size, first, final, bias, head = u
            for c, x in enumerate(grads):
                low = c * width + head * HEAD_DIM
                target[start + first : start + final, low : low + HEAD_DIM] = x[
                    first:final
                ].astype(target.dtype)
    if kind != "time":
        grad_heads[...] = sums[...].astype(BF16)
    return mm(grad_heads[...], weight[:, : 3 * width], NT)


EVENT_NAMES = ("zs", "line", "relay", "across", "core", "first", "second", "third")
BLOCK_ORDER = (1, 2, 3, 0)
ORDER = (
    ("go",),
    ("line", 0, 0), ("zs", 0, 1), ("line", 3, 0), ("zs", 0, 3), ("line", 1, 0), ("zs", 0, 2),
    ("zs", 2, 3), ("ln0",), ("mask",), ("zs", 1, 2), ("line", 2, 0), ("line", 0, 3),
    ("line", 0, 2), ("zs", 1, 1), ("line", 0, 1), ("relay", 0, 2), ("line", 2, 3), ("zs", 1, 3),
    ("relay", 0, 1), ("relay", 0, 3), ("relay", 0, 0), ("across", 0, 1), ("line", 1, 2),
    ("line", 1, 1), ("across", 0, 2), ("zs", 2, 2), ("across", 0, 3), ("across", 0, 0),
    ("relay", 1, 0), ("takeE0",), ("line", 1, 3), ("relay", 2, 0), ("zs", 2, 1), ("zs", 3, 1),
    ("P0", 0), ("relay", 1, 2), ("relay", 2, 3), ("P0", 1), ("P0", 2), ("P0", 3), ("exch1",),
    ("relay", 1, 1), ("across", 1, 2), ("relay", 1, 3), ("line", 2, 2), ("across", 1, 1),
    ("line", 2, 1), ("zs", 3, 2), ("across", 1, 3), ("across", 1, 0), ("line", 3, 1),
    ("across", 2, 0), ("ln1",), ("P1", 0), ("relay", 2, 1), ("zs", 3, 3), ("relay", 2, 2),
    ("P1", 1), ("across", 2, 3), ("line", 3, 2), ("P1", 2), ("P1", 3), ("line", 3, 3),
    ("across", 2, 2), ("across", 2, 1), ("ln2",), ("relay", 3, 0), ("relay", 3, 1),
    ("relay", 3, 2), ("up", 0), ("relay", 3, 3), ("up", 1), ("core", 0), ("across", 3, 2),
    ("across", 3, 0), ("up", 2), ("core", 1), ("across", 3, 3), ("across", 3, 1), ("up", 3),
    ("core", 2), ("dn", 0), ("dn", 1), ("first", 0), ("dn", 2), ("core", 3), ("dn", 3), ("B1", 0),
    ("first", 1), ("first", 2), ("B1", 1), ("second", 0), ("first", 3), ("core", 4), ("B1", 2),
    ("core", 5), ("B1", 3), ("nb2",), ("second", 1), ("core", 6), ("B2", 0), ("second", 2),
    ("first", 4), ("first", 5), ("core", 7), ("B2", 1), ("core", 8), ("first", 6), ("second", 4),
    ("B2", 2), ("second", 5), ("core", 9), ("B2", 3), ("nb1",), ("core", 10), ("second", 3),
    ("first", 8), ("first", 9), ("third", 0), ("core", 11), ("second", 6), ("first", 10),
    ("first", 7), ("second", 8), ("takeE2",), ("B3", 0), ("second", 9), ("B3", 1), ("first", 11),
    ("core", 12), ("second", 10), ("B3", 2), ("core", 13), ("B3", 3), ("exch3",), ("first", 12),
    ("core", 14), ("second", 11), ("second", 12), ("first", 13), ("first", 14), ("core", 15),
    ("second", 13), ("third", 2), ("nb0",), ("second", 14), ("second", 7), ("first", 15),
    ("gain",), ("second", 15), ("third", 1), ("third", 3),
)


def after_each(order):
    found, events = {}, []
    for item in order:
        if item[0] in EVENT_NAMES:
            events.append(item)
        else:
            events = found.setdefault(item, [])
    return found


AFTER = after_each(ORDER)


def layer_kernel(
    live_ref,
    tokens_hbm,
    cotangent_hbm,
    gain_hbm,
    qkv_time_hbm,
    out_time_hbm,
    qkv_space_hbm,
    out_space_hbm,
    up_hbm,
    down_hbm,
    weight_ref,
    out_ref,
    stream_ref,
    own_ref,
    own_gain_ref,
    tokens_ref,
    gain_ref,
    qkv_time_ref,
    out_time_ref,
    qkv_space_ref,
    out_space_ref,
    shard_ref,
    held,
    normed_time_ref,
    time_heads_ref,
    time_mixed_ref,
    after_time_ref,
    normed_space_ref,
    space_heads_ref,
    space_mixed_ref,
    after_space_ref,
    normed_mlp_ref,
    hidden_ref,
    slope_ref,
    low_ref,
    rows_ref,
    patch_ref,
    total_ref,
    mixed_sums,
    sums,
    grad_mixed,
    grad_heads,
    work,
    keep,
    came,
    first,
    second,
    third,
    gains_ref,
    gain_sums,
    gain_line,
    gain_out,
    gain_parts,
    swap_out,
    swap_back,
    piece_sent,
    piece_here,
    core_sent,
    core_here,
    first_sent,
    first_here,
    second_sent,
    second_here,
    third_sent,
    third_here,
    gain_sent,
    gain_here,
    swap_sent,
    swap_here,
    held_sem,
    own_sem,
    load_sem,
    credit,
):
    here = place()
    count, columns = tokens_ref.shape
    width = time_mixed_ref.shape[2]
    own_row = dp_row(here)
    last = CHUNKS * STEPS - 1
    live = jnp.where(here["s"] < live_ref[0], 1.0, 0.0).astype(F32)

    loads = [
        pltpu.make_async_copy(source, target, load_sem.at[i])
        for i, (source, target) in enumerate(
            (
                (gain_hbm, gain_ref),
                (qkv_time_hbm, qkv_time_ref),
                (out_time_hbm, out_time_ref),
                (qkv_space_hbm, qkv_space_ref),
                (out_space_hbm, out_space_ref),
                (up_hbm, shard_ref.at[2]),
                (down_hbm, shard_ref.at[3]),
                (tokens_hbm, tokens_ref),
                (cotangent_hbm, stream_ref),
            )
        )
    ]
    greet(here, "call")
    for load in loads:
        load.start()
    for load in loads[:5]:
        load.wait()

    for k, qkv, out in ((0, qkv_time_ref, out_time_ref), (1, qkv_space_ref, out_space_ref)):
        for c in range(3):
            shard_ref[k, :, c * width : (c + 1) * width] = qkv[c]
        shard_ref[k, :, 3 * width :] = out[...].astype(F32).T.astype(BF16)
    own_gains = gain_ref.shape[1]
    gain_out[0, : gain_ref.shape[0], :own_gains] = gain_ref[...].astype(F32)
    for load in loads[5:7]:
        load.wait()
    greet(here, "answer")

    def row_of(part, r):
        return dp_row(here, y=r // 2, x=r % 2, c=part)

    def slot_of(k, j, row):
        return weight_ref.at[k, j, pl.ds(pl.multiple_of(row * BLOCK_ROWS, BLOCK_ROWS), BLOCK_ROWS)]

    def arrived(k, part, r, j):
        slot = slot_of(k, j, row_of(part, r))
        remote(
            slot, slot, piece_sent.at[k, 0, 0], piece_here.at[k, part, r, j], moved(here, c=1)
        ).wait_recv()

    def send(source, k, j, r, sem, part, r_there, **flips):
        remote(
            source,
            slot_of(k, j, row_of(0, r)),
            piece_sent.at[k, sem, j],
            piece_here.at[k, part, r_there, j],
            moved(here, **flips),
        ).start()

    def piece(k, j, r):
        return slot_of(k, j, row_of(0, r))

    def along_line(k, j):
        remote(
            shard_ref.at[k],
            slot_of(k, j, own_row),
            piece_sent.at[k, 0, j],
            piece_here.at[k, 0, 0, j],
            moved(here, s=j // 2, h=j % 2),
        ).start()

    def spread(source, k, j):
        send(source, k, j, 0, 1, 0, 1, x=1)
        send(source, k, j, 0, 2, 0, 2, y=1)
        send(source, k, j, 0, 4, 1, 0, c=1)

    def line(k, j):
        if j:
            arrived(k, 0, 0, j)
        spread(piece(k, j, 0) if j else shard_ref.at[k], k, j)

    def relay(k, j):
        up = j // 2
        arrived(k, 0, 1, j)
        send(piece(k, j, 1), k, j, 1, 5, 1, 1, c=1)
        arrived(k, 0, 2, j)
        send(piece(k, j, 2), k, j, 2, 6, 1, 2, c=1)
        source = slot_of(k, j, dp_row(here, y=up, x=1 - up))
        remote(
            source,
            source,
            piece_sent.at[k, 3, j],
            piece_here.at[k, 0, 3, j],
            moved(here, y=1 - up, x=up),
        ).start()

    def across(k, j):
        arrived(k, 0, 3, j)
        send(piece(k, j, 3), k, j, 3, 7, 1, 3, c=1)

    def fetch(k, t):
        return pltpu.make_async_copy(weight_ref.at[k, t], held.at[t], held_sem.at[t])

    def ready(k):
        for j in range(STEPS):
            for r in range(4):
                arrived(k, 1, r, j)
        for t in BLOCK_ORDER:
            fetch(k, t).start()

    def weight(k, t):
        fetch(k, t).wait()
        return held.at[t]

    def stored(k):
        return pltpu.make_async_copy(shard_ref.at[k], slot_of(k, 0, own_row), own_sem.at[k])

    half_lanes = keep.shape[4]
    swapped = (0, 2, 1, 3)

    def grad_rows(part, quad):
        row = dp_row(here, y=quad // 2, x=quad % 2, c=part)
        return pl.ds(pl.multiple_of(row * BLOCK_ROWS, BLOCK_ROWS), BLOCK_ROWS)

    def core_copy(step, quad):
        return remote(
            work.at[step % 2, grad_rows(1, quad)],
            came.at[step % 4, quad],
            core_sent.at[step % 2, quad],
            core_here.at[step % 4, quad],
            moved(here, c=1),
        )

    def first_copy(step, half):
        return remote(
            keep.at[step, pl.ds(2, 2), half],
            first.at[step, half],
            first_sent.at[step, half],
            first_here.at[step, half],
            moved(here, y=1 - half, x=half),
        )

    def second_copy(step, half):
        return remote(
            keep.at[step, 1, half],
            second.at[step, half],
            second_sent.at[step, half],
            second_here.at[step, half],
            moved(here, y=half, x=1 - half),
        )

    def third_copy(step):
        j = BLOCK_ORDER[step % STEPS]
        return remote(
            keep.at[step, 0],
            third.at[step],
            third_sent.at[step],
            third_here.at[step],
            moved(here, s=j // 2, h=j % 2),
        )

    def begin(step):
        @pl.when(step >= 2)
        def _():
            for quad in range(4):
                core_copy(step - 2, quad).wait_send()

        return work.at[step % 2]

    def emit(step):
        @pl.when(step >= 4)
        def _():
            pl.semaphore_wait(credit, 1)

        for quad in range(4):
            core_copy(step, quad).start()

    def take_core(step):
        for quad in range(4):
            core_copy(step, quad).wait_recv()
        for index in (2, 3, 1, 0):
            for half in range(2):
                quad = swapped[index] if half else index
                lanes = slice(half * half_lanes, (half + 1) * half_lanes)
                own = work[step % 2, grad_rows(0, quad), lanes].astype(F32)
                both = own + came[step % 4, quad, :, lanes].astype(F32)
                keep[step, index, half] = both.astype(BF16)
                if index == 3:
                    first_copy(step, half).start()
        if step <= last - 4:
            pl.semaphore_signal(
                credit,
                inc=1,
                device_id=moved(here, c=1),
                device_id_type=pl.DeviceIdType.MESH,
            )

    def take_first(step):
        for half in range(2):
            first_copy(step, half).wait_recv()
            for index in (1, 0):
                both = keep[step, index, half].astype(F32) + first[step, half, index].astype(F32)
                keep[step, index, half] = both.astype(BF16)
                if index:
                    second_copy(step, half).start()

    def take_second(step):
        for half in range(2):
            second_copy(step, half).wait_recv()
            both = keep[step, 0, half].astype(F32) + second[step, half].astype(F32)
            keep[step, 0, half] = both.astype(BF16)
        if BLOCK_ORDER[step % STEPS]:
            third_copy(step).start()

    def take_third(index):
        steps = [index * STEPS + i for i in range(STEPS)]
        for step in steps:
            if BLOCK_ORDER[step % STEPS]:
                third_copy(step).wait_recv()
        for half in range(2):
            total = jnp.zeros((BLOCK_ROWS, half_lanes), F32)
            for step in steps:
                source = third[step, half] if BLOCK_ORDER[step % STEPS] else keep[step, 0, half]
                total = total + source.astype(F32)
            own_ref[index, :, half * half_lanes : (half + 1) * half_lanes] = total

    events = {
        "zs": along_line,
        "line": line,
        "relay": relay,
        "across": across,
        "core": take_core,
        "first": take_first,
        "second": take_second,
        "third": take_third,
    }

    def follow(item):
        for name, *args in AFTER.get(item, ()):
            events[name](*args)

    def loop(name, body):
        def step(i, carry):
            body(i, (i + 1) % STEPS)
            for c in range(STEPS - 1):
                if AFTER.get((name, c)):

                    @pl.when(i == c)
                    def _(c=c):
                        follow((name, c))

            return carry

        lax.fori_loop(0, STEPS, step, 0)
        follow((name, STEPS - 1))

    def layer_norm(source_ref, gain, target_ref):
        def body(rows):
            centred, scale = row_stats(source_ref[rows, :])
            target_ref[rows, :] = (centred * scale * gains_ref[gain : gain + 1, :]).astype(
                target_ref.dtype
            )

        by_rows(count, body)

    def norm_back(source_ref, gain, grad_normed_ref):
        def body(rows):
            centred, scale = row_stats(source_ref[rows, :])
            unit = centred * scale
            grad_normed = grad_normed_ref[rows, :]
            e = grad_normed * gains_ref[gain : gain + 1, :]
            mean = jnp.mean(e, -1, keepdims=True)
            tilt = jnp.mean(e * unit, -1, keepdims=True)
            stream_ref[rows, :] += scale * (e - mean - unit * tilt)
            gain_sums[gain : gain + 1, :] += jnp.sum(grad_normed * unit, 0, keepdims=True)

        by_rows(count, body)

    def exchange(index):
        return Exchange(
            here,
            swap_out.at[index % 2],
            swap_back.at[index % 2],
            swap_sent.at[index],
            swap_here.at[index],
        )

    def attention(kind, k, normed_ref, heads_ref, mixed_ref):
        total_ref[...] = jnp.zeros_like(total_ref)

        def compute(i, t):
            total_ref[...] += attend_block(
                kind, t, normed_ref[...], weight(k, t), heads_ref, mixed_ref, mixed_sums
            )

        return compute

    def attention_back(kind, k, normed_ref, heads_ref, mixed_ref):
        total_ref[...] = jnp.zeros_like(total_ref)

        def compute(i, t):
            step = (CHUNKS - 1 - k) * STEPS + i
            out = begin(step)
            total_ref[...] += attend_back_block(
                kind,
                heads_ref.at[t],
                mixed_ref.at[t],
                low_ref,
                weight(k, t),
                grad_mixed,
                sums,
                grad_heads,
            )
            if k:
                fetch(k - 1, t).start()
            out[:, : 3 * width] = mm(normed_ref[...], grad_heads[...], TN).astype(BF16)
            out[:, 3 * width :] = mm(low_ref[...], mixed_ref[t], TN).astype(BF16)
            emit(step)

        return compute

    gain_parts[0, own_row] = gain_out[0]

    def gain_copy(r):
        flips = {"y": r // 4, "x": r // 2 % 2, "c": r % 2}
        return remote(
            gain_out.at[0],
            gain_parts.at[0, own_row],
            gain_sent.at[0, r],
            gain_here.at[0, r],
            moved(here, **flips),
        )

    for r in range(1, 8):
        gain_copy(r).start()
    for k in range(CHUNKS):
        stored(k).start()
    follow(("go",))
    loads[7].wait()

    def unit_rows(rows):
        centred, scale = row_stats(tokens_ref[rows, :])
        rows_ref[rows, :] = centred * scale

    by_rows(count, unit_rows)
    for r in range(1, 8):
        gain_copy(r).wait()
    for d in range(8):
        gains_ref[:, d * own_gains : (d + 1) * own_gains] = gain_parts[0, d, :, :own_gains]

    def scale_rows(rows):
        rows_ref[rows, :] = rows_ref[rows, :] * gains_ref[0:1, :]

    by_rows(count, scale_rows)
    swap = exchange(0)
    swap.send_frames(rows_ref)
    follow(("ln0",))
    loads[8].wait()

    def mask_rows(rows):
        stream_ref[rows, :] = stream_ref[rows, :] * live
        low_ref[rows, :] = stream_ref[rows, :].astype(BF16)

    by_rows(count, mask_rows)
    gain_sums[...] = jnp.zeros_like(gain_sums)
    follow(("mask",))
    swap.take_patches(patch_ref, normed_time_ref)
    for k in range(CHUNKS):
        stored(k).wait()
    follow(("takeE0",))

    ready(0)
    loop("P0", attention("time", 0, normed_time_ref, time_heads_ref, time_mixed_ref))
    swap = exchange(1)
    swap.send_patches(total_ref, patch_ref)
    follow(("exch1",))
    swap.take_frames(rows_ref)
    after_time_ref[...] = tokens_ref[...] + rows_ref[...]
    layer_norm(after_time_ref, 1, normed_space_ref)
    follow(("ln1",))

    ready(1)
    loop("P1", attention("space", 1, normed_space_ref, space_heads_ref, space_mixed_ref))
    after_space_ref[...] = after_time_ref[...] + total_ref[...]
    layer_norm(after_space_ref, 2, normed_mlp_ref)
    follow(("ln2",))

    ready(2)

    def up(i, t):
        out = begin(i)
        pre_act = mm(normed_mlp_ref[...], weight(2, t)[...])
        cdf = 0.5 * (1.0 + lax.erf(pre_act * 0.5**0.5))
        hidden_ref[t] = (pre_act * cdf).astype(BF16)
        density = jnp.exp(-0.5 * pre_act * pre_act) * (0.5 / math.pi) ** 0.5
        slope_ref[t] = (cdf + pre_act * density).astype(BF16)
        out[...] = mm(low_ref[...], hidden_ref[t], TN).astype(BF16)
        emit(i)

    loop("up", up)
    ready(3)
    out_ref[...] = after_space_ref[...]

    def down(i, t):
        out_ref[...] += mm(hidden_ref[t], weight(3, t)[...], NT)
        grad_hidden = mm(low_ref[...], held[t])
        slope_ref[t] = (grad_hidden * slope_ref[t].astype(F32)).astype(BF16)
        fetch(2, t).start()

    loop("dn", down)
    out_ref[...] = out_ref[...] * live
    total_ref[...] = jnp.zeros_like(total_ref)

    def up_back(i, t):
        step = STEPS + i
        out = begin(step)
        total_ref[...] += mm(slope_ref[t], weight(2, t)[...], NT)
        fetch(1, t).start()
        out[...] = mm(normed_mlp_ref[...], slope_ref[t], TN).astype(BF16)
        emit(step)

    loop("B1", up_back)
    norm_back(after_space_ref, 2, total_ref)
    low_ref[...] = stream_ref[...].astype(BF16)
    follow(("nb2",))
    loop("B2", attention_back("space", 1, normed_space_ref, space_heads_ref, space_mixed_ref))
    norm_back(after_time_ref, 1, total_ref)
    swap = exchange(2)
    swap.send_frames(stream_ref)
    follow(("nb1",))
    swap.take_patches(patch_ref, low_ref)
    follow(("takeE2",))
    loop("B3", attention_back("time", 0, normed_time_ref, time_heads_ref, time_mixed_ref))
    swap = exchange(3)
    swap.send_patches(total_ref, patch_ref)
    follow(("exch3",))
    swap.take_frames(rows_ref)
    norm_back(tokens_ref, 0, rows_ref)

    line_index = here["s"] * 2 + here["h"]

    def gain_line_copy(j):
        return remote(
            gain_sums,
            gain_line.at[line_index],
            gain_sent.at[1, j],
            gain_here.at[1, j],
            moved(here, s=j // 2, h=j % 2),
        )

    def gain_back(r):
        flips = {"y": r // 4, "x": r // 2 % 2, "c": r % 2}
        return remote(
            gain_out.at[dp_row(here, **flips)],
            gain_parts.at[1, own_row],
            gain_sent.at[2, r],
            gain_here.at[2, r],
            moved(here, **flips),
        )

    for j in range(1, 4):
        gain_line_copy(j).start()
    gain_line[line_index] = gain_sums[...]
    follow(("nb0",))
    for j in range(1, 4):
        gain_line_copy(j).wait()
    total = gain_line[0] + gain_line[1] + gain_line[2] + gain_line[3]
    for d in range(8):
        gain_out[d, :, :own_gains] = total[:, d * own_gains : (d + 1) * own_gains]
    for r in range(1, 8):
        gain_back(r).start()
    gain_parts[1, own_row] = gain_out[own_row]
    follow(("gain",))
    for r in range(1, 8):
        gain_back(r).wait()
    total = gain_parts[1, 0]
    for d in range(1, 8):
        total = total + gain_parts[1, d]
    own_gain_ref[...] = total

    for k in range(CHUNKS):
        for sem in range(8):
            for j in range(4):
                if sem or j:
                    slot = slot_of(k, 0, own_row)
                    remote(
                        slot,
                        slot,
                        piece_sent.at[k, sem, j],
                        piece_here.at[k, 0, 0, 0],
                        moved(here, c=1),
                    ).wait_send()
    for step in range(last + 1):
        if step > last - 2:
            for quad in range(4):
                core_copy(step, quad).wait_send()
        for half in range(2):
            first_copy(step, half).wait_send()
            second_copy(step, half).wait_send()
        if BLOCK_ORDER[step % STEPS]:
            third_copy(step).wait_send()


def layer(live_clips, tokens, cotangent, norm_gains, *weights):
    count, columns = tokens.shape
    rows, lanes = weights[4].shape
    half = lanes // 2
    width, steps = lanes // 4, CHUNKS * STEPS
    here = pl.BlockSpec(memory_space=pltpu.VMEM)
    there = pl.BlockSpec(memory_space=pl.ANY)
    outputs = (
        shaped(CHUNKS, STEPS, columns, lanes),
        shaped(count, columns, dtype=F32),
        shaped(count, columns, dtype=F32),
        shaped(CHUNKS, rows, lanes, dtype=F32),
        shaped(8, 128, dtype=F32),
    )
    return pl.pallas_call(
        layer_kernel,
        in_specs=[pl.BlockSpec(memory_space=pltpu.SMEM)] + [there] * 9,
        out_specs=[there] + [here] * (len(outputs) - 1),
        out_shape=outputs,
        scratch_shapes=[
            pltpu.VMEM((count, columns), F32),
            pltpu.VMEM(norm_gains.shape, BF16),
            *[pltpu.VMEM(w.shape, BF16) for w in weights[:4]],
            pltpu.VMEM((CHUNKS, rows, lanes), BF16),
            pltpu.VMEM((STEPS, columns, lanes), BF16),
            pltpu.VMEM((count, columns), BF16),
            pltpu.VMEM((STEPS, count, 3 * width), BF16),
            pltpu.VMEM((STEPS, count, width), BF16),
            pltpu.VMEM((count, columns), F32),
            pltpu.VMEM((count, columns), BF16),
            pltpu.VMEM((STEPS, count, 3 * width), BF16),
            pltpu.VMEM((STEPS, count, width), BF16),
            pltpu.VMEM((count, columns), F32),
            pltpu.VMEM((count, columns), BF16),
            pltpu.VMEM((STEPS, count, lanes), BF16),
            pltpu.VMEM((STEPS, count, lanes), BF16),
            pltpu.VMEM((count, columns), BF16),
            pltpu.VMEM((count, columns), F32),
            pltpu.VMEM((columns // 128, count, 128), F32),
            pltpu.VMEM((count, columns), F32),
            pltpu.VMEM((count, width), F32),
            pltpu.VMEM((count, 3 * width), F32),
            pltpu.VMEM((count, width), BF16),
            pltpu.VMEM((count, 3 * width), BF16),
            pltpu.VMEM((2, columns, lanes), BF16),
            pltpu.VMEM((steps, 4, 2, rows, half), BF16),
            pltpu.VMEM((4, 4, rows, lanes), BF16),
            pltpu.VMEM((steps, 2, 2, rows, half), BF16),
            pltpu.VMEM((steps, 2, rows, half), BF16),
            pltpu.VMEM((steps, 2, rows, half), BF16),
            pltpu.VMEM((8, columns), F32),
            pltpu.VMEM((8, columns), F32),
            pltpu.VMEM((4, 8, columns), F32),
            pltpu.VMEM((8, 8, 128), F32),
            pltpu.VMEM((2, 8, 8, 128), F32),
            pltpu.VMEM((2, 4, 2, PAD, columns), BF16),
            pltpu.VMEM((2, 4, 2, PAD, columns), BF16),
            pltpu.SemaphoreType.DMA((CHUNKS, 8, 4)),
            pltpu.SemaphoreType.DMA((CHUNKS, 2, 4, 4)),
            pltpu.SemaphoreType.DMA((2, 4)),
            pltpu.SemaphoreType.DMA((4, 4)),
            pltpu.SemaphoreType.DMA((steps, 2)),
            pltpu.SemaphoreType.DMA((steps, 2)),
            pltpu.SemaphoreType.DMA((steps, 2)),
            pltpu.SemaphoreType.DMA((steps, 2)),
            pltpu.SemaphoreType.DMA((steps,)),
            pltpu.SemaphoreType.DMA((steps,)),
            pltpu.SemaphoreType.DMA((3, 8)),
            pltpu.SemaphoreType.DMA((3, 8)),
            pltpu.SemaphoreType.DMA((4, 4)),
            pltpu.SemaphoreType.DMA((4, 4)),
            pltpu.SemaphoreType.DMA((STEPS,)),
            pltpu.SemaphoreType.DMA((CHUNKS,)),
            pltpu.SemaphoreType.DMA((9,)),
            pltpu.SemaphoreType.REGULAR,
        ],
        compiler_params=pltpu.CompilerParams(
            collective_id=0, has_side_effects=True, vmem_limit_bytes=67043328
        ),
        name="layer",
    )(live_clips, tokens, cotangent, norm_gains, *weights)[1:]


def finish_kernel(output_ref, grad_ref, own_ref, gain_ref, *outs):
    out_ref, stream_ref, gains, time_in, time_out, space_in, space_out, up, down = outs
    width = time_in.shape[2]
    out_ref[...] = output_ref[...]
    stream_ref[...] = grad_ref[...]
    gains[...] = gain_ref[: gains.shape[0], : gains.shape[1]]
    for k, into, out in ((3, time_in, time_out), (2, space_in, space_out)):
        for c in range(3):
            into[c] = own_ref[k, :, c * width : (c + 1) * width]
        out[...] = own_ref[k, :, 3 * width :].T
    up[...] = own_ref[1]
    down[...] = own_ref[0]


def finish(output, grad, own, gain, like):
    shapes = [jax.ShapeDtypeStruct(a.shape, F32) for a in like]
    here = pl.BlockSpec(memory_space=pltpu.VMEM)
    return pl.pallas_call(
        finish_kernel,
        in_specs=[here] * 4,
        out_specs=[here] * len(shapes),
        out_shape=shapes,
        name="finish",
    )(output, grad, own, gain)


def sum_gains(total, own):
    for axes in ("c", "x", "y", TENSOR):
        bit = 1
        while bit < lax.axis_size(axes):
            total = total + along(total, axes, bit)
            bit *= 2
    return lax.dynamic_slice_in_dim(total, lax.axis_index(DP) * own, own, 1)


def on_device(
    routed,
    tokens,
    live_clips,
    norm_gains,
    qkv_time,
    out_time,
    qkv_space,
    out_space,
    up_weight,
    down_weight,
    cotangent,
):
    members = lax.axis_size("c") * lax.axis_size("h")
    share = PATCHES // members
    count, columns = tokens.shape
    width = qkv_time.shape[2]
    live = jnp.where(lax.axis_index("s") < live_clips[0], 1.0, 0.0).astype(F32)

    def pack_heads(qkv, out):
        rows = qkv.shape[1]
        return jnp.concatenate([qkv.transpose(1, 0, 2).reshape(rows, -1), out.T], 1)

    if routed:
        weights = (qkv_time, out_time, qkv_space, out_space, up_weight, down_weight.T)
        done = layer(live_clips, tokens, cotangent, norm_gains, *weights)
        *found, down_own = finish(*done, (tokens, cotangent, norm_gains, *weights))
        return (*found, down_own.T)
    shards = [
        pack_heads(qkv_time, out_time),
        pack_heads(qkv_space, out_space),
        up_weight,
        down_weight.T,
    ]
    grad_stream = cotangent * live
    time_all, space_all, up_all, down_all = [gather_plain(shard) for shard in shards]
    blocks, depth, lanes = up_all.shape
    gains = lax.all_gather(norm_gains, DP, axis=1, tiled=True).astype(F32)
    normed_time = to_patches(normalize(tokens, gains[0]).astype(BF16), members)
    time_heads, time_mixed, change = attend("time", normed_time, time_all, share, BF16)
    after_time = tokens + to_frames(change, members).astype(F32)
    normed_space = normalize(after_time, gains[1]).astype(BF16)
    space_heads, space_mixed, change = attend("space", normed_space, space_all, 1, F32)
    after_space = after_time + change
    normed_mlp = normalize(after_space, gains[2]).astype(BF16)
    hidden, slope = phase(
        up_kernel,
        "up",
        (normed_mlp, up_all),
        (shaped(blocks, count, lanes), shaped(blocks, count, lanes)),
        cost=12,
    )
    (change,) = phase(
        down_kernel, "down", (hidden, down_all), (shaped(count, depth, dtype=F32),), cost=4
    )
    after_mlp = after_space + change
    grad_low = grad_stream.astype(BF16)
    work = (pltpu.VMEM((depth, lanes), BF16),)
    *down_grads, grad_pre = phase(
        down_back_kernel,
        "down_back",
        (grad_low, down_all, hidden, slope),
        (*grad_shapes(down_all, False), shaped(blocks, count, lanes)),
        work,
        cost=8,
    )
    *up_grads, grad_normed = phase(
        up_back_kernel,
        "up_back",
        (normed_mlp, up_all, grad_pre),
        (*grad_shapes(up_all, False), shaped(count, depth, dtype=F32)),
        work,
        cost=8,
    )
    grad_part, gain_mlp = norm_back(after_space, gains[2], grad_normed)
    grad_stream = grad_stream + grad_part
    space_grads, grad_normed = attend_back(
        "space",
        normed_space,
        space_all,
        space_heads,
        space_mixed,
        grad_stream.astype(BF16),
        1,
        F32,
        False,
    )
    grad_part, gain_space = norm_back(after_time, gains[1], grad_normed)
    grad_stream = grad_stream + grad_part
    grad_low = to_patches(grad_stream.astype(BF16), members)
    time_grads, grad_normed = attend_back(
        "time", normed_time, time_all, time_heads, time_mixed, grad_low, share, BF16, routed
    )
    grad_normed = to_frames(grad_normed, members).astype(F32)
    grad_part, gain_time = norm_back(tokens, gains[0], grad_normed)
    grad_tokens = grad_stream + grad_part
    down_own = reduce_plain(down_grads).T
    up_own = reduce_plain(up_grads)
    space_own = reduce_plain(space_grads)
    time_own = reduce_plain(time_grads)
    gains_own = sum_gains(jnp.stack([gain_time, gain_space, gain_mlp]), norm_gains.shape[1])
    output = after_mlp * live

    def unpack(own):
        rows = own.shape[0]
        return own[:, : 3 * width].reshape(rows, 3, width).transpose(1, 0, 2), own[:, 3 * width :].T

    time_in_own, time_out_own = unpack(time_own)
    space_in_own, space_out_own = unpack(space_own)
    return (
        output,
        grad_tokens,
        gains_own,
        time_in_own,
        time_out_own,
        space_in_own,
        space_out_own,
        up_own,
        down_own,
    )


def solution(mesh):
    n_dp, n_tensor = mesh.devices.shape

    def run(*args):
        slots = args[0].shape[0] // (n_dp * HALF * PATCHES)
        fine = Mesh(mesh.devices.reshape(n_dp // 4, 2, 2, slots, n_tensor // slots), ALL)
        in_specs = (
            P(ALL, None),
            P(DP),
            P(None, DP),
            P(None, DP, TENSOR),
            P(TENSOR, DP),
            P(None, DP, TENSOR),
            P(TENSOR, DP),
            P(DP, TENSOR),
            P(TENSOR, DP),
            P(ALL, None),
        )
        out_specs = (in_specs[0], in_specs[0]) + in_specs[2:9]
        routed = fine.devices.shape == (2, 2, 2, 2, 2)
        return jax.shard_map(
            functools.partial(on_device, routed), mesh=fine, in_specs=in_specs, out_specs=out_specs, check_vma=False
        )(*args)

    return run
```

```python
import functools
import math

import jax
import jax.numpy as jnp
from jax import lax
from jax.experimental import pallas as pl
from jax.experimental.pallas import tpu as pltpu
from jax.sharding import Mesh, PartitionSpec as P

HEAD_DIM = 64
PATCHES = 196
HALF = 4
FRAMES = 8
EPSILON = 1e-06
F32 = jnp.float32
BF16 = jnp.bfloat16
ALL = ("y", "x", "c", "s", "h")
DP = ("y", "x", "c")
TENSOR = ("s", "h")
CLIP = ("c", "h")

NN = (((1,), (0,)), ((), ()))
NT = (((1,), (1,)), ((), ()))
TN = (((0,), (0,)), ((), ()))
BLOCK_ROWS = 96


def mm(a, b, dims=NN):
    return lax.dot_general(a, b, dims, preferred_element_type=F32)


def row_ids(shape, dim, start):
    return lax.broadcasted_iota(jnp.int32, shape, dim) + start


def windows(kind, count):
    if kind == "time":
        return [(0, count, None)]
    found = []
    for frame in range(count // PATCHES):
        low = frame * PATCHES // 16 * 16
        high = min(count, -(-(frame + 1) * PATCHES // 16) * 16)
        found.append((low, high - low, frame))
    return found


def key_bias(start, size, group, stride):
    keys = row_ids((size, size), 0, start)
    if group is None:
        together = keys % stride == row_ids((size, size), 1, start) % stride
    else:
        together = (keys >= group * PATCHES) & (keys < (group + 1) * PATCHES)
    return jnp.where(together, 0.0, -1e30)


def row_valid(start, size, group, width):
    rows = row_ids((size, width), 0, start)
    return (rows >= group * PATCHES) & (rows < (group + 1) * PATCHES)


def normalize(rows, scale_row):
    average = jnp.mean(rows, -1, keepdims=True)
    centred = rows - average
    spread = jnp.mean(centred * centred, -1, keepdims=True)
    return centred * lax.rsqrt(spread + EPSILON) * scale_row


def norm_back(rows, scale_row, grad_normed):
    unused, pullback = jax.vjp(normalize, rows, scale_row)
    return pullback(grad_normed)


def row_block(core, part, quad):
    quad_me = lax.axis_index(("y", "x"))
    block = jnp.bitwise_xor(quad_me, quad) * 2 + jnp.bitwise_xor(core, part)
    return pl.multiple_of(block * BLOCK_ROWS, BLOCK_ROWS)


def head_slices(ref, rows, width, head):
    low = head * HEAD_DIM
    return tuple(ref[rows, part * width + low : part * width + low + HEAD_DIM] for part in range(3))


def put_grads(work, outs):
    if len(outs) == 1:
        outs[0][...] = work[...]
        return
    core = lax.axis_index("c")
    for part, out in enumerate(outs):
        for quad in range(out.shape[0]):
            out[quad] = work[pl.ds(row_block(core, part, quad), out.shape[1]), :]


def attend_kernel(kind, stride, normed_ref, weight_ref, heads_ref, mixed_ref, out_ref, sums, total_ref):
    step = pl.program_id(0)
    count, width = mixed_ref.shape
    heads_ref[...] = mm(normed_ref[...], weight_ref[:, : 3 * width]).astype(BF16)
    sums[...] = jnp.zeros_like(sums)
    for start, size, group in windows(kind, count):
        bias = key_bias(start, size, group, stride)
        rows = pl.ds(start, size)
        for head in range(width // HEAD_DIM):
            low = head * HEAD_DIM
            query, key, value = head_slices(heads_ref, rows, width, head)
            scores = mm(key, query * HEAD_DIM**-0.5, NT) + bias
            weights = jnp.exp(scores - jnp.max(scores, 0, keepdims=True))
            total = jnp.sum(weights, 0, keepdims=True)
            blended = (mm(value.T, weights.astype(BF16)) / total).T
            if group is not None:
                blended = jnp.where(row_valid(start, size, group, HEAD_DIM), blended, 0.0)
            sums[rows, low : low + HEAD_DIM] += blended
    mixed_ref[...] = sums[...].astype(BF16)
    share = mm(mixed_ref[...], weight_ref[:, 3 * width :], NT)

    @pl.when(step == 0)
    def _():
        total_ref[...] = share

    @pl.when(step > 0)
    def _():
        total_ref[...] += share

    @pl.when(step == pl.num_programs(0) - 1)
    def _():
        out_ref[...] = total_ref[...].astype(out_ref.dtype)


def attend_back_kernel(
    kind, stride, normed_ref, weight_ref, heads_ref, mixed_ref, grad_ref, *rest
):
    outs, (out_ref, sums, total_ref, grad_mixed, grad_heads, work) = rest[:-6], rest[-6:]
    step = pl.program_id(0)
    count, width = mixed_ref.shape
    scale = HEAD_DIM**-0.5
    grad_mixed[...] = mm(grad_ref[...], weight_ref[:, 3 * width :]).astype(BF16)
    sums[...] = jnp.zeros_like(sums)
    for start, size, group in windows(kind, count):
        bias = key_bias(start, size, group, stride)
        rows = pl.ds(start, size)
        for head in range(width // HEAD_DIM):
            low = head * HEAD_DIM
            query, key, value = head_slices(heads_ref, rows, width, head)
            query = query * scale
            grad = grad_mixed[rows, low : low + HEAD_DIM]
            if group is not None:
                valid = row_valid(start, size, group, HEAD_DIM)
                grad = jnp.where(valid, grad.astype(F32), 0.0).astype(BF16)
            scores = mm(key, query, NT) + bias
            weights = jnp.exp(scores - jnp.max(scores, 0, keepdims=True))
            weights = weights / jnp.sum(weights, 0, keepdims=True)
            grad_weights = mm(value, grad, NT)
            row_terms = jnp.sum(weights * grad_weights, 0, keepdims=True)
            grad_scores = (weights * (grad_weights - row_terms)).astype(BF16)
            sums[rows, low : low + HEAD_DIM] += (mm(key.T, grad_scores) * scale).T
            low += width
            sums[rows, low : low + HEAD_DIM] += mm(grad_scores, query)
            low += width
            sums[rows, low : low + HEAD_DIM] += mm(weights.astype(BF16), grad)
    grad_heads[...] = sums[...].astype(BF16)
    share = mm(grad_heads[...], weight_ref[:, : 3 * width], NT)

    @pl.when(step == 0)
    def _():
        total_ref[...] = share

    @pl.when(step > 0)
    def _():
        total_ref[...] += share

    @pl.when(step == pl.num_programs(0) - 1)
    def _():
        out_ref[...] = total_ref[...].astype(out_ref.dtype)

    work[:, : 3 * width] = mm(normed_ref[...], grad_heads[...], TN).astype(BF16)
    work[:, 3 * width :] = mm(grad_ref[...], mixed_ref[...], TN).astype(BF16)
    put_grads(work, outs)


def up_kernel(normed_ref, weight_ref, hidden_ref, slope_ref):
    pre_act = mm(normed_ref[...], weight_ref[...])
    cdf = 0.5 * (1.0 + lax.erf(pre_act * 0.5**0.5))
    hidden_ref[...] = (pre_act * cdf).astype(BF16)
    density = jnp.exp(-0.5 * pre_act * pre_act) * (0.5 / math.pi) ** 0.5
    slope_ref[...] = (cdf + pre_act * density).astype(slope_ref.dtype)


def down_kernel(hidden_ref, weight_ref, out_ref):
    share = mm(hidden_ref[...], weight_ref[...], NT)

    @pl.when(pl.program_id(0) == 0)
    def _():
        out_ref[...] = share

    @pl.when(pl.program_id(0) > 0)
    def _():
        out_ref[...] += share


def down_back_kernel(grad_ref, weight_ref, hidden_ref, slope_ref, *rest):
    outs, (grad_pre_ref, work) = rest[:-2], rest[-2:]
    grad_hidden = mm(grad_ref[...], weight_ref[...])
    grad_pre_ref[...] = (grad_hidden * slope_ref[...].astype(F32)).astype(BF16)
    work[...] = mm(grad_ref[...], hidden_ref[...], TN).astype(BF16)
    put_grads(work, outs)


def up_back_kernel(normed_ref, weight_ref, grad_pre_ref, *rest):
    outs, (out_ref, work) = rest[:-2], rest[-2:]
    share = mm(grad_pre_ref[...], weight_ref[...], NT)

    @pl.when(pl.program_id(0) == 0)
    def _():
        out_ref[...] = share

    @pl.when(pl.program_id(0) > 0)
    def _():
        out_ref[...] += share

    work[...] = mm(normed_ref[...], grad_pre_ref[...], TN).astype(BF16)
    put_grads(work, outs)


def whole_spec(array):
    return pl.BlockSpec(array.shape, lambda i: (0,) * array.ndim)


def step_spec(array):
    rest = array.shape[1:]
    return pl.BlockSpec((None,) + rest, lambda i: (i,) + (0,) * len(rest))


def phase(kernel, name, inputs, outputs, scratch=(), cost=0):
    blocks = [a for a in inputs if a.ndim > 2][0].shape[0]
    spec = lambda a: whole_spec(a) if a.ndim == 2 else step_spec(a)
    return pl.pallas_call(
        kernel,
        grid=(blocks,),
        in_specs=[spec(a) for a in inputs],
        out_specs=[spec(a) for a in outputs],
        out_shape=outputs,
        scratch_shapes=list(scratch),
        cost_estimate=pl.CostEstimate(
            flops=int(cost * 800e6), bytes_accessed=int(cost * 1e6), transcendentals=0
        ),
        name=name,
    )(*inputs)


def shaped(*shape, dtype=BF16):
    return jax.ShapeDtypeStruct(shape, dtype)


def grad_shapes(weight, routed):
    blocks, depth, lanes = weight.shape
    if not routed:
        return [shaped(blocks, depth, lanes)]
    rows = BLOCK_ROWS
    return [shaped(blocks, depth // rows // 2, rows, lanes) for part in range(2)]


def attend(kind, normed, weight, stride, out_dtype):
    blocks, depth, lanes = weight.shape
    count, width = normed.shape[0], lanes // 4
    return phase(
        functools.partial(attend_kernel, kind, stride),
        kind + "_attend",
        (normed, weight),
        (
            shaped(blocks, count, 3 * width),
            shaped(blocks, count, width),
            shaped(count, depth, dtype=out_dtype),
        ),
        (pltpu.VMEM((count, width), F32), pltpu.VMEM((count, depth), F32)),
        cost=14,
    )


def attend_back(kind, normed, weight, heads, mixed, grad, stride, out_dtype, routed):
    blocks, depth, lanes = weight.shape
    count, width = normed.shape[0], lanes // 4
    *grads, out = phase(
        functools.partial(attend_back_kernel, kind, stride),
        kind + "_attend_back",
        (normed, weight, heads, mixed, grad),
        (*grad_shapes(weight, routed), shaped(count, depth, dtype=out_dtype)),
        (
            pltpu.VMEM((count, 3 * width), F32),
            pltpu.VMEM((count, depth), F32),
            pltpu.VMEM((count, width), BF16),
            pltpu.VMEM((count, 3 * width), BF16),
            pltpu.VMEM((depth, lanes), BF16),
        ),
        cost=20,
    )
    return grads, out


def along(piece, axes, distance):
    size = lax.axis_size(axes)
    return lax.ppermute(piece, axes, [(i, i ^ distance) for i in range(size)])


def after(piece, earlier):
    return piece + earlier[:1, :1] * 0


def gather_plain(shard):
    every = lax.all_gather(shard, TENSOR, axis=0, tiled=False)
    return lax.all_gather(every.reshape(-1, *shard.shape), DP, axis=1, tiled=True)


def reduce_plain(grads):
    part = lax.psum_scatter(grads[0], TENSOR, scatter_dimension=0, tiled=True)[0]
    return lax.psum_scatter(part, DP, scatter_dimension=0, tiled=True).astype(F32)


def by_member(parts, me):
    return jnp.stack(
        [
            lax.dynamic_index_in_dim(parts, jnp.bitwise_xor(me, k), 0, keepdims=False)
            for k in range(parts.shape[0])
        ]
    )


def to_patches(rows, members):
    share, columns = PATCHES // members, rows.shape[1]
    me = lax.axis_index(CLIP)
    parts = rows.reshape(-1, members, share, columns).transpose(1, 0, 2, 3)
    parts = [
        lax.dynamic_index_in_dim(parts, jnp.bitwise_xor(me, k), 0, keepdims=False)
        for k in range(members)
    ]
    parts = [parts[0]] + [along(parts[k], CLIP, k) for k in range(1, members)]
    return by_member(jnp.stack(parts), me).reshape(-1, columns)


def to_frames(rows, members):
    share, columns = PATCHES // members, rows.shape[1]
    me = lax.axis_index(CLIP)
    parts = by_member(rows.reshape(members, -1, share, columns), me)
    parts = [parts[0]] + [along(parts[k], CLIP, k) for k in range(1, members)]
    parts = jnp.stack(parts)
    order = jnp.bitwise_xor(me, jnp.arange(members))
    parts = [
        lax.dynamic_index_in_dim(parts, jnp.bitwise_xor(me, k), 0, keepdims=False)
        for k in range(members)
    ]
    return jnp.stack(parts, 1).reshape(-1, columns)


CHUNKS = 4
STEPS = 4
PAD = 56


def place():
    return {axis: lax.axis_index(axis) for axis in ALL}


def moved(here, **flips):
    return tuple(here[a] + flips.get(a, 0) * (1 - 2 * here[a]) for a in ALL)


def dp_row(here, y=0, x=0, c=0):
    to = lambda a, flip: here[a] + flip * (1 - 2 * here[a])
    return to("y", y) * 4 + to("x", x) * 2 + to("c", c)


def remote(source, target, sent, received, device):
    return pltpu.make_async_remote_copy(
        src_ref=source,
        dst_ref=target,
        send_sem=sent,
        recv_sem=received,
        device_id=device,
        device_id_type=pl.DeviceIdType.MESH,
    )


def peers(here):
    found = [moved(here, s=j // 2, h=j % 2) for j in range(1, 4)]
    found += [moved(here, y=r // 4, x=r // 2 % 2, c=r % 2) for r in range(1, 8)]
    return found + [moved(here, c=1, h=1)]


def greet(here, what):
    barrier = pltpu.get_barrier_semaphore()
    everyone = peers(here)
    if what == "answer":
        pl.semaphore_wait(barrier, len(everyone))
        return
    for device in everyone:
        pl.semaphore_signal(
            barrier, inc=1, device_id=device, device_id_type=pl.DeviceIdType.MESH
        )


class Exchange:
    def __init__(self, here, out, back, sent, received):
        self.here, self.out, self.back = here, out, back
        self.sent, self.received = sent, received
        self.me = here["c"] * 2 + here["h"]

    def device(self, member):
        return tuple({"c": member // 2, "h": member % 2}.get(a, self.here[a]) for a in ALL)

    def start(self, member):
        @pl.when(self.me != member)
        def _():
            remote(
                self.out.at[member],
                self.back.at[self.me],
                self.sent.at[member],
                self.received.at[self.me],
                self.device(member),
            ).start()

        @pl.when(self.me == member)
        def _():
            self.back[member] = self.out[member]

    def finish(self, member):
        @pl.when(self.me != member)
        def _():
            remote(
                self.out.at[member],
                self.back.at[member],
                self.sent.at[member],
                self.received.at[member],
                self.device(member),
            ).wait()

    def send(self, rows_ref, rows_of):
        share = PATCHES // 4
        for member in range(4):
            for frame in range(2):
                rows = rows_of(member, frame)
                self.out[member, frame, :share, :] = rows_ref[rows, :].astype(BF16)
            self.start(member)

    def take(self, rows_ref, rows_of):
        share = PATCHES // 4
        for member in range(4):
            self.finish(member)
            for frame in range(2):
                rows = rows_of(member, frame)
                rows_ref[rows, :] = self.back[member, frame, :share, :].astype(F32)

    @staticmethod
    def by_frame(member, frame):
        low = frame * PATCHES + member * (PATCHES // 4)
        return slice(low, low + PATCHES // 4)

    @staticmethod
    def by_share(member, frame):
        return pl.ds(member * 2 + frame, PATCHES // 4, stride=FRAMES)

    def parts(self, patch_ref):
        for block in range(patch_ref.shape[0]):
            yield block, slice(block * 128, (block + 1) * 128)

    def send_frames(self, rows_ref):
        self.send(rows_ref, self.by_frame)

    def take_patches(self, patch_ref, low_ref):
        share = PATCHES // 4
        for member in range(4):
            self.finish(member)
            for frame in range(2):
                for block, lanes in self.parts(patch_ref):
                    patch_ref[block, self.by_share(member, frame), :] = self.back[
                        member, frame, :share, lanes
                    ].astype(F32)
        for block, lanes in self.parts(patch_ref):
            low_ref[:, lanes] = patch_ref[block].astype(BF16)

    def send_patches(self, rows_ref, patch_ref):
        share = PATCHES // 4
        for block, lanes in self.parts(patch_ref):
            patch_ref[block] = rows_ref[:, lanes]
        for member in range(4):
            for frame in range(2):
                for block, lanes in self.parts(patch_ref):
                    self.out[member, frame, :share, lanes] = patch_ref[
                        block, self.by_share(member, frame), :
                    ].astype(BF16)
            self.start(member)

    def take_frames(self, rows_ref):
        self.take(rows_ref, self.by_frame)


def by_rows(count, body, size=56):
    def step(i, carry):
        body(pl.ds(pl.multiple_of(i * size, size), size))
        return carry

    lax.fori_loop(0, count // size, step, 0)


def row_stats(rows):
    average = jnp.mean(rows, -1, keepdims=True)
    centred = rows - average
    spread = jnp.mean(centred * centred, -1, keepdims=True)
    return centred, lax.rsqrt(spread + EPSILON)


def attention_units(kind, count, width):
    found = []
    if kind == "time":
        tile = 96
        starts = list(range(0, count - tile, tile))
        ends = starts[1:] + [count]
    else:
        starts = [low for low, size, group in windows(kind, count)]
        ends = [low + size for low, size, group in windows(kind, count)]
    for index, (start, end) in enumerate(zip(starts, ends)):
        size = end - start
        keys = row_ids((size, size), 0, 0)
        first, final = 0, size
        if kind == "time":
            together = keys // FRAMES == row_ids((size, size), 1, 0) // FRAMES
        else:
            first = index * PATCHES - start
            final = first + PATCHES
            together = (keys >= first) & (keys < final)
        bias = jnp.where(together, 0.0, -1e30)
        found += [(start, size, first, final, bias, head) for head in range(width // HEAD_DIM)]
    return found


def attend_block(kind, t, normed, weight, heads_ref, mixed_ref, sums):
    count, width = mixed_ref.shape[1:]
    heads_ref[t] = mm(normed, weight[:, : 3 * width]).astype(BF16)
    heads = heads_ref.at[t]
    target = mixed_ref.at[t] if kind == "time" else sums
    units = attention_units(kind, count, width)
    for batch in range(0, len(units), 6):
        some = units[batch : batch + 6]
        parts = [head_slices(heads, pl.ds(u[0], u[1]), width, u[5]) for u in some]
        scores = [
            mm(key, query * HEAD_DIM**-0.5, NT) + u[4] for u, (query, key, value) in zip(some, parts)
        ]
        weights = [jnp.exp(x - jnp.max(x, 0, keepdims=True)) for x in scores]
        scales = [1.0 / jnp.sum(x, 0, keepdims=True) for x in weights]
        blended = [
            (mm(value.T, x.astype(BF16)) * scale).T
            for x, scale, (query, key, value) in zip(weights, scales, parts)
        ]
        for (start, size, first, final, bias, head), x in zip(some, blended):
            lanes = slice(head * HEAD_DIM, (head + 1) * HEAD_DIM)
            target[start + first : start + final, lanes] = x[first:final].astype(target.dtype)
    if kind != "time":
        mixed_ref[t] = sums[...].astype(BF16)
    return mm(mixed_ref[t], weight[:, 3 * width :], NT)


def attend_back_block(kind, heads, mixed, grad, weight, grad_mixed, sums, grad_heads):
    count, width = mixed.shape
    scale = HEAD_DIM**-0.5
    grad_mixed[...] = mm(grad[...], weight[:, 3 * width :]).astype(BF16)
    target = grad_heads if kind == "time" else sums
    units = attention_units(kind, count, width)
    batch_size = 12 if kind == "time" else 3
    for batch in range(0, len(units), batch_size):
        some = units[batch : batch + batch_size]
        parts = []
        for start, size, first, final, bias, head in some:
            rows = pl.ds(start, size)
            query, key, value = head_slices(heads, rows, width, head)
            grad_here = grad_mixed[rows, head * HEAD_DIM : (head + 1) * HEAD_DIM]
            if kind != "time":
                ids = row_ids((size, HEAD_DIM), 0, 0)
                valid = (ids >= first) & (ids < final)
                grad_here = jnp.where(valid, grad_here.astype(F32), 0.0).astype(BF16)
            parts.append((query * scale, key, value, grad_here))
        scores = [mm(p[1], p[0], NT) + u[4] for u, p in zip(some, parts)]
        grad_weights = [mm(p[2], p[3], NT) for p in parts]
        weights = [jnp.exp(x - jnp.max(x, 0, keepdims=True)) for x in scores]
        weights = [x * (1.0 / jnp.sum(x, 0, keepdims=True)) for x in weights]
        grad_values = [mm(x.astype(BF16), p[3]) for x, p in zip(weights, parts)]
        grad_scores = [
            (x * (y - jnp.sum(x * y, 0, keepdims=True))).astype(BF16)
            for x, y in zip(weights, grad_weights)
        ]
        grad_keys = [mm(x, p[0]) for x, p in zip(grad_scores, parts)]
        grad_queries = [(mm(p[1].T, x) * scale).T for x, p in zip(grad_scores, parts)]
        for u, *grads in zip(some, grad_queries, grad_keys, grad_values):
            start, size, first, final, bias, head = u
            for c, x in enumerate(grads):
                low = c * width + head * HEAD_DIM
                target[start + first : start + final, low : low + HEAD_DIM] = x[
                    first:final
                ].astype(target.dtype)
    if kind != "time":
        grad_heads[...] = sums[...].astype(BF16)
    return mm(grad_heads[...], weight[:, : 3 * width], NT)


EVENT_NAMES = ("zs", "line", "relay", "across", "core", "first", "second", "third")
BLOCK_ORDER = (1, 2, 3, 0)
ORDER = (
    ("go",),
    ("zs", 0, 2), ("line", 2, 0), ("line", 1, 0), ("zs", 0, 1), ("line", 0, 0), ("zs", 0, 3),
    ("line", 0, 2), ("line", 0, 1), ("relay", 0, 0), ("zs", 1, 2), ("relay", 0, 2),
    ("line", 0, 3), ("zs", 1, 3), ("line", 1, 2), ("zs", 1, 1), ("ln0",), ("across", 0, 0),
    ("relay", 0, 3), ("relay", 0, 1), ("across", 0, 2), ("relay", 1, 0), ("zs", 2, 1),
    ("zs", 2, 3), ("zs", 2, 2), ("mask",), ("relay", 1, 2), ("across", 0, 1), ("across", 0, 3),
    ("line", 1, 3), ("zs", 3, 3), ("line", 1, 1), ("line", 2, 1), ("takeE0",), ("relay", 1, 3),
    ("P0", 0), ("relay", 1, 1), ("P0", 1), ("line", 2, 3), ("P0", 2), ("P0", 3), ("line", 2, 2),
    ("exch1",), ("relay", 2, 0), ("across", 1, 0), ("relay", 2, 1), ("relay", 2, 3),
    ("line", 3, 0), ("zs", 3, 1), ("across", 1, 3), ("across", 1, 1), ("relay", 2, 2),
    ("line", 3, 3), ("across", 1, 2), ("zs", 3, 2), ("ln1",), ("P1", 0), ("P1", 1),
    ("line", 3, 1), ("P1", 2), ("across", 2, 3), ("across", 2, 0), ("across", 2, 1),
    ("across", 2, 2), ("line", 3, 2), ("P1", 3), ("relay", 3, 0), ("ln2",), ("relay", 3, 3),
    ("up", 0), ("relay", 3, 1), ("relay", 3, 2), ("up", 1), ("core", 0), ("across", 3, 3),
    ("across", 3, 0), ("up", 2), ("core", 1), ("across", 3, 2), ("across", 3, 1), ("up", 3),
    ("core", 2), ("first", 0), ("dn", 0), ("dn", 1), ("dn", 2), ("dn", 3), ("first", 1),
    ("B1", 0), ("core", 3), ("B1", 1), ("second", 0), ("first", 2), ("core", 4), ("second", 1),
    ("B1", 2), ("core", 5), ("B1", 3), ("nb2",), ("first", 4), ("second", 2), ("core", 6),
    ("B2", 0), ("first", 5), ("core", 7), ("second", 4), ("B2", 1), ("core", 8), ("B2", 2),
    ("first", 6), ("core", 9), ("second", 5), ("B2", 3), ("nb1",), ("core", 10), ("first", 9),
    ("second", 6), ("first", 3), ("first", 10), ("first", 8), ("core", 11), ("first", 7),
    ("second", 9), ("takeE2",), ("B3", 0), ("second", 10), ("B3", 1), ("second", 8), ("core", 12),
    ("B3", 2), ("core", 13), ("B3", 3), ("first", 12), ("exch3",), ("second", 3), ("core", 14),
    ("first", 13), ("second", 12), ("core", 15), ("first", 14), ("first", 11), ("second", 13),
    ("third", 0), ("second", 7), ("nb0",), ("second", 14), ("first", 15), ("second", 11),
    ("third", 2), ("third", 1), ("gain",), ("second", 15), ("third", 3),
)


def after_each(order):
    found, events = {}, []
    for item in order:
        if item[0] in EVENT_NAMES:
            events.append(item)
        else:
            events = found.setdefault(item, [])
    return found


LINE_ACROSS = ()
SUM_ACROSS = (0, 1)
AFTER = after_each(ORDER)


def layer_kernel(
    live_ref,
    tokens_hbm,
    cotangent_hbm,
    gain_hbm,
    qkv_time_hbm,
    out_time_hbm,
    qkv_space_hbm,
    out_space_hbm,
    up_hbm,
    down_hbm,
    weight_ref,
    out_hbm,
    stream_hbm,
    own_hbm,
    own_gain_hbm,
    out_ref,
    stream_ref,
    own_ref,
    own_gain_ref,
    tokens_ref,
    gain_ref,
    qkv_time_ref,
    out_time_ref,
    qkv_space_ref,
    out_space_ref,
    shard_ref,
    held,
    normed_time_ref,
    time_heads_ref,
    time_mixed_ref,
    after_time_ref,
    normed_space_ref,
    space_heads_ref,
    space_mixed_ref,
    after_space_ref,
    normed_mlp_ref,
    hidden_ref,
    slope_ref,
    low_ref,
    rows_ref,
    patch_ref,
    total_ref,
    mixed_sums,
    sums,
    grad_mixed,
    grad_heads,
    work,
    keep,
    came,
    first,
    second,
    third,
    fourth,
    gains_ref,
    gain_sums,
    gain_line,
    gain_out,
    gain_parts,
    swap_out,
    swap_back,
    piece_sent,
    piece_here,
    core_sent,
    core_here,
    first_sent,
    first_here,
    second_sent,
    second_here,
    third_sent,
    third_here,
    fourth_sent,
    fourth_here,
    gain_sent,
    gain_here,
    swap_sent,
    swap_here,
    held_sem,
    own_sem,
    load_sem,
    store_sem,
    credit,
):
    here = place()
    count, columns = tokens_ref.shape
    width = time_mixed_ref.shape[2]
    own_row = dp_row(here)
    last = CHUNKS * STEPS - 1
    live = jnp.where(here["s"] < live_ref[0], 1.0, 0.0).astype(F32)

    loads = [
        pltpu.make_async_copy(source, target, load_sem.at[i])
        for i, (source, target) in enumerate(
            (
                (gain_hbm, gain_ref),
                (qkv_time_hbm, qkv_time_ref),
                (out_time_hbm, out_time_ref),
                (qkv_space_hbm, qkv_space_ref),
                (out_space_hbm, out_space_ref),
                (up_hbm, shard_ref.at[2]),
                (down_hbm, shard_ref.at[3]),
                (tokens_hbm, tokens_ref),
                (cotangent_hbm, stream_ref),
            )
        )
    ]
    stores = [
        pltpu.make_async_copy(source, target, store_sem.at[i])
        for i, (source, target) in enumerate(
            [(out_ref, out_hbm), (stream_ref, stream_hbm)]
            + [(own_ref.at[k], own_hbm.at[k]) for k in range(CHUNKS)]
            + [(own_gain_ref, own_gain_hbm)]
        )
    ]
    greet(here, "call")
    for load in loads:
        load.start()
    for load in loads[:5]:
        load.wait()

    for k, qkv, out in ((0, qkv_time_ref, out_time_ref), (1, qkv_space_ref, out_space_ref)):
        for c in range(3):
            shard_ref[k, :, c * width : (c + 1) * width] = qkv[c]
        shard_ref[k, :, 3 * width :] = out[...].astype(F32).T.astype(BF16)
    own_gains = gain_ref.shape[1]
    gain_out[0, : gain_ref.shape[0], :own_gains] = gain_ref[...].astype(F32)
    for load in loads[5:7]:
        load.wait()
    greet(here, "answer")

    def row_of(part, r):
        return dp_row(here, y=r // 2, x=r % 2, c=part)

    def slot_of(k, j, row):
        return weight_ref.at[k, j, pl.ds(pl.multiple_of(row * BLOCK_ROWS, BLOCK_ROWS), BLOCK_ROWS)]

    def arrived(k, part, r, j):
        slot = slot_of(k, j, row_of(part, r))
        remote(
            slot, slot, piece_sent.at[k, 0, 0], piece_here.at[k, part, r, j], moved(here, c=1)
        ).wait_recv()

    def send(source, k, j, r, sem, part, r_there, **flips):
        remote(
            source,
            slot_of(k, j, row_of(0, r)),
            piece_sent.at[k, sem, j],
            piece_here.at[k, part, r_there, j],
            moved(here, **flips),
        ).start()

    def piece(k, j, r):
        return slot_of(k, j, row_of(0, r))

    def along_line(k, j):
        remote(
            shard_ref.at[k],
            slot_of(k, j, own_row),
            piece_sent.at[k, 0, j],
            piece_here.at[k, 0, 0, j],
            moved(here, s=j // 2, h=j % 2),
        ).start()

    def spread(source, k, j):
        send(source, k, j, 0, 1, 0, 1, x=1)
        send(source, k, j, 0, 2, 0, 2, y=1)
        send(source, k, j, 0, 4, 1, 0, c=1)

    def line(k, j):
        if j:
            arrived(k, 0, 0, j)
        spread(piece(k, j, 0) if j else shard_ref.at[k], k, j)

    def relay(k, j):
        arrived(k, 0, 1, j)
        send(piece(k, j, 1), k, j, 1, 5, 1, 1, c=1)
        arrived(k, 0, 2, j)
        send(piece(k, j, 2), k, j, 2, 6, 1, 2, c=1)
        if j == 1 and k in LINE_ACROSS:
            return
        up = (j // 2 + k) % 2
        source = slot_of(k, j, dp_row(here, y=up, x=1 - up))
        remote(
            source,
            source,
            piece_sent.at[k, 3, j],
            piece_here.at[k, 0, 3, j],
            moved(here, y=1 - up, x=up),
        ).start()

    def across(k, j):
        arrived(k, 0, 3, j)
        send(piece(k, j, 3), k, j, 3, 7, 1, 3, c=1)
        if j == 0 and k in LINE_ACROSS:
            remote(
                piece(k, 0, 3),
                piece(k, 1, 3),
                piece_sent.at[k, 3, 1],
                piece_here.at[k, 0, 3, 1],
                moved(here, h=1),
            ).start()

    def fetch(k, t):
        return pltpu.make_async_copy(weight_ref.at[k, t], held.at[t], held_sem.at[t])

    def ready(k):
        for j in range(STEPS):
            for r in range(4):
                arrived(k, 1, r, j)
        for t in BLOCK_ORDER:
            fetch(k, t).start()

    def weight(k, t):
        fetch(k, t).wait()
        return held.at[t]

    def stored(k):
        return pltpu.make_async_copy(shard_ref.at[k], slot_of(k, 0, own_row), own_sem.at[k])

    half_lanes = keep.shape[4]
    swapped = (0, 2, 1, 3)

    def grad_rows(part, quad):
        row = dp_row(here, y=quad // 2, x=quad % 2, c=part)
        return pl.ds(pl.multiple_of(row * BLOCK_ROWS, BLOCK_ROWS), BLOCK_ROWS)

    def core_copy(step, quad):
        return remote(
            work.at[step % 2, grad_rows(1, quad)],
            came.at[step % 4, quad],
            core_sent.at[step % 2, quad],
            core_here.at[step % 4, quad],
            moved(here, c=1),
        )

    def quads_sent(step):
        return 1 if BLOCK_ORDER[step % STEPS] == 1 and step // STEPS in SUM_ACROSS else 2

    def first_copy(step, half):
        quads = quads_sent(step)
        return remote(
            keep.at[step, pl.ds(2, quads), half],
            first.at[step, half, pl.ds(0, quads)],
            first_sent.at[step, half],
            first_here.at[step, half],
            moved(here, y=1 - half, x=half),
        )

    def fourth_copy(index):
        return remote(
            keep.at[index * STEPS + BLOCK_ORDER.index(1), 3],
            fourth.at[index],
            fourth_sent.at[index],
            fourth_here.at[index],
            moved(here, h=1),
        )

    def second_copy(step, half):
        return remote(
            keep.at[step, 1, half],
            second.at[step, half],
            second_sent.at[step, half],
            second_here.at[step, half],
            moved(here, y=half, x=1 - half),
        )

    def third_copy(step):
        j = BLOCK_ORDER[step % STEPS]
        return remote(
            keep.at[step, 0],
            third.at[step],
            third_sent.at[step],
            third_here.at[step],
            moved(here, s=j // 2, h=j % 2),
        )

    def begin(step):
        @pl.when(step >= 2)
        def _():
            for quad in range(4):
                core_copy(step - 2, quad).wait_send()

        return work.at[step % 2]

    def emit(step):
        @pl.when(step >= 4)
        def _():
            pl.semaphore_wait(credit, 1)

        for quad in range(4):
            core_copy(step, quad).start()

    def take_core(step):
        block = BLOCK_ORDER[step % STEPS]
        for quad in range(4):
            core_copy(step, quad).wait_recv()
        for index in (2, 3, 1, 0):
            for half in range(2):
                quad = swapped[index] if half else index
                lanes = slice(half * half_lanes, (half + 1) * half_lanes)
                own = work[step % 2, grad_rows(0, quad), lanes].astype(F32)
                both = own + came[step % 4, quad, :, lanes].astype(F32)
                if index == 3 and block == 0 and step // STEPS in SUM_ACROSS:
                    if half == 0:
                        fourth_copy(step // STEPS).wait_recv()
                    both = both + fourth[step // STEPS, half].astype(F32)
                keep[step, index, half] = both.astype(BF16)
                if index == 1 + quads_sent(step):
                    first_copy(step, half).start()
            if index == 3 and block == 1 and step // STEPS in SUM_ACROSS:
                fourth_copy(step // STEPS).start()
        if step <= last - 4:
            pl.semaphore_signal(
                credit,
                inc=1,
                device_id=moved(here, c=1),
                device_id_type=pl.DeviceIdType.MESH,
            )

    def take_first(step):
        for half in range(2):
            first_copy(step, half).wait_recv()
            for index in (1, 0):
                if index < quads_sent(step):
                    both = keep[step, index, half].astype(F32) + first[step, half, index].astype(F32)
                    keep[step, index, half] = both.astype(BF16)
                if index:
                    second_copy(step, half).start()

    def take_second(step):
        for half in range(2):
            second_copy(step, half).wait_recv()
            both = keep[step, 0, half].astype(F32) + second[step, half].astype(F32)
            keep[step, 0, half] = both.astype(BF16)
        if BLOCK_ORDER[step % STEPS]:
            third_copy(step).start()

    def take_third(index):
        steps = [index * STEPS + i for i in range(STEPS)]
        for step in steps:
            if BLOCK_ORDER[step % STEPS]:
                third_copy(step).wait_recv()
        for half in range(2):
            total = jnp.zeros((BLOCK_ROWS, half_lanes), F32)
            for step in steps:
                source = third[step, half] if BLOCK_ORDER[step % STEPS] else keep[step, 0, half]
                total = total + source.astype(F32)
            own_ref[index, :, half * half_lanes : (half + 1) * half_lanes] = total
        stores[2 + index].start()

    events = {
        "zs": along_line,
        "line": line,
        "relay": relay,
        "across": across,
        "core": take_core,
        "first": take_first,
        "second": take_second,
        "third": take_third,
    }

    def follow(item):
        for name, *args in AFTER.get(item, ()):
            events[name](*args)

    def loop(name, body):
        def step(i, carry):
            body(i, (i + 1) % STEPS)
            for c in range(STEPS - 1):
                if AFTER.get((name, c)):

                    @pl.when(i == c)
                    def _(c=c):
                        follow((name, c))

            return carry

        lax.fori_loop(0, STEPS, step, 0)
        follow((name, STEPS - 1))

    def layer_norm(source_ref, gain, target_ref):
        def body(rows):
            centred, scale = row_stats(source_ref[rows, :])
            target_ref[rows, :] = (centred * scale * gains_ref[gain : gain + 1, :]).astype(
                target_ref.dtype
            )

        by_rows(count, body)

    def norm_back(source_ref, gain, grad_normed_ref):
        def body(rows):
            centred, scale = row_stats(source_ref[rows, :])
            unit = centred * scale
            grad_normed = grad_normed_ref[rows, :]
            e = grad_normed * gains_ref[gain : gain + 1, :]
            mean = jnp.mean(e, -1, keepdims=True)
            tilt = jnp.mean(e * unit, -1, keepdims=True)
            stream_ref[rows, :] += scale * (e - mean - unit * tilt)
            gain_sums[gain : gain + 1, :] += jnp.sum(grad_normed * unit, 0, keepdims=True)

        by_rows(count, body)

    def exchange(index):
        return Exchange(
            here,
            swap_out.at[index % 2],
            swap_back.at[index % 2],
            swap_sent.at[index],
            swap_here.at[index],
        )

    def attention(kind, k, normed_ref, heads_ref, mixed_ref):
        total_ref[...] = jnp.zeros_like(total_ref)

        def compute(i, t):
            total_ref[...] += attend_block(
                kind, t, normed_ref[...], weight(k, t), heads_ref, mixed_ref, mixed_sums
            )

        return compute

    def attention_back(kind, k, normed_ref, heads_ref, mixed_ref):
        total_ref[...] = jnp.zeros_like(total_ref)

        def compute(i, t):
            step = (CHUNKS - 1 - k) * STEPS + i
            out = begin(step)
            total_ref[...] += attend_back_block(
                kind,
                heads_ref.at[t],
                mixed_ref.at[t],
                low_ref,
                weight(k, t),
                grad_mixed,
                sums,
                grad_heads,
            )
            if k:
                fetch(k - 1, t).start()
            out[:, : 3 * width] = mm(normed_ref[...], grad_heads[...], TN).astype(BF16)
            out[:, 3 * width :] = mm(low_ref[...], mixed_ref[t], TN).astype(BF16)
            emit(step)

        return compute

    gain_parts[0, own_row] = gain_out[0]

    def gain_copy(r):
        flips = {"y": r // 4, "x": r // 2 % 2, "c": r % 2}
        return remote(
            gain_out.at[0],
            gain_parts.at[0, own_row],
            gain_sent.at[0, r],
            gain_here.at[0, r],
            moved(here, **flips),
        )

    for r in range(1, 8):
        gain_copy(r).start()
    for k in range(CHUNKS):
        stored(k).start()
    follow(("go",))
    loads[7].wait()

    def unit_rows(rows):
        centred, scale = row_stats(tokens_ref[rows, :])
        rows_ref[rows, :] = centred * scale

    by_rows(count, unit_rows)
    for r in range(1, 8):
        gain_copy(r).wait()
    for d in range(8):
        gains_ref[:, d * own_gains : (d + 1) * own_gains] = gain_parts[0, d, :, :own_gains]

    def scale_rows(rows):
        rows_ref[rows, :] = rows_ref[rows, :] * gains_ref[0:1, :]

    by_rows(count, scale_rows)
    swap = exchange(0)
    swap.send_frames(rows_ref)
    follow(("ln0",))
    loads[8].wait()

    def mask_rows(rows):
        stream_ref[rows, :] = stream_ref[rows, :] * live
        low_ref[rows, :] = stream_ref[rows, :].astype(BF16)

    by_rows(count, mask_rows)
    gain_sums[...] = jnp.zeros_like(gain_sums)
    follow(("mask",))
    swap.take_patches(patch_ref, normed_time_ref)
    for k in range(CHUNKS):
        stored(k).wait()
    follow(("takeE0",))

    ready(0)
    loop("P0", attention("time", 0, normed_time_ref, time_heads_ref, time_mixed_ref))
    swap = exchange(1)
    swap.send_patches(total_ref, patch_ref)
    follow(("exch1",))
    swap.take_frames(rows_ref)
    after_time_ref[...] = tokens_ref[...] + rows_ref[...]
    layer_norm(after_time_ref, 1, normed_space_ref)
    follow(("ln1",))

    ready(1)
    loop("P1", attention("space", 1, normed_space_ref, space_heads_ref, space_mixed_ref))
    after_space_ref[...] = after_time_ref[...] + total_ref[...]
    layer_norm(after_space_ref, 2, normed_mlp_ref)
    follow(("ln2",))

    ready(2)

    def up(i, t):
        out = begin(i)
        pre_act = mm(normed_mlp_ref[...], weight(2, t)[...])
        cdf = 0.5 * (1.0 + lax.erf(pre_act * 0.5**0.5))
        hidden_ref[t] = (pre_act * cdf).astype(BF16)
        density = jnp.exp(-0.5 * pre_act * pre_act) * (0.5 / math.pi) ** 0.5
        slope_ref[t] = (cdf + pre_act * density).astype(BF16)
        out[...] = mm(low_ref[...], hidden_ref[t], TN).astype(BF16)
        emit(i)

    loop("up", up)
    ready(3)
    out_ref[...] = after_space_ref[...]

    def down(i, t):
        out_ref[...] += mm(hidden_ref[t], weight(3, t)[...], NT)
        grad_hidden = mm(low_ref[...], held[t])
        slope_ref[t] = (grad_hidden * slope_ref[t].astype(F32)).astype(BF16)
        fetch(2, t).start()

    loop("dn", down)
    out_ref[...] = out_ref[...] * live
    stores[0].start()
    total_ref[...] = jnp.zeros_like(total_ref)

    def up_back(i, t):
        step = STEPS + i
        out = begin(step)
        total_ref[...] += mm(slope_ref[t], weight(2, t)[...], NT)
        fetch(1, t).start()
        out[...] = mm(normed_mlp_ref[...], slope_ref[t], TN).astype(BF16)
        emit(step)

    loop("B1", up_back)
    norm_back(after_space_ref, 2, total_ref)
    low_ref[...] = stream_ref[...].astype(BF16)
    follow(("nb2",))
    loop("B2", attention_back("space", 1, normed_space_ref, space_heads_ref, space_mixed_ref))
    norm_back(after_time_ref, 1, total_ref)
    swap = exchange(2)
    swap.send_frames(stream_ref)
    follow(("nb1",))
    swap.take_patches(patch_ref, low_ref)
    follow(("takeE2",))
    loop("B3", attention_back("time", 0, normed_time_ref, time_heads_ref, time_mixed_ref))
    swap = exchange(3)
    swap.send_patches(total_ref, patch_ref)
    follow(("exch3",))
    swap.take_frames(rows_ref)
    norm_back(tokens_ref, 0, rows_ref)
    stores[1].start()

    line_index = here["s"] * 2 + here["h"]

    def gain_back(r):
        flips = {"y": r // 4, "x": r // 2 % 2, "c": r % 2}
        return remote(
            gain_out.at[dp_row(here, **flips)],
            gain_parts.at[1, own_row],
            gain_sent.at[1, r],
            gain_here.at[1, r],
            moved(here, **flips),
        )

    def gain_line_copy(j):
        return remote(
            own_gain_ref,
            gain_line.at[line_index],
            gain_sent.at[2, j],
            gain_here.at[2, j],
            moved(here, s=j // 2, h=j % 2),
        )

    total = gain_sums[...]
    for d in range(8):
        gain_out[d, :, :own_gains] = total[:, d * own_gains : (d + 1) * own_gains]
    for r in range(1, 8):
        gain_back(r).start()
    gain_parts[1, own_row] = gain_out[own_row]
    follow(("nb0",))
    for r in range(1, 8):
        gain_back(r).wait()
    total = gain_parts[1, 0]
    for d in range(1, 8):
        total = total + gain_parts[1, d]
    own_gain_ref[...] = total
    for j in range(1, 4):
        gain_line_copy(j).start()
    gain_line[line_index] = total
    follow(("gain",))
    for j in range(1, 4):
        gain_line_copy(j).wait()
    own_gain_ref[...] = gain_line[0] + gain_line[1] + gain_line[2] + gain_line[3]
    stores[2 + CHUNKS].start()

    for k in range(CHUNKS):
        for sem in range(8):
            for j in range(4):
                if sem or j:
                    slot = slot_of(k, 0, own_row)
                    remote(
                        slot,
                        slot,
                        piece_sent.at[k, sem, j],
                        piece_here.at[k, 0, 0, 0],
                        moved(here, c=1),
                    ).wait_send()
    for step in range(last + 1):
        if step > last - 2:
            for quad in range(4):
                core_copy(step, quad).wait_send()
        for half in range(2):
            first_copy(step, half).wait_send()
            second_copy(step, half).wait_send()
        if BLOCK_ORDER[step % STEPS]:
            third_copy(step).wait_send()
    for index in SUM_ACROSS:
        fourth_copy(index).wait_send()
    for store in stores:
        store.wait()


def layer(live_clips, tokens, cotangent, norm_gains, *weights):
    count, columns = tokens.shape
    rows, lanes = weights[4].shape
    half = lanes // 2
    width, steps = lanes // 4, CHUNKS * STEPS
    there = pl.BlockSpec(memory_space=pl.ANY)
    outputs = (
        shaped(CHUNKS, STEPS, columns, lanes),
        shaped(count, columns, dtype=F32),
        shaped(count, columns, dtype=F32),
        shaped(CHUNKS, rows, lanes, dtype=F32),
        shaped(8, 128, dtype=F32),
    )
    return pl.pallas_call(
        layer_kernel,
        in_specs=[pl.BlockSpec(memory_space=pltpu.SMEM)] + [there] * 9,
        out_specs=[there] * len(outputs),
        out_shape=outputs,
        scratch_shapes=[
            pltpu.VMEM((count, columns), F32),
            pltpu.VMEM((count, columns), F32),
            pltpu.VMEM((CHUNKS, rows, lanes), F32),
            pltpu.VMEM((8, 128), F32),
            pltpu.VMEM((count, columns), F32),
            pltpu.VMEM(norm_gains.shape, BF16),
            *[pltpu.VMEM(w.shape, BF16) for w in weights[:4]],
            pltpu.VMEM((CHUNKS, rows, lanes), BF16),
            pltpu.VMEM((STEPS, columns, lanes), BF16),
            pltpu.VMEM((count, columns), BF16),
            pltpu.VMEM((STEPS, count, 3 * width), BF16),
            pltpu.VMEM((STEPS, count, width), BF16),
            pltpu.VMEM((count, columns), F32),
            pltpu.VMEM((count, columns), BF16),
            pltpu.VMEM((STEPS, count, 3 * width), BF16),
            pltpu.VMEM((STEPS, count, width), BF16),
            pltpu.VMEM((count, columns), F32),
            pltpu.VMEM((count, columns), BF16),
            pltpu.VMEM((STEPS, count, lanes), BF16),
            pltpu.VMEM((STEPS, count, lanes), BF16),
            pltpu.VMEM((count, columns), BF16),
            pltpu.VMEM((count, columns), F32),
            pltpu.VMEM((columns // 128, count, 128), F32),
            pltpu.VMEM((count, columns), F32),
            pltpu.VMEM((count, width), F32),
            pltpu.VMEM((count, 3 * width), F32),
            pltpu.VMEM((count, width), BF16),
            pltpu.VMEM((count, 3 * width), BF16),
            pltpu.VMEM((2, columns, lanes), BF16),
            pltpu.VMEM((steps, 4, 2, rows, half), BF16),
            pltpu.VMEM((4, 4, rows, lanes), BF16),
            pltpu.VMEM((steps, 2, 2, rows, half), BF16),
            pltpu.VMEM((steps, 2, rows, half), BF16),
            pltpu.VMEM((steps, 2, rows, half), BF16),
            pltpu.VMEM((CHUNKS, 2, rows, half), BF16),
            pltpu.VMEM((8, columns), F32),
            pltpu.VMEM((8, columns), F32),
            pltpu.VMEM((4, 8, 128), F32),
            pltpu.VMEM((8, 8, 128), F32),
            pltpu.VMEM((2, 8, 8, 128), F32),
            pltpu.VMEM((2, 4, 2, PAD, columns), BF16),
            pltpu.VMEM((2, 4, 2, PAD, columns), BF16),
            pltpu.SemaphoreType.DMA((CHUNKS, 8, 4)),
            pltpu.SemaphoreType.DMA((CHUNKS, 2, 4, 4)),
            pltpu.SemaphoreType.DMA((2, 4)),
            pltpu.SemaphoreType.DMA((4, 4)),
            pltpu.SemaphoreType.DMA((steps, 2)),
            pltpu.SemaphoreType.DMA((steps, 2)),
            pltpu.SemaphoreType.DMA((steps, 2)),
            pltpu.SemaphoreType.DMA((steps, 2)),
            pltpu.SemaphoreType.DMA((steps,)),
            pltpu.SemaphoreType.DMA((steps,)),
            pltpu.SemaphoreType.DMA((CHUNKS,)),
            pltpu.SemaphoreType.DMA((CHUNKS,)),
            pltpu.SemaphoreType.DMA((3, 8)),
            pltpu.SemaphoreType.DMA((3, 8)),
            pltpu.SemaphoreType.DMA((4, 4)),
            pltpu.SemaphoreType.DMA((4, 4)),
            pltpu.SemaphoreType.DMA((STEPS,)),
            pltpu.SemaphoreType.DMA((CHUNKS,)),
            pltpu.SemaphoreType.DMA((9,)),
            pltpu.SemaphoreType.DMA((3 + CHUNKS,)),
            pltpu.SemaphoreType.REGULAR,
        ],
        compiler_params=pltpu.CompilerParams(
            collective_id=0, has_side_effects=True, vmem_limit_bytes=67043328
        ),
        name="layer",
    )(live_clips, tokens, cotangent, norm_gains, *weights)[1:]


def finish_kernel(output_hbm, grad_hbm, own_hbm, gain_ref, *rest):
    targets, buffers, own_ref, load_sem, store_sem = rest[:9], rest[9:18], *rest[18:]
    output, grad, gains, time_in, time_out, space_in, space_out, up, down = buffers
    width = time_in.shape[2]
    sources = [(own_hbm.at[k], into) for k, into in ((0, down), (1, up))]
    sources += [(own_hbm.at[k], own_ref.at[k - 2]) for k in (2, 3)]
    sources += [(output_hbm, output), (grad_hbm, grad)]
    loads = [pltpu.make_async_copy(*pair, load_sem.at[i]) for i, pair in enumerate(sources)]
    stores = [
        pltpu.make_async_copy(*pair, store_sem.at[i]) for i, pair in enumerate(zip(buffers, targets))
    ]
    for i in (2, 3, 0, 1, 4, 5):
        loads[i].start()
    gains[...] = gain_ref[: gains.shape[0], : gains.shape[1]]
    stores[2].start()
    for k, load, into, out, low in ((0, 2, space_in, space_out, 5), (1, 3, time_in, time_out, 3)):
        loads[load].wait()
        for c in range(3):
            into[c] = own_ref[k, :, c * width : (c + 1) * width]
        stores[low].start()
        out[...] = own_ref[k, :, 3 * width :].T
        stores[low + 1].start()
    for load, store in ((0, 8), (1, 7), (4, 0), (5, 1)):
        loads[load].wait()
        stores[store].start()
    for store in stores:
        store.wait()


def finish(output, grad, own, gain, like):
    shapes = [jax.ShapeDtypeStruct(a.shape, F32) for a in like]
    there = pl.BlockSpec(memory_space=pl.ANY)
    return pl.pallas_call(
        finish_kernel,
        in_specs=[there] * 3 + [pl.BlockSpec(memory_space=pltpu.VMEM)],
        out_specs=[there] * len(shapes),
        out_shape=shapes,
        scratch_shapes=[
            *[pltpu.VMEM(a.shape, F32) for a in like],
            pltpu.VMEM((2,) + own.shape[1:], F32),
            pltpu.SemaphoreType.DMA((6,)),
            pltpu.SemaphoreType.DMA((len(shapes),)),
        ],
        name="finish",
    )(output, grad, own, gain)


def sum_gains(total, own):
    for axes in ("c", "x", "y", TENSOR):
        bit = 1
        while bit < lax.axis_size(axes):
            total = total + along(total, axes, bit)
            bit *= 2
    return lax.dynamic_slice_in_dim(total, lax.axis_index(DP) * own, own, 1)


def on_device(
    routed,
    tokens,
    live_clips,
    norm_gains,
    qkv_time,
    out_time,
    qkv_space,
    out_space,
    up_weight,
    down_weight,
    cotangent,
):
    members = lax.axis_size("c") * lax.axis_size("h")
    share = PATCHES // members
    count, columns = tokens.shape
    width = qkv_time.shape[2]
    live = jnp.where(lax.axis_index("s") < live_clips[0], 1.0, 0.0).astype(F32)

    def pack_heads(qkv, out):
        rows = qkv.shape[1]
        return jnp.concatenate([qkv.transpose(1, 0, 2).reshape(rows, -1), out.T], 1)

    if routed:
        weights = (qkv_time, out_time, qkv_space, out_space, up_weight, down_weight.T)
        done = layer(live_clips, tokens, cotangent, norm_gains, *weights)
        *found, down_own = finish(*done, (tokens, cotangent, norm_gains, *weights))
        return (*found, down_own.T)
    shards = [
        pack_heads(qkv_time, out_time),
        pack_heads(qkv_space, out_space),
        up_weight,
        down_weight.T,
    ]
    grad_stream = cotangent * live
    time_all, space_all, up_all, down_all = [gather_plain(shard) for shard in shards]
    blocks, depth, lanes = up_all.shape
    gains = lax.all_gather(norm_gains, DP, axis=1, tiled=True).astype(F32)
    normed_time = to_patches(normalize(tokens, gains[0]).astype(BF16), members)
    time_heads, time_mixed, change = attend("time", normed_time, time_all, share, BF16)
    after_time = tokens + to_frames(change, members).astype(F32)
    normed_space = normalize(after_time, gains[1]).astype(BF16)
    space_heads, space_mixed, change = attend("space", normed_space, space_all, 1, F32)
    after_space = after_time + change
    normed_mlp = normalize(after_space, gains[2]).astype(BF16)
    hidden, slope = phase(
        up_kernel,
        "up",
        (normed_mlp, up_all),
        (shaped(blocks, count, lanes), shaped(blocks, count, lanes)),
        cost=12,
    )
    (change,) = phase(
        down_kernel, "down", (hidden, down_all), (shaped(count, depth, dtype=F32),), cost=4
    )
    after_mlp = after_space + change
    grad_low = grad_stream.astype(BF16)
    work = (pltpu.VMEM((depth, lanes), BF16),)
    *down_grads, grad_pre = phase(
        down_back_kernel,
        "down_back",
        (grad_low, down_all, hidden, slope),
        (*grad_shapes(down_all, False), shaped(blocks, count, lanes)),
        work,
        cost=8,
    )
    *up_grads, grad_normed = phase(
        up_back_kernel,
        "up_back",
        (normed_mlp, up_all, grad_pre),
        (*grad_shapes(up_all, False), shaped(count, depth, dtype=F32)),
        work,
        cost=8,
    )
    grad_part, gain_mlp = norm_back(after_space, gains[2], grad_normed)
    grad_stream = grad_stream + grad_part
    space_grads, grad_normed = attend_back(
        "space",
        normed_space,
        space_all,
        space_heads,
        space_mixed,
        grad_stream.astype(BF16),
        1,
        F32,
        False,
    )
    grad_part, gain_space = norm_back(after_time, gains[1], grad_normed)
    grad_stream = grad_stream + grad_part
    grad_low = to_patches(grad_stream.astype(BF16), members)
    time_grads, grad_normed = attend_back(
        "time", normed_time, time_all, time_heads, time_mixed, grad_low, share, BF16, routed
    )
    grad_normed = to_frames(grad_normed, members).astype(F32)
    grad_part, gain_time = norm_back(tokens, gains[0], grad_normed)
    grad_tokens = grad_stream + grad_part
    down_own = reduce_plain(down_grads).T
    up_own = reduce_plain(up_grads)
    space_own = reduce_plain(space_grads)
    time_own = reduce_plain(time_grads)
    gains_own = sum_gains(jnp.stack([gain_time, gain_space, gain_mlp]), norm_gains.shape[1])
    output = after_mlp * live

    def unpack(own):
        rows = own.shape[0]
        return own[:, : 3 * width].reshape(rows, 3, width).transpose(1, 0, 2), own[:, 3 * width :].T

    time_in_own, time_out_own = unpack(time_own)
    space_in_own, space_out_own = unpack(space_own)
    return (
        output,
        grad_tokens,
        gains_own,
        time_in_own,
        time_out_own,
        space_in_own,
        space_out_own,
        up_own,
        down_own,
    )


def solution(mesh):
    n_dp, n_tensor = mesh.devices.shape

    def run(*args):
        slots = args[0].shape[0] // (n_dp * HALF * PATCHES)
        fine = Mesh(mesh.devices.reshape(n_dp // 4, 2, 2, slots, n_tensor // slots), ALL)
        in_specs = (
            P(ALL, None),
            P(DP),
            P(None, DP),
            P(None, DP, TENSOR),
            P(TENSOR, DP),
            P(None, DP, TENSOR),
            P(TENSOR, DP),
            P(DP, TENSOR),
            P(TENSOR, DP),
            P(ALL, None),
        )
        out_specs = (in_specs[0], in_specs[0]) + in_specs[2:9]
        routed = fine.devices.shape == (2, 2, 2, 2, 2)
        return jax.shard_map(
            functools.partial(on_device, routed), mesh=fine, in_specs=in_specs, out_specs=out_specs, check_vma=False
        )(*args)

    return run
```

```python
import functools
import math

import jax
import jax.numpy as jnp
from jax import lax
from jax.experimental import pallas as pl
from jax.experimental.pallas import tpu as pltpu
from jax.sharding import Mesh, PartitionSpec as P

HEAD_DIM = 64
PATCHES = 196
HALF = 4
FRAMES = 8
EPSILON = 1e-06
F32 = jnp.float32
BF16 = jnp.bfloat16
ALL = ("y", "x", "c", "s", "h")
DP = ("y", "x", "c")
TENSOR = ("s", "h")
CLIP = ("c", "h")

NN = (((1,), (0,)), ((), ()))
NT = (((1,), (1,)), ((), ()))
TN = (((0,), (0,)), ((), ()))
BLOCK_ROWS = 96


def mm(a, b, dims=NN):
    return lax.dot_general(a, b, dims, preferred_element_type=F32)


def row_ids(shape, dim, start):
    return lax.broadcasted_iota(jnp.int32, shape, dim) + start


def windows(kind, count):
    if kind == "time":
        return [(0, count, None)]
    found = []
    for frame in range(count // PATCHES):
        low = frame * PATCHES // 16 * 16
        high = min(count, -(-(frame + 1) * PATCHES // 16) * 16)
        found.append((low, high - low, frame))
    return found


def key_bias(start, size, group, stride):
    keys = row_ids((size, size), 0, start)
    if group is None:
        together = keys % stride == row_ids((size, size), 1, start) % stride
    else:
        together = (keys >= group * PATCHES) & (keys < (group + 1) * PATCHES)
    return jnp.where(together, 0.0, -1e30)


def row_valid(start, size, group, width):
    rows = row_ids((size, width), 0, start)
    return (rows >= group * PATCHES) & (rows < (group + 1) * PATCHES)


def normalize(rows, scale_row):
    average = jnp.mean(rows, -1, keepdims=True)
    centred = rows - average
    spread = jnp.mean(centred * centred, -1, keepdims=True)
    return centred * lax.rsqrt(spread + EPSILON) * scale_row


def norm_back(rows, scale_row, grad_normed):
    unused, pullback = jax.vjp(normalize, rows, scale_row)
    return pullback(grad_normed)


def row_block(core, part, quad):
    quad_me = lax.axis_index(("y", "x"))
    block = jnp.bitwise_xor(quad_me, quad) * 2 + jnp.bitwise_xor(core, part)
    return pl.multiple_of(block * BLOCK_ROWS, BLOCK_ROWS)


def head_slices(ref, rows, width, head):
    low = head * HEAD_DIM
    return tuple(ref[rows, part * width + low : part * width + low + HEAD_DIM] for part in range(3))


def put_grads(work, outs):
    if len(outs) == 1:
        outs[0][...] = work[...]
        return
    core = lax.axis_index("c")
    for part, out in enumerate(outs):
        for quad in range(out.shape[0]):
            out[quad] = work[pl.ds(row_block(core, part, quad), out.shape[1]), :]


def attend_kernel(kind, stride, normed_ref, weight_ref, heads_ref, mixed_ref, out_ref, sums, total_ref):
    step = pl.program_id(0)
    count, width = mixed_ref.shape
    heads_ref[...] = mm(normed_ref[...], weight_ref[:, : 3 * width]).astype(BF16)
    sums[...] = jnp.zeros_like(sums)
    for start, size, group in windows(kind, count):
        bias = key_bias(start, size, group, stride)
        rows = pl.ds(start, size)
        for head in range(width // HEAD_DIM):
            low = head * HEAD_DIM
            query, key, value = head_slices(heads_ref, rows, width, head)
            scores = mm(key, query * HEAD_DIM**-0.5, NT) + bias
            weights = jnp.exp(scores - jnp.max(scores, 0, keepdims=True))
            total = jnp.sum(weights, 0, keepdims=True)
            blended = (mm(value.T, weights.astype(BF16)) / total).T
            if group is not None:
                blended = jnp.where(row_valid(start, size, group, HEAD_DIM), blended, 0.0)
            sums[rows, low : low + HEAD_DIM] += blended
    mixed_ref[...] = sums[...].astype(BF16)
    share = mm(mixed_ref[...], weight_ref[:, 3 * width :], NT)

    @pl.when(step == 0)
    def _():
        total_ref[...] = share

    @pl.when(step > 0)
    def _():
        total_ref[...] += share

    @pl.when(step == pl.num_programs(0) - 1)
    def _():
        out_ref[...] = total_ref[...].astype(out_ref.dtype)


def attend_back_kernel(
    kind, stride, normed_ref, weight_ref, heads_ref, mixed_ref, grad_ref, *rest
):
    outs, (out_ref, sums, total_ref, grad_mixed, grad_heads, work) = rest[:-6], rest[-6:]
    step = pl.program_id(0)
    count, width = mixed_ref.shape
    scale = HEAD_DIM**-0.5
    grad_mixed[...] = mm(grad_ref[...], weight_ref[:, 3 * width :]).astype(BF16)
    sums[...] = jnp.zeros_like(sums)
    for start, size, group in windows(kind, count):
        bias = key_bias(start, size, group, stride)
        rows = pl.ds(start, size)
        for head in range(width // HEAD_DIM):
            low = head * HEAD_DIM
            query, key, value = head_slices(heads_ref, rows, width, head)
            query = query * scale
            grad = grad_mixed[rows, low : low + HEAD_DIM]
            if group is not None:
                valid = row_valid(start, size, group, HEAD_DIM)
                grad = jnp.where(valid, grad.astype(F32), 0.0).astype(BF16)
            scores = mm(key, query, NT) + bias
            weights = jnp.exp(scores - jnp.max(scores, 0, keepdims=True))
            weights = weights / jnp.sum(weights, 0, keepdims=True)
            grad_weights = mm(value, grad, NT)
            row_terms = jnp.sum(weights * grad_weights, 0, keepdims=True)
            grad_scores = (weights * (grad_weights - row_terms)).astype(BF16)
            sums[rows, low : low + HEAD_DIM] += (mm(key.T, grad_scores) * scale).T
            low += width
            sums[rows, low : low + HEAD_DIM] += mm(grad_scores, query)
            low += width
            sums[rows, low : low + HEAD_DIM] += mm(weights.astype(BF16), grad)
    grad_heads[...] = sums[...].astype(BF16)
    share = mm(grad_heads[...], weight_ref[:, : 3 * width], NT)

    @pl.when(step == 0)
    def _():
        total_ref[...] = share

    @pl.when(step > 0)
    def _():
        total_ref[...] += share

    @pl.when(step == pl.num_programs(0) - 1)
    def _():
        out_ref[...] = total_ref[...].astype(out_ref.dtype)

    work[:, : 3 * width] = mm(normed_ref[...], grad_heads[...], TN).astype(BF16)
    work[:, 3 * width :] = mm(grad_ref[...], mixed_ref[...], TN).astype(BF16)
    put_grads(work, outs)


def up_kernel(normed_ref, weight_ref, hidden_ref, slope_ref):
    pre_act = mm(normed_ref[...], weight_ref[...])
    cdf = 0.5 * (1.0 + lax.erf(pre_act * 0.5**0.5))
    hidden_ref[...] = (pre_act * cdf).astype(BF16)
    density = jnp.exp(-0.5 * pre_act * pre_act) * (0.5 / math.pi) ** 0.5
    slope_ref[...] = (cdf + pre_act * density).astype(slope_ref.dtype)


def down_kernel(hidden_ref, weight_ref, out_ref):
    share = mm(hidden_ref[...], weight_ref[...], NT)

    @pl.when(pl.program_id(0) == 0)
    def _():
        out_ref[...] = share

    @pl.when(pl.program_id(0) > 0)
    def _():
        out_ref[...] += share


def down_back_kernel(grad_ref, weight_ref, hidden_ref, slope_ref, *rest):
    outs, (grad_pre_ref, work) = rest[:-2], rest[-2:]
    grad_hidden = mm(grad_ref[...], weight_ref[...])
    grad_pre_ref[...] = (grad_hidden * slope_ref[...].astype(F32)).astype(BF16)
    work[...] = mm(grad_ref[...], hidden_ref[...], TN).astype(BF16)
    put_grads(work, outs)


def up_back_kernel(normed_ref, weight_ref, grad_pre_ref, *rest):
    outs, (out_ref, work) = rest[:-2], rest[-2:]
    share = mm(grad_pre_ref[...], weight_ref[...], NT)

    @pl.when(pl.program_id(0) == 0)
    def _():
        out_ref[...] = share

    @pl.when(pl.program_id(0) > 0)
    def _():
        out_ref[...] += share

    work[...] = mm(normed_ref[...], grad_pre_ref[...], TN).astype(BF16)
    put_grads(work, outs)


def whole_spec(array):
    return pl.BlockSpec(array.shape, lambda i: (0,) * array.ndim)


def step_spec(array):
    rest = array.shape[1:]
    return pl.BlockSpec((None,) + rest, lambda i: (i,) + (0,) * len(rest))


def phase(kernel, name, inputs, outputs, scratch=(), cost=0):
    blocks = [a for a in inputs if a.ndim > 2][0].shape[0]
    spec = lambda a: whole_spec(a) if a.ndim == 2 else step_spec(a)
    return pl.pallas_call(
        kernel,
        grid=(blocks,),
        in_specs=[spec(a) for a in inputs],
        out_specs=[spec(a) for a in outputs],
        out_shape=outputs,
        scratch_shapes=list(scratch),
        cost_estimate=pl.CostEstimate(
            flops=int(cost * 800e6), bytes_accessed=int(cost * 1e6), transcendentals=0
        ),
        name=name,
    )(*inputs)


def shaped(*shape, dtype=BF16):
    return jax.ShapeDtypeStruct(shape, dtype)


def grad_shapes(weight, routed):
    blocks, depth, lanes = weight.shape
    if not routed:
        return [shaped(blocks, depth, lanes)]
    rows = BLOCK_ROWS
    return [shaped(blocks, depth // rows // 2, rows, lanes) for part in range(2)]


def attend(kind, normed, weight, stride, out_dtype):
    blocks, depth, lanes = weight.shape
    count, width = normed.shape[0], lanes // 4
    return phase(
        functools.partial(attend_kernel, kind, stride),
        kind + "_attend",
        (normed, weight),
        (
            shaped(blocks, count, 3 * width),
            shaped(blocks, count, width),
            shaped(count, depth, dtype=out_dtype),
        ),
        (pltpu.VMEM((count, width), F32), pltpu.VMEM((count, depth), F32)),
        cost=14,
    )


def attend_back(kind, normed, weight, heads, mixed, grad, stride, out_dtype, routed):
    blocks, depth, lanes = weight.shape
    count, width = normed.shape[0], lanes // 4
    *grads, out = phase(
        functools.partial(attend_back_kernel, kind, stride),
        kind + "_attend_back",
        (normed, weight, heads, mixed, grad),
        (*grad_shapes(weight, routed), shaped(count, depth, dtype=out_dtype)),
        (
            pltpu.VMEM((count, 3 * width), F32),
            pltpu.VMEM((count, depth), F32),
            pltpu.VMEM((count, width), BF16),
            pltpu.VMEM((count, 3 * width), BF16),
            pltpu.VMEM((depth, lanes), BF16),
        ),
        cost=20,
    )
    return grads, out


def along(piece, axes, distance):
    size = lax.axis_size(axes)
    return lax.ppermute(piece, axes, [(i, i ^ distance) for i in range(size)])


def after(piece, earlier):
    return piece + earlier[:1, :1] * 0


def gather_plain(shard):
    every = lax.all_gather(shard, TENSOR, axis=0, tiled=False)
    return lax.all_gather(every.reshape(-1, *shard.shape), DP, axis=1, tiled=True)


def reduce_plain(grads):
    part = lax.psum_scatter(grads[0], TENSOR, scatter_dimension=0, tiled=True)[0]
    return lax.psum_scatter(part, DP, scatter_dimension=0, tiled=True).astype(F32)


def by_member(parts, me):
    return jnp.stack(
        [
            lax.dynamic_index_in_dim(parts, jnp.bitwise_xor(me, k), 0, keepdims=False)
            for k in range(parts.shape[0])
        ]
    )


def to_patches(rows, members):
    share, columns = PATCHES // members, rows.shape[1]
    me = lax.axis_index(CLIP)
    parts = rows.reshape(-1, members, share, columns).transpose(1, 0, 2, 3)
    parts = [
        lax.dynamic_index_in_dim(parts, jnp.bitwise_xor(me, k), 0, keepdims=False)
        for k in range(members)
    ]
    parts = [parts[0]] + [along(parts[k], CLIP, k) for k in range(1, members)]
    return by_member(jnp.stack(parts), me).reshape(-1, columns)


def to_frames(rows, members):
    share, columns = PATCHES // members, rows.shape[1]
    me = lax.axis_index(CLIP)
    parts = by_member(rows.reshape(members, -1, share, columns), me)
    parts = [parts[0]] + [along(parts[k], CLIP, k) for k in range(1, members)]
    parts = jnp.stack(parts)
    order = jnp.bitwise_xor(me, jnp.arange(members))
    parts = [
        lax.dynamic_index_in_dim(parts, jnp.bitwise_xor(me, k), 0, keepdims=False)
        for k in range(members)
    ]
    return jnp.stack(parts, 1).reshape(-1, columns)


CHUNKS = 4
STEPS = 4
PAD = 56


def place():
    return {axis: lax.axis_index(axis) for axis in ALL}


def moved(here, **flips):
    return tuple(here[a] + flips.get(a, 0) * (1 - 2 * here[a]) for a in ALL)


def dp_row(here, y=0, x=0, c=0):
    to = lambda a, flip: here[a] + flip * (1 - 2 * here[a])
    return to("y", y) * 4 + to("x", x) * 2 + to("c", c)


def remote(source, target, sent, received, device):
    return pltpu.make_async_remote_copy(
        src_ref=source,
        dst_ref=target,
        send_sem=sent,
        recv_sem=received,
        device_id=device,
        device_id_type=pl.DeviceIdType.MESH,
    )


def peers(here):
    found = [moved(here, s=j // 2, h=j % 2) for j in range(1, 4)]
    found += [moved(here, y=r // 4, x=r // 2 % 2, c=r % 2) for r in range(1, 8)]
    return found + [moved(here, c=1, h=1)]


def greet(here, what):
    barrier = pltpu.get_barrier_semaphore()
    everyone = peers(here)
    if what == "answer":
        pl.semaphore_wait(barrier, len(everyone))
        return
    for device in everyone:
        pl.semaphore_signal(
            barrier, inc=1, device_id=device, device_id_type=pl.DeviceIdType.MESH
        )


class Exchange:
    def __init__(self, here, out, back, sent, received):
        self.here, self.out, self.back = here, out, back
        self.sent, self.received = sent, received
        self.me = here["c"] * 2 + here["h"]

    def device(self, member):
        return tuple({"c": member // 2, "h": member % 2}.get(a, self.here[a]) for a in ALL)

    def start(self, member):
        @pl.when(self.me != member)
        def _():
            remote(
                self.out.at[member],
                self.back.at[self.me],
                self.sent.at[member],
                self.received.at[self.me],
                self.device(member),
            ).start()

        @pl.when(self.me == member)
        def _():
            self.back[member] = self.out[member]

    def finish(self, member):
        @pl.when(self.me != member)
        def _():
            remote(
                self.out.at[member],
                self.back.at[member],
                self.sent.at[member],
                self.received.at[member],
                self.device(member),
            ).wait()

    def send(self, rows_ref, rows_of):
        share = PATCHES // 4
        for member in range(4):
            for frame in range(2):
                rows = rows_of(member, frame)
                self.out[member, frame, :share, :] = rows_ref[rows, :].astype(BF16)
            self.start(member)

    def take(self, rows_ref, rows_of):
        share = PATCHES // 4
        for member in range(4):
            self.finish(member)
            for frame in range(2):
                rows = rows_of(member, frame)
                rows_ref[rows, :] = self.back[member, frame, :share, :].astype(F32)

    @staticmethod
    def by_frame(member, frame):
        low = frame * PATCHES + member * (PATCHES // 4)
        return slice(low, low + PATCHES // 4)

    @staticmethod
    def by_share(member, frame):
        return pl.ds(member * 2 + frame, PATCHES // 4, stride=FRAMES)

    def parts(self, patch_ref):
        for block in range(patch_ref.shape[0]):
            yield block, slice(block * 128, (block + 1) * 128)

    def send_frames(self, rows_ref):
        self.send(rows_ref, self.by_frame)

    def take_patches(self, patch_ref, low_ref):
        share = PATCHES // 4
        for member in range(4):
            self.finish(member)
            for frame in range(2):
                for block, lanes in self.parts(patch_ref):
                    patch_ref[block, self.by_share(member, frame), :] = self.back[
                        member, frame, :share, lanes
                    ].astype(F32)
        for block, lanes in self.parts(patch_ref):
            low_ref[:, lanes] = patch_ref[block].astype(BF16)

    def send_patches(self, rows_ref, patch_ref):
        share = PATCHES // 4
        for block, lanes in self.parts(patch_ref):
            patch_ref[block] = rows_ref[:, lanes]
        for member in range(4):
            for frame in range(2):
                for block, lanes in self.parts(patch_ref):
                    self.out[member, frame, :share, lanes] = patch_ref[
                        block, self.by_share(member, frame), :
                    ].astype(BF16)
            self.start(member)

    def take_frames(self, rows_ref):
        self.take(rows_ref, self.by_frame)


def by_rows(count, body, size=56):
    def step(i, carry):
        body(pl.ds(pl.multiple_of(i * size, size), size))
        return carry

    lax.fori_loop(0, count // size, step, 0)


def row_stats(rows):
    average = jnp.mean(rows, -1, keepdims=True)
    centred = rows - average
    spread = jnp.mean(centred * centred, -1, keepdims=True)
    return centred, lax.rsqrt(spread + EPSILON)


def attention_units(kind, count, width):
    found = []
    if kind == "time":
        tile = 96
        starts = list(range(0, count - tile, tile))
        ends = starts[1:] + [count]
    else:
        starts = [low for low, size, group in windows(kind, count)]
        ends = [low + size for low, size, group in windows(kind, count)]
    for index, (start, end) in enumerate(zip(starts, ends)):
        size = end - start
        keys = row_ids((size, size), 0, 0)
        first, final = 0, size
        if kind == "time":
            together = keys // FRAMES == row_ids((size, size), 1, 0) // FRAMES
        else:
            first = index * PATCHES - start
            final = first + PATCHES
            together = (keys >= first) & (keys < final)
        bias = jnp.where(together, 0.0, -1e30)
        found += [(start, size, first, final, bias, head) for head in range(width // HEAD_DIM)]
    return found


def attend_block(kind, t, normed, weight, heads_ref, mixed_ref, sums):
    count, width = mixed_ref.shape[1:]
    heads_ref[t] = mm(normed, weight[:, : 3 * width]).astype(BF16)
    heads = heads_ref.at[t]
    target = mixed_ref.at[t] if kind == "time" else sums
    units = attention_units(kind, count, width)
    for batch in range(0, len(units), 6):
        some = units[batch : batch + 6]
        parts = [head_slices(heads, pl.ds(u[0], u[1]), width, u[5]) for u in some]
        scores = [
            mm(key, query * HEAD_DIM**-0.5, NT) + u[4] for u, (query, key, value) in zip(some, parts)
        ]
        weights = [jnp.exp(x - jnp.max(x, 0, keepdims=True)) for x in scores]
        scales = [1.0 / jnp.sum(x, 0, keepdims=True) for x in weights]
        blended = [
            (mm(value.T, x.astype(BF16)) * scale).T
            for x, scale, (query, key, value) in zip(weights, scales, parts)
        ]
        for (start, size, first, final, bias, head), x in zip(some, blended):
            lanes = slice(head * HEAD_DIM, (head + 1) * HEAD_DIM)
            target[start + first : start + final, lanes] = x[first:final].astype(target.dtype)
    if kind != "time":
        mixed_ref[t] = sums[...].astype(BF16)
    return mm(mixed_ref[t], weight[:, 3 * width :], NT)


def attend_back_block(kind, heads, mixed, grad, weight, grad_mixed, sums, grad_heads):
    count, width = mixed.shape
    scale = HEAD_DIM**-0.5
    grad_mixed[...] = mm(grad[...], weight[:, 3 * width :]).astype(BF16)
    target = grad_heads if kind == "time" else sums
    units = attention_units(kind, count, width)
    batch_size = 12 if kind == "time" else 3
    for batch in range(0, len(units), batch_size):
        some = units[batch : batch + batch_size]
        parts = []
        for start, size, first, final, bias, head in some:
            rows = pl.ds(start, size)
            query, key, value = head_slices(heads, rows, width, head)
            grad_here = grad_mixed[rows, head * HEAD_DIM : (head + 1) * HEAD_DIM]
            if kind != "time":
                ids = row_ids((size, HEAD_DIM), 0, 0)
                valid = (ids >= first) & (ids < final)
                grad_here = jnp.where(valid, grad_here.astype(F32), 0.0).astype(BF16)
            parts.append((query * scale, key, value, grad_here))
        scores = [mm(p[1], p[0], NT) + u[4] for u, p in zip(some, parts)]
        grad_weights = [mm(p[2], p[3], NT) for p in parts]
        weights = [jnp.exp(x - jnp.max(x, 0, keepdims=True)) for x in scores]
        weights = [x * (1.0 / jnp.sum(x, 0, keepdims=True)) for x in weights]
        grad_values = [mm(x.astype(BF16), p[3]) for x, p in zip(weights, parts)]
        grad_scores = [
            (x * (y - jnp.sum(x * y, 0, keepdims=True))).astype(BF16)
            for x, y in zip(weights, grad_weights)
        ]
        grad_keys = [mm(x, p[0]) for x, p in zip(grad_scores, parts)]
        grad_queries = [(mm(p[1].T, x) * scale).T for x, p in zip(grad_scores, parts)]
        for u, *grads in zip(some, grad_queries, grad_keys, grad_values):
            start, size, first, final, bias, head = u
            for c, x in enumerate(grads):
                low = c * width + head * HEAD_DIM
                target[start + first : start + final, low : low + HEAD_DIM] = x[
                    first:final
                ].astype(target.dtype)
    if kind != "time":
        grad_heads[...] = sums[...].astype(BF16)
    return mm(grad_heads[...], weight[:, : 3 * width], NT)


EVENT_NAMES = ("zs", "line", "relay", "across", "core", "first", "second", "third")
BLOCK_ORDER = (1, 2, 3, 0)
ORDER = (
    ("go",),
    ("line", 0, 0), ("zs", 0, 3), ("line", 2, 0), ("zs", 1, 1), ("zs", 0, 1), ("line", 1, 0),
    ("zs", 0, 2), ("zs", 2, 1), ("line", 0, 3), ("zs", 1, 2), ("line", 1, 1), ("zs", 1, 3),
    ("line", 0, 1), ("relay", 2, 0), ("ln0",), ("relay", 0, 3), ("line", 0, 2), ("across", 0, 3),
    ("relay", 1, 1), ("across", 2, 0), ("zs", 2, 2), ("relay", 0, 0), ("relay", 0, 1),
    ("relay", 0, 2), ("line", 2, 1), ("zs", 2, 3), ("line", 1, 2), ("mask",), ("zs", 3, 1),
    ("line", 1, 3), ("across", 0, 0), ("across", 0, 1), ("across", 0, 2), ("zs", 3, 2),
    ("takeE0",), ("P0", 0), ("across", 1, 1), ("line", 2, 2), ("relay", 1, 0), ("P0", 1),
    ("P0", 2), ("relay", 1, 3), ("P0", 3), ("exch1",), ("relay", 1, 2), ("relay", 2, 2),
    ("line", 2, 3), ("across", 1, 2), ("relay", 2, 1), ("across", 2, 2), ("line", 3, 2),
    ("zs", 3, 3), ("across", 1, 0), ("across", 1, 3), ("relay", 2, 3), ("line", 3, 0),
    ("line", 3, 1), ("ln1",), ("P1", 0), ("P1", 1), ("P1", 2), ("across", 2, 3), ("across", 2, 1),
    ("line", 3, 3), ("relay", 3, 2), ("P1", 3), ("relay", 3, 0), ("ln2",), ("up", 0),
    ("relay", 3, 1), ("relay", 3, 3), ("up", 1), ("across", 3, 0), ("across", 3, 2), ("core", 0),
    ("up", 2), ("core", 1), ("across", 3, 1), ("across", 3, 3), ("up", 3), ("core", 2), ("dn", 0),
    ("dn", 1), ("first", 0), ("dn", 2), ("dn", 3), ("first", 2), ("B1", 0), ("core", 3),
    ("B1", 1), ("first", 1), ("second", 2), ("second", 0), ("core", 4), ("B1", 2), ("core", 5),
    ("B1", 3), ("nb2",), ("second", 1), ("core", 6), ("B2", 0), ("core", 7), ("first", 5),
    ("B2", 1), ("core", 8), ("B2", 2), ("core", 9), ("first", 6), ("second", 5), ("B2", 3),
    ("nb1",), ("core", 10), ("first", 4), ("first", 8), ("second", 6), ("first", 10),
    ("core", 11), ("first", 9), ("first", 7), ("second", 4), ("first", 3), ("takeE2",), ("B3", 0),
    ("second", 10), ("B3", 1), ("core", 12), ("second", 8), ("B3", 2), ("second", 9),
    ("core", 13), ("B3", 3), ("exch3",), ("core", 14), ("first", 13), ("second", 3), ("core", 15),
    ("first", 14), ("first", 12), ("second", 13), ("first", 11), ("third", 0), ("second", 7),
    ("first", 15), ("third", 1), ("second", 14), ("nb0",), ("second", 11), ("second", 12),
    ("gain",), ("third", 2), ("second", 15), ("third", 3),
)


def after_each(order):
    found, events = {}, []
    for item in order:
        if item[0] in EVENT_NAMES:
            events.append(item)
        else:
            events = found.setdefault(item, [])
    return found


LINE_ACROSS = ()
SUM_ACROSS = ()
AFTER = after_each(ORDER)


def layer_kernel(
    live_ref,
    tokens_hbm,
    cotangent_hbm,
    gain_hbm,
    qkv_time_hbm,
    out_time_hbm,
    qkv_space_hbm,
    out_space_hbm,
    up_hbm,
    down_hbm,
    weight_ref,
    out_hbm,
    stream_hbm,
    own_hbm,
    own_gain_hbm,
    out_ref,
    stream_ref,
    own_ref,
    own_gain_ref,
    tokens_ref,
    gain_ref,
    qkv_time_ref,
    out_time_ref,
    qkv_space_ref,
    out_space_ref,
    shard_ref,
    held,
    normed_time_ref,
    time_heads_ref,
    time_mixed_ref,
    after_time_ref,
    normed_space_ref,
    space_heads_ref,
    space_mixed_ref,
    after_space_ref,
    normed_mlp_ref,
    hidden_ref,
    slope_ref,
    low_ref,
    rows_ref,
    patch_ref,
    total_ref,
    mixed_sums,
    sums,
    grad_mixed,
    grad_heads,
    work,
    keep,
    came,
    first,
    second,
    third,
    fourth,
    gains_ref,
    gain_sums,
    gain_line,
    gain_out,
    gain_parts,
    swap_out,
    swap_back,
    piece_sent,
    piece_here,
    core_sent,
    core_here,
    first_sent,
    first_here,
    second_sent,
    second_here,
    third_sent,
    third_here,
    fourth_sent,
    fourth_here,
    gain_sent,
    gain_here,
    swap_sent,
    swap_here,
    held_sem,
    own_sem,
    load_sem,
    store_sem,
    credit,
):
    here = place()
    count, columns = tokens_ref.shape
    width = time_mixed_ref.shape[2]
    own_row = dp_row(here)
    last = CHUNKS * STEPS - 1
    live = jnp.where(here["s"] < live_ref[0], 1.0, 0.0).astype(F32)

    loads = [
        pltpu.make_async_copy(source, target, load_sem.at[i])
        for i, (source, target) in enumerate(
            (
                (gain_hbm, gain_ref),
                (qkv_time_hbm, qkv_time_ref),
                (out_time_hbm, out_time_ref),
                (qkv_space_hbm, qkv_space_ref),
                (out_space_hbm, out_space_ref),
                (up_hbm, shard_ref.at[2]),
                (down_hbm, shard_ref.at[3]),
                (tokens_hbm, tokens_ref),
                (cotangent_hbm, stream_ref),
            )
        )
    ]
    stores = [
        pltpu.make_async_copy(source, target, store_sem.at[i])
        for i, (source, target) in enumerate(
            [(out_ref, out_hbm), (stream_ref, stream_hbm)]
            + [(own_ref.at[k], own_hbm.at[k]) for k in range(CHUNKS)]
            + [(own_gain_ref, own_gain_hbm)]
        )
    ]
    greet(here, "call")
    for load in loads:
        load.start()
    for load in loads[:5]:
        load.wait()

    for k, qkv, out in ((0, qkv_time_ref, out_time_ref), (1, qkv_space_ref, out_space_ref)):
        for c in range(3):
            shard_ref[k, :, c * width : (c + 1) * width] = qkv[c]
        shard_ref[k, :, 3 * width :] = out[...].astype(F32).T.astype(BF16)
    own_gains = gain_ref.shape[1]
    gain_out[0, : gain_ref.shape[0], :own_gains] = gain_ref[...].astype(F32)
    for load in loads[5:7]:
        load.wait()
    greet(here, "answer")

    def row_of(part, r):
        return dp_row(here, y=r // 2, x=r % 2, c=part)

    def slot_of(k, j, row):
        return weight_ref.at[k, j, pl.ds(pl.multiple_of(row * BLOCK_ROWS, BLOCK_ROWS), BLOCK_ROWS)]

    def arrived(k, part, r, j):
        slot = slot_of(k, j, row_of(part, r))
        remote(
            slot, slot, piece_sent.at[k, 0, 0], piece_here.at[k, part, r, j], moved(here, c=1)
        ).wait_recv()

    def send(source, k, j, r, sem, part, r_there, **flips):
        remote(
            source,
            slot_of(k, j, row_of(0, r)),
            piece_sent.at[k, sem, j],
            piece_here.at[k, part, r_there, j],
            moved(here, **flips),
        ).start()

    def piece(k, j, r):
        return slot_of(k, j, row_of(0, r))

    def along_line(k, j):
        remote(
            shard_ref.at[k],
            slot_of(k, j, own_row),
            piece_sent.at[k, 0, j],
            piece_here.at[k, 0, 0, j],
            moved(here, s=j // 2, h=j % 2),
        ).start()

    def spread(source, k, j):
        send(source, k, j, 0, 1, 0, 1, x=1)
        send(source, k, j, 0, 2, 0, 2, y=1)
        send(source, k, j, 0, 4, 1, 0, c=1)

    def line(k, j):
        if j:
            arrived(k, 0, 0, j)
        spread(piece(k, j, 0) if j else shard_ref.at[k], k, j)

    def relay(k, j):
        arrived(k, 0, 1, j)
        send(piece(k, j, 1), k, j, 1, 5, 1, 1, c=1)
        arrived(k, 0, 2, j)
        send(piece(k, j, 2), k, j, 2, 6, 1, 2, c=1)
        if j == 1 and k in LINE_ACROSS:
            return
        up = (j // 2 + k) % 2
        source = slot_of(k, j, dp_row(here, y=up, x=1 - up))
        remote(
            source,
            source,
            piece_sent.at[k, 3, j],
            piece_here.at[k, 0, 3, j],
            moved(here, y=1 - up, x=up),
        ).start()

    def across(k, j):
        arrived(k, 0, 3, j)
        send(piece(k, j, 3), k, j, 3, 7, 1, 3, c=1)
        if j == 0 and k in LINE_ACROSS:
            remote(
                piece(k, 0, 3),
                piece(k, 1, 3),
                piece_sent.at[k, 3, 1],
                piece_here.at[k, 0, 3, 1],
                moved(here, h=1),
            ).start()

    def fetch(k, t):
        return pltpu.make_async_copy(weight_ref.at[k, t], held.at[t], held_sem.at[t])

    def ready(k):
        for j in range(STEPS):
            for r in range(4):
                arrived(k, 1, r, j)
        for t in BLOCK_ORDER:
            fetch(k, t).start()

    def weight(k, t):
        fetch(k, t).wait()
        return held.at[t]

    def stored(k):
        return pltpu.make_async_copy(shard_ref.at[k], slot_of(k, 0, own_row), own_sem.at[k])

    half_lanes = keep.shape[4]
    swapped = (0, 2, 1, 3)

    def grad_rows(part, quad):
        row = dp_row(here, y=quad // 2, x=quad % 2, c=part)
        return pl.ds(pl.multiple_of(row * BLOCK_ROWS, BLOCK_ROWS), BLOCK_ROWS)

    def core_copy(step, quad):
        return remote(
            work.at[step % 2, grad_rows(1, quad)],
            came.at[step % 4, quad],
            core_sent.at[step % 2, quad],
            core_here.at[step % 4, quad],
            moved(here, c=1),
        )

    def quads_sent(step):
        return 1 if BLOCK_ORDER[step % STEPS] == 1 and step // STEPS in SUM_ACROSS else 2

    def first_copy(step, half):
        quads = quads_sent(step)
        return remote(
            keep.at[step, pl.ds(2, quads), half],
            first.at[step, half, pl.ds(0, quads)],
            first_sent.at[step, half],
            first_here.at[step, half],
            moved(here, y=1 - half, x=half),
        )

    def fourth_copy(index):
        return remote(
            keep.at[index * STEPS + BLOCK_ORDER.index(1), 3],
            fourth.at[index],
            fourth_sent.at[index],
            fourth_here.at[index],
            moved(here, h=1),
        )

    def second_copy(step, half):
        return remote(
            keep.at[step, 1, half],
            second.at[step, half],
            second_sent.at[step, half],
            second_here.at[step, half],
            moved(here, y=half, x=1 - half),
        )

    def third_copy(step):
        j = BLOCK_ORDER[step % STEPS]
        return remote(
            keep.at[step, 0],
            third.at[step],
            third_sent.at[step],
            third_here.at[step],
            moved(here, s=j // 2, h=j % 2),
        )

    def begin(step):
        @pl.when(step >= 2)
        def _():
            for quad in range(4):
                core_copy(step - 2, quad).wait_send()

        return work.at[step % 2]

    def emit(step):
        @pl.when(step >= 4)
        def _():
            pl.semaphore_wait(credit, 1)

        for quad in range(4):
            core_copy(step, quad).start()

    def take_core(step):
        block = BLOCK_ORDER[step % STEPS]
        for quad in range(4):
            core_copy(step, quad).wait_recv()
        for index in (2, 3, 1, 0):
            for half in range(2):
                quad = swapped[index] if half else index
                lanes = slice(half * half_lanes, (half + 1) * half_lanes)
                own = work[step % 2, grad_rows(0, quad), lanes].astype(F32)
                both = own + came[step % 4, quad, :, lanes].astype(F32)
                if index == 3 and block == 0 and step // STEPS in SUM_ACROSS:
                    if half == 0:
                        fourth_copy(step // STEPS).wait_recv()
                    both = both + fourth[step // STEPS, half].astype(F32)
                keep[step, index, half] = both.astype(BF16)
                if index == 1 + quads_sent(step):
                    first_copy(step, half).start()
            if index == 3 and block == 1 and step // STEPS in SUM_ACROSS:
                fourth_copy(step // STEPS).start()
        if step <= last - 4:
            pl.semaphore_signal(
                credit,
                inc=1,
                device_id=moved(here, c=1),
                device_id_type=pl.DeviceIdType.MESH,
            )

    def take_first(step):
        for half in range(2):
            first_copy(step, half).wait_recv()
            for index in (1, 0):
                if index < quads_sent(step):
                    both = keep[step, index, half].astype(F32) + first[step, half, index].astype(F32)
                    keep[step, index, half] = both.astype(BF16)
                if index:
                    second_copy(step, half).start()

    def take_second(step):
        for half in range(2):
            second_copy(step, half).wait_recv()
            both = keep[step, 0, half].astype(F32) + second[step, half].astype(F32)
            keep[step, 0, half] = both.astype(BF16)
        if BLOCK_ORDER[step % STEPS]:
            third_copy(step).start()

    def take_third(index):
        steps = [index * STEPS + i for i in range(STEPS)]
        for step in steps:
            if BLOCK_ORDER[step % STEPS]:
                third_copy(step).wait_recv()
        for half in range(2):
            total = jnp.zeros((BLOCK_ROWS, half_lanes), F32)
            for step in steps:
                source = third[step, half] if BLOCK_ORDER[step % STEPS] else keep[step, 0, half]
                total = total + source.astype(F32)
            own_ref[index, :, half * half_lanes : (half + 1) * half_lanes] = total
        stores[2 + index].start()

    events = {
        "zs": along_line,
        "line": line,
        "relay": relay,
        "across": across,
        "core": take_core,
        "first": take_first,
        "second": take_second,
        "third": take_third,
    }

    def follow(item):
        for name, *args in AFTER.get(item, ()):
            events[name](*args)

    def loop(name, body):
        def step(i, carry):
            body(i, (i + 1) % STEPS)
            for c in range(STEPS - 1):
                if AFTER.get((name, c)):

                    @pl.when(i == c)
                    def _(c=c):
                        follow((name, c))

            return carry

        lax.fori_loop(0, STEPS, step, 0)
        follow((name, STEPS - 1))

    def layer_norm(source_ref, gain, target_ref):
        def body(rows):
            centred, scale = row_stats(source_ref[rows, :])
            target_ref[rows, :] = (centred * scale * gains_ref[gain : gain + 1, :]).astype(
                target_ref.dtype
            )

        by_rows(count, body)

    def norm_back(source_ref, gain, grad_normed_ref):
        def body(rows):
            centred, scale = row_stats(source_ref[rows, :])
            unit = centred * scale
            grad_normed = grad_normed_ref[rows, :]
            e = grad_normed * gains_ref[gain : gain + 1, :]
            mean = jnp.mean(e, -1, keepdims=True)
            tilt = jnp.mean(e * unit, -1, keepdims=True)
            stream_ref[rows, :] += scale * (e - mean - unit * tilt)
            gain_sums[gain : gain + 1, :] += jnp.sum(grad_normed * unit, 0, keepdims=True)

        by_rows(count, body)

    def exchange(index):
        return Exchange(
            here,
            swap_out.at[index % 2],
            swap_back.at[index % 2],
            swap_sent.at[index],
            swap_here.at[index],
        )

    def attention(kind, k, normed_ref, heads_ref, mixed_ref):
        total_ref[...] = jnp.zeros_like(total_ref)

        def compute(i, t):
            total_ref[...] += attend_block(
                kind, t, normed_ref[...], weight(k, t), heads_ref, mixed_ref, mixed_sums
            )

        return compute

    def attention_back(kind, k, normed_ref, heads_ref, mixed_ref):
        total_ref[...] = jnp.zeros_like(total_ref)

        def compute(i, t):
            step = (CHUNKS - 1 - k) * STEPS + i
            out = begin(step)
            total_ref[...] += attend_back_block(
                kind,
                heads_ref.at[t],
                mixed_ref.at[t],
                low_ref,
                weight(k, t),
                grad_mixed,
                sums,
                grad_heads,
            )
            if k:
                fetch(k - 1, t).start()
            out[:, : 3 * width] = mm(normed_ref[...], grad_heads[...], TN).astype(BF16)
            out[:, 3 * width :] = mm(low_ref[...], mixed_ref[t], TN).astype(BF16)
            emit(step)

        return compute

    gain_parts[0, own_row] = gain_out[0]

    def gain_copy(r):
        flips = {"y": r // 4, "x": r // 2 % 2, "c": r % 2}
        return remote(
            gain_out.at[0],
            gain_parts.at[0, own_row],
            gain_sent.at[0, r],
            gain_here.at[0, r],
            moved(here, **flips),
        )

    for r in range(1, 8):
        gain_copy(r).start()
    for k in range(CHUNKS):
        stored(k).start()
    follow(("go",))
    loads[7].wait()

    def unit_rows(rows):
        centred, scale = row_stats(tokens_ref[rows, :])
        rows_ref[rows, :] = centred * scale

    by_rows(count, unit_rows)
    for r in range(1, 8):
        gain_copy(r).wait()
    for d in range(8):
        gains_ref[:, d * own_gains : (d + 1) * own_gains] = gain_parts[0, d, :, :own_gains]

    def scale_rows(rows):
        rows_ref[rows, :] = rows_ref[rows, :] * gains_ref[0:1, :]

    by_rows(count, scale_rows)
    swap = exchange(0)
    swap.send_frames(rows_ref)
    follow(("ln0",))
    loads[8].wait()

    def mask_rows(rows):
        stream_ref[rows, :] = stream_ref[rows, :] * live
        low_ref[rows, :] = stream_ref[rows, :].astype(BF16)

    by_rows(count, mask_rows)
    gain_sums[...] = jnp.zeros_like(gain_sums)
    follow(("mask",))
    swap.take_patches(patch_ref, normed_time_ref)
    for k in range(CHUNKS):
        stored(k).wait()
    follow(("takeE0",))

    ready(0)
    loop("P0", attention("time", 0, normed_time_ref, time_heads_ref, time_mixed_ref))
    swap = exchange(1)
    swap.send_patches(total_ref, patch_ref)
    follow(("exch1",))
    swap.take_frames(rows_ref)
    after_time_ref[...] = tokens_ref[...] + rows_ref[...]
    layer_norm(after_time_ref, 1, normed_space_ref)
    follow(("ln1",))

    ready(1)
    loop("P1", attention("space", 1, normed_space_ref, space_heads_ref, space_mixed_ref))
    after_space_ref[...] = after_time_ref[...] + total_ref[...]
    layer_norm(after_space_ref, 2, normed_mlp_ref)
    follow(("ln2",))

    ready(2)

    def up(i, t):
        out = begin(i)
        pre_act = mm(normed_mlp_ref[...], weight(2, t)[...])
        cdf = 0.5 * (1.0 + lax.erf(pre_act * 0.5**0.5))
        hidden_ref[t] = (pre_act * cdf).astype(BF16)
        density = jnp.exp(-0.5 * pre_act * pre_act) * (0.5 / math.pi) ** 0.5
        slope_ref[t] = (cdf + pre_act * density).astype(BF16)
        out[...] = mm(low_ref[...], hidden_ref[t], TN).astype(BF16)
        emit(i)

    loop("up", up)
    ready(3)
    out_ref[...] = after_space_ref[...]

    def down(i, t):
        out_ref[...] += mm(hidden_ref[t], weight(3, t)[...], NT)
        grad_hidden = mm(low_ref[...], held[t])
        slope_ref[t] = (grad_hidden * slope_ref[t].astype(F32)).astype(BF16)
        fetch(2, t).start()

    loop("dn", down)
    out_ref[...] = out_ref[...] * live
    stores[0].start()
    total_ref[...] = jnp.zeros_like(total_ref)

    def up_back(i, t):
        step = STEPS + i
        out = begin(step)
        total_ref[...] += mm(slope_ref[t], weight(2, t)[...], NT)
        fetch(1, t).start()
        out[...] = mm(normed_mlp_ref[...], slope_ref[t], TN).astype(BF16)
        emit(step)

    loop("B1", up_back)
    norm_back(after_space_ref, 2, total_ref)
    low_ref[...] = stream_ref[...].astype(BF16)
    follow(("nb2",))
    loop("B2", attention_back("space", 1, normed_space_ref, space_heads_ref, space_mixed_ref))
    norm_back(after_time_ref, 1, total_ref)
    swap = exchange(2)
    swap.send_frames(stream_ref)
    follow(("nb1",))
    swap.take_patches(patch_ref, low_ref)
    follow(("takeE2",))
    loop("B3", attention_back("time", 0, normed_time_ref, time_heads_ref, time_mixed_ref))
    swap = exchange(3)
    swap.send_patches(total_ref, patch_ref)
    follow(("exch3",))
    swap.take_frames(rows_ref)
    norm_back(tokens_ref, 0, rows_ref)
    stores[1].start()

    line_index = here["s"] * 2 + here["h"]

    def gain_back(r):
        flips = {"y": r // 4, "x": r // 2 % 2, "c": r % 2}
        return remote(
            gain_out.at[dp_row(here, **flips)],
            gain_parts.at[1, own_row],
            gain_sent.at[1, r],
            gain_here.at[1, r],
            moved(here, **flips),
        )

    def gain_line_copy(j):
        return remote(
            own_gain_ref,
            gain_line.at[line_index],
            gain_sent.at[2, j],
            gain_here.at[2, j],
            moved(here, s=j // 2, h=j % 2),
        )

    total = gain_sums[...]
    for d in range(8):
        gain_out[d, :, :own_gains] = total[:, d * own_gains : (d + 1) * own_gains]
    for r in range(1, 8):
        gain_back(r).start()
    gain_parts[1, own_row] = gain_out[own_row]
    follow(("nb0",))
    for r in range(1, 8):
        gain_back(r).wait()
    total = gain_parts[1, 0]
    for d in range(1, 8):
        total = total + gain_parts[1, d]
    own_gain_ref[...] = total
    for j in range(1, 4):
        gain_line_copy(j).start()
    gain_line[line_index] = total
    follow(("gain",))
    for j in range(1, 4):
        gain_line_copy(j).wait()
    own_gain_ref[...] = gain_line[0] + gain_line[1] + gain_line[2] + gain_line[3]
    stores[2 + CHUNKS].start()

    for k in range(CHUNKS):
        for sem in range(8):
            for j in range(4):
                if sem or j:
                    slot = slot_of(k, 0, own_row)
                    remote(
                        slot,
                        slot,
                        piece_sent.at[k, sem, j],
                        piece_here.at[k, 0, 0, 0],
                        moved(here, c=1),
                    ).wait_send()
    for step in range(last + 1):
        if step > last - 2:
            for quad in range(4):
                core_copy(step, quad).wait_send()
        for half in range(2):
            first_copy(step, half).wait_send()
            second_copy(step, half).wait_send()
        if BLOCK_ORDER[step % STEPS]:
            third_copy(step).wait_send()
    for index in SUM_ACROSS:
        fourth_copy(index).wait_send()
    for store in stores:
        store.wait()


def layer(live_clips, tokens, cotangent, norm_gains, *weights):
    count, columns = tokens.shape
    rows, lanes = weights[4].shape
    half = lanes // 2
    width, steps = lanes // 4, CHUNKS * STEPS
    there = pl.BlockSpec(memory_space=pl.ANY)
    outputs = (
        shaped(CHUNKS, STEPS, columns, lanes),
        shaped(count, columns, dtype=F32),
        shaped(count, columns, dtype=F32),
        shaped(CHUNKS, rows, lanes, dtype=F32),
        shaped(8, 128, dtype=F32),
    )
    return pl.pallas_call(
        layer_kernel,
        in_specs=[pl.BlockSpec(memory_space=pltpu.SMEM)] + [there] * 9,
        out_specs=[there] * len(outputs),
        out_shape=outputs,
        scratch_shapes=[
            pltpu.VMEM((count, columns), F32),
            pltpu.VMEM((count, columns), F32),
            pltpu.VMEM((CHUNKS, rows, lanes), F32),
            pltpu.VMEM((8, 128), F32),
            pltpu.VMEM((count, columns), F32),
            pltpu.VMEM(norm_gains.shape, BF16),
            *[pltpu.VMEM(w.shape, BF16) for w in weights[:4]],
            pltpu.VMEM((CHUNKS, rows, lanes), BF16),
            pltpu.VMEM((STEPS, columns, lanes), BF16),
            pltpu.VMEM((count, columns), BF16),
            pltpu.VMEM((STEPS, count, 3 * width), BF16),
            pltpu.VMEM((STEPS, count, width), BF16),
            pltpu.VMEM((count, columns), F32),
            pltpu.VMEM((count, columns), BF16),
            pltpu.VMEM((STEPS, count, 3 * width), BF16),
            pltpu.VMEM((STEPS, count, width), BF16),
            pltpu.VMEM((count, columns), F32),
            pltpu.VMEM((count, columns), BF16),
            pltpu.VMEM((STEPS, count, lanes), BF16),
            pltpu.VMEM((STEPS, count, lanes), BF16),
            pltpu.VMEM((count, columns), BF16),
            pltpu.VMEM((count, columns), F32),
            pltpu.VMEM((columns // 128, count, 128), F32),
            pltpu.VMEM((count, columns), F32),
            pltpu.VMEM((count, width), F32),
            pltpu.VMEM((count, 3 * width), F32),
            pltpu.VMEM((count, width), BF16),
            pltpu.VMEM((count, 3 * width), BF16),
            pltpu.VMEM((2, columns, lanes), BF16),
            pltpu.VMEM((steps, 4, 2, rows, half), BF16),
            pltpu.VMEM((4, 4, rows, lanes), BF16),
            pltpu.VMEM((steps, 2, 2, rows, half), BF16),
            pltpu.VMEM((steps, 2, rows, half), BF16),
            pltpu.VMEM((steps, 2, rows, half), BF16),
            pltpu.VMEM((CHUNKS, 2, rows, half), BF16),
            pltpu.VMEM((8, columns), F32),
            pltpu.VMEM((8, columns), F32),
            pltpu.VMEM((4, 8, 128), F32),
            pltpu.VMEM((8, 8, 128), F32),
            pltpu.VMEM((2, 8, 8, 128), F32),
            pltpu.VMEM((2, 4, 2, PAD, columns), BF16),
            pltpu.VMEM((2, 4, 2, PAD, columns), BF16),
            pltpu.SemaphoreType.DMA((CHUNKS, 8, 4)),
            pltpu.SemaphoreType.DMA((CHUNKS, 2, 4, 4)),
            pltpu.SemaphoreType.DMA((2, 4)),
            pltpu.SemaphoreType.DMA((4, 4)),
            pltpu.SemaphoreType.DMA((steps, 2)),
            pltpu.SemaphoreType.DMA((steps, 2)),
            pltpu.SemaphoreType.DMA((steps, 2)),
            pltpu.SemaphoreType.DMA((steps, 2)),
            pltpu.SemaphoreType.DMA((steps,)),
            pltpu.SemaphoreType.DMA((steps,)),
            pltpu.SemaphoreType.DMA((CHUNKS,)),
            pltpu.SemaphoreType.DMA((CHUNKS,)),
            pltpu.SemaphoreType.DMA((3, 8)),
            pltpu.SemaphoreType.DMA((3, 8)),
            pltpu.SemaphoreType.DMA((4, 4)),
            pltpu.SemaphoreType.DMA((4, 4)),
            pltpu.SemaphoreType.DMA((STEPS,)),
            pltpu.SemaphoreType.DMA((CHUNKS,)),
            pltpu.SemaphoreType.DMA((9,)),
            pltpu.SemaphoreType.DMA((3 + CHUNKS,)),
            pltpu.SemaphoreType.REGULAR,
        ],
        compiler_params=pltpu.CompilerParams(
            collective_id=0, has_side_effects=True, vmem_limit_bytes=67043328
        ),
        name="layer",
    )(live_clips, tokens, cotangent, norm_gains, *weights)[1:]


def finish_kernel(output_hbm, grad_hbm, own_hbm, gain_ref, *rest):
    targets, buffers, own_ref, load_sem, store_sem = rest[:9], rest[9:18], *rest[18:]
    output, grad, gains, time_in, time_out, space_in, space_out, up, down = buffers
    width = time_in.shape[2]
    sources = [(own_hbm.at[k], into) for k, into in ((0, down), (1, up))]
    sources += [(own_hbm.at[k], own_ref.at[k - 2]) for k in (2, 3)]
    sources += [(output_hbm, output), (grad_hbm, grad)]
    loads = [pltpu.make_async_copy(*pair, load_sem.at[i]) for i, pair in enumerate(sources)]
    stores = [
        pltpu.make_async_copy(*pair, store_sem.at[i]) for i, pair in enumerate(zip(buffers, targets))
    ]
    for i in (2, 3, 0, 1, 4, 5):
        loads[i].start()
    gains[...] = gain_ref[: gains.shape[0], : gains.shape[1]]
    stores[2].start()
    for k, load, into, out, low in ((0, 2, space_in, space_out, 5), (1, 3, time_in, time_out, 3)):
        loads[load].wait()
        for c in range(3):
            into[c] = own_ref[k, :, c * width : (c + 1) * width]
        stores[low].start()
        out[...] = own_ref[k, :, 3 * width :].T
        stores[low + 1].start()
    for load, store in ((0, 8), (1, 7), (4, 0), (5, 1)):
        loads[load].wait()
        stores[store].start()
    for store in stores:
        store.wait()


def finish(output, grad, own, gain, like):
    shapes = [jax.ShapeDtypeStruct(a.shape, F32) for a in like]
    there = pl.BlockSpec(memory_space=pl.ANY)
    return pl.pallas_call(
        finish_kernel,
        in_specs=[there] * 3 + [pl.BlockSpec(memory_space=pltpu.VMEM)],
        out_specs=[there] * len(shapes),
        out_shape=shapes,
        scratch_shapes=[
            *[pltpu.VMEM(a.shape, F32) for a in like],
            pltpu.VMEM((2,) + own.shape[1:], F32),
            pltpu.SemaphoreType.DMA((6,)),
            pltpu.SemaphoreType.DMA((len(shapes),)),
        ],
        name="finish",
    )(output, grad, own, gain)


def sum_gains(total, own):
    for axes in ("c", "x", "y", TENSOR):
        bit = 1
        while bit < lax.axis_size(axes):
            total = total + along(total, axes, bit)
            bit *= 2
    return lax.dynamic_slice_in_dim(total, lax.axis_index(DP) * own, own, 1)


def on_device(
    routed,
    tokens,
    live_clips,
    norm_gains,
    qkv_time,
    out_time,
    qkv_space,
    out_space,
    up_weight,
    down_weight,
    cotangent,
):
    members = lax.axis_size("c") * lax.axis_size("h")
    share = PATCHES // members
    count, columns = tokens.shape
    width = qkv_time.shape[2]
    live = jnp.where(lax.axis_index("s") < live_clips[0], 1.0, 0.0).astype(F32)

    def pack_heads(qkv, out):
        rows = qkv.shape[1]
        return jnp.concatenate([qkv.transpose(1, 0, 2).reshape(rows, -1), out.T], 1)

    if routed:
        weights = (qkv_time, out_time, qkv_space, out_space, up_weight, down_weight.T)
        done = layer(live_clips, tokens, cotangent, norm_gains, *weights)
        *found, down_own = finish(*done, (tokens, cotangent, norm_gains, *weights))
        return (*found, down_own.T)
    shards = [
        pack_heads(qkv_time, out_time),
        pack_heads(qkv_space, out_space),
        up_weight,
        down_weight.T,
    ]
    grad_stream = cotangent * live
    time_all, space_all, up_all, down_all = [gather_plain(shard) for shard in shards]
    blocks, depth, lanes = up_all.shape
    gains = lax.all_gather(norm_gains, DP, axis=1, tiled=True).astype(F32)
    normed_time = to_patches(normalize(tokens, gains[0]).astype(BF16), members)
    time_heads, time_mixed, change = attend("time", normed_time, time_all, share, BF16)
    after_time = tokens + to_frames(change, members).astype(F32)
    normed_space = normalize(after_time, gains[1]).astype(BF16)
    space_heads, space_mixed, change = attend("space", normed_space, space_all, 1, F32)
    after_space = after_time + change
    normed_mlp = normalize(after_space, gains[2]).astype(BF16)
    hidden, slope = phase(
        up_kernel,
        "up",
        (normed_mlp, up_all),
        (shaped(blocks, count, lanes), shaped(blocks, count, lanes)),
        cost=12,
    )
    (change,) = phase(
        down_kernel, "down", (hidden, down_all), (shaped(count, depth, dtype=F32),), cost=4
    )
    after_mlp = after_space + change
    grad_low = grad_stream.astype(BF16)
    work = (pltpu.VMEM((depth, lanes), BF16),)
    *down_grads, grad_pre = phase(
        down_back_kernel,
        "down_back",
        (grad_low, down_all, hidden, slope),
        (*grad_shapes(down_all, False), shaped(blocks, count, lanes)),
        work,
        cost=8,
    )
    *up_grads, grad_normed = phase(
        up_back_kernel,
        "up_back",
        (normed_mlp, up_all, grad_pre),
        (*grad_shapes(up_all, False), shaped(count, depth, dtype=F32)),
        work,
        cost=8,
    )
    grad_part, gain_mlp = norm_back(after_space, gains[2], grad_normed)
    grad_stream = grad_stream + grad_part
    space_grads, grad_normed = attend_back(
        "space",
        normed_space,
        space_all,
        space_heads,
        space_mixed,
        grad_stream.astype(BF16),
        1,
        F32,
        False,
    )
    grad_part, gain_space = norm_back(after_time, gains[1], grad_normed)
    grad_stream = grad_stream + grad_part
    grad_low = to_patches(grad_stream.astype(BF16), members)
    time_grads, grad_normed = attend_back(
        "time", normed_time, time_all, time_heads, time_mixed, grad_low, share, BF16, routed
    )
    grad_normed = to_frames(grad_normed, members).astype(F32)
    grad_part, gain_time = norm_back(tokens, gains[0], grad_normed)
    grad_tokens = grad_stream + grad_part
    down_own = reduce_plain(down_grads).T
    up_own = reduce_plain(up_grads)
    space_own = reduce_plain(space_grads)
    time_own = reduce_plain(time_grads)
    gains_own = sum_gains(jnp.stack([gain_time, gain_space, gain_mlp]), norm_gains.shape[1])
    output = after_mlp * live

    def unpack(own):
        rows = own.shape[0]
        return own[:, : 3 * width].reshape(rows, 3, width).transpose(1, 0, 2), own[:, 3 * width :].T

    time_in_own, time_out_own = unpack(time_own)
    space_in_own, space_out_own = unpack(space_own)
    return (
        output,
        grad_tokens,
        gains_own,
        time_in_own,
        time_out_own,
        space_in_own,
        space_out_own,
        up_own,
        down_own,
    )


def solution(mesh):
    n_dp, n_tensor = mesh.devices.shape

    def run(*args):
        slots = args[0].shape[0] // (n_dp * HALF * PATCHES)
        fine = Mesh(mesh.devices.reshape(n_dp // 4, 2, 2, slots, n_tensor // slots), ALL)
        in_specs = (
            P(ALL, None),
            P(DP),
            P(None, DP),
            P(None, DP, TENSOR),
            P(TENSOR, DP),
            P(None, DP, TENSOR),
            P(TENSOR, DP),
            P(DP, TENSOR),
            P(TENSOR, DP),
            P(ALL, None),
        )
        out_specs = (in_specs[0], in_specs[0]) + in_specs[2:9]
        routed = fine.devices.shape == (2, 2, 2, 2, 2)
        return jax.shard_map(
            functools.partial(on_device, routed), mesh=fine, in_specs=in_specs, out_specs=out_specs, check_vma=False
        )(*args)

    return run
```

```python
import functools
import math

import jax
import jax.numpy as jnp
from jax import lax
from jax.experimental import pallas as pl
from jax.experimental.pallas import tpu as pltpu
from jax.sharding import Mesh, PartitionSpec as P

HEAD_DIM = 64
PATCHES = 196
HALF = 4
FRAMES = 8
EPSILON = 1e-06
F32 = jnp.float32
BF16 = jnp.bfloat16
ALL = ("y", "x", "c", "s", "h")
DP = ("y", "x", "c")
TENSOR = ("s", "h")
CLIP = ("c", "h")

NN = (((1,), (0,)), ((), ()))
NT = (((1,), (1,)), ((), ()))
TN = (((0,), (0,)), ((), ()))
BLOCK_ROWS = 96


def mm(a, b, dims=NN):
    return lax.dot_general(a, b, dims, preferred_element_type=F32)


def row_ids(shape, dim, start):
    return lax.broadcasted_iota(jnp.int32, shape, dim) + start


def windows(kind, count):
    if kind == "time":
        return [(0, count, None)]
    found = []
    for frame in range(count // PATCHES):
        low = frame * PATCHES // 16 * 16
        high = min(count, -(-(frame + 1) * PATCHES // 16) * 16)
        found.append((low, high - low, frame))
    return found


def key_bias(start, size, group, stride):
    keys = row_ids((size, size), 0, start)
    if group is None:
        together = keys % stride == row_ids((size, size), 1, start) % stride
    else:
        together = (keys >= group * PATCHES) & (keys < (group + 1) * PATCHES)
    return jnp.where(together, 0.0, -1e30)


def row_valid(start, size, group, width):
    rows = row_ids((size, width), 0, start)
    return (rows >= group * PATCHES) & (rows < (group + 1) * PATCHES)


def normalize(rows, scale_row):
    average = jnp.mean(rows, -1, keepdims=True)
    centred = rows - average
    spread = jnp.mean(centred * centred, -1, keepdims=True)
    return centred * lax.rsqrt(spread + EPSILON) * scale_row


def norm_back(rows, scale_row, grad_normed):
    unused, pullback = jax.vjp(normalize, rows, scale_row)
    return pullback(grad_normed)


def row_block(core, part, quad):
    quad_me = lax.axis_index(("y", "x"))
    block = jnp.bitwise_xor(quad_me, quad) * 2 + jnp.bitwise_xor(core, part)
    return pl.multiple_of(block * BLOCK_ROWS, BLOCK_ROWS)


def head_slices(ref, rows, width, head):
    low = head * HEAD_DIM
    return tuple(ref[rows, part * width + low : part * width + low + HEAD_DIM] for part in range(3))


def put_grads(work, outs):
    if len(outs) == 1:
        outs[0][...] = work[...]
        return
    core = lax.axis_index("c")
    for part, out in enumerate(outs):
        for quad in range(out.shape[0]):
            out[quad] = work[pl.ds(row_block(core, part, quad), out.shape[1]), :]


def attend_kernel(kind, stride, normed_ref, weight_ref, heads_ref, mixed_ref, out_ref, sums, total_ref):
    step = pl.program_id(0)
    count, width = mixed_ref.shape
    heads_ref[...] = mm(normed_ref[...], weight_ref[:, : 3 * width]).astype(BF16)
    sums[...] = jnp.zeros_like(sums)
    for start, size, group in windows(kind, count):
        bias = key_bias(start, size, group, stride)
        rows = pl.ds(start, size)
        for head in range(width // HEAD_DIM):
            low = head * HEAD_DIM
            query, key, value = head_slices(heads_ref, rows, width, head)
            scores = mm(key, query * HEAD_DIM**-0.5, NT) + bias
            weights = jnp.exp(scores - jnp.max(scores, 0, keepdims=True))
            total = jnp.sum(weights, 0, keepdims=True)
            blended = (mm(value.T, weights.astype(BF16)) / total).T
            if group is not None:
                blended = jnp.where(row_valid(start, size, group, HEAD_DIM), blended, 0.0)
            sums[rows, low : low + HEAD_DIM] += blended
    mixed_ref[...] = sums[...].astype(BF16)
    share = mm(mixed_ref[...], weight_ref[:, 3 * width :], NT)

    @pl.when(step == 0)
    def _():
        total_ref[...] = share

    @pl.when(step > 0)
    def _():
        total_ref[...] += share

    @pl.when(step == pl.num_programs(0) - 1)
    def _():
        out_ref[...] = total_ref[...].astype(out_ref.dtype)


def attend_back_kernel(
    kind, stride, normed_ref, weight_ref, heads_ref, mixed_ref, grad_ref, *rest
):
    outs, (out_ref, sums, total_ref, grad_mixed, grad_heads, work) = rest[:-6], rest[-6:]
    step = pl.program_id(0)
    count, width = mixed_ref.shape
    scale = HEAD_DIM**-0.5
    grad_mixed[...] = mm(grad_ref[...], weight_ref[:, 3 * width :]).astype(BF16)
    sums[...] = jnp.zeros_like(sums)
    for start, size, group in windows(kind, count):
        bias = key_bias(start, size, group, stride)
        rows = pl.ds(start, size)
        for head in range(width // HEAD_DIM):
            low = head * HEAD_DIM
            query, key, value = head_slices(heads_ref, rows, width, head)
            query = query * scale
            grad = grad_mixed[rows, low : low + HEAD_DIM]
            if group is not None:
                valid = row_valid(start, size, group, HEAD_DIM)
                grad = jnp.where(valid, grad.astype(F32), 0.0).astype(BF16)
            scores = mm(key, query, NT) + bias
            weights = jnp.exp(scores - jnp.max(scores, 0, keepdims=True))
            weights = weights / jnp.sum(weights, 0, keepdims=True)
            grad_weights = mm(value, grad, NT)
            row_terms = jnp.sum(weights * grad_weights, 0, keepdims=True)
            grad_scores = (weights * (grad_weights - row_terms)).astype(BF16)
            sums[rows, low : low + HEAD_DIM] += (mm(key.T, grad_scores) * scale).T
            low += width
            sums[rows, low : low + HEAD_DIM] += mm(grad_scores, query)
            low += width
            sums[rows, low : low + HEAD_DIM] += mm(weights.astype(BF16), grad)
    grad_heads[...] = sums[...].astype(BF16)
    share = mm(grad_heads[...], weight_ref[:, : 3 * width], NT)

    @pl.when(step == 0)
    def _():
        total_ref[...] = share

    @pl.when(step > 0)
    def _():
        total_ref[...] += share

    @pl.when(step == pl.num_programs(0) - 1)
    def _():
        out_ref[...] = total_ref[...].astype(out_ref.dtype)

    work[:, : 3 * width] = mm(normed_ref[...], grad_heads[...], TN).astype(BF16)
    work[:, 3 * width :] = mm(grad_ref[...], mixed_ref[...], TN).astype(BF16)
    put_grads(work, outs)


def up_kernel(normed_ref, weight_ref, hidden_ref, slope_ref):
    pre_act = mm(normed_ref[...], weight_ref[...])
    cdf = 0.5 * (1.0 + lax.erf(pre_act * 0.5**0.5))
    hidden_ref[...] = (pre_act * cdf).astype(BF16)
    density = jnp.exp(-0.5 * pre_act * pre_act) * (0.5 / math.pi) ** 0.5
    slope_ref[...] = (cdf + pre_act * density).astype(slope_ref.dtype)


def down_kernel(hidden_ref, weight_ref, out_ref):
    share = mm(hidden_ref[...], weight_ref[...], NT)

    @pl.when(pl.program_id(0) == 0)
    def _():
        out_ref[...] = share

    @pl.when(pl.program_id(0) > 0)
    def _():
        out_ref[...] += share


def down_back_kernel(grad_ref, weight_ref, hidden_ref, slope_ref, *rest):
    outs, (grad_pre_ref, work) = rest[:-2], rest[-2:]
    grad_hidden = mm(grad_ref[...], weight_ref[...])
    grad_pre_ref[...] = (grad_hidden * slope_ref[...].astype(F32)).astype(BF16)
    work[...] = mm(grad_ref[...], hidden_ref[...], TN).astype(BF16)
    put_grads(work, outs)


def up_back_kernel(normed_ref, weight_ref, grad_pre_ref, *rest):
    outs, (out_ref, work) = rest[:-2], rest[-2:]
    share = mm(grad_pre_ref[...], weight_ref[...], NT)

    @pl.when(pl.program_id(0) == 0)
    def _():
        out_ref[...] = share

    @pl.when(pl.program_id(0) > 0)
    def _():
        out_ref[...] += share

    work[...] = mm(normed_ref[...], grad_pre_ref[...], TN).astype(BF16)
    put_grads(work, outs)


def whole_spec(array):
    return pl.BlockSpec(array.shape, lambda i: (0,) * array.ndim)


def step_spec(array):
    rest = array.shape[1:]
    return pl.BlockSpec((None,) + rest, lambda i: (i,) + (0,) * len(rest))


def phase(kernel, name, inputs, outputs, scratch=(), cost=0):
    blocks = [a for a in inputs if a.ndim > 2][0].shape[0]
    spec = lambda a: whole_spec(a) if a.ndim == 2 else step_spec(a)
    return pl.pallas_call(
        kernel,
        grid=(blocks,),
        in_specs=[spec(a) for a in inputs],
        out_specs=[spec(a) for a in outputs],
        out_shape=outputs,
        scratch_shapes=list(scratch),
        cost_estimate=pl.CostEstimate(
            flops=int(cost * 800e6), bytes_accessed=int(cost * 1e6), transcendentals=0
        ),
        name=name,
    )(*inputs)


def shaped(*shape, dtype=BF16):
    return jax.ShapeDtypeStruct(shape, dtype)


def grad_shapes(weight, routed):
    blocks, depth, lanes = weight.shape
    if not routed:
        return [shaped(blocks, depth, lanes)]
    rows = BLOCK_ROWS
    return [shaped(blocks, depth // rows // 2, rows, lanes) for part in range(2)]


def attend(kind, normed, weight, stride, out_dtype):
    blocks, depth, lanes = weight.shape
    count, width = normed.shape[0], lanes // 4
    return phase(
        functools.partial(attend_kernel, kind, stride),
        kind + "_attend",
        (normed, weight),
        (
            shaped(blocks, count, 3 * width),
            shaped(blocks, count, width),
            shaped(count, depth, dtype=out_dtype),
        ),
        (pltpu.VMEM((count, width), F32), pltpu.VMEM((count, depth), F32)),
        cost=14,
    )


def attend_back(kind, normed, weight, heads, mixed, grad, stride, out_dtype, routed):
    blocks, depth, lanes = weight.shape
    count, width = normed.shape[0], lanes // 4
    *grads, out = phase(
        functools.partial(attend_back_kernel, kind, stride),
        kind + "_attend_back",
        (normed, weight, heads, mixed, grad),
        (*grad_shapes(weight, routed), shaped(count, depth, dtype=out_dtype)),
        (
            pltpu.VMEM((count, 3 * width), F32),
            pltpu.VMEM((count, depth), F32),
            pltpu.VMEM((count, width), BF16),
            pltpu.VMEM((count, 3 * width), BF16),
            pltpu.VMEM((depth, lanes), BF16),
        ),
        cost=20,
    )
    return grads, out


def along(piece, axes, distance):
    size = lax.axis_size(axes)
    return lax.ppermute(piece, axes, [(i, i ^ distance) for i in range(size)])


def after(piece, earlier):
    return piece + earlier[:1, :1] * 0


def gather_plain(shard):
    every = lax.all_gather(shard, TENSOR, axis=0, tiled=False)
    return lax.all_gather(every.reshape(-1, *shard.shape), DP, axis=1, tiled=True)


def reduce_plain(grads):
    part = lax.psum_scatter(grads[0], TENSOR, scatter_dimension=0, tiled=True)[0]
    return lax.psum_scatter(part, DP, scatter_dimension=0, tiled=True).astype(F32)


def by_member(parts, me):
    return jnp.stack(
        [
            lax.dynamic_index_in_dim(parts, jnp.bitwise_xor(me, k), 0, keepdims=False)
            for k in range(parts.shape[0])
        ]
    )


def to_patches(rows, members):
    share, columns = PATCHES // members, rows.shape[1]
    me = lax.axis_index(CLIP)
    parts = rows.reshape(-1, members, share, columns).transpose(1, 0, 2, 3)
    parts = [
        lax.dynamic_index_in_dim(parts, jnp.bitwise_xor(me, k), 0, keepdims=False)
        for k in range(members)
    ]
    parts = [parts[0]] + [along(parts[k], CLIP, k) for k in range(1, members)]
    return by_member(jnp.stack(parts), me).reshape(-1, columns)


def to_frames(rows, members):
    share, columns = PATCHES // members, rows.shape[1]
    me = lax.axis_index(CLIP)
    parts = by_member(rows.reshape(members, -1, share, columns), me)
    parts = [parts[0]] + [along(parts[k], CLIP, k) for k in range(1, members)]
    parts = jnp.stack(parts)
    order = jnp.bitwise_xor(me, jnp.arange(members))
    parts = [
        lax.dynamic_index_in_dim(parts, jnp.bitwise_xor(me, k), 0, keepdims=False)
        for k in range(members)
    ]
    return jnp.stack(parts, 1).reshape(-1, columns)


CHUNKS = 4
STEPS = 4
PAD = 56


def place():
    return {axis: lax.axis_index(axis) for axis in ALL}


def moved(here, **flips):
    return tuple(here[a] + flips.get(a, 0) * (1 - 2 * here[a]) for a in ALL)


def dp_row(here, y=0, x=0, c=0):
    to = lambda a, flip: here[a] + flip * (1 - 2 * here[a])
    return to("y", y) * 4 + to("x", x) * 2 + to("c", c)


def remote(source, target, sent, received, device):
    return pltpu.make_async_remote_copy(
        src_ref=source,
        dst_ref=target,
        send_sem=sent,
        recv_sem=received,
        device_id=device,
        device_id_type=pl.DeviceIdType.MESH,
    )


def peers(here):
    found = [moved(here, s=j // 2, h=j % 2) for j in range(1, 4)]
    found += [moved(here, y=r // 4, x=r // 2 % 2, c=r % 2) for r in range(1, 8)]
    return found + [moved(here, c=1, h=1)]


def greet(here, what):
    barrier = pltpu.get_barrier_semaphore()
    everyone = peers(here)
    if what == "answer":
        pl.semaphore_wait(barrier, len(everyone))
        return
    for device in everyone:
        pl.semaphore_signal(
            barrier, inc=1, device_id=device, device_id_type=pl.DeviceIdType.MESH
        )


class Exchange:
    def __init__(self, here, out, back, sent, received):
        self.here, self.out, self.back = here, out, back
        self.sent, self.received = sent, received
        self.me = here["c"] * 2 + here["h"]

    def device(self, member):
        return tuple({"c": member // 2, "h": member % 2}.get(a, self.here[a]) for a in ALL)

    def start(self, member):
        @pl.when(self.me != member)
        def _():
            remote(
                self.out.at[member],
                self.back.at[self.me],
                self.sent.at[member],
                self.received.at[self.me],
                self.device(member),
            ).start()

        @pl.when(self.me == member)
        def _():
            self.back[member] = self.out[member]

    def finish(self, member):
        @pl.when(self.me != member)
        def _():
            remote(
                self.out.at[member],
                self.back.at[member],
                self.sent.at[member],
                self.received.at[member],
                self.device(member),
            ).wait()

    def send(self, rows_ref, rows_of):
        share = PATCHES // 4
        for member in range(4):
            for frame in range(2):
                rows = rows_of(member, frame)
                self.out[member, frame, :share, :] = rows_ref[rows, :].astype(BF16)
            self.start(member)

    def take(self, rows_ref, rows_of):
        share = PATCHES // 4
        for member in range(4):
            self.finish(member)
            for frame in range(2):
                rows = rows_of(member, frame)
                rows_ref[rows, :] = self.back[member, frame, :share, :].astype(F32)

    @staticmethod
    def by_frame(member, frame):
        low = frame * PATCHES + member * (PATCHES // 4)
        return slice(low, low + PATCHES // 4)

    @staticmethod
    def by_share(member, frame):
        return pl.ds(member * 2 + frame, PATCHES // 4, stride=FRAMES)

    def parts(self, patch_ref):
        for block in range(patch_ref.shape[0]):
            yield block, slice(block * 128, (block + 1) * 128)

    def send_frames(self, rows_ref):
        self.send(rows_ref, self.by_frame)

    def take_patches(self, patch_ref, low_ref):
        share = PATCHES // 4
        for member in range(4):
            self.finish(member)
            for frame in range(2):
                for block, lanes in self.parts(patch_ref):
                    patch_ref[block, self.by_share(member, frame), :] = self.back[
                        member, frame, :share, lanes
                    ].astype(F32)
        for block, lanes in self.parts(patch_ref):
            low_ref[:, lanes] = patch_ref[block].astype(BF16)

    def send_patches(self, rows_ref, patch_ref):
        share = PATCHES // 4
        for block, lanes in self.parts(patch_ref):
            patch_ref[block] = rows_ref[:, lanes]
        for member in range(4):
            for frame in range(2):
                for block, lanes in self.parts(patch_ref):
                    self.out[member, frame, :share, lanes] = patch_ref[
                        block, self.by_share(member, frame), :
                    ].astype(BF16)
            self.start(member)

    def take_frames(self, rows_ref):
        self.take(rows_ref, self.by_frame)


def by_rows(count, body, size=56):
    def step(i, carry):
        body(pl.ds(pl.multiple_of(i * size, size), size))
        return carry

    lax.fori_loop(0, count // size, step, 0)


def row_stats(rows):
    average = jnp.mean(rows, -1, keepdims=True)
    centred = rows - average
    spread = jnp.mean(centred * centred, -1, keepdims=True)
    return centred, lax.rsqrt(spread + EPSILON)


def attention_units(kind, count, width):
    found = []
    if kind == "time":
        tile = 96
        starts = list(range(0, count - tile, tile))
        ends = starts[1:] + [count]
    else:
        starts = [low for low, size, group in windows(kind, count)]
        ends = [low + size for low, size, group in windows(kind, count)]
    for index, (start, end) in enumerate(zip(starts, ends)):
        size = end - start
        keys = row_ids((size, size), 0, 0)
        first, final = 0, size
        if kind == "time":
            together = keys // FRAMES == row_ids((size, size), 1, 0) // FRAMES
        else:
            first = index * PATCHES - start
            final = first + PATCHES
            together = (keys >= first) & (keys < final)
        bias = jnp.where(together, 0.0, -1e30)
        found += [(start, size, first, final, bias, head) for head in range(width // HEAD_DIM)]
    return found


def attend_block(kind, t, normed, weight, heads_ref, mixed_ref, sums):
    count, width = mixed_ref.shape[1:]
    heads_ref[t] = mm(normed, weight[:, : 3 * width]).astype(BF16)
    heads = heads_ref.at[t]
    target = mixed_ref.at[t] if kind == "time" else sums
    units = attention_units(kind, count, width)
    batch_size = 12 if kind == "time" else 6
    for batch in range(0, len(units), batch_size):
        some = units[batch : batch + batch_size]
        parts = [head_slices(heads, pl.ds(u[0], u[1]), width, u[5]) for u in some]
        scores = [
            mm(key, query * HEAD_DIM**-0.5, NT) + u[4] for u, (query, key, value) in zip(some, parts)
        ]
        weights = [jnp.exp(x - jnp.max(x, 0, keepdims=True)) for x in scores]
        scales = [1.0 / jnp.sum(x, 0, keepdims=True) for x in weights]
        blended = [
            (mm(value.T, x.astype(BF16)) * scale).T
            for x, scale, (query, key, value) in zip(weights, scales, parts)
        ]
        for (start, size, first, final, bias, head), x in zip(some, blended):
            lanes = slice(head * HEAD_DIM, (head + 1) * HEAD_DIM)
            target[start + first : start + final, lanes] = x[first:final].astype(target.dtype)
    if kind != "time":
        mixed_ref[t] = sums[...].astype(BF16)
    return mm(mixed_ref[t], weight[:, 3 * width :], NT)


def attend_back_block(kind, heads, mixed, grad, weight, grad_mixed, sums, grad_heads):
    count, width = mixed.shape
    scale = HEAD_DIM**-0.5
    grad_mixed[...] = mm(grad[...], weight[:, 3 * width :]).astype(BF16)
    target = grad_heads if kind == "time" else sums
    units = attention_units(kind, count, width)
    batch_size = 12 if kind == "time" else 3
    for batch in range(0, len(units), batch_size):
        some = units[batch : batch + batch_size]
        parts = []
        for start, size, first, final, bias, head in some:
            rows = pl.ds(start, size)
            query, key, value = head_slices(heads, rows, width, head)
            grad_here = grad_mixed[rows, head * HEAD_DIM : (head + 1) * HEAD_DIM]
            if kind != "time":
                ids = row_ids((size, HEAD_DIM), 0, 0)
                valid = (ids >= first) & (ids < final)
                grad_here = jnp.where(valid, grad_here.astype(F32), 0.0).astype(BF16)
            parts.append((query * scale, key, value, grad_here))
        scores = [mm(p[1], p[0], NT) + u[4] for u, p in zip(some, parts)]
        grad_weights = [mm(p[2], p[3], NT) for p in parts]
        weights = [jnp.exp(x - jnp.max(x, 0, keepdims=True)) for x in scores]
        weights = [x * (1.0 / jnp.sum(x, 0, keepdims=True)) for x in weights]
        grad_values = [mm(x.astype(BF16), p[3]) for x, p in zip(weights, parts)]
        grad_scores = [
            (x * (y - jnp.sum(x * y, 0, keepdims=True))).astype(BF16)
            for x, y in zip(weights, grad_weights)
        ]
        grad_keys = [mm(x, p[0]) for x, p in zip(grad_scores, parts)]
        grad_queries = [(mm(p[1].T, x) * scale).T for x, p in zip(grad_scores, parts)]
        for u, *grads in zip(some, grad_queries, grad_keys, grad_values):
            start, size, first, final, bias, head = u
            for c, x in enumerate(grads):
                low = c * width + head * HEAD_DIM
                target[start + first : start + final, low : low + HEAD_DIM] = x[
                    first:final
                ].astype(target.dtype)
    if kind != "time":
        grad_heads[...] = sums[...].astype(BF16)
    return mm(grad_heads[...], weight[:, : 3 * width], NT)


EVENT_NAMES = ("zs", "line", "relay", "across", "core", "first", "second", "third")
BLOCK_ORDER = (1, 2, 3, 0)
ORDER = (
    ("go",),
    ("line", 0, 0), ("zs", 0, 3), ("line", 2, 0), ("zs", 1, 1), ("zs", 0, 1), ("line", 1, 0),
    ("zs", 0, 2), ("zs", 2, 1), ("line", 0, 3), ("zs", 1, 2), ("line", 1, 1), ("zs", 1, 3),
    ("line", 0, 1), ("relay", 2, 0), ("ln0",), ("relay", 0, 3), ("line", 0, 2), ("across", 0, 3),
    ("relay", 1, 1), ("across", 2, 0), ("zs", 2, 2), ("relay", 0, 0), ("relay", 0, 1),
    ("relay", 0, 2), ("line", 2, 1), ("zs", 2, 3), ("line", 1, 2), ("mask",), ("zs", 3, 1),
    ("line", 1, 3), ("across", 0, 0), ("across", 0, 1), ("across", 0, 2), ("zs", 3, 2),
    ("takeE0",), ("P0", 0), ("across", 1, 1), ("line", 2, 2), ("relay", 1, 0), ("P0", 1),
    ("P0", 2), ("relay", 1, 3), ("P0", 3), ("exch1",), ("relay", 1, 2), ("relay", 2, 2),
    ("line", 2, 3), ("across", 1, 2), ("relay", 2, 1), ("across", 2, 2), ("line", 3, 2),
    ("zs", 3, 3), ("across", 1, 0), ("across", 1, 3), ("relay", 2, 3), ("line", 3, 0),
    ("line", 3, 1), ("ln1",), ("P1", 0), ("P1", 1), ("P1", 2), ("across", 2, 3), ("across", 2, 1),
    ("line", 3, 3), ("relay", 3, 2), ("P1", 3), ("relay", 3, 0), ("ln2",), ("up", 0),
    ("relay", 3, 1), ("relay", 3, 3), ("up", 1), ("across", 3, 0), ("across", 3, 2), ("core", 0),
    ("up", 2), ("core", 1), ("across", 3, 1), ("across", 3, 3), ("up", 3), ("core", 2), ("dn", 0),
    ("dn", 1), ("first", 0), ("dn", 2), ("dn", 3), ("first", 2), ("B1", 0), ("core", 3),
    ("B1", 1), ("first", 1), ("second", 2), ("second", 0), ("core", 4), ("B1", 2), ("core", 5),
    ("B1", 3), ("nb2",), ("second", 1), ("core", 6), ("B2", 0), ("core", 7), ("first", 5),
    ("B2", 1), ("core", 8), ("B2", 2), ("core", 9), ("first", 6), ("second", 5), ("B2", 3),
    ("nb1",), ("core", 10), ("first", 4), ("first", 8), ("second", 6), ("first", 10),
    ("core", 11), ("first", 9), ("first", 7), ("second", 4), ("first", 3), ("takeE2",), ("B3", 0),
    ("second", 10), ("B3", 1), ("core", 12), ("second", 8), ("B3", 2), ("second", 9),
    ("core", 13), ("B3", 3), ("exch3",), ("core", 14), ("first", 13), ("second", 3), ("core", 15),
    ("first", 14), ("first", 12), ("second", 13), ("first", 11), ("third", 0), ("second", 7),
    ("first", 15), ("third", 1), ("second", 14), ("nb0",), ("second", 11), ("second", 12),
    ("gain",), ("third", 2), ("second", 15), ("third", 3),
)


def after_each(order):
    found, events = {}, []
    for item in order:
        if item[0] in EVENT_NAMES:
            events.append(item)
        else:
            events = found.setdefault(item, [])
    return found


LINE_ACROSS = ()
SUM_ACROSS = ()
AFTER = after_each(ORDER)


def layer_kernel(
    live_ref,
    tokens_hbm,
    cotangent_hbm,
    gain_hbm,
    qkv_time_hbm,
    out_time_hbm,
    qkv_space_hbm,
    out_space_hbm,
    up_hbm,
    down_hbm,
    weight_ref,
    out_hbm,
    stream_hbm,
    own_hbm,
    own_gain_hbm,
    out_ref,
    stream_ref,
    own_ref,
    own_gain_ref,
    tokens_ref,
    gain_ref,
    qkv_time_ref,
    out_time_ref,
    qkv_space_ref,
    out_space_ref,
    shard_ref,
    held,
    normed_time_ref,
    time_heads_ref,
    time_mixed_ref,
    after_time_ref,
    normed_space_ref,
    space_heads_ref,
    space_mixed_ref,
    after_space_ref,
    normed_mlp_ref,
    hidden_ref,
    slope_ref,
    low_ref,
    rows_ref,
    patch_ref,
    total_ref,
    mixed_sums,
    sums,
    grad_mixed,
    grad_heads,
    work,
    keep,
    came,
    first,
    second,
    third,
    fourth,
    gains_ref,
    gain_sums,
    gain_line,
    gain_out,
    gain_parts,
    swap_out,
    swap_back,
    piece_sent,
    piece_here,
    core_sent,
    core_here,
    first_sent,
    first_here,
    second_sent,
    second_here,
    third_sent,
    third_here,
    fourth_sent,
    fourth_here,
    gain_sent,
    gain_here,
    swap_sent,
    swap_here,
    held_sem,
    own_sem,
    load_sem,
    store_sem,
    credit,
):
    here = place()
    count, columns = tokens_ref.shape
    width = time_mixed_ref.shape[2]
    own_row = dp_row(here)
    last = CHUNKS * STEPS - 1
    live = jnp.where(here["s"] < live_ref[0], 1.0, 0.0).astype(F32)

    loads = [
        pltpu.make_async_copy(source, target, load_sem.at[i])
        for i, (source, target) in enumerate(
            (
                (gain_hbm, gain_ref),
                (qkv_time_hbm, qkv_time_ref),
                (out_time_hbm, out_time_ref),
                (qkv_space_hbm, qkv_space_ref),
                (out_space_hbm, out_space_ref),
                (up_hbm, shard_ref.at[2]),
                (down_hbm, shard_ref.at[3]),
                (tokens_hbm, tokens_ref),
                (cotangent_hbm, stream_ref),
            )
        )
    ]
    stores = [
        pltpu.make_async_copy(source, target, store_sem.at[i])
        for i, (source, target) in enumerate(
            [(out_ref, out_hbm), (stream_ref, stream_hbm)]
            + [(own_ref.at[k], own_hbm.at[k]) for k in range(CHUNKS)]
            + [(own_gain_ref, own_gain_hbm)]
        )
    ]
    greet(here, "call")
    for load in loads:
        load.start()
    for load in loads[:5]:
        load.wait()

    for k, qkv, out in ((0, qkv_time_ref, out_time_ref), (1, qkv_space_ref, out_space_ref)):
        for c in range(3):
            shard_ref[k, :, c * width : (c + 1) * width] = qkv[c]
        shard_ref[k, :, 3 * width :] = out[...].astype(F32).T.astype(BF16)
    own_gains = gain_ref.shape[1]
    gain_out[0, : gain_ref.shape[0], :own_gains] = gain_ref[...].astype(F32)
    for load in loads[5:7]:
        load.wait()
    greet(here, "answer")

    def row_of(part, r):
        return dp_row(here, y=r // 2, x=r % 2, c=part)

    def slot_of(k, j, row):
        return weight_ref.at[k, j, pl.ds(pl.multiple_of(row * BLOCK_ROWS, BLOCK_ROWS), BLOCK_ROWS)]

    def arrived(k, part, r, j):
        slot = slot_of(k, j, row_of(part, r))
        remote(
            slot, slot, piece_sent.at[k, 0, 0], piece_here.at[k, part, r, j], moved(here, c=1)
        ).wait_recv()

    def send(source, k, j, r, sem, part, r_there, **flips):
        remote(
            source,
            slot_of(k, j, row_of(0, r)),
            piece_sent.at[k, sem, j],
            piece_here.at[k, part, r_there, j],
            moved(here, **flips),
        ).start()

    def piece(k, j, r):
        return slot_of(k, j, row_of(0, r))

    def along_line(k, j):
        remote(
            shard_ref.at[k],
            slot_of(k, j, own_row),
            piece_sent.at[k, 0, j],
            piece_here.at[k, 0, 0, j],
            moved(here, s=j // 2, h=j % 2),
        ).start()

    def spread(source, k, j):
        send(source, k, j, 0, 1, 0, 1, x=1)
        send(source, k, j, 0, 2, 0, 2, y=1)
        send(source, k, j, 0, 4, 1, 0, c=1)

    def line(k, j):
        if j:
            arrived(k, 0, 0, j)
        spread(piece(k, j, 0) if j else shard_ref.at[k], k, j)

    def relay(k, j):
        arrived(k, 0, 1, j)
        send(piece(k, j, 1), k, j, 1, 5, 1, 1, c=1)
        arrived(k, 0, 2, j)
        send(piece(k, j, 2), k, j, 2, 6, 1, 2, c=1)
        if j == 1 and k in LINE_ACROSS:
            return
        up = (j // 2 + k) % 2
        source = slot_of(k, j, dp_row(here, y=up, x=1 - up))
        remote(
            source,
            source,
            piece_sent.at[k, 3, j],
            piece_here.at[k, 0, 3, j],
            moved(here, y=1 - up, x=up),
        ).start()

    def across(k, j):
        arrived(k, 0, 3, j)
        send(piece(k, j, 3), k, j, 3, 7, 1, 3, c=1)
        if j == 0 and k in LINE_ACROSS:
            remote(
                piece(k, 0, 3),
                piece(k, 1, 3),
                piece_sent.at[k, 3, 1],
                piece_here.at[k, 0, 3, 1],
                moved(here, h=1),
            ).start()

    def fetch(k, t):
        return pltpu.make_async_copy(weight_ref.at[k, t], held.at[t], held_sem.at[t])

    def ready(k):
        for j in range(STEPS):
            for r in range(4):
                arrived(k, 1, r, j)
        for t in BLOCK_ORDER:
            fetch(k, t).start()

    def weight(k, t):
        fetch(k, t).wait()
        return held.at[t]

    def stored(k):
        return pltpu.make_async_copy(shard_ref.at[k], slot_of(k, 0, own_row), own_sem.at[k])

    half_lanes = keep.shape[4]
    swapped = (0, 2, 1, 3)

    def grad_rows(part, quad):
        row = dp_row(here, y=quad // 2, x=quad % 2, c=part)
        return pl.ds(pl.multiple_of(row * BLOCK_ROWS, BLOCK_ROWS), BLOCK_ROWS)

    def core_copy(step, quad):
        return remote(
            work.at[step % 2, grad_rows(1, quad)],
            came.at[step % 4, quad],
            core_sent.at[step % 2, quad],
            core_here.at[step % 4, quad],
            moved(here, c=1),
        )

    def quads_sent(step):
        return 1 if BLOCK_ORDER[step % STEPS] == 1 and step // STEPS in SUM_ACROSS else 2

    def first_copy(step, half):
        quads = quads_sent(step)
        return remote(
            keep.at[step, pl.ds(2, quads), half],
            first.at[step, half, pl.ds(0, quads)],
            first_sent.at[step, half],
            first_here.at[step, half],
            moved(here, y=1 - half, x=half),
        )

    def fourth_copy(index):
        return remote(
            keep.at[index * STEPS + BLOCK_ORDER.index(1), 3],
            fourth.at[index],
            fourth_sent.at[index],
            fourth_here.at[index],
            moved(here, h=1),
        )

    def second_copy(step, half):
        return remote(
            keep.at[step, 1, half],
            second.at[step, half],
            second_sent.at[step, half],
            second_here.at[step, half],
            moved(here, y=half, x=1 - half),
        )

    def third_copy(step):
        j = BLOCK_ORDER[step % STEPS]
        return remote(
            keep.at[step, 0],
            third.at[step],
            third_sent.at[step],
            third_here.at[step],
            moved(here, s=j // 2, h=j % 2),
        )

    def begin(step):
        @pl.when(step >= 2)
        def _():
            for quad in range(4):
                core_copy(step - 2, quad).wait_send()

        return work.at[step % 2]

    def emit(step):
        @pl.when(step >= 4)
        def _():
            pl.semaphore_wait(credit, 1)

        for quad in range(4):
            core_copy(step, quad).start()

    def take_core(step):
        block = BLOCK_ORDER[step % STEPS]
        for quad in range(4):
            core_copy(step, quad).wait_recv()
        for index in (2, 3, 1, 0):
            for half in range(2):
                quad = swapped[index] if half else index
                lanes = slice(half * half_lanes, (half + 1) * half_lanes)
                own = work[step % 2, grad_rows(0, quad), lanes].astype(F32)
                both = own + came[step % 4, quad, :, lanes].astype(F32)
                if index == 3 and block == 0 and step // STEPS in SUM_ACROSS:
                    if half == 0:
                        fourth_copy(step // STEPS).wait_recv()
                    both = both + fourth[step // STEPS, half].astype(F32)
                keep[step, index, half] = both.astype(BF16)
                if index == 1 + quads_sent(step):
                    first_copy(step, half).start()
            if index == 3 and block == 1 and step // STEPS in SUM_ACROSS:
                fourth_copy(step // STEPS).start()
        if step <= last - 4:
            pl.semaphore_signal(
                credit,
                inc=1,
                device_id=moved(here, c=1),
                device_id_type=pl.DeviceIdType.MESH,
            )

    def take_first(step):
        for half in range(2):
            first_copy(step, half).wait_recv()
            for index in (1, 0):
                if index < quads_sent(step):
                    both = keep[step, index, half].astype(F32) + first[step, half, index].astype(F32)
                    keep[step, index, half] = both.astype(BF16)
                if index:
                    second_copy(step, half).start()

    def take_second(step):
        for half in range(2):
            second_copy(step, half).wait_recv()
            both = keep[step, 0, half].astype(F32) + second[step, half].astype(F32)
            keep[step, 0, half] = both.astype(BF16)
        if BLOCK_ORDER[step % STEPS]:
            third_copy(step).start()

    def take_third(index):
        steps = [index * STEPS + i for i in range(STEPS)]
        for step in steps:
            if BLOCK_ORDER[step % STEPS]:
                third_copy(step).wait_recv()
        for half in range(2):
            total = jnp.zeros((BLOCK_ROWS, half_lanes), F32)
            for step in steps:
                source = third[step, half] if BLOCK_ORDER[step % STEPS] else keep[step, 0, half]
                total = total + source.astype(F32)
            own_ref[index, :, half * half_lanes : (half + 1) * half_lanes] = total
        stores[2 + index].start()

    events = {
        "zs": along_line,
        "line": line,
        "relay": relay,
        "across": across,
        "core": take_core,
        "first": take_first,
        "second": take_second,
        "third": take_third,
    }

    def follow(item):
        for name, *args in AFTER.get(item, ()):
            events[name](*args)

    def loop(name, body):
        def step(i, carry):
            body(i, (i + 1) % STEPS)
            for c in range(STEPS - 1):
                if AFTER.get((name, c)):

                    @pl.when(i == c)
                    def _(c=c):
                        follow((name, c))

            return carry

        lax.fori_loop(0, STEPS, step, 0)
        follow((name, STEPS - 1))

    def layer_norm(source_ref, gain, target_ref):
        def body(rows):
            centred, scale = row_stats(source_ref[rows, :])
            target_ref[rows, :] = (centred * scale * gains_ref[gain : gain + 1, :]).astype(
                target_ref.dtype
            )

        by_rows(count, body)

    def norm_back(source_ref, gain, grad_normed_ref):
        def body(rows):
            centred, scale = row_stats(source_ref[rows, :])
            unit = centred * scale
            grad_normed = grad_normed_ref[rows, :]
            e = grad_normed * gains_ref[gain : gain + 1, :]
            mean = jnp.mean(e, -1, keepdims=True)
            tilt = jnp.mean(e * unit, -1, keepdims=True)
            stream_ref[rows, :] += scale * (e - mean - unit * tilt)
            gain_sums[gain : gain + 1, :] += jnp.sum(grad_normed * unit, 0, keepdims=True)

        by_rows(count, body)

    def exchange(index):
        return Exchange(
            here,
            swap_out.at[index % 2],
            swap_back.at[index % 2],
            swap_sent.at[index],
            swap_here.at[index],
        )

    def attention(kind, k, normed_ref, heads_ref, mixed_ref):
        total_ref[...] = jnp.zeros_like(total_ref)

        def compute(i, t):
            total_ref[...] += attend_block(
                kind, t, normed_ref[...], weight(k, t), heads_ref, mixed_ref, mixed_sums
            )

        return compute

    def attention_back(kind, k, normed_ref, heads_ref, mixed_ref):
        total_ref[...] = jnp.zeros_like(total_ref)

        def compute(i, t):
            step = (CHUNKS - 1 - k) * STEPS + i
            out = begin(step)
            total_ref[...] += attend_back_block(
                kind,
                heads_ref.at[t],
                mixed_ref.at[t],
                low_ref,
                weight(k, t),
                grad_mixed,
                sums,
                grad_heads,
            )
            if k:
                fetch(k - 1, t).start()
            out[:, : 3 * width] = mm(normed_ref[...], grad_heads[...], TN).astype(BF16)
            out[:, 3 * width :] = mm(low_ref[...], mixed_ref[t], TN).astype(BF16)
            emit(step)

        return compute

    gain_parts[0, own_row] = gain_out[0]

    def gain_copy(r):
        flips = {"y": r // 4, "x": r // 2 % 2, "c": r % 2}
        return remote(
            gain_out.at[0],
            gain_parts.at[0, own_row],
            gain_sent.at[0, r],
            gain_here.at[0, r],
            moved(here, **flips),
        )

    for r in range(1, 8):
        gain_copy(r).start()
    for k in range(CHUNKS):
        stored(k).start()
    follow(("go",))
    loads[7].wait()

    def unit_rows(rows):
        centred, scale = row_stats(tokens_ref[rows, :])
        rows_ref[rows, :] = centred * scale

    by_rows(count, unit_rows)
    for r in range(1, 8):
        gain_copy(r).wait()
    for d in range(8):
        gains_ref[:, d * own_gains : (d + 1) * own_gains] = gain_parts[0, d, :, :own_gains]

    def scale_rows(rows):
        rows_ref[rows, :] = rows_ref[rows, :] * gains_ref[0:1, :]

    by_rows(count, scale_rows)
    swap = exchange(0)
    swap.send_frames(rows_ref)
    follow(("ln0",))
    loads[8].wait()

    def mask_rows(rows):
        stream_ref[rows, :] = stream_ref[rows, :] * live
        low_ref[rows, :] = stream_ref[rows, :].astype(BF16)

    by_rows(count, mask_rows)
    gain_sums[...] = jnp.zeros_like(gain_sums)
    follow(("mask",))
    swap.take_patches(patch_ref, normed_time_ref)
    for k in range(CHUNKS):
        stored(k).wait()
    follow(("takeE0",))

    ready(0)
    loop("P0", attention("time", 0, normed_time_ref, time_heads_ref, time_mixed_ref))
    swap = exchange(1)
    swap.send_patches(total_ref, patch_ref)
    follow(("exch1",))
    swap.take_frames(rows_ref)
    after_time_ref[...] = tokens_ref[...] + rows_ref[...]
    layer_norm(after_time_ref, 1, normed_space_ref)
    follow(("ln1",))

    ready(1)
    loop("P1", attention("space", 1, normed_space_ref, space_heads_ref, space_mixed_ref))
    after_space_ref[...] = after_time_ref[...] + total_ref[...]
    layer_norm(after_space_ref, 2, normed_mlp_ref)
    follow(("ln2",))

    ready(2)

    def up(i, t):
        out = begin(i)
        pre_act = mm(normed_mlp_ref[...], weight(2, t)[...])
        cdf = 0.5 * (1.0 + lax.erf(pre_act * 0.5**0.5))
        hidden_ref[t] = (pre_act * cdf).astype(BF16)
        density = jnp.exp(-0.5 * pre_act * pre_act) * (0.5 / math.pi) ** 0.5
        slope_ref[t] = (cdf + pre_act * density).astype(BF16)
        out[...] = mm(low_ref[...], hidden_ref[t], TN).astype(BF16)
        emit(i)

    loop("up", up)
    ready(3)
    out_ref[...] = after_space_ref[...]

    def down(i, t):
        out_ref[...] += mm(hidden_ref[t], weight(3, t)[...], NT)
        grad_hidden = mm(low_ref[...], held[t])
        slope_ref[t] = (grad_hidden * slope_ref[t].astype(F32)).astype(BF16)
        fetch(2, t).start()

    loop("dn", down)
    out_ref[...] = out_ref[...] * live
    stores[0].start()
    total_ref[...] = jnp.zeros_like(total_ref)

    def up_back(i, t):
        step = STEPS + i
        out = begin(step)
        total_ref[...] += mm(slope_ref[t], weight(2, t)[...], NT)
        fetch(1, t).start()
        out[...] = mm(normed_mlp_ref[...], slope_ref[t], TN).astype(BF16)
        emit(step)

    loop("B1", up_back)
    norm_back(after_space_ref, 2, total_ref)
    low_ref[...] = stream_ref[...].astype(BF16)
    follow(("nb2",))
    loop("B2", attention_back("space", 1, normed_space_ref, space_heads_ref, space_mixed_ref))
    norm_back(after_time_ref, 1, total_ref)
    swap = exchange(2)
    swap.send_frames(stream_ref)
    follow(("nb1",))
    swap.take_patches(patch_ref, low_ref)
    follow(("takeE2",))
    loop("B3", attention_back("time", 0, normed_time_ref, time_heads_ref, time_mixed_ref))
    swap = exchange(3)
    swap.send_patches(total_ref, patch_ref)
    follow(("exch3",))
    swap.take_frames(rows_ref)
    norm_back(tokens_ref, 0, rows_ref)
    stores[1].start()

    line_index = here["s"] * 2 + here["h"]

    def gain_back(r):
        flips = {"y": r // 4, "x": r // 2 % 2, "c": r % 2}
        return remote(
            gain_out.at[dp_row(here, **flips)],
            gain_parts.at[1, own_row],
            gain_sent.at[1, r],
            gain_here.at[1, r],
            moved(here, **flips),
        )

    def gain_line_copy(j):
        return remote(
            own_gain_ref,
            gain_line.at[line_index],
            gain_sent.at[2, j],
            gain_here.at[2, j],
            moved(here, s=j // 2, h=j % 2),
        )

    total = gain_sums[...]
    for d in range(8):
        gain_out[d, :, :own_gains] = total[:, d * own_gains : (d + 1) * own_gains]
    for r in range(1, 8):
        gain_back(r).start()
    gain_parts[1, own_row] = gain_out[own_row]
    follow(("nb0",))
    for r in range(1, 8):
        gain_back(r).wait()
    total = gain_parts[1, 0]
    for d in range(1, 8):
        total = total + gain_parts[1, d]
    own_gain_ref[...] = total
    for j in range(1, 4):
        gain_line_copy(j).start()
    gain_line[line_index] = total
    follow(("gain",))
    for j in range(1, 4):
        gain_line_copy(j).wait()
    own_gain_ref[...] = gain_line[0] + gain_line[1] + gain_line[2] + gain_line[3]
    stores[2 + CHUNKS].start()

    for k in range(CHUNKS):
        for sem in range(8):
            for j in range(4):
                if sem or j:
                    slot = slot_of(k, 0, own_row)
                    remote(
                        slot,
                        slot,
                        piece_sent.at[k, sem, j],
                        piece_here.at[k, 0, 0, 0],
                        moved(here, c=1),
                    ).wait_send()
    for step in range(last + 1):
        if step > last - 2:
            for quad in range(4):
                core_copy(step, quad).wait_send()
        for half in range(2):
            first_copy(step, half).wait_send()
            second_copy(step, half).wait_send()
        if BLOCK_ORDER[step % STEPS]:
            third_copy(step).wait_send()
    for index in SUM_ACROSS:
        fourth_copy(index).wait_send()
    for store in stores:
        store.wait()


def layer(live_clips, tokens, cotangent, norm_gains, *weights):
    count, columns = tokens.shape
    rows, lanes = weights[4].shape
    half = lanes // 2
    width, steps = lanes // 4, CHUNKS * STEPS
    there = pl.BlockSpec(memory_space=pl.ANY)
    outputs = (
        shaped(CHUNKS, STEPS, columns, lanes),
        shaped(count, columns, dtype=F32),
        shaped(count, columns, dtype=F32),
        shaped(CHUNKS, rows, lanes, dtype=F32),
        shaped(8, 128, dtype=F32),
    )
    return pl.pallas_call(
        layer_kernel,
        in_specs=[pl.BlockSpec(memory_space=pltpu.SMEM)] + [there] * 9,
        out_specs=[there] * len(outputs),
        out_shape=outputs,
        scratch_shapes=[
            pltpu.VMEM((count, columns), F32),
            pltpu.VMEM((count, columns), F32),
            pltpu.VMEM((CHUNKS, rows, lanes), F32),
            pltpu.VMEM((8, 128), F32),
            pltpu.VMEM((count, columns), F32),
            pltpu.VMEM(norm_gains.shape, BF16),
            *[pltpu.VMEM(w.shape, BF16) for w in weights[:4]],
            pltpu.VMEM((CHUNKS, rows, lanes), BF16),
            pltpu.VMEM((STEPS, columns, lanes), BF16),
            pltpu.VMEM((count, columns), BF16),
            pltpu.VMEM((STEPS, count, 3 * width), BF16),
            pltpu.VMEM((STEPS, count, width), BF16),
            pltpu.VMEM((count, columns), F32),
            pltpu.VMEM((count, columns), BF16),
            pltpu.VMEM((STEPS, count, 3 * width), BF16),
            pltpu.VMEM((STEPS, count, width), BF16),
            pltpu.VMEM((count, columns), F32),
            pltpu.VMEM((count, columns), BF16),
            pltpu.VMEM((STEPS, count, lanes), BF16),
            pltpu.VMEM((STEPS, count, lanes), BF16),
            pltpu.VMEM((count, columns), BF16),
            pltpu.VMEM((count, columns), F32),
            pltpu.VMEM((columns // 128, count, 128), F32),
            pltpu.VMEM((count, columns), F32),
            pltpu.VMEM((count, width), F32),
            pltpu.VMEM((count, 3 * width), F32),
            pltpu.VMEM((count, width), BF16),
            pltpu.VMEM((count, 3 * width), BF16),
            pltpu.VMEM((2, columns, lanes), BF16),
            pltpu.VMEM((steps, 4, 2, rows, half), BF16),
            pltpu.VMEM((4, 4, rows, lanes), BF16),
            pltpu.VMEM((steps, 2, 2, rows, half), BF16),
            pltpu.VMEM((steps, 2, rows, half), BF16),
            pltpu.VMEM((steps, 2, rows, half), BF16),
            pltpu.VMEM((CHUNKS, 2, rows, half), BF16),
            pltpu.VMEM((8, columns), F32),
            pltpu.VMEM((8, columns), F32),
            pltpu.VMEM((4, 8, 128), F32),
            pltpu.VMEM((8, 8, 128), F32),
            pltpu.VMEM((2, 8, 8, 128), F32),
            pltpu.VMEM((2, 4, 2, PAD, columns), BF16),
            pltpu.VMEM((2, 4, 2, PAD, columns), BF16),
            pltpu.SemaphoreType.DMA((CHUNKS, 8, 4)),
            pltpu.SemaphoreType.DMA((CHUNKS, 2, 4, 4)),
            pltpu.SemaphoreType.DMA((2, 4)),
            pltpu.SemaphoreType.DMA((4, 4)),
            pltpu.SemaphoreType.DMA((steps, 2)),
            pltpu.SemaphoreType.DMA((steps, 2)),
            pltpu.SemaphoreType.DMA((steps, 2)),
            pltpu.SemaphoreType.DMA((steps, 2)),
            pltpu.SemaphoreType.DMA((steps,)),
            pltpu.SemaphoreType.DMA((steps,)),
            pltpu.SemaphoreType.DMA((CHUNKS,)),
            pltpu.SemaphoreType.DMA((CHUNKS,)),
            pltpu.SemaphoreType.DMA((3, 8)),
            pltpu.SemaphoreType.DMA((3, 8)),
            pltpu.SemaphoreType.DMA((4, 4)),
            pltpu.SemaphoreType.DMA((4, 4)),
            pltpu.SemaphoreType.DMA((STEPS,)),
            pltpu.SemaphoreType.DMA((CHUNKS,)),
            pltpu.SemaphoreType.DMA((9,)),
            pltpu.SemaphoreType.DMA((3 + CHUNKS,)),
            pltpu.SemaphoreType.REGULAR,
        ],
        compiler_params=pltpu.CompilerParams(
            collective_id=0, has_side_effects=True, vmem_limit_bytes=67043328
        ),
        name="layer",
    )(live_clips, tokens, cotangent, norm_gains, *weights)[1:]


def finish_kernel(output_hbm, grad_hbm, own_hbm, gain_ref, *rest):
    targets, buffers, own_ref, load_sem, store_sem = rest[:9], rest[9:18], *rest[18:]
    output, grad, gains, time_in, time_out, space_in, space_out, up, down = buffers
    width = time_in.shape[2]
    sources = [(own_hbm.at[k], into) for k, into in ((0, down), (1, up))]
    sources += [(own_hbm.at[k], own_ref.at[k - 2]) for k in (2, 3)]
    sources += [(output_hbm, output), (grad_hbm, grad)]
    loads = [pltpu.make_async_copy(*pair, load_sem.at[i]) for i, pair in enumerate(sources)]
    stores = [
        pltpu.make_async_copy(*pair, store_sem.at[i]) for i, pair in enumerate(zip(buffers, targets))
    ]
    for i in (2, 3, 0, 1, 4, 5):
        loads[i].start()
    gains[...] = gain_ref[: gains.shape[0], : gains.shape[1]]
    stores[2].start()
    for k, load, into, out, low in ((0, 2, space_in, space_out, 5), (1, 3, time_in, time_out, 3)):
        loads[load].wait()
        for c in range(3):
            into[c] = own_ref[k, :, c * width : (c + 1) * width]
        stores[low].start()
        out[...] = own_ref[k, :, 3 * width :].T
        stores[low + 1].start()
    for load, store in ((0, 8), (1, 7), (4, 0), (5, 1)):
        loads[load].wait()
        stores[store].start()
    for store in stores:
        store.wait()


def finish(output, grad, own, gain, like):
    shapes = [jax.ShapeDtypeStruct(a.shape, F32) for a in like]
    there = pl.BlockSpec(memory_space=pl.ANY)
    return pl.pallas_call(
        finish_kernel,
        in_specs=[there] * 3 + [pl.BlockSpec(memory_space=pltpu.VMEM)],
        out_specs=[there] * len(shapes),
        out_shape=shapes,
        scratch_shapes=[
            *[pltpu.VMEM(a.shape, F32) for a in like],
            pltpu.VMEM((2,) + own.shape[1:], F32),
            pltpu.SemaphoreType.DMA((6,)),
            pltpu.SemaphoreType.DMA((len(shapes),)),
        ],
        name="finish",
    )(output, grad, own, gain)


def sum_gains(total, own):
    for axes in ("c", "x", "y", TENSOR):
        bit = 1
        while bit < lax.axis_size(axes):
            total = total + along(total, axes, bit)
            bit *= 2
    return lax.dynamic_slice_in_dim(total, lax.axis_index(DP) * own, own, 1)


def on_device(
    routed,
    tokens,
    live_clips,
    norm_gains,
    qkv_time,
    out_time,
    qkv_space,
    out_space,
    up_weight,
    down_weight,
    cotangent,
):
    members = lax.axis_size("c") * lax.axis_size("h")
    share = PATCHES // members
    count, columns = tokens.shape
    width = qkv_time.shape[2]
    live = jnp.where(lax.axis_index("s") < live_clips[0], 1.0, 0.0).astype(F32)

    def pack_heads(qkv, out):
        rows = qkv.shape[1]
        return jnp.concatenate([qkv.transpose(1, 0, 2).reshape(rows, -1), out.T], 1)

    if routed:
        weights = (qkv_time, out_time, qkv_space, out_space, up_weight, down_weight.T)
        done = layer(live_clips, tokens, cotangent, norm_gains, *weights)
        *found, down_own = finish(*done, (tokens, cotangent, norm_gains, *weights))
        return (*found, down_own.T)
    shards = [
        pack_heads(qkv_time, out_time),
        pack_heads(qkv_space, out_space),
        up_weight,
        down_weight.T,
    ]
    grad_stream = cotangent * live
    time_all, space_all, up_all, down_all = [gather_plain(shard) for shard in shards]
    blocks, depth, lanes = up_all.shape
    gains = lax.all_gather(norm_gains, DP, axis=1, tiled=True).astype(F32)
    normed_time = to_patches(normalize(tokens, gains[0]).astype(BF16), members)
    time_heads, time_mixed, change = attend("time", normed_time, time_all, share, BF16)
    after_time = tokens + to_frames(change, members).astype(F32)
    normed_space = normalize(after_time, gains[1]).astype(BF16)
    space_heads, space_mixed, change = attend("space", normed_space, space_all, 1, F32)
    after_space = after_time + change
    normed_mlp = normalize(after_space, gains[2]).astype(BF16)
    hidden, slope = phase(
        up_kernel,
        "up",
        (normed_mlp, up_all),
        (shaped(blocks, count, lanes), shaped(blocks, count, lanes)),
        cost=12,
    )
    (change,) = phase(
        down_kernel, "down", (hidden, down_all), (shaped(count, depth, dtype=F32),), cost=4
    )
    after_mlp = after_space + change
    grad_low = grad_stream.astype(BF16)
    work = (pltpu.VMEM((depth, lanes), BF16),)
    *down_grads, grad_pre = phase(
        down_back_kernel,
        "down_back",
        (grad_low, down_all, hidden, slope),
        (*grad_shapes(down_all, False), shaped(blocks, count, lanes)),
        work,
        cost=8,
    )
    *up_grads, grad_normed = phase(
        up_back_kernel,
        "up_back",
        (normed_mlp, up_all, grad_pre),
        (*grad_shapes(up_all, False), shaped(count, depth, dtype=F32)),
        work,
        cost=8,
    )
    grad_part, gain_mlp = norm_back(after_space, gains[2], grad_normed)
    grad_stream = grad_stream + grad_part
    space_grads, grad_normed = attend_back(
        "space",
        normed_space,
        space_all,
        space_heads,
        space_mixed,
        grad_stream.astype(BF16),
        1,
        F32,
        False,
    )
    grad_part, gain_space = norm_back(after_time, gains[1], grad_normed)
    grad_stream = grad_stream + grad_part
    grad_low = to_patches(grad_stream.astype(BF16), members)
    time_grads, grad_normed = attend_back(
        "time", normed_time, time_all, time_heads, time_mixed, grad_low, share, BF16, routed
    )
    grad_normed = to_frames(grad_normed, members).astype(F32)
    grad_part, gain_time = norm_back(tokens, gains[0], grad_normed)
    grad_tokens = grad_stream + grad_part
    down_own = reduce_plain(down_grads).T
    up_own = reduce_plain(up_grads)
    space_own = reduce_plain(space_grads)
    time_own = reduce_plain(time_grads)
    gains_own = sum_gains(jnp.stack([gain_time, gain_space, gain_mlp]), norm_gains.shape[1])
    output = after_mlp * live

    def unpack(own):
        rows = own.shape[0]
        return own[:, : 3 * width].reshape(rows, 3, width).transpose(1, 0, 2), own[:, 3 * width :].T

    time_in_own, time_out_own = unpack(time_own)
    space_in_own, space_out_own = unpack(space_own)
    return (
        output,
        grad_tokens,
        gains_own,
        time_in_own,
        time_out_own,
        space_in_own,
        space_out_own,
        up_own,
        down_own,
    )


def solution(mesh):
    n_dp, n_tensor = mesh.devices.shape

    def run(*args):
        slots = args[0].shape[0] // (n_dp * HALF * PATCHES)
        fine = Mesh(mesh.devices.reshape(n_dp // 4, 2, 2, slots, n_tensor // slots), ALL)
        in_specs = (
            P(ALL, None),
            P(DP),
            P(None, DP),
            P(None, DP, TENSOR),
            P(TENSOR, DP),
            P(None, DP, TENSOR),
            P(TENSOR, DP),
            P(DP, TENSOR),
            P(TENSOR, DP),
            P(ALL, None),
        )
        out_specs = (in_specs[0], in_specs[0]) + in_specs[2:9]
        routed = fine.devices.shape == (2, 2, 2, 2, 2)
        return jax.shard_map(
            functools.partial(on_device, routed), mesh=fine, in_specs=in_specs, out_specs=out_specs, check_vma=False
        )(*args)

    return run
```
